32 devices in a mesh: parts: 2 (over y), row: 4 (over x, core), col: 4 (over z).
Axes of the slice: x: 2, y: 2, z: 4, core: 2. Of those that a mesh axis runs over, the one named last changes fastest.
Arguments:
- alignment_tensor: bfloat16 [256, 256, 256], P(('parts', 'col'), 'row'), parts along dimension 0, may hold values from -6 to 6
- standardizer_scaling: float32 [256], replicated, may hold values from 0.25 to 1.75
- standardizer_offset: float32 [256], replicated, may hold values from -3 to 3
- first_projector: bfloat16 [256, 32], replicated, may hold values from -0.375 to 0.375
- second_projector: bfloat16 [256, 32], replicated, may hold values from -0.375 to 0.375
- final_projector: bfloat16 [1024, 128], replicated, may hold values from -1 to 1
- final_offset: float32 [128], replicated, may hold values from -3 to 3
- amino_strand_label: int32 [512], P('parts'), parts along dimension 0, may hold values from 0 to 7, never falling along the last dimension, each value on 1 to 128 neighbouring positions
- matched_strand_count: int32 [16, 8], P('parts'), parts along dimension 0, may hold values from 32 to 128, as said below
- couple_delta_adjoint: bfloat16 [512, 256, 128], P(('parts', 'row'), 'col'), parts along dimension 0, may hold values from -6 to 6
Outputs:
- pair_update: bfloat16 [512, 256, 128], P(('parts', 'row'), 'col'), parts along dimension 0
- adjoint_first_factor: bfloat16 [256, 8192], P(('parts', 'col'), 'row'), parts along dimension 0
- grad_right: bfloat16 [256, 8192], P(('parts', 'col'), 'row'), parts along dimension 0
- grad_w_out: float32 [2048, 128], P('parts'), parts along dimension 0
The draws below stay inside these ranges and needn't reach their ends.
There are 2 independent parts, one for each index of `parts`. The reference program is written for one: setup_inputs(seed, part) draws one part's arguments, and reference() takes and returns one part's arrays. A program takes and returns all parts, laid end to end along the dimension named above; an argument that names none is the same for every part. Nothing has to cross between parts.
Inputs may be any that keep to these rules, and one draw needn't show every extreme that they name: `amino_strand_label`: chain numbers never fall along the residues; a chain has 1 to 128 residues. `matched_strand_count`: every entry is a multiple of 32.
All inputs are finite; a program needn't handle non-finite values.
Results may differ from the reference program's by a relative error of at most 0.018.
Values may be sent and summed in bfloat16 or wider, within the bound.
No kernel may reach another device: no remote copies, remote signals or barrier semaphores. Data moves between devices by JAX's collectives and lax.ppermute only.
A program may use at most 256 MiB of HBM per device.

```python
import math
import jax
import jax.numpy as jnp
import numpy as np
from jax import lax

ALIGNED_HOMOLOGS = 128
ALIGNED_FEATS = 256
PROJECTED_SIZE = 32
CZ = 128
WINDOW_AMINOS = 256
DEPTH_STEP = 32
CHAINS = 8
LEVELS = 4
N_ROW = 4


def draw_matched_strand_count(key, part):
    levels = jax.random.randint(jax.random.fold_in(key, 11), (CHAINS * CHAINS,), 1, LEVELS + 1)
    spots = jax.random.permutation(jax.random.fold_in(key, 12), CHAINS * CHAINS)
    levels = levels.at[spots[0]].set(LEVELS).at[spots[1]].set(1)
    return (levels * DEPTH_STEP).reshape(CHAINS, CHAINS).astype(jnp.int32)


def steps_of(key, shape, shards, smallest, top_value):
    def one(dim, shards_of):
        steps = jax.random.uniform(jax.random.fold_in(jax.random.fold_in(key, 6), dim), (shards_of,), jnp.float32, smallest / len(shards), top_value / len(shards))
        return jnp.repeat(jnp.exp(steps), shape[dim] // shards_of).reshape((-1,) + (1,) * (len(shape) - dim - 1))

    loudness = one(*shards[0])
    for cut in shards[1:]:
        loudness = loudness * one(*cut)
    return loudness


def length_profile(amount, total, reach, lean):
    weights = [(1 << 20) // math.isqrt(grade ** lean) + 1 for grade in range(2, amount + 1)]
    rest, counts = total - reach - (amount - 1), [1] * (amount - 1)
    while rest > 0:
        free = [i for i in range(amount - 1) if counts[i] < reach]
        pool, budget = sum([weights[i] for i in free]), rest
        for i in free:
            more = min(reach - counts[i], max(1, budget * weights[i] // pool), rest)
            counts[i] = counts[i] + more
            rest = rest - more
    return np.array([reach] + counts)


def uneven(stream_key, amount, total, bound, slope):
    if amount == 2:
        one = jax.random.randint(stream_key, (), max(1, total - bound), min(bound, total - 1) + 1)
        return jnp.stack([one, total - one])
    sizes = jnp.asarray(length_profile(amount, total, bound, slope), jnp.int32)
    twos = (amount - 1) // 2
    donor, taker = sizes[1:1 + 2 * twos:2], sizes[2:2 + 2 * twos:2]
    slack = jnp.minimum(donor - 1, bound - taker)
    shifted = jax.random.randint(jax.random.fold_in(stream_key, 1), (twos,), 0, 1 << 20) % (slack + 1)
    sizes = sizes.at[1:1 + 2 * twos:2].set(donor - shifted).at[2:2 + 2 * twos:2].set(taker + shifted)
    return sizes[jax.random.permutation(jax.random.fold_in(stream_key, 2), amount)]


def bell_draw(own_key, shape, scale, limit, cuts=(), held_as=jnp.bfloat16):
    array = scale * jax.random.normal(own_key, shape, jnp.float32)
    if cuts:
        array = array * steps_of(own_key, shape, cuts, -0.22, 0.18)
    return jnp.clip(array, -limit, limit).astype(held_as)


def setup_inputs(seed: int = 0, part: int = 0) -> dict:
    key_of = jax.random.split(jax.random.key(seed), 11)
    part_splits = jax.random.split(jax.random.fold_in(key_of[10], part), 11)
    return {
        "alignment_tensor": bell_draw(part_splits[0], (ALIGNED_HOMOLOGS, WINDOW_AMINOS, ALIGNED_FEATS), 1.0, 6.0, ((0, 4), (1, 4))),
        "standardizer_scaling": jnp.clip(1.0 + 0.15 * jax.random.normal(key_of[1], (ALIGNED_FEATS,), jnp.float32), 0.25, 1.75),
        "standardizer_offset": bell_draw(key_of[2], (ALIGNED_FEATS,), 0.5, 3.0, (), jnp.float32),
        "first_projector": bell_draw(key_of[3], (ALIGNED_FEATS, PROJECTED_SIZE), ALIGNED_FEATS ** -0.5, 0.375),
        "second_projector": bell_draw(key_of[4], (ALIGNED_FEATS, PROJECTED_SIZE), ALIGNED_FEATS ** -0.5, 0.375),
        "final_projector": bell_draw(key_of[5], (PROJECTED_SIZE * PROJECTED_SIZE, CZ), PROJECTED_SIZE ** -0.5, 1.0),
        "final_offset": bell_draw(key_of[6], (CZ,), 0.5, 3.0, (), jnp.float32),
        "amino_strand_label": jnp.searchsorted(jnp.cumsum(uneven(part_splits[7], CHAINS, WINDOW_AMINOS, WINDOW_AMINOS // 2, 1)), jnp.arange(WINDOW_AMINOS), side="right").astype(jnp.int32),
        "matched_strand_count": draw_matched_strand_count(jax.random.fold_in(jax.random.fold_in(key_of[10], part), 71), part),
        "couple_delta_adjoint": bell_draw(part_splits[9], (WINDOW_AMINOS, WINDOW_AMINOS, CZ), 1.0, 6.0, ((0, 4), (1, 4))),
    }


def standardize_entries(alignment_tensor, standard_multiplier, additive_offset):
    incoming_entries = alignment_tensor.astype(jnp.float32)
    center = incoming_entries - lax.optimization_barrier(jnp.mean(incoming_entries, axis=-1, keepdims=True))
    spread = lax.optimization_barrier(jnp.mean(center * center, axis=-1, keepdims=True))
    return (center * lax.rsqrt(spread + 1e-05) * standard_multiplier + additive_offset).astype(jnp.bfloat16)

def reference(alignment_tensor, standardizer_scaling, standardizer_offset, first_projector, second_projector, final_projector, final_offset, amino_strand_label, matched_strand_count, couple_delta_adjoint):
    standardized_entries = standardize_entries(alignment_tensor, standardizer_scaling, standardizer_offset).reshape(-1, ALIGNED_FEATS)
    first_factor = jnp.dot(standardized_entries, first_projector, preferred_element_type=jnp.float32).astype(jnp.bfloat16).reshape(ALIGNED_HOMOLOGS, WINDOW_AMINOS * PROJECTED_SIZE)
    second_factor = jnp.dot(standardized_entries, second_projector, preferred_element_type=jnp.float32).astype(jnp.bfloat16).reshape(ALIGNED_HOMOLOGS, WINDOW_AMINOS * PROJECTED_SIZE)
    chains = jnp.arange(CHAINS, dtype=jnp.int32)
    onehot = (amino_strand_label[:, None] == chains[None, :]).astype(jnp.float32)
    table = matched_strand_count.astype(jnp.float32)
    depth = jnp.dot(jnp.dot(onehot, table, precision=lax.Precision.HIGHEST), onehot.T, precision=lax.Precision.HIGHEST)
    block = WINDOW_AMINOS // N_ROW
    right_wide = second_factor.astype(jnp.float32)

    def row_block(index):
        start = (index * block).astype(jnp.int32)
        left_rows = lax.dynamic_slice_in_dim(first_factor, start * PROJECTED_SIZE, block * PROJECTED_SIZE, 1).astype(jnp.float32)
        depth_rows = lax.dynamic_slice_in_dim(depth, start, block, 0)
        grad_rows = lax.dynamic_slice_in_dim(couple_delta_adjoint, start, block, 0)
        acc = jnp.zeros((block, WINDOW_AMINOS, PROJECTED_SIZE * PROJECTED_SIZE), jnp.float32)
        for level in range(LEVELS):
            low = level * DEPTH_STEP
            prod = jnp.einsum('sa,sb->ab', left_rows[low:low + DEPTH_STEP], right_wide[low:low + DEPTH_STEP])
            prod = prod.reshape(block, PROJECTED_SIZE, WINDOW_AMINOS, PROJECTED_SIZE).transpose(0, 2, 1, 3).reshape(block, WINDOW_AMINOS, PROJECTED_SIZE * PROJECTED_SIZE)
            acc = acc + (depth_rows > low).astype(jnp.float32)[:, :, None] * prod
        outer = (acc / depth_rows[:, :, None]).astype(jnp.bfloat16)
        flat_outer = outer.reshape(-1, PROJECTED_SIZE * PROJECTED_SIZE)
        pair = (jnp.dot(flat_outer, final_projector, preferred_element_type=jnp.float32) + final_offset).astype(jnp.bfloat16)
        flat_grad = grad_rows.reshape(-1, CZ)
        back = jnp.dot(flat_grad, final_projector.T, preferred_element_type=jnp.float32).reshape(block, WINDOW_AMINOS, PROJECTED_SIZE * PROJECTED_SIZE)
        scaled = (back / depth_rows[:, :, None]).astype(jnp.bfloat16)
        weight_part = jnp.dot(flat_outer.T, flat_grad, preferred_element_type=jnp.float32)
        turned = scaled.reshape(block, WINDOW_AMINOS, PROJECTED_SIZE, PROJECTED_SIZE).transpose(0, 2, 1, 3).reshape(block * PROJECTED_SIZE, WINDOW_AMINOS * PROJECTED_SIZE).astype(jnp.float32)
        left_parts = []
        right_parts = []
        for level in range(LEVELS):
            low = level * DEPTH_STEP
            keep = (depth_rows > low).astype(jnp.float32)
            keep_wide = jnp.broadcast_to(keep[:, None, :, None], (block, PROJECTED_SIZE, WINDOW_AMINOS, PROJECTED_SIZE)).reshape(block * PROJECTED_SIZE, WINDOW_AMINOS * PROJECTED_SIZE)
            masked = turned * keep_wide
            left_parts.append(jnp.einsum('sb,ab->sa', right_wide[low:low + DEPTH_STEP], masked))
            right_parts.append(jnp.einsum('sa,ab->sb', left_rows[low:low + DEPTH_STEP], masked))
        return (pair.reshape(block, WINDOW_AMINOS, CZ), jnp.concatenate(left_parts, 0), jnp.concatenate(right_parts, 0), weight_part)
    pairs, first_factor_adjoint, right_grads, weight_parts = lax.map(row_block, jnp.arange(N_ROW, dtype=jnp.int32))
    pair_update = pairs.reshape(WINDOW_AMINOS, WINDOW_AMINOS, CZ)
    adjoint_first_factor = first_factor_adjoint.transpose(1, 0, 2).reshape(ALIGNED_HOMOLOGS, WINDOW_AMINOS * PROJECTED_SIZE).astype(jnp.bfloat16)
    grad_right = lax.optimization_barrier(jnp.sum(right_grads, axis=0)).astype(jnp.bfloat16)
    grad_w_out = lax.optimization_barrier(jnp.sum(weight_parts, axis=0)) / WINDOW_AMINOS
    return (pair_update, adjoint_first_factor, grad_right, grad_w_out)
```

```python
import functools

import jax
import jax.numpy as jnp
from jax import lax
from jax.experimental import pallas as pl
from jax.experimental.pallas import tpu as pltpu
from jax.sharding import PartitionSpec as P

PROJ = 32
CHAINS = 8
LANES = 128
PER_TILE = LANES // PROJ
WIDE = 256
F32 = jnp.float32
BF16 = jnp.bfloat16


def standardize_entries(alignment_tensor, standard_multiplier, additive_offset):
    incoming_entries = alignment_tensor.astype(F32)
    center = incoming_entries - jnp.mean(incoming_entries, axis=-1, keepdims=True)
    spread = jnp.mean(center * center, axis=-1, keepdims=True)
    return (center * lax.rsqrt(spread + 1e-05) * standard_multiplier + additive_offset).astype(BF16)


def swap_blocks(parts):
    return [
        jnp.concatenate([part[:, q * PROJ : (q + 1) * PROJ] for part in parts], axis=1)
        for q in range(PER_TILE)
    ]


def nt_dot(a, b):
    return lax.dot_general(a, b, (((1,), (1,)), ((), ())), preferred_element_type=F32)


def nn_dot(a, b):
    return lax.dot_general(a, b, (((1,), (0,)), ((), ())), preferred_element_type=F32)


def back_body(grad_ref, wt_ref, out_ref):
    rows, cols, width = grad_ref.shape
    for half in range(rows // PER_TILE):
        block = grad_ref[half * PER_TILE : (half + 1) * PER_TILE].reshape(PER_TILE * cols, width)
        for t in range(PROJ // PER_TILE):
            prod = nn_dot(block, wt_ref[:, t * LANES : (t + 1) * LANES]).astype(BF16)
            turned = swap_blocks([prod[p * cols : (p + 1) * cols] for p in range(PER_TILE)])
            for q in range(PER_TILE):
                e = t * PER_TILE + q
                out_ref[e * cols : (e + 1) * cols, half * LANES : (half + 1) * LANES] = turned[q]


def back_call(grad, wt):
    rows, cols, width = grad.shape
    step = WIDE // PROJ
    return pl.pallas_call(
        back_body,
        grid=(rows // step,),
        in_specs=[
            pl.BlockSpec((step, cols, width), lambda g: (g, 0, 0)),
            pl.BlockSpec((width, PROJ * PROJ), lambda g: (0, 0)),
        ],
        out_specs=pl.BlockSpec((PROJ * cols, WIDE), lambda g: (0, g)),
        out_shape=jax.ShapeDtypeStruct((PROJ * cols, rows * PROJ), BF16),
        compiler_params=pltpu.CompilerParams(dimension_semantics=("arbitrary",)),
        name="back",
    )(grad, wt)


def masked_left(left_ref, lab_ref, lb_ref, pair):
    seqs = left_ref.shape[0]
    left = left_ref[...].astype(F32)
    for side in range(2):
        keep = (lab_ref[...] == 2 * pair + side).astype(F32)
        lb_ref[side * seqs : (side + 1) * seqs] = (left * keep).astype(BF16)


def grads_body(lo_ref, hi_ref, back_ref, left_ref, lab_ref, right_ref, wide_ref, tall_ref,
               left_out, right_out, rm_ref, q_ref, lb_ref, flip_ref, turn_ref):
    g = pl.program_id(0)
    seqs = left_ref.shape[0]
    span = back_ref.shape[0]
    cols = span // PROJ
    chunk = min(512, span)

    @pl.when(g == 0)
    def _():
        for a in range(CHAINS):
            weight = tall_ref[a * seqs : (a + 1) * seqs]
            row = (a % 2) * seqs
            for t in range(span // LANES):
                lanes = slice(t * LANES, (t + 1) * LANES)
                rm_ref[a // 2, row : row + seqs, lanes] = (
                    right_ref[:, lanes].astype(F32) * weight
                ).astype(BF16)
        q_ref[...] = jnp.zeros_like(q_ref)

    left_out[...] = jnp.zeros_like(left_out)

    def one_pair(pair, carry):
        masked_left(left_ref, lab_ref, lb_ref, pair)
        part = nn_dot(rm_ref[pair], back_ref[...])
        keep0 = lab_ref[...] == 2 * pair
        keep1 = lab_ref[...] == 2 * pair + 1
        left_out[...] += jnp.where(keep0, part[:seqs], 0.0) + jnp.where(keep1, part[seqs:], 0.0)

        def rows_of(m, c):
            rows = pl.ds(pl.multiple_of(m * chunk, chunk), chunk)
            q_ref[pair, rows] += nt_dot(back_ref[rows], lb_ref[...])
            return c

        lax.fori_loop(0, span // chunk, rows_of, 0)
        return carry

    lax.fori_loop(lo_ref[g], hi_ref[g] + 1, one_pair, 0)

    @pl.when(g == pl.num_programs(0) - 1)
    def _():
        for e in range(PROJ):
            rows = slice(e * cols, (e + 1) * cols)
            total = jnp.zeros((cols, seqs), F32)
            for a in range(CHAINS):
                lanes = slice((a % 2) * seqs, (a % 2 + 1) * seqs)
                total += q_ref[a // 2, rows, lanes] * wide_ref[:, a * seqs : (a + 1) * seqs]
            flip_ref[rows] = total
        for j in range(cols):
            turn_ref[j * PROJ : (j + 1) * PROJ] = flip_ref[pl.ds(j, PROJ, stride=cols)]
        for t in range(span // LANES):
            rows = slice(t * LANES, (t + 1) * LANES)
            right_out[:, rows] = turn_ref[rows].T.astype(BF16)


def grads_call(lo, hi, back, left, lab, right, wide, tall):
    span, total = back.shape
    seqs = left.shape[0]
    whole = lambda shape: pl.BlockSpec(shape, lambda g, lo, hi: (0, 0))
    return pl.pallas_call(
        grads_body,
        grid_spec=pltpu.PrefetchScalarGridSpec(
            num_scalar_prefetch=2,
            grid=(total // WIDE,),
            in_specs=[
                pl.BlockSpec((span, WIDE), lambda g, lo, hi: (0, g)),
                pl.BlockSpec((seqs, WIDE), lambda g, lo, hi: (0, g)),
                pl.BlockSpec((1, WIDE), lambda g, lo, hi: (0, g)),
                whole(right.shape),
                whole(wide.shape),
                whole(tall.shape),
            ],
            out_specs=[
                pl.BlockSpec((seqs, WIDE), lambda g, lo, hi: (0, g)),
                whole((seqs, span)),
            ],
            scratch_shapes=[
                pltpu.VMEM((CHAINS // 2, 2 * seqs, span), BF16),
                pltpu.VMEM((CHAINS // 2, span, 2 * seqs), F32),
                pltpu.VMEM((2 * seqs, WIDE), BF16),
                pltpu.VMEM((span, seqs), F32),
                pltpu.VMEM((span, seqs), F32),
            ],
        ),
        out_shape=[
            jax.ShapeDtypeStruct((seqs, total), F32),
            jax.ShapeDtypeStruct((seqs, span), BF16),
        ],
        compiler_params=pltpu.CompilerParams(dimension_semantics=("arbitrary",)),
        name="grads",
    )(lo, hi, back, left, lab, right, wide, tall)


def forward_body(lo_ref, hi_ref, left_ref, lab_ref, right_ref, wide_ref, w_ref, bias_ref, grad_ref,
                 pair_out, weight_out, rm_ref, lb_ref, acc_ref, x_ref, sum_ref, turn_ref):
    g = pl.program_id(0)
    seqs = left_ref.shape[0]
    span = right_ref.shape[0]
    cols = span // PROJ
    chunk = min(512, span)
    rows_here, _, width = grad_ref.shape

    @pl.when(g == 0)
    def _():
        for a in range(CHAINS):
            weight = wide_ref[:, a * seqs : (a + 1) * seqs]
            lanes = slice((a % 2) * seqs, (a % 2 + 1) * seqs)
            for e in range(PROJ):
                rows = slice(e * cols, (e + 1) * cols)
                rm_ref[a // 2, rows, lanes] = (right_ref[rows].astype(F32) * weight).astype(BF16)
        sum_ref[...] = jnp.zeros_like(sum_ref)

    def product(pair, add):
        masked_left(left_ref, lab_ref, lb_ref, pair)

        def rows_of(m, c):
            rows = pl.ds(pl.multiple_of(m * chunk, chunk), chunk)
            part = nn_dot(rm_ref[pair, rows], lb_ref[...])
            acc_ref[rows] = acc_ref[rows] + part if add else part
            return c

        lax.fori_loop(0, span // chunk, rows_of, 0)

    product(lo_ref[g], False)

    def more(pair, carry):
        product(pair, True)
        return carry

    lax.fori_loop(lo_ref[g] + 1, hi_ref[g] + 1, more, 0)

    for half in range(WIDE // LANES):
        lanes = slice(half * LANES, (half + 1) * LANES)
        for t in range(PROJ // PER_TILE):
            parts = []
            for q in range(PER_TILE):
                e = t * PER_TILE + q
                parts.append(acc_ref[e * cols : (e + 1) * cols, lanes].astype(BF16))
            turned = swap_blocks(parts)
            for p in range(PER_TILE):
                i = half * PER_TILE + p
                x_ref[i * cols : (i + 1) * cols, t * LANES : (t + 1) * LANES] = turned[p]

    pair = nn_dot(x_ref[...], w_ref[...]) + bias_ref[...]
    pair_out[...] = pair.astype(BF16).reshape(rows_here, cols, width)
    flat = grad_ref[...].reshape(rows_here * cols, width)
    sum_ref[...] += nn_dot(flat.T, x_ref[...])

    @pl.when(g == pl.num_programs(0) - 1)
    def _():
        for t in range(PROJ * PROJ // LANES):
            part = slice(t * LANES, (t + 1) * LANES)
            turn_ref[part] = sum_ref[:, part].T
        for c in range(PROJ):
            weight_out[c * PROJ : (c + 1) * PROJ] = turn_ref[pl.ds(c, PROJ, stride=PROJ)]


def forward_call(lo, hi, left, lab, right, wide, w, bias, grad):
    rows, cols, width = grad.shape
    seqs, total = left.shape
    span = right.shape[0]
    step = WIDE // PROJ
    whole = lambda shape: pl.BlockSpec(shape, lambda g, lo, hi: (0, 0))
    return pl.pallas_call(
        forward_body,
        grid_spec=pltpu.PrefetchScalarGridSpec(
            num_scalar_prefetch=2,
            grid=(total // WIDE,),
            in_specs=[
                pl.BlockSpec((seqs, WIDE), lambda g, lo, hi: (0, g)),
                pl.BlockSpec((1, WIDE), lambda g, lo, hi: (0, g)),
                whole(right.shape),
                whole(wide.shape),
                whole(w.shape),
                whole(bias.shape),
                pl.BlockSpec((step, cols, width), lambda g, lo, hi: (g, 0, 0)),
            ],
            out_specs=[
                pl.BlockSpec((step, cols, width), lambda g, lo, hi: (g, 0, 0)),
                whole((PROJ * PROJ, width)),
            ],
            scratch_shapes=[
                pltpu.VMEM((CHAINS // 2, span, 2 * seqs), BF16),
                pltpu.VMEM((2 * seqs, WIDE), BF16),
                pltpu.VMEM((span, WIDE), F32),
                pltpu.VMEM((step * cols, PROJ * PROJ), BF16),
                pltpu.VMEM((width, PROJ * PROJ), F32),
                pltpu.VMEM((PROJ * PROJ, width), F32),
            ],
        ),
        out_shape=[
            jax.ShapeDtypeStruct((rows, cols, width), BF16),
            jax.ShapeDtypeStruct((PROJ * PROJ, width), F32),
        ],
        compiler_params=pltpu.CompilerParams(dimension_semantics=("arbitrary",)),
        name="forward",
    )(lo, hi, left, lab, right, wide, w, bias, grad)


def shards(n_row, n_col, alignment_tensor, gain, shift, first_projector, second_projector,
           final_projector, final_offset, labels, counts, grad):
    here, rows, feats = alignment_tensor.shape
    cols, width = grad.shape[1:]
    seqs = here * n_col
    my_row, my_col = lax.axis_index("row"), lax.axis_index("col")
    normed = standardize_entries(alignment_tensor, gain, shift).reshape(-1, feats)
    left = jnp.dot(normed, first_projector, preferred_element_type=F32).astype(BF16)
    right = jnp.dot(normed, second_projector, preferred_element_type=F32).astype(BF16)
    left = left.reshape(here, rows * PROJ)
    right = right.reshape(here, rows * PROJ)

    left = lax.all_gather(left, "col", axis=0, tiled=True)
    right = lax.all_gather(right, "row", axis=1, tiled=True)
    right = lax.all_to_all(right, "col", split_axis=1, concat_axis=0, tiled=True)

    w = final_projector.reshape(PROJ, PROJ, width).transpose(1, 0, 2).reshape(PROJ * PROJ, width)
    back = back_call(grad, w.T)

    row_labels = lax.dynamic_slice_in_dim(labels, my_row * rows, rows, 0)
    col_labels = lax.dynamic_slice_in_dim(labels, my_col * cols, cols, 0)
    lab = jnp.repeat(row_labels, PROJ)[None, :]
    step = WIDE // PROJ
    lo = row_labels[::step] // 2
    hi = row_labels[step - 1 :: step] // 2
    chains = jnp.arange(CHAINS, dtype=jnp.int32)
    col_hot = col_labels[:, None, None] == chains[None, None, :]
    depth = jnp.sum(jnp.where(col_hot, counts[None, :, :], 0), axis=-1)
    seq = jnp.arange(seqs, dtype=jnp.int32)
    wide = jnp.where(seq[None, None, :] < depth[:, :, None], 1.0 / depth.astype(F32)[:, :, None], 0.0)
    tall = jnp.tile(wide.transpose(1, 2, 0).reshape(CHAINS * seqs, cols), (1, LANES // cols))
    wide = wide.reshape(cols, CHAINS * seqs)

    turned = right.reshape(seqs, cols, PROJ).transpose(0, 2, 1).reshape(seqs, PROJ * cols)
    left_grad, right_grad = grads_call(lo, hi, back, left, lab, turned, wide, tall)
    pair_update, weight = forward_call(
        lo, hi, left, lab, turned.T, wide, w, final_offset[None, :], grad
    )

    adjoint_first = lax.psum_scatter(left_grad.astype(BF16), "col", scatter_dimension=0, tiled=True)
    parts = lax.all_to_all(right_grad, "col", split_axis=0, concat_axis=1, tiled=True)
    grad_right = lax.psum_scatter(parts, "row", scatter_dimension=1, tiled=True)
    grad_w_out = lax.psum(weight, ("row", "col")) / (n_row * rows)
    return pair_update, adjoint_first, grad_right, grad_w_out


def solution(mesh):
    in_specs = (
        P(("parts", "col"), "row", None),
        P(),
        P(),
        P(),
        P(),
        P(),
        P(),
        P("parts"),
        P("parts", None),
        P(("parts", "row"), "col", None),
    )
    out_specs = (
        P(("parts", "row"), "col", None),
        P(("parts", "col"), "row"),
        P(("parts", "col"), "row"),
        P("parts", None),
    )
    body = functools.partial(shards, mesh.shape["row"], mesh.shape["col"])
    return jax.shard_map(body, mesh=mesh, in_specs=in_specs, out_specs=out_specs, check_vma=False)
```

```python
import functools

import jax
import jax.numpy as jnp
from jax import lax
from jax.experimental import pallas as pl
from jax.experimental.pallas import tpu as pltpu
from jax.sharding import PartitionSpec as P

PROJ = 32
CHAINS = 8
LANES = 128
PER_TILE = LANES // PROJ
WIDE = 256
F32 = jnp.float32
BF16 = jnp.bfloat16


def standardize_entries(alignment_tensor, standard_multiplier, additive_offset):
    incoming_entries = alignment_tensor.astype(F32)
    center = incoming_entries - jnp.mean(incoming_entries, axis=-1, keepdims=True)
    spread = jnp.mean(center * center, axis=-1, keepdims=True)
    return (center * lax.rsqrt(spread + 1e-05) * standard_multiplier + additive_offset).astype(BF16)


def swap_blocks(parts):
    return [
        jnp.concatenate([part[:, q * PROJ : (q + 1) * PROJ] for part in parts], axis=1)
        for q in range(PER_TILE)
    ]


def nt_dot(a, b):
    return lax.dot_general(a, b, (((1,), (1,)), ((), ())), preferred_element_type=F32)


def nn_dot(a, b):
    return lax.dot_general(a, b, (((1,), (0,)), ((), ())), preferred_element_type=F32)


def cost(passes, span, total, seqs):
    return pl.CostEstimate(
        flops=4 * passes * span * total * seqs, bytes_accessed=2 * span * total, transcendentals=0
    )


def back_body(grad_ref, wt_ref, out_ref):
    rows, cols, width = grad_ref.shape
    for half in range(rows // PER_TILE):
        block = grad_ref[half * PER_TILE : (half + 1) * PER_TILE].reshape(PER_TILE * cols, width)
        for t in range(PROJ // PER_TILE):
            prod = nn_dot(block, wt_ref[:, t * LANES : (t + 1) * LANES]).astype(BF16)
            turned = swap_blocks([prod[p * cols : (p + 1) * cols] for p in range(PER_TILE)])
            for q in range(PER_TILE):
                e = t * PER_TILE + q
                out_ref[e * cols : (e + 1) * cols, half * LANES : (half + 1) * LANES] = turned[q]


def back_call(grad, wt):
    rows, cols, width = grad.shape
    step = WIDE // PROJ
    return pl.pallas_call(
        back_body,
        grid=(rows // step,),
        in_specs=[
            pl.BlockSpec((step, cols, width), lambda g: (g, 0, 0)),
            pl.BlockSpec((width, PROJ * PROJ), lambda g: (0, 0)),
        ],
        out_specs=pl.BlockSpec((PROJ * cols, WIDE), lambda g: (0, g)),
        out_shape=jax.ShapeDtypeStruct((PROJ * cols, rows * PROJ), BF16),
        compiler_params=pltpu.CompilerParams(dimension_semantics=("arbitrary",)),
        cost_estimate=cost(10, PROJ * cols, rows * PROJ, width),
        name="back",
    )(grad, wt)


def masked_left(left_ref, lab_ref, lb_ref, pair):
    seqs = left_ref.shape[0]
    left = left_ref[...].astype(F32)
    for side in range(2):
        keep = (lab_ref[...] == 2 * pair + side).astype(F32)
        lb_ref[side * seqs : (side + 1) * seqs] = (left * keep).astype(BF16)


def right_grad_body(lo_ref, hi_ref, back_ref, left_ref, lab_ref, wide_ref,
                    right_out, q_ref, lb_ref, flip_ref, turn_ref):
    g = pl.program_id(0)
    seqs = left_ref.shape[0]
    span = back_ref.shape[0]
    cols = span // PROJ
    chunk = min(512, span)

    @pl.when(g == 0)
    def _():
        q_ref[...] = jnp.zeros_like(q_ref)

    def one_pair(pair, carry):
        masked_left(left_ref, lab_ref, lb_ref, pair)

        def rows_of(m, c):
            rows = pl.ds(pl.multiple_of(m * chunk, chunk), chunk)
            q_ref[pair, rows] += nt_dot(back_ref[rows], lb_ref[...])
            return c

        lax.fori_loop(0, span // chunk, rows_of, 0)
        return carry

    lax.fori_loop(lo_ref[g], hi_ref[g] + 1, one_pair, 0)

    @pl.when(g == pl.num_programs(0) - 1)
    def _():
        for e in range(PROJ):
            rows = slice(e * cols, (e + 1) * cols)
            total = jnp.zeros((cols, seqs), F32)
            for a in range(CHAINS):
                lanes = slice((a % 2) * seqs, (a % 2 + 1) * seqs)
                total += q_ref[a // 2, rows, lanes] * wide_ref[:, a * seqs : (a + 1) * seqs]
            flip_ref[rows] = total
        for j in range(cols):
            turn_ref[j * PROJ : (j + 1) * PROJ] = flip_ref[pl.ds(j, PROJ, stride=cols)]
        for t in range(span // LANES):
            rows = slice(t * LANES, (t + 1) * LANES)
            right_out[:, rows] = turn_ref[rows].T.astype(BF16)


def right_grad_call(lo, hi, back, left, lab, wide):
    span, total = back.shape
    seqs = left.shape[0]
    whole = lambda shape: pl.BlockSpec(shape, lambda g, lo, hi: (0, 0))
    return pl.pallas_call(
        right_grad_body,
        grid_spec=pltpu.PrefetchScalarGridSpec(
            num_scalar_prefetch=2,
            grid=(total // WIDE,),
            in_specs=[
                pl.BlockSpec((span, WIDE), lambda g, lo, hi: (0, g)),
                pl.BlockSpec((seqs, WIDE), lambda g, lo, hi: (0, g)),
                pl.BlockSpec((1, WIDE), lambda g, lo, hi: (0, g)),
                whole(wide.shape),
            ],
            out_specs=whole((seqs, span)),
            scratch_shapes=[
                pltpu.VMEM((CHAINS // 2, span, 2 * seqs), F32),
                pltpu.VMEM((2 * seqs, WIDE), BF16),
                pltpu.VMEM((span, seqs), F32),
                pltpu.VMEM((span, seqs), F32),
            ],
        ),
        out_shape=jax.ShapeDtypeStruct((seqs, span), BF16),
        compiler_params=pltpu.CompilerParams(dimension_semantics=("arbitrary",)),
        cost_estimate=cost(10, span, total, seqs),
        name="right_grad",
    )(lo, hi, back, left, lab, wide)


def left_grad_body(lo_ref, hi_ref, back_ref, lab_ref, right_ref, tall_ref, left_out, rm_ref):
    g = pl.program_id(0)
    seqs = right_ref.shape[0]
    span = back_ref.shape[0]

    @pl.when(g == 0)
    def _():
        for a in range(CHAINS):
            weight = tall_ref[a * seqs : (a + 1) * seqs]
            row = (a % 2) * seqs
            for t in range(span // LANES):
                lanes = slice(t * LANES, (t + 1) * LANES)
                rm_ref[a // 2, row : row + seqs, lanes] = (
                    right_ref[:, lanes].astype(F32) * weight
                ).astype(BF16)

    def one_pair(pair, total):
        part = nn_dot(rm_ref[pair], back_ref[...])
        keep0 = lab_ref[...] == 2 * pair
        keep1 = lab_ref[...] == 2 * pair + 1
        return total + jnp.where(keep0, part[:seqs], 0.0) + jnp.where(keep1, part[seqs:], 0.0)

    total = lax.fori_loop(lo_ref[g], hi_ref[g] + 1, one_pair, jnp.zeros(left_out.shape, F32))
    left_out[...] = total.astype(BF16)


def left_grad_call(lo, hi, back, lab, right, tall):
    span, total = back.shape
    seqs = right.shape[0]
    whole = lambda shape: pl.BlockSpec(shape, lambda g, lo, hi: (0, 0))
    return pl.pallas_call(
        left_grad_body,
        grid_spec=pltpu.PrefetchScalarGridSpec(
            num_scalar_prefetch=2,
            grid=(total // WIDE,),
            in_specs=[
                pl.BlockSpec((span, WIDE), lambda g, lo, hi: (0, g)),
                pl.BlockSpec((1, WIDE), lambda g, lo, hi: (0, g)),
                whole(right.shape),
                whole(tall.shape),
            ],
            out_specs=pl.BlockSpec((seqs, WIDE), lambda g, lo, hi: (0, g)),
            scratch_shapes=[pltpu.VMEM((CHAINS // 2, 2 * seqs, span), BF16)],
        ),
        out_shape=jax.ShapeDtypeStruct((seqs, total), BF16),
        compiler_params=pltpu.CompilerParams(dimension_semantics=("arbitrary",)),
        cost_estimate=cost(10, span, total, seqs),
        name="left_grad",
    )(lo, hi, back, lab, right, tall)


def forward_body(lo_ref, hi_ref, left_ref, lab_ref, right_ref, wide_ref, w_ref, bias_ref, grad_ref,
                 pair_out, weight_out, rm_ref, lb_ref, acc_ref, x_ref, sum_ref, turn_ref):
    g = pl.program_id(0)
    seqs = left_ref.shape[0]
    span = right_ref.shape[0]
    cols = span // PROJ
    chunk = min(512, span)
    rows_here, _, width = grad_ref.shape

    @pl.when(g == 0)
    def _():
        for a in range(CHAINS):
            weight = wide_ref[:, a * seqs : (a + 1) * seqs]
            lanes = slice((a % 2) * seqs, (a % 2 + 1) * seqs)
            for e in range(PROJ):
                rows = slice(e * cols, (e + 1) * cols)
                rm_ref[a // 2, rows, lanes] = (right_ref[rows].astype(F32) * weight).astype(BF16)
        sum_ref[...] = jnp.zeros_like(sum_ref)

    def product(pair, add):
        masked_left(left_ref, lab_ref, lb_ref, pair)

        def rows_of(m, c):
            rows = pl.ds(pl.multiple_of(m * chunk, chunk), chunk)
            part = nn_dot(rm_ref[pair, rows], lb_ref[...])
            acc_ref[rows] = acc_ref[rows] + part if add else part
            return c

        lax.fori_loop(0, span // chunk, rows_of, 0)

    product(lo_ref[g], False)

    def more(pair, carry):
        product(pair, True)
        return carry

    lax.fori_loop(lo_ref[g] + 1, hi_ref[g] + 1, more, 0)

    for half in range(WIDE // LANES):
        lanes = slice(half * LANES, (half + 1) * LANES)
        for t in range(PROJ // PER_TILE):
            parts = []
            for q in range(PER_TILE):
                e = t * PER_TILE + q
                parts.append(acc_ref[e * cols : (e + 1) * cols, lanes].astype(BF16))
            turned = swap_blocks(parts)
            for p in range(PER_TILE):
                i = half * PER_TILE + p
                x_ref[i * cols : (i + 1) * cols, t * LANES : (t + 1) * LANES] = turned[p]

    pair = nn_dot(x_ref[...], w_ref[...]) + bias_ref[...]
    pair_out[...] = pair.astype(BF16).reshape(rows_here, cols, width)
    flat = grad_ref[...].reshape(rows_here * cols, width)
    sum_ref[...] += nn_dot(flat.T, x_ref[...])

    @pl.when(g == pl.num_programs(0) - 1)
    def _():
        for t in range(PROJ * PROJ // LANES):
            part = slice(t * LANES, (t + 1) * LANES)
            turn_ref[part] = sum_ref[:, part].T
        for c in range(PROJ):
            weight_out[c * PROJ : (c + 1) * PROJ] = turn_ref[pl.ds(c, PROJ, stride=PROJ)]


def forward_call(lo, hi, left, lab, right, wide, w, bias, grad):
    rows, cols, width = grad.shape
    seqs, total = left.shape
    span = right.shape[0]
    step = WIDE // PROJ
    whole = lambda shape: pl.BlockSpec(shape, lambda g, lo, hi: (0, 0))
    return pl.pallas_call(
        forward_body,
        grid_spec=pltpu.PrefetchScalarGridSpec(
            num_scalar_prefetch=2,
            grid=(total // WIDE,),
            in_specs=[
                pl.BlockSpec((seqs, WIDE), lambda g, lo, hi: (0, g)),
                pl.BlockSpec((1, WIDE), lambda g, lo, hi: (0, g)),
                whole(right.shape),
                whole(wide.shape),
                whole(w.shape),
                whole(bias.shape),
                pl.BlockSpec((step, cols, width), lambda g, lo, hi: (g, 0, 0)),
            ],
            out_specs=[
                pl.BlockSpec((step, cols, width), lambda g, lo, hi: (g, 0, 0)),
                whole((PROJ * PROJ, width)),
            ],
            scratch_shapes=[
                pltpu.VMEM((CHAINS // 2, span, 2 * seqs), BF16),
                pltpu.VMEM((2 * seqs, WIDE), BF16),
                pltpu.VMEM((span, WIDE), F32),
                pltpu.VMEM((step * cols, PROJ * PROJ), BF16),
                pltpu.VMEM((width, PROJ * PROJ), F32),
                pltpu.VMEM((PROJ * PROJ, width), F32),
            ],
        ),
        out_shape=[
            jax.ShapeDtypeStruct((rows, cols, width), BF16),
            jax.ShapeDtypeStruct((PROJ * PROJ, width), F32),
        ],
        compiler_params=pltpu.CompilerParams(dimension_semantics=("arbitrary",)),
        cost_estimate=cost(20, span, total, seqs),
        name="forward",
    )(lo, hi, left, lab, right, wide, w, bias, grad)


class Ring:
    def __init__(self, n_row, n_col):
        self.n_row, self.n_col = n_row, n_col
        self.n_x = n_row // 2
        self.per_row = n_col // n_row
        self.row = lax.axis_index("row").astype(jnp.uint32)
        self.col = lax.axis_index("col").astype(jnp.uint32)
        self.x, self.core = self.row // 2, self.row % 2

    def core_of(self, col):
        return (col // self.per_row) % 2

    def col_shift(self, value, k):
        n = self.n_col
        return lax.ppermute(value, "col", [((t + k) % n, t) for t in range(n)])

    def row_shift(self, value, k):
        n = self.n_row
        return lax.ppermute(value, "row", [((t + k) % n, t) for t in range(n)])

    def x_shift(self, value, k):
        return self.row_shift(value, 2 * k)

    def other_core(self, value):
        return lax.ppermute(value, "row", [(t ^ 1, t) for t in range(self.n_row)])

    def along_col(self, value, k, outward):
        pairs = []
        for r in range(self.n_row):
            for t in range(self.n_col):
                q = (t - k) % self.n_col
                if self.core_of(q) == r % 2:
                    far, near = r * self.n_col + t, r * self.n_col + q
                    pairs.append((far, near) if outward else (near, far))
        return lax.ppermute(value, ("row", "col"), pairs)

    def right_to_cols(self, right):
        here, lanes = right.shape
        lanes //= self.per_row
        by_x = jnp.stack([right] + [self.x_shift(right, k) for k in range(1, self.n_x)])
        blocks = []
        for k in range(self.n_col):
            q = (self.col + (self.n_col - k)) % self.n_col
            which = ((q // self.per_row) // 2 + self.n_x - self.x) % self.n_x
            piece = lax.dynamic_slice(
                by_x, (which, jnp.uint32(0), (q % self.per_row) * lanes), (1, here, lanes)
            )
            blocks.append(self.along_col(piece[0], k, True) if k else piece[0])
        mine = jnp.concatenate(blocks, axis=0)
        return jnp.where(self.core_of(self.col) == self.core, mine, self.other_core(mine))

    def right_from_cols(self, grad):
        lanes = grad.shape[1]
        here = grad.shape[0] // self.n_col
        both = (grad.astype(F32) + self.other_core(grad).astype(F32)).astype(BF16)
        by_row = jnp.zeros((self.n_x, here, self.per_row * lanes), BF16)
        for k in range(self.n_col):
            block = both[k * here : (k + 1) * here]
            q = (self.col + (self.n_col - k)) % self.n_col
            fits = self.core_of(q) == self.core
            got = self.along_col(block, k, False) if k else block
            got = jnp.where(fits, got, 0)
            which = ((q // self.per_row) // 2 + self.n_x - self.x) % self.n_x
            at = (which, jnp.uint32(0), (q % self.per_row) * lanes)
            old = lax.dynamic_slice(by_row, at, (1, here, lanes))
            by_row = lax.dynamic_update_slice(by_row, old + got[None], at)
        total = by_row[0].astype(F32)
        for k in range(1, self.n_x):
            total += self.x_shift(by_row[k], self.n_x - k).astype(F32)
        return total.astype(BF16)

    def weight_sum(self, weight):
        n = self.n_row
        size = weight.shape[0] // n
        sent = weight.astype(BF16).reshape(n, size, -1)
        pick = lambda k: lax.dynamic_index_in_dim(sent, (self.row + k) % n, 0, keepdims=False)
        total = lax.dynamic_index_in_dim(weight.reshape(n, size, -1), self.row, 0, keepdims=False)
        for k in range(1, n):
            total += self.row_shift(pick(k), n - k).astype(F32)
        mine = total.astype(BF16)
        for k in range(1, self.n_col):
            total += self.col_shift(mine, k).astype(F32)
        mine = total.astype(BF16)
        turns = jnp.stack([mine] + [self.row_shift(mine, k) for k in range(1, n)])
        turns = jnp.concatenate([turns, turns])
        return lax.dynamic_slice_in_dim(turns, (n - self.row) % n, n, 0).reshape(weight.shape)


def shards(n_row, n_col, alignment_tensor, gain, shift, first_projector, second_projector,
           final_projector, final_offset, labels, counts, grad):
    ring = Ring(n_row, n_col)
    here, rows, feats = alignment_tensor.shape
    cols, width = grad.shape[1:]
    seqs = here * n_col
    normed = standardize_entries(alignment_tensor, gain, shift).reshape(-1, feats)
    left = jnp.dot(normed, first_projector, preferred_element_type=F32).astype(BF16)
    right = jnp.dot(normed, second_projector, preferred_element_type=F32).astype(BF16)
    left = left.reshape(here, rows * PROJ)
    right = right.reshape(here, rows // cols, cols, PROJ).transpose(0, 1, 3, 2)
    right = ring.right_to_cols(right.reshape(here, rows * PROJ))
    left = jnp.concatenate([left] + [ring.col_shift(left, k) for k in range(1, n_col)])

    w = final_projector.reshape(PROJ, PROJ, width).transpose(1, 0, 2).reshape(PROJ * PROJ, width)
    back = back_call(grad, w.T)

    row_labels = lax.dynamic_slice_in_dim(labels, ring.row * rows, rows, 0)
    col_labels = lax.dynamic_slice_in_dim(labels, ring.col * cols, cols, 0)
    lab = jnp.repeat(row_labels, PROJ)[None, :]
    step = WIDE // PROJ
    lo = row_labels[::step] // 2
    hi = row_labels[step - 1 :: step] // 2
    chains = jnp.arange(CHAINS, dtype=jnp.int32)
    col_hot = col_labels[:, None, None] == chains[None, None, :]
    depth = jnp.sum(jnp.where(col_hot, counts[None, :, :], 0), axis=-1)
    seq = (jnp.arange(seqs, dtype=jnp.uint32) + ring.col * here) % seqs
    seq = seq.astype(jnp.int32)
    wide = jnp.where(seq[None, None, :] < depth[:, :, None], 1.0 / depth.astype(F32)[:, :, None], 0.0)
    tall = jnp.tile(wide.transpose(1, 2, 0).reshape(CHAINS * seqs, cols), (1, LANES // cols))
    wide = wide.reshape(cols, CHAINS * seqs)

    right_grad = right_grad_call(lo, hi, back, left, lab, wide)
    left_grad = left_grad_call(lo, hi, back, lab, right, tall)
    pair_update, weight = forward_call(
        lo, hi, left, lab, right.T, wide, w, final_offset[None, :], grad
    )

    grad_right = ring.right_from_cols(right_grad)
    total = left_grad[:here].astype(F32)
    for k in range(1, n_col):
        total += ring.col_shift(left_grad[k * here : (k + 1) * here], n_col - k).astype(F32)
    adjoint_first = total.astype(BF16)
    grad_w_out = ring.weight_sum(weight).astype(F32) / (n_row * rows)
    return pair_update, adjoint_first, grad_right, grad_w_out


def solution(mesh):
    in_specs = (
        P(("parts", "col"), "row", None),
        P(),
        P(),
        P(),
        P(),
        P(),
        P(),
        P("parts"),
        P("parts", None),
        P(("parts", "row"), "col", None),
    )
    out_specs = (
        P(("parts", "row"), "col", None),
        P(("parts", "col"), "row"),
        P(("parts", "col"), "row"),
        P("parts", None),
    )
    body = functools.partial(shards, mesh.shape["row"], mesh.shape["col"])
    return jax.shard_map(body, mesh=mesh, in_specs=in_specs, out_specs=out_specs, check_vma=False)
```

```python
import jax
import jax.numpy as jnp
from jax import lax
from jax.experimental import pallas as pl
from jax.experimental.pallas import tpu as pltpu
from jax.sharding import PartitionSpec as P


PROJ = 32
CHAINS = 8
LANES = 128
PER_TILE = LANES // PROJ
WIDE = 256
F32 = jnp.float32
BF16 = jnp.bfloat16


def standardize_entries(alignment_tensor, standard_multiplier, additive_offset):
    incoming_entries = alignment_tensor.astype(F32)
    center = incoming_entries - jnp.mean(incoming_entries, axis=-1, keepdims=True)
    spread = jnp.mean(center * center, axis=-1, keepdims=True)
    return (center * lax.rsqrt(spread + 1e-05) * standard_multiplier + additive_offset).astype(BF16)


def swap_blocks(parts):
    lane = lax.broadcasted_iota(jnp.int32, parts[0].shape, 1)
    for bit in (2, 1):
        shift = bit * PROJ
        low = (lane & shift) == 0
        out = list(parts)
        for p in range(PER_TILE):
            if not p & bit:
                a, b = parts[p], parts[p | bit]
                out[p] = jnp.where(low, a, pltpu.roll(b, shift, 1))
                out[p | bit] = jnp.where(low, pltpu.roll(a, LANES - shift, 1), b)
        parts = out
    return parts


def nt_dot(a, b):
    return lax.dot_general(a, b, (((1,), (1,)), ((), ())), preferred_element_type=F32)


def nn_dot(a, b):
    return lax.dot_general(a, b, (((1,), (0,)), ((), ())), preferred_element_type=F32)


def cost(passes, span, total, seqs):
    return pl.CostEstimate(
        flops=4 * passes * span * total * seqs, bytes_accessed=2 * span * total, transcendentals=0
    )


def back_body(grad_ref, wt_ref, out_ref):
    rows, cols, width = grad_ref.shape
    block = grad_ref[...].reshape(rows * cols, width)
    for u in range(PROJ * PROJ // WIDE):
        prod = nn_dot(block, wt_ref[:, u * WIDE : (u + 1) * WIDE]).astype(BF16)
        for half in range(rows // PER_TILE):
            for t in range(WIDE // LANES):
                parts = [
                    prod[(half * PER_TILE + p) * cols : (half * PER_TILE + p + 1) * cols,
                         t * LANES : (t + 1) * LANES]
                    for p in range(PER_TILE)
                ]
                for q, part in enumerate(swap_blocks(parts)):
                    e = u * (WIDE // PROJ) + t * PER_TILE + q
                    out_ref[0, e * cols : (e + 1) * cols, half * LANES : (half + 1) * LANES] = part


def back_call(grad, wt):
    rows, cols, width = grad.shape
    step = WIDE // PROJ
    return pl.pallas_call(
        back_body,
        grid=(rows // step,),
        in_specs=[
            pl.BlockSpec((step, cols, width), lambda g: (g, 0, 0)),
            pl.BlockSpec((width, PROJ * PROJ), lambda g: (0, 0)),
        ],
        out_specs=pl.BlockSpec((1, PROJ * cols, WIDE), lambda g: (g, 0, 0)),
        out_shape=jax.ShapeDtypeStruct((rows // step, PROJ * cols, WIDE), BF16),
        compiler_params=pltpu.CompilerParams(dimension_semantics=("arbitrary",)),
        cost_estimate=cost(10, PROJ * cols, rows * PROJ, width),
        name="back",
    )(grad, wt)


def masked_left(left_ref, lab_ref, lb_ref, pair):
    seqs = left_ref.shape[0]
    for side in range(2):
        keep = (lab_ref[...] == 2 * pair + side).astype(F32).astype(BF16)
        lb_ref[side * seqs : (side + 1) * seqs] = left_ref[...] * keep


def right_grad_body(lo_ref, hi_ref, back_ref, left_ref, lab_ref, wide_ref,
                    right_out, q_ref, lb_ref, flip_ref, turn_ref):
    g = pl.program_id(0)
    seqs = left_ref.shape[0]
    span = back_ref.shape[1]
    cols = span // PROJ
    last = pl.num_programs(0) - 1

    def over_pairs(fn):
        def step(pair, carry):
            fn(pair)
            return carry

        return step

    @pl.when(g == 0)
    def _():
        def clear(pair):
            q_ref[pair] = jnp.zeros(q_ref.shape[1:], F32)

        lax.fori_loop(lo_ref[0], hi_ref[last] + 1, over_pairs(clear), 0)
        flip_ref[...] = jnp.zeros_like(flip_ref)

    def one_pair(pair):
        masked_left(left_ref, lab_ref, lb_ref, pair)
        q_ref[pair] += nt_dot(back_ref[0], lb_ref[...])

    lax.fori_loop(lo_ref[g], hi_ref[g] + 1, over_pairs(one_pair), 0)

    @pl.when(g == last)
    def _():
        def combine(pair):
            for e in range(PROJ):
                rows = slice(e * cols, (e + 1) * cols)
                both = q_ref[pair, rows] * wide_ref[pair]
                flip_ref[rows] += both[:, :seqs] + both[:, seqs:]

        lax.fori_loop(lo_ref[0], hi_ref[last] + 1, over_pairs(combine), 0)
        for j in range(cols):
            turn_ref[j * PROJ : (j + 1) * PROJ] = flip_ref[pl.ds(j, PROJ, stride=cols)]
        for t in range(span // LANES):
            rows = slice(t * LANES, (t + 1) * LANES)
            right_out[:, rows] = turn_ref[rows].T.astype(BF16)


def right_grad_call(lo, hi, back, left, lab, wide):
    groups, span, _ = back.shape
    total = groups * WIDE
    seqs = left.shape[0]
    whole = lambda shape: pl.BlockSpec(shape, lambda g, lo, hi: (0,) * len(shape))
    return pl.pallas_call(
        right_grad_body,
        grid_spec=pltpu.PrefetchScalarGridSpec(
            num_scalar_prefetch=2,
            grid=(total // WIDE,),
            in_specs=[
                pl.BlockSpec((1, span, WIDE), lambda g, lo, hi: (g, 0, 0)),
                pl.BlockSpec((seqs, WIDE), lambda g, lo, hi: (0, g)),
                pl.BlockSpec((1, WIDE), lambda g, lo, hi: (0, g)),
                whole(wide.shape),
            ],
            out_specs=whole((seqs, span)),
            scratch_shapes=[
                pltpu.VMEM((CHAINS // 2, span, 2 * seqs), F32),
                pltpu.VMEM((2 * seqs, WIDE), BF16),
                pltpu.VMEM((span, seqs), F32),
                pltpu.VMEM((span, seqs), F32),
            ],
        ),
        out_shape=jax.ShapeDtypeStruct((seqs, span), BF16),
        compiler_params=pltpu.CompilerParams(dimension_semantics=("arbitrary",)),
        cost_estimate=cost(10, span, total, seqs),
        name="right_grad",
    )(lo, hi, back, left, lab, wide)


def left_grad_body(lo_ref, hi_ref, back_ref, lab_ref, right_ref, tall_ref, left_out, rm_ref):
    g = pl.program_id(0)
    seqs = right_ref.shape[1]
    span = back_ref.shape[1]

    last = pl.num_programs(0) - 1

    @pl.when(g == 0)
    def _():
        def build(pair, carry):
            for side in range(2):
                row = side * seqs
                plain, third = tall_ref[pair, 0, row : row + seqs], tall_ref[pair, 1, row : row + seqs]
                for t in range(span // LANES):
                    lanes = slice(t * LANES, (t + 1) * LANES)
                    rm_ref[pair, row : row + seqs, lanes] = (
                        right_ref[0, :, lanes] * plain + right_ref[1, :, lanes] * third
                    )
            return carry

        lax.fori_loop(lo_ref[0], hi_ref[last] + 1, build, 0)

    def one_pair(pair, total):
        part = nn_dot(rm_ref[pair], back_ref[0])
        keep0 = lab_ref[...] == 2 * pair
        keep1 = lab_ref[...] == 2 * pair + 1
        return total + jnp.where(keep0, part[:seqs], 0.0) + jnp.where(keep1, part[seqs:], 0.0)

    total = lax.fori_loop(lo_ref[g], hi_ref[g] + 1, one_pair, jnp.zeros(left_out.shape, F32))
    left_out[...] = total.astype(BF16)


def left_grad_call(lo, hi, back, lab, right, tall):
    groups, span, _ = back.shape
    total = groups * WIDE
    seqs = right.shape[1]
    whole = lambda shape: pl.BlockSpec(shape, lambda g, lo, hi: (0,) * len(shape))
    return pl.pallas_call(
        left_grad_body,
        grid_spec=pltpu.PrefetchScalarGridSpec(
            num_scalar_prefetch=2,
            grid=(total // WIDE,),
            in_specs=[
                pl.BlockSpec((1, span, WIDE), lambda g, lo, hi: (g, 0, 0)),
                pl.BlockSpec((1, WIDE), lambda g, lo, hi: (0, g)),
                whole(right.shape),
                whole(tall.shape),
            ],
            out_specs=pl.BlockSpec((seqs, WIDE), lambda g, lo, hi: (0, g)),
            scratch_shapes=[pltpu.VMEM((CHAINS // 2, 2 * seqs, span), BF16)],
        ),
        out_shape=jax.ShapeDtypeStruct((seqs, total), BF16),
        compiler_params=pltpu.CompilerParams(dimension_semantics=("arbitrary",)),
        cost_estimate=cost(10, span, total, seqs),
        name="left_grad",
    )(lo, hi, back, lab, right, tall)


def outer_body(lo_ref, hi_ref, left_ref, lab_ref, right_ref, wide_ref, grad_ref,
               x_ref, weight_out, rm_ref, lb_ref, acc_ref, sum_ref, turn_ref):
    g = pl.program_id(0)
    seqs = left_ref.shape[0]
    span = right_ref.shape[1]
    cols = span // PROJ
    rows_here, _, width = grad_ref.shape

    last = pl.num_programs(0) - 1

    @pl.when(g == 0)
    def _():
        def build(pair, carry):
            plain, third = wide_ref[pair, 0], wide_ref[pair, 1]
            for e in range(PROJ):
                rows = slice(e * cols, (e + 1) * cols)
                for side in range(2):
                    lanes = slice(side * seqs, (side + 1) * seqs)
                    rm_ref[pair, rows, lanes] = (
                        right_ref[0, rows] * plain[:, lanes] + right_ref[1, rows] * third[:, lanes]
                    )
            return carry

        lax.fori_loop(lo_ref[0], hi_ref[last] + 1, build, 0)
        sum_ref[...] = jnp.zeros_like(sum_ref)

    def product(pair):
        masked_left(left_ref, lab_ref, lb_ref, pair)
        return nn_dot(rm_ref[pair], lb_ref[...])

    acc_ref[...] = product(lo_ref[g])

    def more(pair, carry):
        acc_ref[...] += product(pair)
        return carry

    lax.fori_loop(lo_ref[g] + 1, hi_ref[g] + 1, more, 0)

    for half in range(WIDE // LANES):
        lanes = slice(half * LANES, (half + 1) * LANES)
        for t in range(PROJ // PER_TILE):
            parts = []
            for q in range(PER_TILE):
                e = t * PER_TILE + q
                parts.append(acc_ref[e * cols : (e + 1) * cols, lanes].astype(BF16))
            turned = swap_blocks(parts)
            for p in range(PER_TILE):
                i = half * PER_TILE + p
                x_ref[i * cols : (i + 1) * cols, t * LANES : (t + 1) * LANES] = turned[p]

    flat = grad_ref[...].reshape(rows_here * cols, width)
    sum_ref[...] += nn_dot(flat.T, x_ref[...])

    @pl.when(g == last)
    def _():
        for t in range(PROJ * PROJ // LANES):
            part = slice(t * LANES, (t + 1) * LANES)
            turn_ref[part] = sum_ref[:, part].T
        for c in range(PROJ):
            weight_out[c * PROJ : (c + 1) * PROJ] = turn_ref[pl.ds(c, PROJ, stride=PROJ)]


def outer_call(lo, hi, left, lab, right, wide, grad):
    rows, cols, width = grad.shape
    seqs, total = left.shape
    span = right.shape[1]
    step = WIDE // PROJ
    whole = lambda shape: pl.BlockSpec(shape, lambda g, lo, hi: (0,) * len(shape))
    return pl.pallas_call(
        outer_body,
        grid_spec=pltpu.PrefetchScalarGridSpec(
            num_scalar_prefetch=2,
            grid=(total // WIDE,),
            in_specs=[
                pl.BlockSpec((seqs, WIDE), lambda g, lo, hi: (0, g)),
                pl.BlockSpec((1, WIDE), lambda g, lo, hi: (0, g)),
                whole(right.shape),
                whole(wide.shape),
                pl.BlockSpec((step, cols, width), lambda g, lo, hi: (g, 0, 0)),
            ],
            out_specs=[
                pl.BlockSpec((step * cols, PROJ * PROJ), lambda g, lo, hi: (g, 0)),
                whole((PROJ * PROJ, width)),
            ],
            scratch_shapes=[
                pltpu.VMEM((CHAINS // 2, span, 2 * seqs), BF16),
                pltpu.VMEM((2 * seqs, WIDE), BF16),
                pltpu.VMEM((span, WIDE), F32),
                pltpu.VMEM((width, PROJ * PROJ), F32),
                pltpu.VMEM((PROJ * PROJ, width), F32),
            ],
        ),
        out_shape=[
            jax.ShapeDtypeStruct((rows * cols, PROJ * PROJ), BF16),
            jax.ShapeDtypeStruct((PROJ * PROJ, width), F32),
        ],
        compiler_params=pltpu.CompilerParams(dimension_semantics=("arbitrary",)),
        cost_estimate=cost(20, span, total, seqs),
        name="outer",
    )(lo, hi, left, lab, right, wide, grad)


class Ring:
    def __init__(self, n_row, n_col):
        self.n_row, self.n_col = n_row, n_col
        self.n_x = n_row // 2
        self.per_row = n_col // n_row
        self.row = lax.axis_index("row").astype(jnp.uint32)
        self.col = lax.axis_index("col").astype(jnp.uint32)
        self.x, self.core = self.row // 2, self.row % 2

    def core_of(self, col):
        return (col // self.per_row) % 2

    def col_shift(self, value, k):
        n = self.n_col
        return lax.ppermute(value, "col", [((t + k) % n, t) for t in range(n)])

    def row_shift(self, value, k):
        n = self.n_row
        return lax.ppermute(value, "row", [((t + k) % n, t) for t in range(n)])

    def x_shift(self, value, k):
        return self.row_shift(value, 2 * k)

    def other_core(self, value):
        return lax.ppermute(value, "row", [(t ^ 1, t) for t in range(self.n_row)])

    def along_col(self, value, k, outward):
        pairs = []
        for r in range(self.n_row):
            for t in range(self.n_col):
                q = (t - k) % self.n_col
                if self.core_of(q) == r % 2:
                    far, near = r * self.n_col + t, r * self.n_col + q
                    pairs.append((far, near) if outward else (near, far))
        return lax.ppermute(value, ("row", "col"), pairs)

    def right_along_x(self, right):
        here, lanes = right.shape
        lanes //= self.per_row
        by_x = jnp.stack([right] + [self.x_shift(right, k) for k in range(1, self.n_x)])
        pieces = []
        for k in range(self.n_col):
            q = (self.col + (self.n_col - k)) % self.n_col
            which = ((q // self.per_row) // 2 + self.n_x - self.x) % self.n_x
            at = (which, jnp.uint32(0), (q % self.per_row) * lanes)
            pieces.append(lax.dynamic_slice(by_x, at, (1, here, lanes))[0])
        return pieces

    def right_along_col(self, pieces):
        blocks = [self.along_col(p, k, True) if k else p for k, p in enumerate(pieces)]
        return jnp.concatenate(blocks, axis=0)

    def right_to_both(self, mine):
        return jnp.where(self.core_of(self.col) == self.core, mine, self.other_core(mine))

    def grad_of_chip(self, grad):
        return (grad.astype(F32) + self.other_core(grad).astype(F32)).astype(BF16)

    def grad_along_col(self, both):
        lanes = both.shape[1]
        here = both.shape[0] // self.n_col
        by_row = jnp.zeros((self.n_x, here, self.per_row * lanes), BF16)
        for k in range(self.n_col):
            block = both[k * here : (k + 1) * here]
            q = (self.col + (self.n_col - k)) % self.n_col
            fits = self.core_of(q) == self.core
            got = self.along_col(block, k, False) if k else block
            got = jnp.where(fits, got, 0)
            which = ((q // self.per_row) // 2 + self.n_x - self.x) % self.n_x
            at = (which, jnp.uint32(0), (q % self.per_row) * lanes)
            old = lax.dynamic_slice(by_row, at, (1, here, lanes))
            by_row = lax.dynamic_update_slice(by_row, old + got[None], at)
        return by_row

    def grad_along_x(self, by_row):
        total = by_row[0].astype(F32)
        for k in range(1, self.n_x):
            total += self.x_shift(by_row[k], self.n_x - k).astype(F32)
        return total.astype(BF16)

    def weight_over_row(self, weight):
        n = self.n_row
        size = weight.shape[0] // n
        sent = weight.astype(BF16).reshape(n, size, -1)
        total = lax.dynamic_index_in_dim(weight.reshape(n, size, -1), self.row, 0, keepdims=False)
        for k in range(1, n):
            piece = lax.dynamic_index_in_dim(sent, (self.row + k) % n, 0, keepdims=False)
            total += self.row_shift(piece, n - k).astype(F32)
        return total

    def weight_over_col(self, total):
        mine = total.astype(BF16)
        for k in range(1, self.n_col):
            total += self.col_shift(mine, k).astype(F32)
        return total.astype(BF16)

    def weight_to_all(self, mine):
        n = self.n_row
        which = (lax.broadcasted_iota(jnp.uint32, (n, 1, 1), 0) + (n - self.row)) % n
        shares = mine[None]
        for k in range(1, n):
            shares = jnp.where(which == k, self.row_shift(mine, k)[None], shares)
        return shares.reshape(n * mine.shape[0], mine.shape[1])


def after(value, *others):
    return lax.optimization_barrier((value,) + others)[0]


def shards(n_row, n_col, alignment_tensor, gain, shift, first_projector, second_projector,
           final_projector, final_offset, labels, counts, grad):
    ring = Ring(n_row, n_col)
    here, rows, feats = alignment_tensor.shape
    cols, width = grad.shape[1:]
    seqs = here * n_col
    normed = standardize_entries(alignment_tensor, gain, shift).reshape(-1, feats)
    left = jnp.dot(normed, first_projector, preferred_element_type=F32).astype(BF16)
    right = jnp.dot(normed, second_projector, preferred_element_type=F32).astype(BF16)
    left = left.reshape(here, rows * PROJ)
    right = right.reshape(here, rows // cols, cols, PROJ).transpose(0, 1, 3, 2)
    pieces = ring.right_along_x(right.reshape(here, rows * PROJ))
    left = jnp.concatenate([left] + [ring.col_shift(left, k) for k in range(1, n_col)])

    row_labels = lax.dynamic_slice_in_dim(labels, ring.row * rows, rows, 0)
    col_labels = lax.dynamic_slice_in_dim(labels, ring.col * cols, cols, 0)
    lab = jnp.repeat(row_labels, PROJ)[None, :]
    step = WIDE // PROJ
    lo = row_labels[::step] // 2
    hi = row_labels[step - 1 :: step] // 2
    chains = jnp.arange(CHAINS, dtype=jnp.int32)
    col_hot = col_labels[:, None, None] == chains[None, None, :]
    depth = jnp.sum(jnp.where(col_hot, counts[None, :, :], 0), axis=-1)
    seq = (jnp.arange(seqs, dtype=jnp.uint32) + ring.col * here) % seqs
    seq = seq.astype(jnp.int32)
    keep = seq[None, None, :] < depth[:, :, None]
    weight = jnp.where(keep, 1.0 / depth.astype(F32)[:, :, None], 0.0)
    third = (depth % 3 == 0)[:, :, None]
    weights = jnp.stack([jnp.where(third, 0.0, weight), jnp.where(third, 3.0 * weight, 0.0)])
    weights = weights.astype(BF16)
    pairs = CHAINS // 2
    tall = weights.transpose(2, 0, 3, 1).reshape(pairs, 2, 2, seqs, cols).swapaxes(1, 2)
    tall = jnp.tile(tall.reshape(pairs, 2, 2 * seqs, cols), (1, 1, 1, LANES // cols))
    wide = weights.reshape(2, cols, pairs, 2 * seqs).transpose(2, 0, 1, 3)
    plain = weight.reshape(cols, pairs, 2 * seqs).transpose(1, 0, 2)

    w = final_projector.reshape(PROJ, PROJ, width).transpose(1, 0, 2).reshape(PROJ * PROJ, width)
    back = back_call(after(grad, *pieces), w.T)
    mine = ring.right_along_col(pieces)
    right_grad = right_grad_call(lo, hi, back, left, lab, plain)

    mine = after(mine, right_grad)
    right = ring.right_to_both(mine)
    right = jnp.stack([right, (right.astype(F32) / 3).astype(BF16)])
    both = ring.grad_of_chip(right_grad)
    by_row = ring.grad_along_col(both)
    outer, weight = outer_call(
        lo, hi, after(left, both), lab, right.swapaxes(1, 2), wide, grad
    )
    by_row = after(by_row, weight)
    share = ring.weight_over_row(weight)
    left_grad = left_grad_call(lo, hi, after(back, weight), lab, right, tall)
    share = after(share, left_grad)
    by_row = after(by_row, left_grad)
    grad_right = ring.grad_along_x(by_row)

    total = left_grad[:here].astype(F32)
    for k in range(1, n_col):
        total += ring.col_shift(left_grad[k * here : (k + 1) * here], n_col - k).astype(F32)
    adjoint_first = total.astype(BF16)
    pair = jnp.dot(after(outer, left_grad, share), w, preferred_element_type=F32) + final_offset
    pair_update = pair.astype(BF16).reshape(rows, cols, width)
    mine = after(ring.weight_over_col(share), pair_update)
    grad_w_out = ring.weight_to_all(mine).astype(F32) / (n_row * rows)
    return pair_update, adjoint_first, grad_right, grad_w_out


def solution(mesh):
    in_specs = (
        P(("parts", "col"), "row", None),
        P(),
        P(),
        P(),
        P(),
        P(),
        P(),
        P("parts"),
        P("parts", None),
        P(("parts", "row"), "col", None),
    )
    out_specs = (
        P(("parts", "row"), "col", None),
        P(("parts", "col"), "row"),
        P(("parts", "col"), "row"),
        P("parts", None),
    )

    def body(*args):
        return shards(mesh.shape["row"], mesh.shape["col"], *args)

    return jax.shard_map(body, mesh=mesh, in_specs=in_specs, out_specs=out_specs, check_vma=False)
```

```python
import jax
import jax.numpy as jnp
from jax import lax
from jax.experimental import pallas as pl
from jax.experimental.pallas import tpu as pltpu
from jax.sharding import PartitionSpec as P


PROJ = 32
CHAINS = 8
LANES = 128
PER_TILE = LANES // PROJ
WIDE = 256
F32 = jnp.float32
BF16 = jnp.bfloat16


def swap_blocks(parts):
    lane = lax.broadcasted_iota(jnp.int32, parts[0].shape, 1)
    for bit in (2, 1):
        shift = bit * PROJ
        low = (lane & shift) == 0
        out = list(parts)
        for p in range(PER_TILE):
            if not p & bit:
                a, b = parts[p], parts[p | bit]
                out[p] = jnp.where(low, a, pltpu.roll(b, shift, 1))
                out[p | bit] = jnp.where(low, pltpu.roll(a, LANES - shift, 1), b)
        parts = out
    return parts


def nt_dot(a, b):
    return lax.dot_general(a, b, (((1,), (1,)), ((), ())), preferred_element_type=F32)


def nn_dot(a, b):
    return lax.dot_general(a, b, (((1,), (0,)), ((), ())), preferred_element_type=F32)


def project_body(x_ref, gain_ref, shift_ref, w_ref, left_ref, right_ref, proj_ref, turn_ref, out_ref,
                 *, cols):
    here, rows, feats = x_ref.shape
    chunk = max(1, WIDE // rows)

    def norm(step, carry):
        x = x_ref[pl.ds(step * chunk, chunk)].astype(F32).reshape(chunk * rows, feats)
        center = x - jnp.mean(x, axis=-1, keepdims=True)
        spread = jnp.mean(center * center, axis=-1, keepdims=True)
        normed = center * lax.rsqrt(spread + 1e-05) * gain_ref[...] + shift_ref[...]
        at = pl.multiple_of(step * (chunk * rows), chunk * rows)
        proj_ref[pl.ds(at, chunk * rows)] = nn_dot(normed.astype(BF16), w_ref[...])
        return carry

    lax.fori_loop(0, here // chunk, norm, 0)

    lane = lax.broadcasted_iota(jnp.int32, (here, LANES), 1)
    for t in range(rows // PER_TILE):
        tile = proj_ref[pl.ds(t * PER_TILE, here, stride=rows)]
        for p in range(1, PER_TILE):
            part = proj_ref[pl.ds(t * PER_TILE + p, here, stride=rows)]
            tile = jnp.where(lane < p * PROJ, tile, pltpu.roll(part, p * PROJ, 1))
        left_ref[:, t * LANES : (t + 1) * LANES] = tile.astype(BF16)

    tiles = here * rows // LANES
    for t in range(tiles):
        flipped = proj_ref[t * LANES : (t + 1) * LANES].T
        turn_ref[t * PROJ : (t + 1) * PROJ] = flipped[PROJ : 2 * PROJ]
    seqs = LANES // rows
    per = LANES // cols
    lane = lax.broadcasted_iota(jnp.int32, (tiles, LANES), 1)
    for block in range(rows // cols):
        for t in range(PROJ // per):
            at = (block * (PROJ // per) + t) * LANES
            parts = [turn_ref[pl.ds(t * per + p, tiles, stride=PROJ)] for p in range(per)]
            for u in range(seqs):
                start = u * rows + block * cols
                tile = None
                for p, part in enumerate(parts):
                    amount = (p * cols - start) % LANES
                    part = pltpu.roll(part, amount, 1) if amount else part
                    tile = part if tile is None else jnp.where(lane < p * cols, tile, part)
                out_ref[pl.ds(u, tiles, stride=seqs), :] = tile
            right_ref[:, at : at + LANES] = out_ref[...].astype(BF16)


def project_call(x, gain, shift, w, cols):
    here, rows, _ = x.shape
    return pl.pallas_call(
        lambda *refs: project_body(*refs, cols=cols),
        out_shape=[jax.ShapeDtypeStruct((here, rows * PROJ), BF16)] * 2,
        scratch_shapes=[
            pltpu.VMEM((here * rows, LANES), F32),
            pltpu.VMEM((here * rows // LANES * PROJ, LANES), F32),
            pltpu.VMEM((here, LANES), F32),
        ],
        name="project",
    )(x, gain, shift, w)


def prep_body(at_ref, labels_ref, counts_ref, w_ref, lab_ref, tall_ref, wide_ref, plain_ref,
              w_out, wt_out, wide_w_ref, *, rows, cols, seqs):
    res = labels_ref.shape[1]
    labels = jnp.broadcast_to(labels_ref[...], (8, res))
    own = pltpu.roll(labels, (res - at_ref[0]) % res, 1)[:, :rows]
    spread = (
        lax.broadcasted_iota(jnp.int32, (rows, rows * PROJ), 1) // PROJ
        == lax.broadcasted_iota(jnp.int32, (rows, rows * PROJ), 0)
    )
    lab = nn_dot(own.astype(F32).astype(BF16), spread.astype(F32).astype(BF16))
    lab_ref[...] = lab[:1].astype(jnp.int32)

    there = pltpu.roll(labels, (res - at_ref[1]) % res, 1)[:, :LANES]
    there = jnp.where(lax.broadcasted_iota(jnp.int32, (8, LANES), 1) < cols, there, 0)
    reach = cols
    while reach < LANES:
        there = there + pltpu.roll(there, reach, 1)
        reach *= 2
    depth = jnp.zeros((CHAINS, LANES), jnp.int32)
    for b in range(CHAINS):
        depth += jnp.where(there == b, counts_ref[:, b : b + 1], 0)
    seq = (lax.broadcasted_iota(jnp.int32, (seqs, LANES), 0) + at_ref[2]) % seqs
    for a in range(CHAINS):
        deep = jnp.broadcast_to(depth[a : a + 1], (seqs, LANES))
        weight = jnp.where(seq < deep, 1.0 / deep.astype(F32), 0.0)
        three = deep % 3 == 0
        side = slice((a % 2) * seqs, (a % 2 + 1) * seqs)
        for x, part in enumerate((jnp.where(three, 0.0, weight), jnp.where(three, 3.0 * weight, 0.0))):
            tall_ref[a // 2, x, side] = part.astype(BF16)
            wide_ref[a // 2, x, :, side] = part.T[:cols].astype(BF16)
        plain_ref[a // 2, :, side] = weight.T[:cols]

    wide_w_ref[...] = w_ref[...].astype(F32)
    for t in range(PROJ // PER_TILE):
        for q in range(PER_TILE):
            e = t * PER_TILE + q
            w_out[e * PROJ : (e + 1) * PROJ] = wide_w_ref[pl.ds(e, PROJ, stride=PROJ)].astype(BF16)
        block = w_out[t * LANES : (t + 1) * LANES].astype(F32)
        wt_out[:, t * LANES : (t + 1) * LANES] = block.T.astype(BF16)


def prep_call(at, labels, counts, w, rows, cols, seqs):
    pairs = CHAINS // 2
    width = w.shape[1]
    vmem = pl.BlockSpec(memory_space=pltpu.VMEM)
    return pl.pallas_call(
        lambda *refs: prep_body(*refs, rows=rows, cols=cols, seqs=seqs),
        in_specs=[pl.BlockSpec(memory_space=pltpu.SMEM), vmem, vmem, vmem],
        out_specs=[vmem] * 6,
        out_shape=[
            jax.ShapeDtypeStruct((1, rows * PROJ), jnp.int32),
            jax.ShapeDtypeStruct((pairs, 2, 2 * seqs, LANES), BF16),
            jax.ShapeDtypeStruct((pairs, 2, cols, 2 * seqs), BF16),
            jax.ShapeDtypeStruct((pairs, cols, 2 * seqs), F32),
            jax.ShapeDtypeStruct(w.shape, BF16),
            jax.ShapeDtypeStruct((width, PROJ * PROJ), BF16),
        ],
        scratch_shapes=[pltpu.VMEM(w.shape, F32)],
        name="prep",
    )(at, labels[None, :], counts, w)


def cost(passes, span, total, seqs):
    return pl.CostEstimate(
        flops=4 * passes * span * total * seqs, bytes_accessed=2 * span * total, transcendentals=0
    )


def back_body(grad_ref, wt_ref, out_ref):
    rows, cols, width = grad_ref.shape
    block = grad_ref[...].reshape(rows * cols, width)
    for u in range(PROJ * PROJ // WIDE):
        prod = nn_dot(block, wt_ref[:, u * WIDE : (u + 1) * WIDE]).astype(BF16)
        for half in range(rows // PER_TILE):
            for t in range(WIDE // LANES):
                parts = [
                    prod[(half * PER_TILE + p) * cols : (half * PER_TILE + p + 1) * cols,
                         t * LANES : (t + 1) * LANES]
                    for p in range(PER_TILE)
                ]
                for q, part in enumerate(swap_blocks(parts)):
                    e = u * (WIDE // PROJ) + t * PER_TILE + q
                    out_ref[0, e * cols : (e + 1) * cols, half * LANES : (half + 1) * LANES] = part


def back_call(grad, wt):
    rows, cols, width = grad.shape
    step = WIDE // PROJ
    return pl.pallas_call(
        back_body,
        grid=(rows // step,),
        in_specs=[
            pl.BlockSpec((step, cols, width), lambda g: (g, 0, 0)),
            pl.BlockSpec((width, PROJ * PROJ), lambda g: (0, 0)),
        ],
        out_specs=pl.BlockSpec((1, PROJ * cols, WIDE), lambda g: (g, 0, 0)),
        out_shape=jax.ShapeDtypeStruct((rows // step, PROJ * cols, WIDE), BF16),
        compiler_params=pltpu.CompilerParams(dimension_semantics=("arbitrary",)),
        cost_estimate=cost(10, PROJ * cols, rows * PROJ, width),
        name="back",
    )(grad, wt)


def first_pair(at_ref, labels_ref, group):
    return labels_ref[at_ref[0] + group * (WIDE // PROJ)] // 2


def last_pair(at_ref, labels_ref, group):
    return labels_ref[at_ref[0] + (group + 1) * (WIDE // PROJ) - 1] // 2


def masked_left(left_ref, lab_ref, lb_ref, pair):
    seqs = left_ref.shape[0]
    for side in range(2):
        keep = (lab_ref[...] == 2 * pair + side).astype(F32).astype(BF16)
        lb_ref[side * seqs : (side + 1) * seqs] = left_ref[...] * keep


def right_grad_body(at_ref, labels_ref, back_ref, left_ref, lab_ref, wide_ref,
                    right_out, q_ref, lb_ref, flip_ref, turn_ref):
    g = pl.program_id(0)
    seqs = left_ref.shape[0]
    span = back_ref.shape[1]
    cols = span // PROJ
    last = pl.num_programs(0) - 1

    def over_pairs(fn):
        def step(pair, carry):
            fn(pair)
            return carry

        return step

    @pl.when(g == 0)
    def _():
        def clear(pair):
            q_ref[pair] = jnp.zeros(q_ref.shape[1:], F32)

        lax.fori_loop(first_pair(at_ref, labels_ref, 0), last_pair(at_ref, labels_ref, last) + 1, over_pairs(clear), 0)
        flip_ref[...] = jnp.zeros_like(flip_ref)

    def one_pair(pair):
        masked_left(left_ref, lab_ref, lb_ref, pair)
        q_ref[pair] += nt_dot(back_ref[0], lb_ref[...])

    lax.fori_loop(first_pair(at_ref, labels_ref, g), last_pair(at_ref, labels_ref, g) + 1, over_pairs(one_pair), 0)

    @pl.when(g == last)
    def _():
        def combine(pair):
            for e in range(PROJ):
                rows = slice(e * cols, (e + 1) * cols)
                both = q_ref[pair, rows] * wide_ref[pair]
                flip_ref[rows] += both[:, :seqs] + both[:, seqs:]

        lax.fori_loop(first_pair(at_ref, labels_ref, 0), last_pair(at_ref, labels_ref, last) + 1, over_pairs(combine), 0)
        for j in range(cols):
            turn_ref[j * PROJ : (j + 1) * PROJ] = flip_ref[pl.ds(j, PROJ, stride=cols)]
        for t in range(span // LANES):
            rows = slice(t * LANES, (t + 1) * LANES)
            right_out[:, rows] = turn_ref[rows].T.astype(BF16)


def right_grad_call(at, labels, back, left, lab, wide):
    groups, span, _ = back.shape
    total = groups * WIDE
    seqs = left.shape[0]
    whole = lambda shape: pl.BlockSpec(shape, lambda g, *_: (0,) * len(shape))
    return pl.pallas_call(
        right_grad_body,
        grid_spec=pltpu.PrefetchScalarGridSpec(
            num_scalar_prefetch=2,
            grid=(total // WIDE,),
            in_specs=[
                pl.BlockSpec((1, span, WIDE), lambda g, *_: (g, 0, 0)),
                pl.BlockSpec((seqs, WIDE), lambda g, *_: (0, g)),
                pl.BlockSpec((1, WIDE), lambda g, *_: (0, g)),
                whole(wide.shape),
            ],
            out_specs=whole((seqs, span)),
            scratch_shapes=[
                pltpu.VMEM((CHAINS // 2, span, 2 * seqs), F32),
                pltpu.VMEM((2 * seqs, WIDE), BF16),
                pltpu.VMEM((span, seqs), F32),
                pltpu.VMEM((span, seqs), F32),
            ],
        ),
        out_shape=jax.ShapeDtypeStruct((seqs, span), BF16),
        compiler_params=pltpu.CompilerParams(dimension_semantics=("arbitrary",)),
        cost_estimate=cost(10, span, total, seqs),
        name="right_grad",
    )(at, labels, back, left, lab, wide)


def left_grad_body(at_ref, labels_ref, back_ref, lab_ref, right_ref, tall_ref, left_out, rm_ref, part_ref):
    g = pl.program_id(0)
    seqs = right_ref.shape[0]
    span = back_ref.shape[1]

    last = pl.num_programs(0) - 1

    @pl.when(g == 0)
    def _():
        part_ref[...] = (right_ref[...].astype(F32) / 3).astype(BF16)

        def build(pair, carry):
            for side in range(2):
                row = side * seqs
                plain, third = tall_ref[pair, 0, row : row + seqs], tall_ref[pair, 1, row : row + seqs]
                for t in range(span // LANES):
                    lanes = slice(t * LANES, (t + 1) * LANES)
                    rm_ref[pair, row : row + seqs, lanes] = (
                        right_ref[:, lanes] * plain + part_ref[:, lanes] * third
                    )
            return carry

        lax.fori_loop(first_pair(at_ref, labels_ref, 0), last_pair(at_ref, labels_ref, last) + 1, build, 0)

    def one_pair(pair, total):
        part = nn_dot(rm_ref[pair], back_ref[0])
        keep0 = lab_ref[...] == 2 * pair
        keep1 = lab_ref[...] == 2 * pair + 1
        return total + jnp.where(keep0, part[:seqs], 0.0) + jnp.where(keep1, part[seqs:], 0.0)

    total = lax.fori_loop(first_pair(at_ref, labels_ref, g), last_pair(at_ref, labels_ref, g) + 1, one_pair, jnp.zeros(left_out.shape, F32))
    left_out[...] = total.astype(BF16)


def left_grad_call(at, labels, back, lab, right, tall):
    groups, span, _ = back.shape
    total = groups * WIDE
    seqs = right.shape[0]
    whole = lambda shape: pl.BlockSpec(shape, lambda g, *_: (0,) * len(shape))
    return pl.pallas_call(
        left_grad_body,
        grid_spec=pltpu.PrefetchScalarGridSpec(
            num_scalar_prefetch=2,
            grid=(total // WIDE,),
            in_specs=[
                pl.BlockSpec((1, span, WIDE), lambda g, *_: (g, 0, 0)),
                pl.BlockSpec((1, WIDE), lambda g, *_: (0, g)),
                whole(right.shape),
                whole(tall.shape),
            ],
            out_specs=pl.BlockSpec((seqs, WIDE), lambda g, *_: (0, g)),
            scratch_shapes=[
                pltpu.VMEM((CHAINS // 2, 2 * seqs, span), BF16),
                pltpu.VMEM((seqs, span), BF16),
            ],
        ),
        out_shape=jax.ShapeDtypeStruct((seqs, total), BF16),
        compiler_params=pltpu.CompilerParams(dimension_semantics=("arbitrary",)),
        cost_estimate=cost(10, span, total, seqs),
        name="left_grad",
    )(at, labels, back, lab, right, tall)


def outer_body(at_ref, labels_ref, left_ref, lab_ref, right_ref, wide_ref, grad_ref,
               x_ref, weight_out, rm_ref, lb_ref, acc_ref, sum_ref, turn_ref, flip_ref, part_ref):
    g = pl.program_id(0)
    seqs = left_ref.shape[0]
    span = right_ref.shape[1]
    cols = span // PROJ
    rows_here, _, width = grad_ref.shape

    last = pl.num_programs(0) - 1

    @pl.when(g == 0)
    def _():
        for t in range(span // LANES):
            lanes = slice(t * LANES, (t + 1) * LANES)
            flipped = right_ref[:, lanes].astype(F32).T
            flip_ref[lanes] = flipped.astype(BF16)
            part_ref[lanes] = (flipped / 3).astype(BF16)

        def build(pair, carry):
            plain, third = wide_ref[pair, 0], wide_ref[pair, 1]
            for e in range(PROJ):
                rows = slice(e * cols, (e + 1) * cols)
                for side in range(2):
                    lanes = slice(side * seqs, (side + 1) * seqs)
                    rm_ref[pair, rows, lanes] = (
                        flip_ref[rows] * plain[:, lanes] + part_ref[rows] * third[:, lanes]
                    )
            return carry

        lax.fori_loop(first_pair(at_ref, labels_ref, 0), last_pair(at_ref, labels_ref, last) + 1, build, 0)
        sum_ref[...] = jnp.zeros_like(sum_ref)

    def product(pair):
        masked_left(left_ref, lab_ref, lb_ref, pair)
        return nn_dot(rm_ref[pair], lb_ref[...])

    acc_ref[...] = product(first_pair(at_ref, labels_ref, g))

    def more(pair, carry):
        acc_ref[...] += product(pair)
        return carry

    lax.fori_loop(first_pair(at_ref, labels_ref, g) + 1, last_pair(at_ref, labels_ref, g) + 1, more, 0)

    for half in range(WIDE // LANES):
        lanes = slice(half * LANES, (half + 1) * LANES)
        for t in range(PROJ // PER_TILE):
            parts = []
            for q in range(PER_TILE):
                e = t * PER_TILE + q
                parts.append(acc_ref[e * cols : (e + 1) * cols, lanes].astype(BF16))
            turned = swap_blocks(parts)
            for p in range(PER_TILE):
                i = half * PER_TILE + p
                x_ref[i * cols : (i + 1) * cols, t * LANES : (t + 1) * LANES] = turned[p]

    flat = grad_ref[...].reshape(rows_here * cols, width)
    sum_ref[...] += nn_dot(flat.T, x_ref[...])

    @pl.when(g == last)
    def _():
        for t in range(PROJ * PROJ // LANES):
            part = slice(t * LANES, (t + 1) * LANES)
            turn_ref[part] = sum_ref[:, part].T
        for c in range(PROJ):
            weight_out[c * PROJ : (c + 1) * PROJ] = turn_ref[pl.ds(c, PROJ, stride=PROJ)]


def outer_call(at, labels, left, lab, right, wide, grad):
    rows, cols, width = grad.shape
    seqs, total = left.shape
    span = right.shape[1]
    step = WIDE // PROJ
    whole = lambda shape: pl.BlockSpec(shape, lambda g, *_: (0,) * len(shape))
    return pl.pallas_call(
        outer_body,
        grid_spec=pltpu.PrefetchScalarGridSpec(
            num_scalar_prefetch=2,
            grid=(total // WIDE,),
            in_specs=[
                pl.BlockSpec((seqs, WIDE), lambda g, *_: (0, g)),
                pl.BlockSpec((1, WIDE), lambda g, *_: (0, g)),
                whole(right.shape),
                whole(wide.shape),
                pl.BlockSpec((step, cols, width), lambda g, *_: (g, 0, 0)),
            ],
            out_specs=[
                pl.BlockSpec((step * cols, PROJ * PROJ), lambda g, *_: (g, 0)),
                whole((PROJ * PROJ, width)),
            ],
            scratch_shapes=[
                pltpu.VMEM((CHAINS // 2, span, 2 * seqs), BF16),
                pltpu.VMEM((2 * seqs, WIDE), BF16),
                pltpu.VMEM((span, WIDE), F32),
                pltpu.VMEM((width, PROJ * PROJ), F32),
                pltpu.VMEM((PROJ * PROJ, width), F32),
                pltpu.VMEM((span, seqs), BF16),
                pltpu.VMEM((span, seqs), BF16),
            ],
        ),
        out_shape=[
            jax.ShapeDtypeStruct((rows * cols, PROJ * PROJ), BF16),
            jax.ShapeDtypeStruct((PROJ * PROJ, width), F32),
        ],
        compiler_params=pltpu.CompilerParams(dimension_semantics=("arbitrary",)),
        cost_estimate=cost(20, span, total, seqs),
        name="outer",
    )(at, labels, left, lab, right, wide, grad)


class Ring:
    def __init__(self, n_row, n_col):
        self.n_row, self.n_col = n_row, n_col
        self.per_row = n_col // n_row
        self.row = lax.axis_index("row").astype(jnp.uint32)
        self.col = lax.axis_index("col").astype(jnp.uint32)

    def col_shift(self, value, k):
        n = self.n_col
        return lax.ppermute(value, "col", [((t + k) % n, t) for t in range(n)])

    def row_shift(self, value, k):
        n = self.n_row
        return lax.ppermute(value, "row", [((t + k) % n, t) for t in range(n)])

    def right_along_row(self, right):
        n, m = self.n_row, self.per_row
        here, lanes = right.shape
        lanes //= m
        by_row = jnp.stack([right] + [self.row_shift(right, k) for k in range(1, n)])
        pieces = []
        for k in range(self.n_col):
            q = (self.col + (self.n_col - k)) % self.n_col
            at = ((q // m + (n - self.row)) % n, jnp.uint32(0), (q % m) * lanes)
            pieces.append(lax.dynamic_slice(by_row, at, (1, here, lanes))[0])
        return pieces

    def right_along_col(self, pieces):
        return jnp.concatenate([self.col_shift(p, k) if k else p for k, p in enumerate(pieces)])

    def right_grad_home(self, grad):
        n, m = self.n_col, self.per_row
        here, lanes = grad.shape[0] // n, grad.shape[1]
        total = jnp.zeros((m, here, lanes), F32)
        slot = lax.broadcasted_iota(jnp.uint32, (m, 1, 1), 0)
        for k in range(n):
            t = (self.row * m + self.col % m + k) % n
            block = lax.dynamic_slice_in_dim(grad, ((t + n - self.col) % n) * here, here, 0)
            pairs = []
            for r in range(self.n_row):
                for q in range(n):
                    pairs.append((r * n + q, (q // m) * n + (r * m + q % m + k) % n))
            got = lax.ppermute(block, ("row", "col"), pairs).astype(F32)[None]
            total += got if m == 1 else jnp.where(slot == (self.col + (n - k)) % n % m, got, 0)
        return total.swapaxes(0, 1).reshape(here, m * lanes).astype(BF16)

    def weight_over_row(self, weight):
        n = self.n_row
        size = weight.shape[0] // n
        sent = weight.astype(BF16).reshape(n, size, -1)
        total = lax.dynamic_index_in_dim(weight.reshape(n, size, -1), self.row, 0, keepdims=False)
        for k in range(1, n):
            piece = lax.dynamic_index_in_dim(sent, (self.row + k) % n, 0, keepdims=False)
            total += self.row_shift(piece, n - k).astype(F32)
        return total

    def weight_over_col(self, total):
        mine = total.astype(BF16)
        for k in range(1, self.n_col):
            total += self.col_shift(mine, k).astype(F32)
        return total.astype(BF16)

    def weight_to_all(self, mine):
        n = self.n_row
        which = (lax.broadcasted_iota(jnp.uint32, (n, 1, 1), 0) + (n - self.row)) % n
        shares = mine[None]
        for k in range(1, n):
            shares = jnp.where(which == k, self.row_shift(mine, k)[None], shares)
        return shares.reshape(n * mine.shape[0], mine.shape[1])


def after(value, *others):
    return lax.optimization_barrier((value,) + others)[0]


def shards(n_row, n_col, alignment_tensor, gain, shift, first_projector, second_projector,
           final_projector, final_offset, labels, counts, grad):
    ring = Ring(n_row, n_col)
    here, rows, _ = alignment_tensor.shape
    cols, width = grad.shape[1:]
    seqs = here * n_col
    both = jnp.concatenate([first_projector, second_projector], axis=1)
    both = jnp.pad(both, ((0, 0), (0, LANES - 2 * PROJ)))
    left, right = project_call(alignment_tensor, gain[None, :], shift[None, :], both, cols)
    pieces = ring.right_along_row(right)
    left = jnp.concatenate([left] + [ring.col_shift(left, k) for k in range(1, n_col)])

    at = jnp.stack([ring.row * rows, ring.col * cols, ring.col * here]).astype(jnp.int32)
    lab, tall, wide, plain, w, wt = prep_call(
        at, labels, counts, after(final_projector, right), rows, cols, seqs
    )
    back = back_call(after(grad, *pieces), wt)
    mine = ring.right_along_col(pieces)
    right_grad = right_grad_call(at, labels, back, left, lab, plain)

    right = after(mine, right_grad)
    grad_right = ring.right_grad_home(right_grad)
    outer, weight = outer_call(
        at, labels, left, lab, right, wide, grad
    )
    share = ring.weight_over_row(weight)
    left_grad = left_grad_call(at, labels, after(back, weight), lab, right, tall)
    share = after(share, left_grad)

    total = left_grad[:here].astype(F32)
    for k in range(1, n_col):
        total += ring.col_shift(left_grad[k * here : (k + 1) * here], n_col - k).astype(F32)
    adjoint_first = total.astype(BF16)
    pair = jnp.dot(after(outer, left_grad, share), w, preferred_element_type=F32) + final_offset
    pair_update = pair.astype(BF16).reshape(rows, cols, width)
    mine = after(ring.weight_over_col(share), pair_update)
    grad_w_out = ring.weight_to_all(mine).astype(F32) / (n_row * rows)
    return pair_update, adjoint_first, grad_right, grad_w_out


def solution(mesh):
    in_specs = (
        P(("parts", "col"), "row", None),
        P(),
        P(),
        P(),
        P(),
        P(),
        P(),
        P("parts"),
        P("parts", None),
        P(("parts", "row"), "col", None),
    )
    out_specs = (
        P(("parts", "row"), "col", None),
        P(("parts", "col"), "row"),
        P(("parts", "col"), "row"),
        P("parts", None),
    )

    def body(*args):
        return shards(mesh.shape["row"], mesh.shape["col"], *args)

    return jax.shard_map(body, mesh=mesh, in_specs=in_specs, out_specs=out_specs, check_vma=False)
```

```python
import jax
import jax.numpy as jnp
from jax import lax
from jax.experimental import pallas as pl
from jax.experimental.pallas import tpu as pltpu
from jax.sharding import PartitionSpec as P


PROJ = 32
CHAINS = 8
LANES = 128
PER_TILE = LANES // PROJ
WIDE = 256
F32 = jnp.float32
BF16 = jnp.bfloat16
VMEM = pl.BlockSpec(memory_space=pltpu.VMEM)
KERNEL = pltpu.CompilerParams(dimension_semantics=("arbitrary",), vmem_limit_bytes=24 << 20)


def swap_blocks(parts):
    lane = lax.broadcasted_iota(jnp.int32, parts[0].shape, 1)
    for bit in (2, 1):
        shift = bit * PROJ
        low = (lane & shift) == 0
        out = list(parts)
        for p in range(PER_TILE):
            if not p & bit:
                a, b = parts[p], parts[p | bit]
                out[p] = jnp.where(low, a, pltpu.roll(b, shift, 1))
                out[p | bit] = jnp.where(low, pltpu.roll(a, LANES - shift, 1), b)
        parts = out
    return parts


def nt_dot(a, b):
    return lax.dot_general(a, b, (((1,), (1,)), ((), ())), preferred_element_type=F32)


def nn_dot(a, b):
    return lax.dot_general(a, b, (((1,), (0,)), ((), ())), preferred_element_type=F32)


def project_body(x_ref, gain_ref, shift_ref, w_ref, left_ref, right_ref, proj_ref, turn_ref, out_ref,
                 *, cols):
    here, rows, feats = x_ref.shape
    chunk = max(1, WIDE // rows)

    def norm(step, carry):
        x = x_ref[pl.ds(step * chunk, chunk)].astype(F32).reshape(chunk * rows, feats)
        center = x - jnp.mean(x, axis=-1, keepdims=True)
        spread = jnp.mean(center * center, axis=-1, keepdims=True)
        normed = center * lax.rsqrt(spread + 1e-05) * gain_ref[...] + shift_ref[...]
        at = pl.multiple_of(step * (chunk * rows), chunk * rows)
        proj_ref[pl.ds(at, chunk * rows)] = nn_dot(normed.astype(BF16), w_ref[...])
        return carry

    lax.fori_loop(0, here // chunk, norm, 0)

    lane = lax.broadcasted_iota(jnp.int32, (here, LANES), 1)
    for t in range(rows // PER_TILE):
        tile = proj_ref[pl.ds(t * PER_TILE, here, stride=rows)]
        for p in range(1, PER_TILE):
            part = proj_ref[pl.ds(t * PER_TILE + p, here, stride=rows)]
            tile = jnp.where(lane < p * PROJ, tile, pltpu.roll(part, p * PROJ, 1))
        left_ref[:, t * LANES : (t + 1) * LANES] = tile.astype(BF16)

    tiles = here * rows // LANES
    for t in range(tiles):
        flipped = proj_ref[t * LANES : (t + 1) * LANES].T
        turn_ref[t * PROJ : (t + 1) * PROJ] = flipped[PROJ : 2 * PROJ]
    seqs = LANES // rows
    per = LANES // cols
    lane = lax.broadcasted_iota(jnp.int32, (tiles, LANES), 1)
    for block in range(rows // cols):
        for t in range(PROJ // per):
            at = (block * (PROJ // per) + t) * LANES
            parts = [turn_ref[pl.ds(t * per + p, tiles, stride=PROJ)] for p in range(per)]
            for u in range(seqs):
                start = u * rows + block * cols
                tile = None
                for p, part in enumerate(parts):
                    amount = (p * cols - start) % LANES
                    part = pltpu.roll(part, amount, 1) if amount else part
                    tile = part if tile is None else jnp.where(lane < p * cols, tile, part)
                out_ref[pl.ds(u, tiles, stride=seqs), :] = tile
            right_ref[:, at : at + LANES] = out_ref[...].astype(BF16)


def project_call(x, gain, shift, w, cols):
    here, rows, _ = x.shape
    return pl.pallas_call(
        lambda *refs: project_body(*refs, cols=cols),
        out_shape=[jax.ShapeDtypeStruct((here, rows * PROJ), BF16)] * 2,
        scratch_shapes=[
            pltpu.VMEM((here * rows, LANES), F32),
            pltpu.VMEM((here * rows // LANES * PROJ, LANES), F32),
            pltpu.VMEM((here, LANES), F32),
        ],
        compiler_params=pltpu.CompilerParams(vmem_limit_bytes=24 << 20),
        name="project",
    )(x, gain, shift, w)


def prep_body(at_ref, labels_ref, counts_ref, w_ref, lab_ref, tall_ref, wide_ref, plain_ref,
              w_out, wt_out, wide_w_ref, *, rows, cols, seqs):
    res = labels_ref.shape[1]
    labels = jnp.broadcast_to(labels_ref[...], (8, res))
    own = pltpu.roll(labels, (res - at_ref[0]) % res, 1)[:, :rows]
    spread = (
        lax.broadcasted_iota(jnp.int32, (rows, rows * PROJ), 1) // PROJ
        == lax.broadcasted_iota(jnp.int32, (rows, rows * PROJ), 0)
    )
    lab = nn_dot(own.astype(F32).astype(BF16), spread.astype(F32).astype(BF16))
    lab_ref[...] = lab[:1].astype(jnp.int32)

    there = pltpu.roll(labels, (res - at_ref[1]) % res, 1)[:, :LANES]
    there = jnp.where(lax.broadcasted_iota(jnp.int32, (8, LANES), 1) < cols, there, 0)
    reach = cols
    while reach < LANES:
        there = there + pltpu.roll(there, reach, 1)
        reach *= 2
    depth = jnp.zeros((CHAINS, LANES), jnp.int32)
    for b in range(CHAINS):
        depth += jnp.where(there == b, counts_ref[:, b : b + 1], 0)
    seq = (lax.broadcasted_iota(jnp.int32, (seqs, LANES), 0) + at_ref[2]) % seqs
    for a in range(CHAINS):
        deep = jnp.broadcast_to(depth[a : a + 1], (seqs, LANES))
        weight = jnp.where(seq < deep, 1.0 / deep.astype(F32), 0.0)
        three = deep % 3 == 0
        side = slice((a % 2) * seqs, (a % 2 + 1) * seqs)
        for x, part in enumerate((jnp.where(three, 0.0, weight), jnp.where(three, 3.0 * weight, 0.0))):
            tall_ref[a // 2, x, side] = part.astype(BF16)
            wide_ref[a // 2, x, :, side] = part.T[:cols].astype(BF16)
        plain_ref[a // 2, :, side] = weight.T[:cols]

    wide_w_ref[...] = w_ref[...].astype(F32)
    for t in range(PROJ // PER_TILE):
        for q in range(PER_TILE):
            e = t * PER_TILE + q
            w_out[e * PROJ : (e + 1) * PROJ] = wide_w_ref[pl.ds(e, PROJ, stride=PROJ)].astype(BF16)
        block = w_out[t * LANES : (t + 1) * LANES].astype(F32)
        wt_out[:, t * LANES : (t + 1) * LANES] = block.T.astype(BF16)


def prep_call(at, labels, counts, w, rows, cols, seqs):
    pairs = CHAINS // 2
    width = w.shape[1]
    return pl.pallas_call(
        lambda *refs: prep_body(*refs, rows=rows, cols=cols, seqs=seqs),
        in_specs=[pl.BlockSpec(memory_space=pltpu.SMEM), VMEM, VMEM, VMEM],
        out_specs=[VMEM] * 6,
        out_shape=[
            jax.ShapeDtypeStruct((1, rows * PROJ), jnp.int32),
            jax.ShapeDtypeStruct((pairs, 2, 2 * seqs, LANES), BF16),
            jax.ShapeDtypeStruct((pairs, 2, cols, 2 * seqs), BF16),
            jax.ShapeDtypeStruct((pairs, cols, 2 * seqs), F32),
            jax.ShapeDtypeStruct(w.shape, BF16),
            jax.ShapeDtypeStruct((width, PROJ * PROJ), BF16),
        ],
        scratch_shapes=[pltpu.VMEM(w.shape, F32)],
        compiler_params=pltpu.CompilerParams(vmem_limit_bytes=24 << 20),
        name="prep",
    )(at, labels[None, :], counts, w)


def cost(passes, span, total, seqs):
    return pl.CostEstimate(
        flops=4 * passes * span * total * seqs, bytes_accessed=2 * span * total, transcendentals=0
    )


def back_body(grad_ref, wt_ref, out_ref):
    rows, cols, width = grad_ref.shape
    g = pl.program_id(0)
    block = grad_ref[...].reshape(rows * cols, width)
    for u in range(PROJ * PROJ // WIDE):
        prod = nn_dot(block, wt_ref[:, u * WIDE : (u + 1) * WIDE]).astype(BF16)
        for half in range(rows // PER_TILE):
            for t in range(WIDE // LANES):
                parts = [
                    prod[(half * PER_TILE + p) * cols : (half * PER_TILE + p + 1) * cols,
                         t * LANES : (t + 1) * LANES]
                    for p in range(PER_TILE)
                ]
                for q, part in enumerate(swap_blocks(parts)):
                    e = u * (WIDE // PROJ) + t * PER_TILE + q
                    out_ref[g, e * cols : (e + 1) * cols, half * LANES : (half + 1) * LANES] = part


def back_call(grad, wt):
    rows, cols, width = grad.shape
    step = WIDE // PROJ
    return pl.pallas_call(
        back_body,
        grid=(rows // step,),
        in_specs=[
            pl.BlockSpec((step, cols, width), lambda g: (g, 0, 0)),
            pl.BlockSpec((width, PROJ * PROJ), lambda g: (0, 0)),
        ],
        out_specs=VMEM,
        out_shape=pltpu.VMEM((rows // step, PROJ * cols, WIDE), BF16),
        compiler_params=KERNEL,
        cost_estimate=cost(10, PROJ * cols, rows * PROJ, width),
        name="back",
    )(grad, wt)


def first_pair(at_ref, labels_ref, group):
    return labels_ref[at_ref[0] + group * (WIDE // PROJ)] // 2


def last_pair(at_ref, labels_ref, group):
    return labels_ref[at_ref[0] + (group + 1) * (WIDE // PROJ) - 1] // 2


def masked_left(left_ref, lab_ref, lb_ref, pair):
    seqs = left_ref.shape[0]
    for side in range(2):
        keep = (lab_ref[...] == 2 * pair + side).astype(F32).astype(BF16)
        lb_ref[side * seqs : (side + 1) * seqs] = left_ref[...] * keep


def right_grad_body(at_ref, labels_ref, back_ref, left_ref, lab_ref, wide_ref,
                    right_out, q_ref, lb_ref, flip_ref, turn_ref):
    g = pl.program_id(0)
    seqs = left_ref.shape[0]
    span = back_ref.shape[1]
    cols = span // PROJ
    last = pl.num_programs(0) - 1

    def over_pairs(fn):
        def step(pair, carry):
            fn(pair)
            return carry

        return step

    @pl.when(g == 0)
    def _():
        def clear(pair):
            q_ref[pair] = jnp.zeros(q_ref.shape[1:], F32)

        lax.fori_loop(first_pair(at_ref, labels_ref, 0), last_pair(at_ref, labels_ref, last) + 1, over_pairs(clear), 0)
        flip_ref[...] = jnp.zeros_like(flip_ref)

    def one_pair(pair):
        masked_left(left_ref, lab_ref, lb_ref, pair)
        q_ref[pair] += nt_dot(back_ref[g], lb_ref[...])

    lax.fori_loop(first_pair(at_ref, labels_ref, g), last_pair(at_ref, labels_ref, g) + 1, over_pairs(one_pair), 0)

    @pl.when(g == last)
    def _():
        def combine(pair):
            for e in range(PROJ):
                rows = slice(e * cols, (e + 1) * cols)
                both = q_ref[pair, rows] * wide_ref[pair]
                flip_ref[rows] += both[:, :seqs] + both[:, seqs:]

        lax.fori_loop(first_pair(at_ref, labels_ref, 0), last_pair(at_ref, labels_ref, last) + 1, over_pairs(combine), 0)
        for j in range(cols):
            turn_ref[j * PROJ : (j + 1) * PROJ] = flip_ref[pl.ds(j, PROJ, stride=cols)]
        for t in range(span // LANES):
            rows = slice(t * LANES, (t + 1) * LANES)
            right_out[:, rows] = turn_ref[rows].T.astype(BF16)


def right_grad_call(at, labels, back, left, lab, wide):
    groups, span, _ = back.shape
    total = groups * WIDE
    seqs = left.shape[0]
    whole = lambda shape: pl.BlockSpec(shape, lambda g, *_: (0,) * len(shape))
    return pl.pallas_call(
        right_grad_body,
        grid_spec=pltpu.PrefetchScalarGridSpec(
            num_scalar_prefetch=2,
            grid=(total // WIDE,),
            in_specs=[
                VMEM,
                pl.BlockSpec((seqs, WIDE), lambda g, *_: (0, g)),
                pl.BlockSpec((1, WIDE), lambda g, *_: (0, g)),
                whole(wide.shape),
            ],
            out_specs=whole((seqs, span)),
            scratch_shapes=[
                pltpu.VMEM((CHAINS // 2, span, 2 * seqs), F32),
                pltpu.VMEM((2 * seqs, WIDE), BF16),
                pltpu.VMEM((span, seqs), F32),
                pltpu.VMEM((span, seqs), F32),
            ],
        ),
        out_shape=jax.ShapeDtypeStruct((seqs, span), BF16),
        compiler_params=KERNEL,
        cost_estimate=cost(10, span, total, seqs),
        name="right_grad",
    )(at, labels, back, left, lab, wide)


def left_grad_body(at_ref, labels_ref, back_ref, lab_ref, right_ref, tall_ref, left_out, rm_ref, part_ref):
    g = pl.program_id(0)
    seqs = right_ref.shape[0]
    span = back_ref.shape[1]

    last = pl.num_programs(0) - 1

    @pl.when(g == 0)
    def _():
        part_ref[...] = (right_ref[...].astype(F32) / 3).astype(BF16)

        def build(pair, carry):
            for side in range(2):
                row = side * seqs
                plain, third = tall_ref[pair, 0, row : row + seqs], tall_ref[pair, 1, row : row + seqs]
                for t in range(span // LANES):
                    lanes = slice(t * LANES, (t + 1) * LANES)
                    rm_ref[pair, row : row + seqs, lanes] = (
                        right_ref[:, lanes] * plain + part_ref[:, lanes] * third
                    )
            return carry

        lax.fori_loop(first_pair(at_ref, labels_ref, 0), last_pair(at_ref, labels_ref, last) + 1, build, 0)

    def one_pair(pair, total):
        part = nn_dot(rm_ref[pair], back_ref[g])
        keep0 = lab_ref[...] == 2 * pair
        keep1 = lab_ref[...] == 2 * pair + 1
        return total + jnp.where(keep0, part[:seqs], 0.0) + jnp.where(keep1, part[seqs:], 0.0)

    total = lax.fori_loop(first_pair(at_ref, labels_ref, g), last_pair(at_ref, labels_ref, g) + 1, one_pair, jnp.zeros(left_out.shape, F32))
    left_out[...] = total.astype(BF16)


def left_grad_call(at, labels, back, lab, right, tall):
    groups, span, _ = back.shape
    total = groups * WIDE
    seqs = right.shape[0]
    whole = lambda shape: pl.BlockSpec(shape, lambda g, *_: (0,) * len(shape))
    return pl.pallas_call(
        left_grad_body,
        grid_spec=pltpu.PrefetchScalarGridSpec(
            num_scalar_prefetch=2,
            grid=(total // WIDE,),
            in_specs=[
                VMEM,
                pl.BlockSpec((1, WIDE), lambda g, *_: (0, g)),
                whole(right.shape),
                whole(tall.shape),
            ],
            out_specs=pl.BlockSpec((seqs, WIDE), lambda g, *_: (0, g)),
            scratch_shapes=[
                pltpu.VMEM((CHAINS // 2, 2 * seqs, span), BF16),
                pltpu.VMEM((seqs, span), BF16),
            ],
        ),
        out_shape=jax.ShapeDtypeStruct((seqs, total), BF16),
        compiler_params=KERNEL,
        cost_estimate=cost(10, span, total, seqs),
        name="left_grad",
    )(at, labels, back, lab, right, tall)


def outer_body(at_ref, labels_ref, left_ref, lab_ref, right_ref, wide_ref, grad_ref,
               outer_ref, weight_out, rm_ref, lb_ref, acc_ref, sum_ref, turn_ref, flip_ref, part_ref):
    g = pl.program_id(0)
    seqs = left_ref.shape[0]
    span = right_ref.shape[1]
    cols = span // PROJ
    rows_here, _, width = grad_ref.shape

    last = pl.num_programs(0) - 1

    @pl.when(g == 0)
    def _():
        for t in range(span // LANES):
            lanes = slice(t * LANES, (t + 1) * LANES)
            flipped = right_ref[:, lanes].astype(F32).T
            flip_ref[lanes] = flipped.astype(BF16)
            part_ref[lanes] = (flipped / 3).astype(BF16)

        def build(pair, carry):
            plain, third = wide_ref[pair, 0], wide_ref[pair, 1]
            for e in range(PROJ):
                rows = slice(e * cols, (e + 1) * cols)
                for side in range(2):
                    lanes = slice(side * seqs, (side + 1) * seqs)
                    rm_ref[pair, rows, lanes] = (
                        flip_ref[rows] * plain[:, lanes] + part_ref[rows] * third[:, lanes]
                    )
            return carry

        lax.fori_loop(first_pair(at_ref, labels_ref, 0), last_pair(at_ref, labels_ref, last) + 1, build, 0)
        sum_ref[...] = jnp.zeros_like(sum_ref)

    def product(pair):
        masked_left(left_ref, lab_ref, lb_ref, pair)
        return nn_dot(rm_ref[pair], lb_ref[...])

    acc_ref[...] = product(first_pair(at_ref, labels_ref, g))

    def more(pair, carry):
        acc_ref[...] += product(pair)
        return carry

    lax.fori_loop(first_pair(at_ref, labels_ref, g) + 1, last_pair(at_ref, labels_ref, g) + 1, more, 0)

    for half in range(WIDE // LANES):
        lanes = slice(half * LANES, (half + 1) * LANES)
        for t in range(PROJ // PER_TILE):
            parts = []
            for q in range(PER_TILE):
                e = t * PER_TILE + q
                parts.append(acc_ref[e * cols : (e + 1) * cols, lanes].astype(BF16))
            turned = swap_blocks(parts)
            for p in range(PER_TILE):
                i = half * PER_TILE + p
                outer_ref[g, i * cols : (i + 1) * cols, t * LANES : (t + 1) * LANES] = turned[p]

    flat = grad_ref[...].reshape(rows_here * cols, width)
    sum_ref[...] += nn_dot(flat.T, outer_ref[g])

    @pl.when(g == last)
    def _():
        for t in range(PROJ * PROJ // LANES):
            part = slice(t * LANES, (t + 1) * LANES)
            turn_ref[part] = sum_ref[:, part].T
        for c in range(PROJ):
            weight_out[c * PROJ : (c + 1) * PROJ] = turn_ref[pl.ds(c, PROJ, stride=PROJ)]


def outer_call(at, labels, left, lab, right, wide, grad):
    rows, cols, width = grad.shape
    seqs, total = left.shape
    span = right.shape[1]
    step = WIDE // PROJ
    whole = lambda shape: pl.BlockSpec(shape, lambda g, *_: (0,) * len(shape))
    return pl.pallas_call(
        outer_body,
        grid_spec=pltpu.PrefetchScalarGridSpec(
            num_scalar_prefetch=2,
            grid=(total // WIDE,),
            in_specs=[
                pl.BlockSpec((seqs, WIDE), lambda g, *_: (0, g)),
                pl.BlockSpec((1, WIDE), lambda g, *_: (0, g)),
                whole(right.shape),
                whole(wide.shape),
                pl.BlockSpec((step, cols, width), lambda g, *_: (g, 0, 0)),
            ],
            out_specs=[
                VMEM,
                whole((PROJ * PROJ, width)),
            ],
            scratch_shapes=[
                pltpu.VMEM((CHAINS // 2, span, 2 * seqs), BF16),
                pltpu.VMEM((2 * seqs, WIDE), BF16),
                pltpu.VMEM((span, WIDE), F32),
                pltpu.VMEM((width, PROJ * PROJ), F32),
                pltpu.VMEM((PROJ * PROJ, width), F32),
                pltpu.VMEM((span, seqs), BF16),
                pltpu.VMEM((span, seqs), BF16),
            ],
        ),
        out_shape=[
            pltpu.VMEM((rows // step, step * cols, PROJ * PROJ), BF16),
            jax.ShapeDtypeStruct((PROJ * PROJ, width), F32),
        ],
        compiler_params=KERNEL,
        cost_estimate=cost(20, span, total, seqs),
        name="outer",
    )(at, labels, left, lab, right, wide, grad)


def pair_body(outer_ref, w_ref, offset_ref, pair_ref):
    pair = nn_dot(outer_ref[pl.program_id(0)], w_ref[...]) + offset_ref[...]
    pair_ref[...] = pair.astype(BF16)


def pair_call(outer, w, offset):
    groups, pairs, feats = outer.shape
    width = w.shape[1]
    return pl.pallas_call(
        pair_body,
        grid=(groups,),
        in_specs=[
            VMEM,
            pl.BlockSpec(w.shape, lambda g: (0, 0)),
            pl.BlockSpec(offset.shape, lambda g: (0, 0)),
        ],
        out_specs=pl.BlockSpec((pairs, width), lambda g: (g, 0)),
        out_shape=jax.ShapeDtypeStruct((groups * pairs, width), BF16),
        compiler_params=KERNEL,
        cost_estimate=pl.CostEstimate(
            flops=2 * groups * pairs * feats * width,
            bytes_accessed=2 * groups * pairs * width,
            transcendentals=0,
        ),
        name="pair",
    )(outer, w, offset)


class Ring:
    def __init__(self, n_row, n_col):
        self.n_row, self.n_col = n_row, n_col
        self.per_row = n_col // n_row
        self.row = lax.axis_index("row").astype(jnp.uint32)
        self.col = lax.axis_index("col").astype(jnp.uint32)

    def col_shift(self, value, k):
        n = self.n_col
        return lax.ppermute(value, "col", [((t + k) % n, t) for t in range(n)])

    def row_shift(self, value, k):
        n = self.n_row
        return lax.ppermute(value, "row", [((t + k) % n, t) for t in range(n)])

    def right_along_row(self, right):
        n, m = self.n_row, self.per_row
        here, lanes = right.shape
        lanes //= m
        by_row = jnp.stack([right] + [self.row_shift(right, k) for k in range(1, n)])
        pieces = []
        for k in range(self.n_col):
            q = (self.col + (self.n_col - k)) % self.n_col
            at = ((q // m + (n - self.row)) % n, jnp.uint32(0), (q % m) * lanes)
            pieces.append(lax.dynamic_slice(by_row, at, (1, here, lanes))[0])
        return pieces

    def right_along_col(self, pieces):
        return jnp.concatenate([self.col_shift(p, k) if k else p for k, p in enumerate(pieces)])

    def right_grad_home(self, grad):
        n, m = self.n_col, self.per_row
        here, lanes = grad.shape[0] // n, grad.shape[1]
        total = jnp.zeros((m, here, lanes), F32)
        slot = lax.broadcasted_iota(jnp.uint32, (m, 1, 1), 0)
        for k in range(n):
            t = (self.row * m + self.col % m + k) % n
            block = lax.dynamic_slice_in_dim(grad, ((t + n - self.col) % n) * here, here, 0)
            pairs = []
            for r in range(self.n_row):
                for q in range(n):
                    pairs.append((r * n + q, (q // m) * n + (r * m + q % m + k) % n))
            got = lax.ppermute(block, ("row", "col"), pairs).astype(F32)[None]
            total += got if m == 1 else jnp.where(slot == (self.col + (n - k)) % n % m, got, 0)
        return total.swapaxes(0, 1).reshape(here, m * lanes).astype(BF16)

    def weight_over_row(self, weight):
        n = self.n_row
        size = weight.shape[0] // n
        sent = weight.astype(BF16).reshape(n, size, -1)
        total = lax.dynamic_index_in_dim(weight.reshape(n, size, -1), self.row, 0, keepdims=False)
        for k in range(1, n):
            piece = lax.dynamic_index_in_dim(sent, (self.row + k) % n, 0, keepdims=False)
            total += self.row_shift(piece, n - k).astype(F32)
        return total

    def weight_over_col(self, total):
        mine = total.astype(BF16)
        for k in range(1, self.n_col):
            total += self.col_shift(mine, k).astype(F32)
        return total.astype(BF16)

    def weight_to_all(self, mine):
        n = self.n_row
        which = (lax.broadcasted_iota(jnp.uint32, (n, 1, 1), 0) + (n - self.row)) % n
        shares = mine[None]
        for k in range(1, n):
            shares = jnp.where(which == k, self.row_shift(mine, k)[None], shares)
        return shares.reshape(n * mine.shape[0], mine.shape[1])


def in_vmem(value):
    return pltpu.with_memory_space_constraint(value, pltpu.VMEM)


def after(value, *others):
    return lax.optimization_barrier((value,) + others)[0]


def shards(n_row, n_col, alignment_tensor, gain, shift, first_projector, second_projector,
           final_projector, final_offset, labels, counts, grad):
    ring = Ring(n_row, n_col)
    here, rows, _ = alignment_tensor.shape
    cols, width = grad.shape[1:]
    seqs = here * n_col
    both = jnp.concatenate([first_projector, second_projector], axis=1)
    both = jnp.pad(both, ((0, 0), (0, LANES - 2 * PROJ)))
    left, right = project_call(alignment_tensor, gain[None, :], shift[None, :], both, cols)
    pieces = ring.right_along_row(right)
    left = jnp.concatenate([left] + [ring.col_shift(left, k) for k in range(1, n_col)])

    at = jnp.stack([ring.row * rows, ring.col * cols, ring.col * here]).astype(jnp.int32)
    lab, tall, wide, plain, w, wt = prep_call(
        at, labels, counts, after(final_projector, right), rows, cols, seqs
    )
    back = back_call(after(grad, *pieces), wt)
    mine = ring.right_along_col(pieces)
    back = in_vmem(back)
    right_grad = right_grad_call(at, labels, back, left, lab, plain)

    right = after(mine, right_grad)
    grad_right = ring.right_grad_home(right_grad)
    outer, weight = outer_call(
        at, labels, left, lab, right, wide, grad
    )
    share = ring.weight_over_row(weight)
    left_grad = left_grad_call(at, labels, back, after(lab, weight), right, tall)
    share = after(share, left_grad)

    total = left_grad[:here].astype(F32)
    for k in range(1, n_col):
        total += ring.col_shift(left_grad[k * here : (k + 1) * here], n_col - k).astype(F32)
    adjoint_first = total.astype(BF16)
    pair_update = pair_call(in_vmem(outer), after(w, left_grad, share), final_offset[None, :])
    pair_update = pair_update.reshape(rows, cols, width)
    mine = after(ring.weight_over_col(share), pair_update)
    grad_w_out = ring.weight_to_all(mine).astype(F32) / (n_row * rows)
    return pair_update, adjoint_first, grad_right, grad_w_out


def solution(mesh):
    in_specs = (
        P(("parts", "col"), "row", None),
        P(),
        P(),
        P(),
        P(),
        P(),
        P(),
        P("parts"),
        P("parts", None),
        P(("parts", "row"), "col", None),
    )
    out_specs = (
        P(("parts", "row"), "col", None),
        P(("parts", "col"), "row"),
        P(("parts", "col"), "row"),
        P("parts", None),
    )

    def body(*args):
        return shards(mesh.shape["row"], mesh.shape["col"], *args)

    return jax.shard_map(body, mesh=mesh, in_specs=in_specs, out_specs=out_specs, check_vma=False)
```

```python
import jax
import jax.numpy as jnp
from jax import lax
from jax.experimental import pallas as pl
from jax.experimental.pallas import tpu as pltpu
from jax.sharding import PartitionSpec as P


PROJ = 32
CHAINS = 8
LANES = 128
PER_TILE = LANES // PROJ
WIDE = 256
F32 = jnp.float32
BF16 = jnp.bfloat16
VMEM = pl.BlockSpec(memory_space=pltpu.VMEM)
KERNEL = pltpu.CompilerParams(dimension_semantics=("arbitrary",), vmem_limit_bytes=24 << 20)


def swap_blocks(parts):
    lane = lax.broadcasted_iota(jnp.int32, parts[0].shape, 1)
    outs = []
    for q in range(PER_TILE):
        out = parts[(PER_TILE - 1 - q) % PER_TILE]
        for block in range(PER_TILE - 2, -1, -1):
            out = jnp.where(lane < (block + 1) * PROJ, parts[(block - q) % PER_TILE], out)
        outs.append(pltpu.roll(out, LANES - q * PROJ, 1) if q else out)
    return outs


def rolled(value, p):
    if not p:
        return value
    return jnp.concatenate(
        [pltpu.roll(value[:, t : t + LANES], p * PROJ, 1) for t in range(0, value.shape[1], LANES)],
        axis=1,
    )


def nt_dot(a, b):
    return lax.dot_general(a, b, (((1,), (1,)), ((), ())), preferred_element_type=F32)


def nn_dot(a, b):
    return lax.dot_general(a, b, (((1,), (0,)), ((), ())), preferred_element_type=F32)


def in_vmem(value):
    return pltpu.with_memory_space_constraint(value, pltpu.VMEM)


def in_hbm(value):
    return pltpu.with_memory_space_constraint(value, pltpu.HBM)


def project_body(x_ref, gain_ref, shift_ref, first_ref, second_ref, left_ref, right_ref, proj_ref, turn_ref, out_ref,
                 *, cols):
    here, rows, feats = x_ref.shape
    chunk = max(1, WIDE // rows)
    blank = jnp.zeros((LANES - 2 * PROJ, feats), BF16)
    w = jnp.concatenate([first_ref[...], second_ref[...], blank], axis=0)

    def norm(step, carry):
        x = x_ref[pl.ds(step * chunk, chunk)].astype(F32).reshape(chunk * rows, feats)
        center = x - jnp.mean(x, axis=-1, keepdims=True)
        spread = jnp.mean(center * center, axis=-1, keepdims=True)
        normed = center * lax.rsqrt(spread + 1e-05) * gain_ref[...] + shift_ref[...]
        at = pl.multiple_of(step * (chunk * rows), chunk * rows)
        proj_ref[pl.ds(at, chunk * rows)] = nt_dot(normed.astype(BF16), w)
        return carry

    lax.fori_loop(0, here // chunk, norm, 0)

    lane = lax.broadcasted_iota(jnp.int32, (here, LANES), 1)
    for t in range(rows // PER_TILE):
        tile = proj_ref[pl.ds(t * PER_TILE, here, stride=rows)]
        for p in range(1, PER_TILE):
            part = proj_ref[pl.ds(t * PER_TILE + p, here, stride=rows)]
            tile = jnp.where(lane < p * PROJ, tile, pltpu.roll(part, p * PROJ, 1))
        left_ref[:, t * LANES : (t + 1) * LANES] = tile.astype(BF16)

    tiles = here * rows // LANES
    for t in range(tiles):
        flipped = proj_ref[t * LANES : (t + 1) * LANES].T
        turn_ref[t * PROJ : (t + 1) * PROJ] = flipped[PROJ : 2 * PROJ]
    seqs = LANES // rows
    per = LANES // cols
    lane = lax.broadcasted_iota(jnp.int32, (tiles, LANES), 1)
    for block in range(rows // cols):
        for t in range(PROJ // per):
            at = (block * (PROJ // per) + t) * LANES
            parts = [turn_ref[pl.ds(t * per + p, tiles, stride=PROJ)] for p in range(per)]
            for u in range(seqs):
                start = u * rows + block * cols
                tile = None
                for p, part in enumerate(parts):
                    amount = (p * cols - start) % LANES
                    part = pltpu.roll(part, amount, 1) if amount else part
                    tile = part if tile is None else jnp.where(lane < p * cols, tile, part)
                out_ref[pl.ds(u, tiles, stride=seqs), :] = tile
            right_ref[:, at : at + LANES] = out_ref[...].astype(BF16)


def project_call(x, gain, shift, first, second, cols):
    here, rows, _ = x.shape
    return pl.pallas_call(
        lambda *refs: project_body(*refs, cols=cols),
        out_shape=[jax.ShapeDtypeStruct((here, rows * PROJ), BF16)] * 2,
        scratch_shapes=[
            pltpu.VMEM((here * rows, LANES), F32),
            pltpu.VMEM((here * rows // LANES * PROJ, LANES), F32),
            pltpu.VMEM((here, LANES), F32),
        ],
        compiler_params=pltpu.CompilerParams(vmem_limit_bytes=24 << 20),
        name="project",
    )(*map(in_hbm, (x, gain, shift, first, second)))


def prep_body(at_ref, labels_ref, counts_ref, w_ref, lab_ref, tall_ref, wide_ref, plain_ref,
              w_out, wt_out, wide_w_ref, *, rows, cols, seqs):
    res = labels_ref.shape[1]
    labels = jnp.broadcast_to(labels_ref[...], (8, res))
    own = pltpu.roll(labels, (res - at_ref[0]) % res, 1)[:, :rows]
    spread = (
        lax.broadcasted_iota(jnp.int32, (rows, rows * PROJ), 1) // PROJ
        == lax.broadcasted_iota(jnp.int32, (rows, rows * PROJ), 0)
    )
    lab = nn_dot(own.astype(F32).astype(BF16), spread.astype(F32).astype(BF16))
    lab_ref[...] = lab[:1].astype(jnp.int32)

    there = pltpu.roll(labels, (res - at_ref[1]) % res, 1)[:, :LANES]
    there = jnp.where(lax.broadcasted_iota(jnp.int32, (8, LANES), 1) < cols, there, 0)
    reach = cols
    while reach < LANES:
        there = there + pltpu.roll(there, reach, 1)
        reach *= 2
    depth = jnp.zeros((CHAINS, LANES), jnp.int32)
    for b in range(CHAINS):
        depth += jnp.where(there == b, counts_ref[:, b : b + 1], 0)
    seq = (lax.broadcasted_iota(jnp.int32, (seqs, LANES), 0) + at_ref[2]) % seqs
    for a in range(CHAINS):
        deep = jnp.broadcast_to(depth[a : a + 1], (seqs, LANES))
        weight = jnp.where(seq < deep, 1.0 / deep.astype(F32), 0.0)
        three = deep % 3 == 0
        side = slice((a % 2) * seqs, (a % 2 + 1) * seqs)
        for x, part in enumerate((jnp.where(three, 0.0, weight), jnp.where(three, 3.0 * weight, 0.0))):
            tall_ref[a // 2, x, side] = part.astype(BF16)
            wide_ref[a // 2, x, :, side] = part.T[:cols].astype(BF16)
        plain_ref[a // 2, :, side] = weight.T[:cols]

    wide_w_ref[...] = w_ref[...].astype(F32)
    for t in range(PROJ // PER_TILE):
        for q in range(PER_TILE):
            e = t * PER_TILE + q
            w_out[e * PROJ : (e + 1) * PROJ] = wide_w_ref[pl.ds(e, PROJ, stride=PROJ)].astype(BF16)
        block = w_out[t * LANES : (t + 1) * LANES].astype(F32)
        for p in range(PER_TILE):
            wt_out[p, :, t * LANES : (t + 1) * LANES] = rolled(block.T, p).astype(BF16)


def prep_call(at, labels, counts, w, rows, cols, seqs):
    pairs = CHAINS // 2
    width = w.shape[1]
    return pl.pallas_call(
        lambda *refs: prep_body(*refs, rows=rows, cols=cols, seqs=seqs),
        in_specs=[pl.BlockSpec(memory_space=pltpu.SMEM), VMEM, VMEM, VMEM],
        out_specs=[VMEM] * 6,
        out_shape=[
            jax.ShapeDtypeStruct((1, rows * PROJ), jnp.int32),
            jax.ShapeDtypeStruct((pairs, 2, 2 * seqs, LANES), BF16),
            jax.ShapeDtypeStruct((pairs, 2, cols, 2 * seqs), BF16),
            jax.ShapeDtypeStruct((pairs, cols, 2 * seqs), F32),
            jax.ShapeDtypeStruct(w.shape, BF16),
            jax.ShapeDtypeStruct((PER_TILE, width, PROJ * PROJ), BF16),
        ],
        scratch_shapes=[pltpu.VMEM(w.shape, F32)],
        compiler_params=pltpu.CompilerParams(vmem_limit_bytes=24 << 20),
        name="prep",
    )(at, in_hbm(labels[None, :]), in_hbm(counts), in_hbm(w))


def cost(passes, span, total, seqs):
    return pl.CostEstimate(
        flops=4 * passes * span * total * seqs, bytes_accessed=2 * span * total, transcendentals=0
    )


def back_body(grad_ref, wt_ref, out_ref):
    rows, cols, _ = grad_ref.shape
    g = pl.program_id(0)
    halves = rows // PER_TILE
    blocks = [
        jnp.concatenate([grad_ref[half * PER_TILE + p] for half in range(halves)], axis=0)
        for p in range(PER_TILE)
    ]
    for u in range(PROJ * PROJ // WIDE):
        prods = [
            nn_dot(block, wt_ref[p, :, u * WIDE : (u + 1) * WIDE]).astype(BF16)
            for p, block in enumerate(blocks)
        ]
        for half in range(halves):
            for t in range(WIDE // LANES):
                parts = [
                    prod[half * cols : (half + 1) * cols, t * LANES : (t + 1) * LANES]
                    for prod in prods
                ]
                for q, part in enumerate(swap_blocks(parts)):
                    e = u * (WIDE // PROJ) + t * PER_TILE + q
                    out_ref[g, e * cols : (e + 1) * cols, half * LANES : (half + 1) * LANES] = part


def back_call(grad, wt):
    rows, cols, width = grad.shape
    step = WIDE // PROJ
    return pl.pallas_call(
        back_body,
        grid=(rows // step,),
        in_specs=[
            pl.BlockSpec((step, cols, width), lambda g: (g, 0, 0)),
            pl.BlockSpec(wt.shape, lambda g: (0, 0, 0)),
        ],
        out_specs=VMEM,
        out_shape=pltpu.VMEM((rows // step, PROJ * cols, WIDE), BF16),
        compiler_params=KERNEL,
        cost_estimate=cost(10, PROJ * cols, rows * PROJ, width),
        name="back",
    )(in_hbm(grad), wt)


def first_pair(at_ref, labels_ref, group):
    return labels_ref[at_ref[0] + group * (WIDE // PROJ)] // 2


def last_pair(at_ref, labels_ref, group):
    return labels_ref[at_ref[0] + (group + 1) * (WIDE // PROJ) - 1] // 2


def masked_left(left_ref, lab_ref, lb_ref, pair):
    seqs = left_ref.shape[0]
    for side in range(2):
        keep = (lab_ref[...] == 2 * pair + side).astype(F32).astype(BF16)
        lb_ref[side * seqs : (side + 1) * seqs] = left_ref[...] * keep


def right_grad_body(at_ref, labels_ref, back_ref, left_ref, lab_ref, wide_ref,
                    right_out, q_ref, lb_ref, flip_ref, turn_ref):
    g = pl.program_id(0)
    seqs = left_ref.shape[0]
    span = back_ref.shape[1]
    cols = span // PROJ
    last = pl.num_programs(0) - 1

    def over_pairs(fn):
        def step(pair, carry):
            fn(pair)
            return carry

        return step

    @pl.when(g == 0)
    def _():
        def clear(pair):
            q_ref[pair] = jnp.zeros(q_ref.shape[1:], F32)

        lax.fori_loop(first_pair(at_ref, labels_ref, 0), last_pair(at_ref, labels_ref, last) + 1, over_pairs(clear), 0)
        flip_ref[...] = jnp.zeros_like(flip_ref)

    def one_pair(pair):
        masked_left(left_ref, lab_ref, lb_ref, pair)
        q_ref[pair] += nt_dot(back_ref[g], lb_ref[...])

    lax.fori_loop(first_pair(at_ref, labels_ref, g), last_pair(at_ref, labels_ref, g) + 1, over_pairs(one_pair), 0)

    @pl.when(g == last)
    def _():
        def combine(pair):
            for e in range(PROJ):
                rows = slice(e * cols, (e + 1) * cols)
                both = q_ref[pair, rows] * wide_ref[pair]
                flip_ref[rows] += both[:, :seqs] + both[:, seqs:]

        lax.fori_loop(first_pair(at_ref, labels_ref, 0), last_pair(at_ref, labels_ref, last) + 1, over_pairs(combine), 0)
        for j in range(cols):
            turn_ref[j * PROJ : (j + 1) * PROJ] = flip_ref[pl.ds(j, PROJ, stride=cols)]
        for t in range(span // LANES):
            rows = slice(t * LANES, (t + 1) * LANES)
            right_out[:, rows] = turn_ref[rows].T.astype(BF16)


def right_grad_call(at, labels, back, left, lab, wide):
    groups, span, _ = back.shape
    total = groups * WIDE
    seqs = left.shape[0]
    whole = lambda shape: pl.BlockSpec(shape, lambda g, *_: (0,) * len(shape))
    return pl.pallas_call(
        right_grad_body,
        grid_spec=pltpu.PrefetchScalarGridSpec(
            num_scalar_prefetch=2,
            grid=(total // WIDE,),
            in_specs=[
                VMEM,
                pl.BlockSpec((seqs, WIDE), lambda g, *_: (0, g)),
                pl.BlockSpec((1, WIDE), lambda g, *_: (0, g)),
                whole(wide.shape),
            ],
            out_specs=whole((seqs, span)),
            scratch_shapes=[
                pltpu.VMEM((CHAINS // 2, span, 2 * seqs), F32),
                pltpu.VMEM((2 * seqs, WIDE), BF16),
                pltpu.VMEM((span, seqs), F32),
                pltpu.VMEM((span, seqs), F32),
            ],
        ),
        out_shape=jax.ShapeDtypeStruct((seqs, span), BF16),
        compiler_params=KERNEL,
        cost_estimate=cost(10, span, total, seqs),
        name="right_grad",
    )(at, labels, back, left, lab, wide)


def left_grad_body(at_ref, labels_ref, back_ref, lab_ref, right_ref, tall_ref, left_out, rm_ref, part_ref):
    g = pl.program_id(0)
    seqs = right_ref.shape[0]
    span = back_ref.shape[1]

    last = pl.num_programs(0) - 1

    @pl.when(g == 0)
    def _():
        part_ref[...] = (right_ref[...].astype(F32) / 3).astype(BF16)

        def build(pair, carry):
            for side in range(2):
                row = side * seqs
                plain, third = tall_ref[pair, 0, row : row + seqs], tall_ref[pair, 1, row : row + seqs]
                for t in range(span // LANES):
                    lanes = slice(t * LANES, (t + 1) * LANES)
                    rm_ref[pair, row : row + seqs, lanes] = (
                        right_ref[:, lanes] * plain + part_ref[:, lanes] * third
                    )
            return carry

        lax.fori_loop(first_pair(at_ref, labels_ref, 0), last_pair(at_ref, labels_ref, last) + 1, build, 0)

    def one_pair(pair, total):
        part = nn_dot(rm_ref[pair], back_ref[g])
        keep0 = lab_ref[...] == 2 * pair
        keep1 = lab_ref[...] == 2 * pair + 1
        return total + jnp.where(keep0, part[:seqs], 0.0) + jnp.where(keep1, part[seqs:], 0.0)

    total = lax.fori_loop(first_pair(at_ref, labels_ref, g), last_pair(at_ref, labels_ref, g) + 1, one_pair, jnp.zeros(left_out.shape, F32))
    left_out[...] = total.astype(BF16)


def left_grad_call(at, labels, back, lab, right, tall):
    groups, span, _ = back.shape
    total = groups * WIDE
    seqs = right.shape[0]
    whole = lambda shape: pl.BlockSpec(shape, lambda g, *_: (0,) * len(shape))
    return pl.pallas_call(
        left_grad_body,
        grid_spec=pltpu.PrefetchScalarGridSpec(
            num_scalar_prefetch=2,
            grid=(total // WIDE,),
            in_specs=[
                VMEM,
                pl.BlockSpec((1, WIDE), lambda g, *_: (0, g)),
                whole(right.shape),
                whole(tall.shape),
            ],
            out_specs=pl.BlockSpec((seqs, WIDE), lambda g, *_: (0, g)),
            scratch_shapes=[
                pltpu.VMEM((CHAINS // 2, 2 * seqs, span), BF16),
                pltpu.VMEM((seqs, span), BF16),
            ],
        ),
        out_shape=jax.ShapeDtypeStruct((seqs, total), BF16),
        compiler_params=KERNEL,
        cost_estimate=cost(10, span, total, seqs),
        name="left_grad",
    )(at, labels, back, lab, right, tall)


def outer_body(at_ref, labels_ref, left_ref, lab_ref, right_ref, wide_ref, grad_ref,
               outer_ref, weight_out, rm_ref, lb_ref, acc_ref, sum_ref, turn_ref, flip_ref, part_ref):
    g = pl.program_id(0)
    seqs = left_ref.shape[0]
    span = right_ref.shape[1]
    cols = span // PROJ
    rows_here, _, width = grad_ref.shape

    last = pl.num_programs(0) - 1

    @pl.when(g == 0)
    def _():
        for t in range(span // LANES):
            lanes = slice(t * LANES, (t + 1) * LANES)
            flipped = right_ref[:, lanes].astype(F32).T
            flip_ref[lanes] = flipped.astype(BF16)
            part_ref[lanes] = (flipped / 3).astype(BF16)

        def build(pair, carry):
            plain, third = wide_ref[pair, 0], wide_ref[pair, 1]
            for e in range(PROJ):
                rows = slice(e * cols, (e + 1) * cols)
                to = e % PER_TILE * (PROJ // PER_TILE) + e // PER_TILE
                into = slice(to * cols, (to + 1) * cols)
                for side in range(2):
                    lanes = slice(side * seqs, (side + 1) * seqs)
                    rm_ref[pair, into, lanes] = (
                        flip_ref[rows] * plain[:, lanes] + part_ref[rows] * third[:, lanes]
                    )
            return carry

        lax.fori_loop(first_pair(at_ref, labels_ref, 0), last_pair(at_ref, labels_ref, last) + 1, build, 0)
        sum_ref[...] = jnp.zeros_like(sum_ref)

    quarter = span // PER_TILE

    def product(pair, add):
        masked_left(left_ref, lab_ref, lb_ref, pair)
        for q in range(PER_TILE):
            rows = slice(q * quarter, (q + 1) * quarter)
            part = nn_dot(rm_ref[pair, rows], rolled(lb_ref[...], q))
            acc_ref[rows] = acc_ref[rows] + part if add else part

    product(first_pair(at_ref, labels_ref, g), False)

    def more(pair, carry):
        product(pair, True)
        return carry

    lax.fori_loop(
        first_pair(at_ref, labels_ref, g) + 1, last_pair(at_ref, labels_ref, g) + 1, more, 0
    )

    for half in range(WIDE // LANES):
        lanes = slice(half * LANES, (half + 1) * LANES)
        for t in range(PROJ // PER_TILE):
            parts = []
            for q in range(PER_TILE):
                e = q * (PROJ // PER_TILE) + t
                parts.append(acc_ref[e * cols : (e + 1) * cols, lanes].astype(BF16))
            turned = swap_blocks(parts)
            for p in range(PER_TILE):
                i = half * PER_TILE + p
                outer_ref[g, i * cols : (i + 1) * cols, t * LANES : (t + 1) * LANES] = turned[p]

    flat = grad_ref[...].reshape(rows_here * cols, width)
    sum_ref[...] += nn_dot(flat.T, outer_ref[g])

    @pl.when(g == last)
    def _():
        for t in range(PROJ * PROJ // LANES):
            part = slice(t * LANES, (t + 1) * LANES)
            turn_ref[part] = sum_ref[:, part].T
        for c in range(PROJ):
            weight_out[c * PROJ : (c + 1) * PROJ] = turn_ref[pl.ds(c, PROJ, stride=PROJ)]


def outer_call(at, labels, left, lab, right, wide, grad):
    rows, cols, width = grad.shape
    seqs, total = left.shape
    span = right.shape[1]
    step = WIDE // PROJ
    whole = lambda shape: pl.BlockSpec(shape, lambda g, *_: (0,) * len(shape))
    return pl.pallas_call(
        outer_body,
        grid_spec=pltpu.PrefetchScalarGridSpec(
            num_scalar_prefetch=2,
            grid=(total // WIDE,),
            in_specs=[
                pl.BlockSpec((seqs, WIDE), lambda g, *_: (0, g)),
                pl.BlockSpec((1, WIDE), lambda g, *_: (0, g)),
                whole(right.shape),
                whole(wide.shape),
                pl.BlockSpec((step, cols, width), lambda g, *_: (g, 0, 0)),
            ],
            out_specs=[
                VMEM,
                whole((PROJ * PROJ, width)),
            ],
            scratch_shapes=[
                pltpu.VMEM((CHAINS // 2, span, 2 * seqs), BF16),
                pltpu.VMEM((2 * seqs, WIDE), BF16),
                pltpu.VMEM((span, WIDE), F32),
                pltpu.VMEM((width, PROJ * PROJ), F32),
                pltpu.VMEM((PROJ * PROJ, width), F32),
                pltpu.VMEM((span, seqs), BF16),
                pltpu.VMEM((span, seqs), BF16),
            ],
        ),
        out_shape=[
            pltpu.VMEM((rows // step, step * cols, PROJ * PROJ), BF16),
            jax.ShapeDtypeStruct((PROJ * PROJ, width), F32),
        ],
        compiler_params=KERNEL,
        cost_estimate=cost(20, span, total, seqs),
        name="outer",
    )(at, labels, left, lab, right, wide, grad)


def pair_body(outer_ref, w_ref, offset_ref, pair_ref):
    pair = nn_dot(outer_ref[pl.program_id(0)], w_ref[...]) + offset_ref[...]
    pair_ref[...] = pair.astype(BF16)


def pair_call(outer, w, offset):
    groups, pairs, feats = outer.shape
    width = w.shape[1]
    return pl.pallas_call(
        pair_body,
        grid=(groups,),
        in_specs=[
            VMEM,
            pl.BlockSpec(w.shape, lambda g: (0, 0)),
            pl.BlockSpec(offset.shape, lambda g: (0, 0)),
        ],
        out_specs=pl.BlockSpec((pairs, width), lambda g: (g, 0)),
        out_shape=jax.ShapeDtypeStruct((groups * pairs, width), BF16),
        compiler_params=KERNEL,
        cost_estimate=pl.CostEstimate(
            flops=2 * groups * pairs * feats * width,
            bytes_accessed=2 * groups * pairs * width,
            transcendentals=0,
        ),
        name="pair",
    )(outer, w, offset)


class Ring:
    def __init__(self, n_row, n_col):
        self.n_row, self.n_col = n_row, n_col
        self.per_row = n_col // n_row
        self.row = lax.axis_index("row").astype(jnp.uint32)
        self.col = lax.axis_index("col").astype(jnp.uint32)

    def col_shift(self, value, k):
        n = self.n_col
        return lax.ppermute(value, "col", [((t + k) % n, t) for t in range(n)])

    def row_shift(self, value, k):
        n = self.n_row
        return lax.ppermute(value, "row", [((t + k) % n, t) for t in range(n)])

    def right_along_row(self, right):
        n, m = self.n_row, self.per_row
        here, lanes = right.shape
        lanes //= m
        by_row = jnp.stack([right] + [self.row_shift(right, k) for k in range(1, n)])
        pieces = []
        for k in range(self.n_col):
            q = (self.col + (self.n_col - k)) % self.n_col
            at = ((q // m + (n - self.row)) % n, jnp.uint32(0), (q % m) * lanes)
            pieces.append(lax.dynamic_slice(by_row, at, (1, here, lanes))[0])
        return pieces

    def right_along_col(self, pieces):
        return jnp.concatenate([self.col_shift(p, k) if k else p for k, p in enumerate(pieces)])

    def right_grad_home(self, grad):
        n, m = self.n_col, self.per_row
        here, lanes = grad.shape[0] // n, grad.shape[1]
        total = jnp.zeros((m, here, lanes), F32)
        slot = lax.broadcasted_iota(jnp.uint32, (m, 1, 1), 0)
        for k in range(n):
            t = (self.row * m + self.col % m + k) % n
            block = lax.dynamic_slice_in_dim(grad, ((t + n - self.col) % n) * here, here, 0)
            pairs = []
            for r in range(self.n_row):
                for q in range(n):
                    pairs.append((r * n + q, (q // m) * n + (r * m + q % m + k) % n))
            got = lax.ppermute(block, ("row", "col"), pairs).astype(F32)[None]
            total += got if m == 1 else jnp.where(slot == (self.col + (n - k)) % n % m, got, 0)
        return total.swapaxes(0, 1).reshape(here, m * lanes).astype(BF16)

    def weight_over_row(self, weight):
        n = self.n_row
        size = weight.shape[0] // n
        sent = weight.astype(BF16).reshape(n, size, -1)
        total = lax.dynamic_index_in_dim(weight.reshape(n, size, -1), self.row, 0, keepdims=False)
        for k in range(1, n):
            piece = lax.dynamic_index_in_dim(sent, (self.row + k) % n, 0, keepdims=False)
            total += self.row_shift(piece, n - k).astype(F32)
        return total

    def weight_over_col(self, total):
        mine = total.astype(BF16)
        for k in range(1, self.n_col):
            total += self.col_shift(mine, k).astype(F32)
        return total.astype(BF16)

    def weight_to_all(self, mine):
        n = self.n_row
        which = (lax.broadcasted_iota(jnp.uint32, (n, 1, 1), 0) + (n - self.row)) % n
        shares = mine[None]
        for k in range(1, n):
            shares = jnp.where(which == k, self.row_shift(mine, k)[None], shares)
        return shares.reshape(n * mine.shape[0], mine.shape[1])


def after(value, *others):
    return lax.optimization_barrier((value,) + others)[0]


def shards(n_row, n_col, alignment_tensor, gain, shift, first_projector, second_projector,
           final_projector, final_offset, labels, counts, grad):
    ring = Ring(n_row, n_col)
    here, rows, _ = alignment_tensor.shape
    cols, width = grad.shape[1:]
    seqs = here * n_col
    left, right = project_call(
        alignment_tensor, gain[None, :], shift[None, :], first_projector.T, second_projector.T, cols
    )
    pieces = ring.right_along_row(right)
    left = jnp.concatenate([left] + [ring.col_shift(left, k) for k in range(1, n_col)])

    at = jnp.stack([ring.row * rows, ring.col * cols, ring.col * here]).astype(jnp.int32)
    lab, tall, wide, plain, w, wt = prep_call(
        at, labels, counts, after(final_projector, right), rows, cols, seqs
    )
    back = back_call(after(grad, *pieces), wt)
    mine = ring.right_along_col(pieces)
    back = in_vmem(back)
    right_grad = right_grad_call(at, labels, back, left, lab, plain)

    right = after(mine, right_grad)
    grad_right = ring.right_grad_home(right_grad)
    outer, weight = outer_call(
        at, labels, left, lab, right, wide, grad
    )
    share = ring.weight_over_row(weight)
    left_grad = left_grad_call(at, labels, back, after(lab, weight), right, tall)
    share = after(share, left_grad)

    total = left_grad[:here].astype(F32)
    for k in range(1, n_col):
        total += ring.col_shift(left_grad[k * here : (k + 1) * here], n_col - k).astype(F32)
    adjoint_first = total.astype(BF16)
    pair_update = pair_call(in_vmem(outer), after(w, left_grad, share), final_offset[None, :])
    pair_update = pair_update.reshape(rows, cols, width)
    mine = after(ring.weight_over_col(share), pair_update)
    grad_w_out = ring.weight_to_all(mine).astype(F32) / (n_row * rows)
    return pair_update, adjoint_first, grad_right, grad_w_out


def solution(mesh):
    in_specs = (
        P(("parts", "col"), "row", None),
        P(),
        P(),
        P(),
        P(),
        P(),
        P(),
        P("parts"),
        P("parts", None),
        P(("parts", "row"), "col", None),
    )
    out_specs = (
        P(("parts", "row"), "col", None),
        P(("parts", "col"), "row"),
        P(("parts", "col"), "row"),
        P("parts", None),
    )

    def body(*args):
        return shards(mesh.shape["row"], mesh.shape["col"], *args)

    return jax.shard_map(body, mesh=mesh, in_specs=in_specs, out_specs=out_specs, check_vma=False)
```

```python
import jax
import jax.numpy as jnp
from jax import lax
from jax.experimental import pallas as pl
from jax.experimental.pallas import tpu as pltpu
from jax.sharding import PartitionSpec as P


PROJ = 32
CHAINS = 8
LANES = 128
PER_TILE = LANES // PROJ
WIDE = 256
F32 = jnp.float32
BF16 = jnp.bfloat16
VMEM = pl.BlockSpec(memory_space=pltpu.VMEM)
KERNEL = pltpu.CompilerParams(dimension_semantics=("arbitrary",), vmem_limit_bytes=24 << 20)


def swap_blocks(parts):
    lane = lax.broadcasted_iota(jnp.int32, parts[0].shape, 1)
    outs = []
    for q in range(PER_TILE):
        out = parts[(PER_TILE - 1 - q) % PER_TILE]
        for block in range(PER_TILE - 2, -1, -1):
            out = jnp.where(lane < (block + 1) * PROJ, parts[(block - q) % PER_TILE], out)
        outs.append(pltpu.roll(out, LANES - q * PROJ, 1) if q else out)
    return outs


def rolled(value, p):
    if not p:
        return value
    return jnp.concatenate(
        [pltpu.roll(value[:, t : t + LANES], p * PROJ, 1) for t in range(0, value.shape[1], LANES)],
        axis=1,
    )


def nt_dot(a, b):
    return lax.dot_general(a, b, (((1,), (1,)), ((), ())), preferred_element_type=F32)


def nn_dot(a, b):
    return lax.dot_general(a, b, (((1,), (0,)), ((), ())), preferred_element_type=F32)


def in_vmem(value):
    return pltpu.with_memory_space_constraint(value, pltpu.VMEM)


def in_hbm(value):
    return pltpu.with_memory_space_constraint(value, pltpu.HBM)


def project_body(x_ref, gain_ref, shift_ref, first_ref, second_ref, left_ref, right_ref, proj_ref, turn_ref, out_ref,
                 *, cols):
    here, rows, feats = x_ref.shape
    chunk = max(1, 2 * WIDE // rows)
    blank = jnp.zeros((LANES - 2 * PROJ, feats), BF16)
    w = jnp.concatenate([first_ref[...], second_ref[...], blank], axis=0)

    def norm(step, carry):
        x = x_ref[pl.ds(step * chunk, chunk)].astype(F32).reshape(chunk * rows, feats)
        center = x - jnp.mean(x, axis=-1, keepdims=True)
        spread = jnp.mean(center * center, axis=-1, keepdims=True)
        normed = center * lax.rsqrt(spread + 1e-05) * gain_ref[...] + shift_ref[...]
        at = pl.multiple_of(step * (chunk * rows), chunk * rows)
        proj_ref[pl.ds(at, chunk * rows)] = nt_dot(normed.astype(BF16), w)
        return carry

    lax.fori_loop(0, here // chunk, norm, 0)

    lane = lax.broadcasted_iota(jnp.int32, (here, LANES), 1)
    for t in range(rows // PER_TILE):
        tile = proj_ref[pl.ds(t * PER_TILE, here, stride=rows)]
        for p in range(1, PER_TILE):
            part = proj_ref[pl.ds(t * PER_TILE + p, here, stride=rows)]
            tile = jnp.where(lane < p * PROJ, tile, pltpu.roll(part, p * PROJ, 1))
        left_ref[:, t * LANES : (t + 1) * LANES] = tile.astype(BF16)

    tiles = here * rows // LANES
    for t in range(tiles):
        flipped = proj_ref[t * LANES : (t + 1) * LANES].T
        turn_ref[t * PROJ : (t + 1) * PROJ] = flipped[PROJ : 2 * PROJ]
    seqs = LANES // rows
    per = LANES // cols
    lane = lax.broadcasted_iota(jnp.int32, (tiles, LANES), 1)
    for block in range(rows // cols):
        for t in range(PROJ // per):
            at = (block * (PROJ // per) + t) * LANES
            parts = [turn_ref[pl.ds(t * per + p, tiles, stride=PROJ)] for p in range(per)]
            for u in range(seqs):
                start = u * rows + block * cols
                tile = None
                for p, part in enumerate(parts):
                    amount = (p * cols - start) % LANES
                    part = pltpu.roll(part, amount, 1) if amount else part
                    tile = part if tile is None else jnp.where(lane < p * cols, tile, part)
                out_ref[pl.ds(u, tiles, stride=seqs), :] = tile
            right_ref[:, at : at + LANES] = out_ref[...].astype(BF16)


def project_call(x, gain, shift, first, second, cols):
    here, rows, _ = x.shape
    return pl.pallas_call(
        lambda *refs: project_body(*refs, cols=cols),
        out_shape=[jax.ShapeDtypeStruct((here, rows * PROJ), BF16)] * 2,
        scratch_shapes=[
            pltpu.VMEM((here * rows, LANES), F32),
            pltpu.VMEM((here * rows // LANES * PROJ, LANES), F32),
            pltpu.VMEM((here, LANES), F32),
        ],
        compiler_params=pltpu.CompilerParams(vmem_limit_bytes=24 << 20),
        name="project",
    )(*map(in_hbm, (x, gain, shift, first, second)))


def prep_body(at_ref, labels_ref, counts_ref, w_ref, lab_ref, tall_ref, wide_ref, plain_ref,
              w_out, wt_out, wide_w_ref, *, rows, cols, seqs):
    res = labels_ref.shape[1]
    labels = jnp.broadcast_to(labels_ref[...], (8, res))
    own = pltpu.roll(labels, (res - at_ref[0]) % res, 1)[:, :rows]
    spread = (
        lax.broadcasted_iota(jnp.int32, (rows, rows * PROJ), 1) // PROJ
        == lax.broadcasted_iota(jnp.int32, (rows, rows * PROJ), 0)
    )
    lab = nn_dot(own.astype(F32).astype(BF16), spread.astype(F32).astype(BF16))
    lab_ref[...] = lab[:1].astype(jnp.int32)

    there = pltpu.roll(labels, (res - at_ref[1]) % res, 1)[:, :LANES]
    there = jnp.where(lax.broadcasted_iota(jnp.int32, (8, LANES), 1) < cols, there, 0)
    reach = cols
    while reach < LANES:
        there = there + pltpu.roll(there, reach, 1)
        reach *= 2
    depth = jnp.zeros((CHAINS, LANES), jnp.int32)
    for b in range(CHAINS):
        depth += jnp.where(there == b, counts_ref[:, b : b + 1], 0)
    seq = (lax.broadcasted_iota(jnp.int32, (seqs, LANES), 0) + at_ref[2]) % seqs
    for a in range(CHAINS):
        deep = jnp.broadcast_to(depth[a : a + 1], (seqs, LANES))
        weight = jnp.where(seq < deep, 1.0 / deep.astype(F32), 0.0)
        three = deep % 3 == 0
        side = slice((a % 2) * seqs, (a % 2 + 1) * seqs)
        for x, part in enumerate((jnp.where(three, 0.0, weight), jnp.where(three, 3.0 * weight, 0.0))):
            tall_ref[a // 2, x, side] = part.astype(BF16)
            wide_ref[a // 2, x, :, side] = part.T[:cols].astype(BF16)
        plain_ref[a // 2, :, side] = weight.T[:cols]

    wide_w_ref[...] = w_ref[...].astype(F32)
    for t in range(PROJ // PER_TILE):
        for q in range(PER_TILE):
            e = t * PER_TILE + q
            w_out[e * PROJ : (e + 1) * PROJ] = wide_w_ref[pl.ds(e, PROJ, stride=PROJ)].astype(BF16)
        block = w_out[t * LANES : (t + 1) * LANES].astype(F32)
        for p in range(PER_TILE):
            wt_out[p, :, t * LANES : (t + 1) * LANES] = rolled(block.T, p).astype(BF16)


def prep_call(at, labels, counts, w, rows, cols, seqs):
    pairs = CHAINS // 2
    width = w.shape[1]
    return pl.pallas_call(
        lambda *refs: prep_body(*refs, rows=rows, cols=cols, seqs=seqs),
        in_specs=[pl.BlockSpec(memory_space=pltpu.SMEM), VMEM, VMEM, VMEM],
        out_specs=[VMEM] * 6,
        out_shape=[
            jax.ShapeDtypeStruct((1, rows * PROJ), jnp.int32),
            jax.ShapeDtypeStruct((pairs, 2, 2 * seqs, LANES), BF16),
            jax.ShapeDtypeStruct((pairs, 2, cols, 2 * seqs), BF16),
            jax.ShapeDtypeStruct((pairs, cols, 2 * seqs), F32),
            jax.ShapeDtypeStruct(w.shape, BF16),
            jax.ShapeDtypeStruct((PER_TILE, width, PROJ * PROJ), BF16),
        ],
        scratch_shapes=[pltpu.VMEM(w.shape, F32)],
        compiler_params=pltpu.CompilerParams(vmem_limit_bytes=24 << 20),
        name="prep",
    )(at, in_hbm(labels[None, :]), in_hbm(counts), in_hbm(w))


def cost(passes, span, total, seqs):
    return pl.CostEstimate(
        flops=4 * passes * span * total * seqs, bytes_accessed=2 * span * total, transcendentals=0
    )


def back_body(grad_ref, wt_ref, out_ref):
    rows, cols, _ = grad_ref.shape
    g = pl.program_id(0)
    halves = rows // PER_TILE
    blocks = [
        jnp.concatenate([grad_ref[half * PER_TILE + p] for half in range(halves)], axis=0)
        for p in range(PER_TILE)
    ]
    for u in range(PROJ * PROJ // WIDE):
        prods = [
            nn_dot(block, wt_ref[p, :, u * WIDE : (u + 1) * WIDE]).astype(BF16)
            for p, block in enumerate(blocks)
        ]
        for half in range(halves):
            for t in range(WIDE // LANES):
                parts = [
                    prod[half * cols : (half + 1) * cols, t * LANES : (t + 1) * LANES]
                    for prod in prods
                ]
                for q, part in enumerate(swap_blocks(parts)):
                    e = u * (WIDE // PROJ) + t * PER_TILE + q
                    out_ref[g, e * cols : (e + 1) * cols, half * LANES : (half + 1) * LANES] = part


def back_call(grad, wt):
    rows, cols, width = grad.shape
    step = WIDE // PROJ
    return pl.pallas_call(
        back_body,
        grid=(rows // step,),
        in_specs=[
            pl.BlockSpec((step, cols, width), lambda g: (g, 0, 0)),
            pl.BlockSpec(wt.shape, lambda g: (0, 0, 0)),
        ],
        out_specs=VMEM,
        out_shape=pltpu.VMEM((rows // step, PROJ * cols, WIDE), BF16),
        compiler_params=KERNEL,
        cost_estimate=cost(10, PROJ * cols, rows * PROJ, width),
        name="back",
    )(in_hbm(grad), wt)


def first_pair(at_ref, labels_ref, group):
    return labels_ref[at_ref[0] + group * (WIDE // PROJ)] // 2


def last_pair(at_ref, labels_ref, group):
    return labels_ref[at_ref[0] + (group + 1) * (WIDE // PROJ) - 1] // 2


def masked_left(left_ref, lab_ref, lb_ref, pair):
    seqs = left_ref.shape[0]
    for side in range(2):
        keep = (lab_ref[...] == 2 * pair + side).astype(F32).astype(BF16)
        lb_ref[side * seqs : (side + 1) * seqs] = left_ref[...] * keep


def right_grad_body(at_ref, labels_ref, back_ref, left_ref, lab_ref, wide_ref,
                    right_out, q_ref, lb_ref, flip_ref, turn_ref):
    g = pl.program_id(0)
    seqs = left_ref.shape[0]
    span = back_ref.shape[1]
    cols = span // PROJ
    last = pl.num_programs(0) - 1

    def over_pairs(fn):
        def step(pair, carry):
            fn(pair)
            return carry

        return step

    @pl.when(g == 0)
    def _():
        def clear(pair):
            q_ref[pair] = jnp.zeros(q_ref.shape[1:], F32)

        lax.fori_loop(first_pair(at_ref, labels_ref, 0), last_pair(at_ref, labels_ref, last) + 1, over_pairs(clear), 0)
        flip_ref[...] = jnp.zeros_like(flip_ref)

    def one_pair(pair):
        masked_left(left_ref, lab_ref, lb_ref, pair)
        q_ref[pair] += nt_dot(back_ref[g], lb_ref[...])

    lax.fori_loop(first_pair(at_ref, labels_ref, g), last_pair(at_ref, labels_ref, g) + 1, over_pairs(one_pair), 0)

    @pl.when(g == last)
    def _():
        def combine(pair):
            for e in range(PROJ):
                rows = slice(e * cols, (e + 1) * cols)
                both = q_ref[pair, rows] * wide_ref[pair]
                flip_ref[rows] += both[:, :seqs] + both[:, seqs:]

        lax.fori_loop(first_pair(at_ref, labels_ref, 0), last_pair(at_ref, labels_ref, last) + 1, over_pairs(combine), 0)
        for j in range(cols):
            turn_ref[j * PROJ : (j + 1) * PROJ] = flip_ref[pl.ds(j, PROJ, stride=cols)]
        for t in range(span // LANES):
            rows = slice(t * LANES, (t + 1) * LANES)
            right_out[:, rows] = turn_ref[rows].T.astype(BF16)


def right_grad_call(at, labels, back, left, lab, wide):
    groups, span, _ = back.shape
    total = groups * WIDE
    seqs = left.shape[0]
    whole = lambda shape: pl.BlockSpec(shape, lambda g, *_: (0,) * len(shape))
    return pl.pallas_call(
        right_grad_body,
        grid_spec=pltpu.PrefetchScalarGridSpec(
            num_scalar_prefetch=2,
            grid=(total // WIDE,),
            in_specs=[
                VMEM,
                pl.BlockSpec((seqs, WIDE), lambda g, *_: (0, g)),
                pl.BlockSpec((1, WIDE), lambda g, *_: (0, g)),
                whole(wide.shape),
            ],
            out_specs=whole((seqs, span)),
            scratch_shapes=[
                pltpu.VMEM((CHAINS // 2, span, 2 * seqs), F32),
                pltpu.VMEM((2 * seqs, WIDE), BF16),
                pltpu.VMEM((span, seqs), F32),
                pltpu.VMEM((span, seqs), F32),
            ],
        ),
        out_shape=jax.ShapeDtypeStruct((seqs, span), BF16),
        compiler_params=KERNEL,
        cost_estimate=cost(10, span, total, seqs),
        name="right_grad",
    )(at, labels, back, left, lab, wide)


def left_grad_body(at_ref, labels_ref, back_ref, lab_ref, right_ref, tall_ref, left_out, rm_ref, part_ref):
    g = pl.program_id(0)
    seqs = right_ref.shape[0]
    span = back_ref.shape[1]

    last = pl.num_programs(0) - 1

    @pl.when(g == 0)
    def _():
        part_ref[...] = (right_ref[...].astype(F32) / 3).astype(BF16)

        def build(pair, carry):
            for side in range(2):
                row = side * seqs
                plain, third = tall_ref[pair, 0, row : row + seqs], tall_ref[pair, 1, row : row + seqs]
                for t in range(span // LANES):
                    lanes = slice(t * LANES, (t + 1) * LANES)
                    rm_ref[pair, row : row + seqs, lanes] = (
                        right_ref[:, lanes] * plain + part_ref[:, lanes] * third
                    )
            return carry

        lax.fori_loop(first_pair(at_ref, labels_ref, 0), last_pair(at_ref, labels_ref, last) + 1, build, 0)

    def one_pair(pair, total):
        part = nn_dot(rm_ref[pair], back_ref[g])
        keep0 = lab_ref[...] == 2 * pair
        keep1 = lab_ref[...] == 2 * pair + 1
        return total + jnp.where(keep0, part[:seqs], 0.0) + jnp.where(keep1, part[seqs:], 0.0)

    total = lax.fori_loop(first_pair(at_ref, labels_ref, g), last_pair(at_ref, labels_ref, g) + 1, one_pair, jnp.zeros(left_out.shape, F32))
    left_out[...] = total.astype(BF16)


def left_grad_call(at, labels, back, lab, right, tall):
    groups, span, _ = back.shape
    total = groups * WIDE
    seqs = right.shape[0]
    whole = lambda shape: pl.BlockSpec(shape, lambda g, *_: (0,) * len(shape))
    return pl.pallas_call(
        left_grad_body,
        grid_spec=pltpu.PrefetchScalarGridSpec(
            num_scalar_prefetch=2,
            grid=(total // WIDE,),
            in_specs=[
                VMEM,
                pl.BlockSpec((1, WIDE), lambda g, *_: (0, g)),
                whole(right.shape),
                whole(tall.shape),
            ],
            out_specs=pl.BlockSpec((seqs, WIDE), lambda g, *_: (0, g)),
            scratch_shapes=[
                pltpu.VMEM((CHAINS // 2, 2 * seqs, span), BF16),
                pltpu.VMEM((seqs, span), BF16),
            ],
        ),
        out_shape=jax.ShapeDtypeStruct((seqs, total), BF16),
        compiler_params=KERNEL,
        cost_estimate=cost(10, span, total, seqs),
        name="left_grad",
    )(at, labels, back, lab, right, tall)


def outer_body(at_ref, labels_ref, left_ref, lab_ref, right_ref, wide_ref, grad_ref,
               outer_ref, weight_out, rm_ref, lb_ref, acc_ref, sum_ref, turn_ref, flip_ref, part_ref):
    g = pl.program_id(0)
    seqs = left_ref.shape[0]
    span = right_ref.shape[1]
    cols = span // PROJ
    rows_here, _, width = grad_ref.shape

    last = pl.num_programs(0) - 1

    @pl.when(g == 0)
    def _():
        for t in range(span // LANES):
            lanes = slice(t * LANES, (t + 1) * LANES)
            flipped = right_ref[:, lanes].astype(F32).T
            flip_ref[lanes] = flipped.astype(BF16)
            part_ref[lanes] = (flipped / 3).astype(BF16)

        def build(pair, carry):
            plain, third = wide_ref[pair, 0], wide_ref[pair, 1]
            for e in range(PROJ):
                rows = slice(e * cols, (e + 1) * cols)
                to = e % PER_TILE * (PROJ // PER_TILE) + e // PER_TILE
                into = slice(to * cols, (to + 1) * cols)
                for side in range(2):
                    lanes = slice(side * seqs, (side + 1) * seqs)
                    rm_ref[pair, into, lanes] = (
                        flip_ref[rows] * plain[:, lanes] + part_ref[rows] * third[:, lanes]
                    )
            return carry

        lax.fori_loop(first_pair(at_ref, labels_ref, 0), last_pair(at_ref, labels_ref, last) + 1, build, 0)
        sum_ref[...] = jnp.zeros_like(sum_ref)

    quarter = span // PER_TILE

    def product(pair, add):
        masked_left(left_ref, lab_ref, lb_ref, pair)
        for q in range(PER_TILE):
            rows = slice(q * quarter, (q + 1) * quarter)
            part = nn_dot(rm_ref[pair, rows], rolled(lb_ref[...], q))
            acc_ref[rows] = acc_ref[rows] + part if add else part

    product(first_pair(at_ref, labels_ref, g), False)

    def more(pair, carry):
        product(pair, True)
        return carry

    lax.fori_loop(
        first_pair(at_ref, labels_ref, g) + 1, last_pair(at_ref, labels_ref, g) + 1, more, 0
    )

    for half in range(WIDE // LANES):
        lanes = slice(half * LANES, (half + 1) * LANES)
        for t in range(PROJ // PER_TILE):
            parts = []
            for q in range(PER_TILE):
                e = q * (PROJ // PER_TILE) + t
                parts.append(acc_ref[e * cols : (e + 1) * cols, lanes].astype(BF16))
            turned = swap_blocks(parts)
            for p in range(PER_TILE):
                i = half * PER_TILE + p
                outer_ref[g, i * cols : (i + 1) * cols, t * LANES : (t + 1) * LANES] = turned[p]

    flat = grad_ref[...].reshape(rows_here * cols, width)
    sum_ref[...] += nn_dot(flat.T, outer_ref[g])

    @pl.when(g == last)
    def _():
        for t in range(PROJ * PROJ // LANES):
            part = slice(t * LANES, (t + 1) * LANES)
            turn_ref[part] = sum_ref[:, part].T
        for c in range(PROJ):
            weight_out[c * PROJ : (c + 1) * PROJ] = turn_ref[pl.ds(c, PROJ, stride=PROJ)]


def outer_call(at, labels, left, lab, right, wide, grad):
    rows, cols, width = grad.shape
    seqs, total = left.shape
    span = right.shape[1]
    step = WIDE // PROJ
    whole = lambda shape: pl.BlockSpec(shape, lambda g, *_: (0,) * len(shape))
    return pl.pallas_call(
        outer_body,
        grid_spec=pltpu.PrefetchScalarGridSpec(
            num_scalar_prefetch=2,
            grid=(total // WIDE,),
            in_specs=[
                pl.BlockSpec((seqs, WIDE), lambda g, *_: (0, g)),
                pl.BlockSpec((1, WIDE), lambda g, *_: (0, g)),
                whole(right.shape),
                whole(wide.shape),
                pl.BlockSpec((step, cols, width), lambda g, *_: (g, 0, 0)),
            ],
            out_specs=[
                VMEM,
                whole((PROJ * PROJ, width)),
            ],
            scratch_shapes=[
                pltpu.VMEM((CHAINS // 2, span, 2 * seqs), BF16),
                pltpu.VMEM((2 * seqs, WIDE), BF16),
                pltpu.VMEM((span, WIDE), F32),
                pltpu.VMEM((width, PROJ * PROJ), F32),
                pltpu.VMEM((PROJ * PROJ, width), F32),
                pltpu.VMEM((span, seqs), BF16),
                pltpu.VMEM((span, seqs), BF16),
            ],
        ),
        out_shape=[
            pltpu.VMEM((rows // step, step * cols, PROJ * PROJ), BF16),
            jax.ShapeDtypeStruct((PROJ * PROJ, width), F32),
        ],
        compiler_params=KERNEL,
        cost_estimate=cost(20, span, total, seqs),
        name="outer",
    )(at, labels, left, lab, right, wide, grad)


def pair_body(outer_ref, w_ref, offset_ref, pair_ref):
    pair = nn_dot(outer_ref[pl.program_id(0)], w_ref[...]) + offset_ref[...]
    pair_ref[...] = pair.astype(BF16)


def pair_call(outer, w, offset):
    groups, pairs, feats = outer.shape
    width = w.shape[1]
    return pl.pallas_call(
        pair_body,
        grid=(groups,),
        in_specs=[
            VMEM,
            pl.BlockSpec(w.shape, lambda g: (0, 0)),
            pl.BlockSpec(offset.shape, lambda g: (0, 0)),
        ],
        out_specs=pl.BlockSpec((pairs, width), lambda g: (g, 0)),
        out_shape=jax.ShapeDtypeStruct((groups * pairs, width), BF16),
        compiler_params=KERNEL,
        cost_estimate=pl.CostEstimate(
            flops=2 * groups * pairs * feats * width,
            bytes_accessed=2 * groups * pairs * width,
            transcendentals=0,
        ),
        name="pair",
    )(outer, w, offset)


class Ring:
    def __init__(self, n_row, n_col):
        self.n_row, self.n_col = n_row, n_col
        self.per_row = n_col // n_row
        self.row = lax.axis_index("row").astype(jnp.uint32)
        self.col = lax.axis_index("col").astype(jnp.uint32)

    def col_shift(self, value, k):
        n = self.n_col
        return lax.ppermute(value, "col", [((t + k) % n, t) for t in range(n)])

    def row_shift(self, value, k):
        n = self.n_row
        return lax.ppermute(value, "row", [((t + k) % n, t) for t in range(n)])

    def right_along_row(self, right):
        others = [self.row_shift(right, k) for k in range(1, self.n_row)]
        return [right] + others

    def right_pieces(self, by_row):
        n, m = self.n_row, self.per_row
        here, lanes = by_row[0].shape
        lanes //= m
        by_row = jnp.stack(by_row)
        pieces = []
        for k in range(self.n_col):
            q = (self.col + (self.n_col - k)) % self.n_col
            at = ((q // m + (n - self.row)) % n, jnp.uint32(0), (q % m) * lanes)
            pieces.append(lax.dynamic_slice(by_row, at, (1, here, lanes))[0])
        return pieces

    def right_along_col(self, pieces):
        return jnp.concatenate([self.col_shift(p, k) if k else p for k, p in enumerate(pieces)])

    def right_grad_home(self, grad):
        n, m = self.n_col, self.per_row
        here, lanes = grad.shape[0] // n, grad.shape[1]
        total = jnp.zeros((m, here, lanes), F32)
        slot = lax.broadcasted_iota(jnp.uint32, (m, 1, 1), 0)
        for k in range(n):
            t = (self.row * m + self.col % m + k) % n
            block = lax.dynamic_slice_in_dim(grad, ((t + n - self.col) % n) * here, here, 0)
            pairs = []
            for r in range(self.n_row):
                for q in range(n):
                    pairs.append((r * n + q, (q // m) * n + (r * m + q % m + k) % n))
            got = lax.ppermute(block, ("row", "col"), pairs).astype(F32)[None]
            total += got if m == 1 else jnp.where(slot == (self.col + (n - k)) % n % m, got, 0)
        return total.swapaxes(0, 1).reshape(here, m * lanes).astype(BF16)

    def weight_over_row(self, weight):
        n = self.n_row
        size = weight.shape[0] // n
        sent = weight.astype(BF16).reshape(n, size, -1)
        total = lax.dynamic_index_in_dim(weight.reshape(n, size, -1), self.row, 0, keepdims=False)
        for k in range(1, n):
            piece = lax.dynamic_index_in_dim(sent, (self.row + k) % n, 0, keepdims=False)
            total += self.row_shift(piece, n - k).astype(F32)
        return total

    def weight_over_col(self, total):
        mine = total.astype(BF16)
        for k in range(1, self.n_col):
            total += self.col_shift(mine, k).astype(F32)
        return total.astype(BF16)

    def weight_to_all(self, mine):
        n = self.n_row
        which = (lax.broadcasted_iota(jnp.uint32, (n, 1, 1), 0) + (n - self.row)) % n
        shares = mine[None]
        for k in range(1, n):
            shares = jnp.where(which == k, self.row_shift(mine, k)[None], shares)
        return shares.reshape(n * mine.shape[0], mine.shape[1])


def after(value, *others):
    return lax.optimization_barrier((value,) + others)[0]


def shards(n_row, n_col, alignment_tensor, gain, shift, first_projector, second_projector,
           final_projector, final_offset, labels, counts, grad):
    ring = Ring(n_row, n_col)
    here, rows, _ = alignment_tensor.shape
    cols, width = grad.shape[1:]
    seqs = here * n_col
    left, right = project_call(
        alignment_tensor, gain[None, :], shift[None, :], first_projector.T, second_projector.T, cols
    )
    by_row = ring.right_along_row(right)
    left = jnp.concatenate([left] + [ring.col_shift(left, k) for k in range(1, n_col)])

    at = jnp.stack([ring.row * rows, ring.col * cols, ring.col * here]).astype(jnp.int32)
    lab, tall, wide, plain, w, wt = prep_call(
        at, labels, counts, after(final_projector, right), rows, cols, seqs
    )
    back = back_call(grad, wt)
    mine = ring.right_along_col(ring.right_pieces(by_row))
    back = in_vmem(back)
    right_grad = right_grad_call(at, labels, back, left, lab, plain)

    right = after(mine, right_grad)
    grad_right = ring.right_grad_home(right_grad)
    outer, weight = outer_call(
        at, labels, left, lab, right, wide, grad
    )
    share = ring.weight_over_row(weight)
    left_grad = left_grad_call(at, labels, back, after(lab, weight), right, tall)
    share = after(share, left_grad)

    total = left_grad[:here].astype(F32)
    for k in range(1, n_col):
        total += ring.col_shift(left_grad[k * here : (k + 1) * here], n_col - k).astype(F32)
    adjoint_first = total.astype(BF16)
    pair_update = pair_call(in_vmem(outer), after(w, left_grad, share), final_offset[None, :])
    pair_update = pair_update.reshape(rows, cols, width)
    mine = after(ring.weight_over_col(share), pair_update)
    grad_w_out = ring.weight_to_all(mine).astype(F32) / (n_row * rows)
    return pair_update, adjoint_first, grad_right, grad_w_out


def solution(mesh):
    in_specs = (
        P(("parts", "col"), "row", None),
        P(),
        P(),
        P(),
        P(),
        P(),
        P(),
        P("parts"),
        P("parts", None),
        P(("parts", "row"), "col", None),
    )
    out_specs = (
        P(("parts", "row"), "col", None),
        P(("parts", "col"), "row"),
        P(("parts", "col"), "row"),
        P("parts", None),
    )

    def body(*args):
        return shards(mesh.shape["row"], mesh.shape["col"], *args)

    return jax.shard_map(body, mesh=mesh, in_specs=in_specs, out_specs=out_specs, check_vma=False)
```

```python
import jax
import jax.numpy as jnp
from jax import lax
from jax.experimental import pallas as pl
from jax.experimental.pallas import tpu as pltpu
from jax.sharding import PartitionSpec as P


PROJ = 32
CHAINS = 8
LANES = 128
PER_TILE = LANES // PROJ
WIDE = 256
F32 = jnp.float32
BF16 = jnp.bfloat16
VMEM = pl.BlockSpec(memory_space=pltpu.VMEM)
KERNEL = pltpu.CompilerParams(dimension_semantics=("arbitrary",), vmem_limit_bytes=24 << 20)


def swap_blocks(parts):
    lane = lax.broadcasted_iota(jnp.int32, parts[0].shape, 1)
    outs = []
    for q in range(PER_TILE):
        out = parts[(PER_TILE - 1 - q) % PER_TILE]
        for block in range(PER_TILE - 2, -1, -1):
            out = jnp.where(lane < (block + 1) * PROJ, parts[(block - q) % PER_TILE], out)
        outs.append(pltpu.roll(out, LANES - q * PROJ, 1) if q else out)
    return outs


def rolled(value, p):
    if not p:
        return value
    return jnp.concatenate(
        [pltpu.roll(value[:, t : t + LANES], p * PROJ, 1) for t in range(0, value.shape[1], LANES)],
        axis=1,
    )


def nt_dot(a, b):
    return lax.dot_general(a, b, (((1,), (1,)), ((), ())), preferred_element_type=F32)


def nn_dot(a, b):
    return lax.dot_general(a, b, (((1,), (0,)), ((), ())), preferred_element_type=F32)


def in_vmem(value):
    return pltpu.with_memory_space_constraint(value, pltpu.VMEM)


def in_hbm(value):
    return pltpu.with_memory_space_constraint(value, pltpu.HBM)


def project_body(x_ref, gain_ref, shift_ref, first_ref, second_ref, left_ref, right_ref, proj_ref, turn_ref, out_ref,
                 *, cols):
    chunk, rows, feats = x_ref.shape
    g = pl.program_id(0)
    blank = jnp.zeros((LANES - 2 * PROJ, feats), BF16)
    w = jnp.concatenate([first_ref[...], second_ref[...], blank], axis=0)

    x = x_ref[...].astype(F32).reshape(chunk * rows, feats)
    center = x - jnp.mean(x, axis=-1, keepdims=True)
    spread = jnp.mean(center * center, axis=-1, keepdims=True)
    normed = center * lax.rsqrt(spread + 1e-05) * gain_ref[...] + shift_ref[...]
    at = pl.multiple_of(g * (chunk * rows), chunk * rows)
    proj_ref[pl.ds(at, chunk * rows)] = nt_dot(normed.astype(BF16), w)

    @pl.when(g == pl.num_programs(0) - 1)
    def _():
        project_layout(proj_ref, turn_ref, out_ref, left_ref, right_ref, rows, cols)


def project_layout(proj_ref, turn_ref, out_ref, left_ref, right_ref, rows, cols):
    here = left_ref.shape[0]
    lane = lax.broadcasted_iota(jnp.int32, (here, LANES), 1)
    for t in range(rows // PER_TILE):
        tile = proj_ref[pl.ds(t * PER_TILE, here, stride=rows)]
        for p in range(1, PER_TILE):
            part = proj_ref[pl.ds(t * PER_TILE + p, here, stride=rows)]
            tile = jnp.where(lane < p * PROJ, tile, pltpu.roll(part, p * PROJ, 1))
        left_ref[:, t * LANES : (t + 1) * LANES] = tile.astype(BF16)

    tiles = here * rows // LANES
    for t in range(tiles):
        flipped = proj_ref[t * LANES : (t + 1) * LANES].T
        turn_ref[t * PROJ : (t + 1) * PROJ] = flipped[PROJ : 2 * PROJ]
    seqs = LANES // rows
    per = LANES // cols
    lane = lax.broadcasted_iota(jnp.int32, (tiles, LANES), 1)
    for block in range(rows // cols):
        for t in range(PROJ // per):
            at = (block * (PROJ // per) + t) * LANES
            parts = [turn_ref[pl.ds(t * per + p, tiles, stride=PROJ)] for p in range(per)]
            for u in range(seqs):
                start = u * rows + block * cols
                tile = None
                for p, part in enumerate(parts):
                    amount = (p * cols - start) % LANES
                    part = pltpu.roll(part, amount, 1) if amount else part
                    tile = part if tile is None else jnp.where(lane < p * cols, tile, part)
                out_ref[pl.ds(u, tiles, stride=seqs), :] = tile
            right_ref[:, at : at + LANES] = out_ref[...].astype(BF16)


def project_call(x, gain, shift, first, second, cols):
    here, rows, feats = x.shape
    chunk = min(here, max(1, 2 * WIDE // rows))
    whole = lambda a: pl.BlockSpec(a.shape, lambda g: (0,) * a.ndim)
    return pl.pallas_call(
        lambda *refs: project_body(*refs, cols=cols),
        grid=(here // chunk,),
        in_specs=[pl.BlockSpec((chunk, rows, feats), lambda g: (g, 0, 0))]
        + [whole(a) for a in (gain, shift, first, second)],
        out_specs=[VMEM] * 2,
        out_shape=[jax.ShapeDtypeStruct((here, rows * PROJ), BF16)] * 2,
        scratch_shapes=[
            pltpu.VMEM((here * rows, LANES), F32),
            pltpu.VMEM((here * rows // LANES * PROJ, LANES), F32),
            pltpu.VMEM((here, LANES), F32),
        ],
        compiler_params=KERNEL,
        name="project",
    )(*map(in_hbm, (x, gain, shift, first, second)))


def prep_body(at_ref, labels_ref, counts_ref, w_ref, lab_ref, tall_ref, wide_ref, plain_ref,
              w_out, wt_out, wide_w_ref, *, rows, cols, seqs):
    res = labels_ref.shape[1]
    labels = jnp.broadcast_to(labels_ref[...], (8, res))
    own = pltpu.roll(labels, (res - at_ref[0]) % res, 1)[:, :rows]
    spread = (
        lax.broadcasted_iota(jnp.int32, (rows, rows * PROJ), 1) // PROJ
        == lax.broadcasted_iota(jnp.int32, (rows, rows * PROJ), 0)
    )
    lab = nn_dot(own.astype(F32).astype(BF16), spread.astype(F32).astype(BF16))
    lab_ref[...] = lab[:1].astype(jnp.int32)

    there = pltpu.roll(labels, (res - at_ref[1]) % res, 1)[:, :LANES]
    there = jnp.where(lax.broadcasted_iota(jnp.int32, (8, LANES), 1) < cols, there, 0)
    reach = cols
    while reach < LANES:
        there = there + pltpu.roll(there, reach, 1)
        reach *= 2
    depth = jnp.zeros((CHAINS, LANES), jnp.int32)
    for b in range(CHAINS):
        depth += jnp.where(there == b, counts_ref[:, b : b + 1], 0)
    seq = (lax.broadcasted_iota(jnp.int32, (seqs, LANES), 0) + at_ref[2]) % seqs
    for a in range(CHAINS):
        deep = jnp.broadcast_to(depth[a : a + 1], (seqs, LANES))
        weight = jnp.where(seq < deep, 1.0 / deep.astype(F32), 0.0)
        three = deep % 3 == 0
        side = slice((a % 2) * seqs, (a % 2 + 1) * seqs)
        for x, part in enumerate((jnp.where(three, 0.0, weight), jnp.where(three, 3.0 * weight, 0.0))):
            tall_ref[a // 2, x, side] = part.astype(BF16)
            wide_ref[a // 2, x, :, side] = part.T[:cols].astype(BF16)
        plain_ref[a // 2, :, side] = weight.T[:cols]

    wide_w_ref[...] = w_ref[...].astype(F32)
    for t in range(PROJ // PER_TILE):
        for q in range(PER_TILE):
            e = t * PER_TILE + q
            w_out[e * PROJ : (e + 1) * PROJ] = wide_w_ref[pl.ds(e, PROJ, stride=PROJ)].astype(BF16)
        block = w_out[t * LANES : (t + 1) * LANES].astype(F32)
        for p in range(PER_TILE):
            wt_out[p, :, t * LANES : (t + 1) * LANES] = rolled(block.T, p).astype(BF16)


def prep_call(at, labels, counts, w, rows, cols, seqs):
    pairs = CHAINS // 2
    width = w.shape[1]
    return pl.pallas_call(
        lambda *refs: prep_body(*refs, rows=rows, cols=cols, seqs=seqs),
        in_specs=[pl.BlockSpec(memory_space=pltpu.SMEM), VMEM, VMEM, VMEM],
        out_specs=[VMEM] * 6,
        out_shape=[
            jax.ShapeDtypeStruct((1, rows * PROJ), jnp.int32),
            jax.ShapeDtypeStruct((pairs, 2, 2 * seqs, LANES), BF16),
            jax.ShapeDtypeStruct((pairs, 2, cols, 2 * seqs), BF16),
            jax.ShapeDtypeStruct((pairs, cols, 2 * seqs), F32),
            jax.ShapeDtypeStruct(w.shape, BF16),
            jax.ShapeDtypeStruct((PER_TILE, width, PROJ * PROJ), BF16),
        ],
        scratch_shapes=[pltpu.VMEM(w.shape, F32)],
        compiler_params=pltpu.CompilerParams(vmem_limit_bytes=24 << 20),
        name="prep",
    )(at, in_hbm(labels[None, :]), in_hbm(counts), in_hbm(w))


def cost(passes, span, total, seqs):
    return pl.CostEstimate(
        flops=4 * passes * span * total * seqs, bytes_accessed=2 * span * total, transcendentals=0
    )


def back_body(grad_ref, wt_ref, out_ref):
    rows, cols, _ = grad_ref.shape
    g = pl.program_id(0)
    halves = rows // PER_TILE
    blocks = [
        jnp.concatenate([grad_ref[half * PER_TILE + p] for half in range(halves)], axis=0)
        for p in range(PER_TILE)
    ]
    for u in range(PROJ * PROJ // WIDE):
        prods = [
            nn_dot(block, wt_ref[p, :, u * WIDE : (u + 1) * WIDE]).astype(BF16)
            for p, block in enumerate(blocks)
        ]
        for half in range(halves):
            for t in range(WIDE // LANES):
                parts = [
                    prod[half * cols : (half + 1) * cols, t * LANES : (t + 1) * LANES]
                    for prod in prods
                ]
                for q, part in enumerate(swap_blocks(parts)):
                    e = u * (WIDE // PROJ) + t * PER_TILE + q
                    out_ref[g, e * cols : (e + 1) * cols, half * LANES : (half + 1) * LANES] = part


def back_call(grad, wt):
    rows, cols, width = grad.shape
    step = WIDE // PROJ
    return pl.pallas_call(
        back_body,
        grid=(rows // step,),
        in_specs=[
            pl.BlockSpec((step, cols, width), lambda g: (g, 0, 0)),
            VMEM,
        ],
        out_specs=VMEM,
        out_shape=pltpu.VMEM((rows // step, PROJ * cols, WIDE), BF16),
        compiler_params=KERNEL,
        cost_estimate=cost(10, PROJ * cols, rows * PROJ, width),
        name="back",
    )(in_hbm(grad), wt)


def first_pair(at_ref, labels_ref, group):
    return labels_ref[at_ref[0] + group * (WIDE // PROJ)] // 2


def last_pair(at_ref, labels_ref, group):
    return labels_ref[at_ref[0] + (group + 1) * (WIDE // PROJ) - 1] // 2


def lanes_of(group):
    return pl.ds(pl.multiple_of(group * WIDE, WIDE), WIDE)


def masked_left(left_ref, lab_ref, lb_ref, pair):
    seqs = left_ref.shape[0]
    lanes = lanes_of(pl.program_id(0))
    for side in range(2):
        keep = (lab_ref[:, lanes] == 2 * pair + side).astype(F32).astype(BF16)
        lb_ref[side * seqs : (side + 1) * seqs] = left_ref[:, lanes] * keep


def right_grad_body(at_ref, labels_ref, back_ref, left_ref, lab_ref, wide_ref,
                    right_out, q_ref, lb_ref, flip_ref, turn_ref):
    g = pl.program_id(0)
    seqs = left_ref.shape[0]
    span = back_ref.shape[1]
    cols = span // PROJ
    last = pl.num_programs(0) - 1

    def over_pairs(fn):
        def step(pair, carry):
            fn(pair)
            return carry

        return step

    @pl.when(g == 0)
    def _():
        def clear(pair):
            q_ref[pair] = jnp.zeros(q_ref.shape[1:], F32)

        lax.fori_loop(first_pair(at_ref, labels_ref, 0), last_pair(at_ref, labels_ref, last) + 1, over_pairs(clear), 0)
        flip_ref[...] = jnp.zeros_like(flip_ref)

    def one_pair(pair):
        masked_left(left_ref, lab_ref, lb_ref, pair)
        q_ref[pair] += nt_dot(back_ref[g], lb_ref[...])

    lax.fori_loop(first_pair(at_ref, labels_ref, g), last_pair(at_ref, labels_ref, g) + 1, over_pairs(one_pair), 0)

    @pl.when(g == last)
    def _():
        def combine(pair):
            for e in range(PROJ):
                rows = slice(e * cols, (e + 1) * cols)
                both = q_ref[pair, rows] * wide_ref[pair]
                flip_ref[rows] += both[:, :seqs] + both[:, seqs:]

        lax.fori_loop(first_pair(at_ref, labels_ref, 0), last_pair(at_ref, labels_ref, last) + 1, over_pairs(combine), 0)
        for j in range(cols):
            turn_ref[j * PROJ : (j + 1) * PROJ] = flip_ref[pl.ds(j, PROJ, stride=cols)]
        for t in range(span // LANES):
            rows = slice(t * LANES, (t + 1) * LANES)
            right_out[:, rows] = turn_ref[rows].T.astype(BF16)


def right_grad_call(at, labels, back, left, lab, wide):
    groups, span, _ = back.shape
    total = groups * WIDE
    seqs = left.shape[0]
    return pl.pallas_call(
        right_grad_body,
        grid_spec=pltpu.PrefetchScalarGridSpec(
            num_scalar_prefetch=2,
            grid=(total // WIDE,),
            in_specs=[
                VMEM,
                VMEM,
                VMEM,
                VMEM,
            ],
            out_specs=VMEM,
            scratch_shapes=[
                pltpu.VMEM((CHAINS // 2, span, 2 * seqs), F32),
                pltpu.VMEM((2 * seqs, WIDE), BF16),
                pltpu.VMEM((span, seqs), F32),
                pltpu.VMEM((span, seqs), F32),
            ],
        ),
        out_shape=jax.ShapeDtypeStruct((seqs, span), BF16),
        compiler_params=KERNEL,
        cost_estimate=cost(10, span, total, seqs),
        name="right_grad",
    )(at, labels, back, left, lab, wide)


def left_grad_body(at_ref, labels_ref, back_ref, lab_ref, right_ref, tall_ref, left_out, rm_ref, part_ref):
    g = pl.program_id(0)
    seqs = right_ref.shape[0]
    span = back_ref.shape[1]

    last = pl.num_programs(0) - 1

    @pl.when(g == 0)
    def _():
        part_ref[...] = (right_ref[...].astype(F32) / 3).astype(BF16)

        def build(pair, carry):
            for side in range(2):
                row = side * seqs
                plain, third = tall_ref[pair, 0, row : row + seqs], tall_ref[pair, 1, row : row + seqs]
                for t in range(span // LANES):
                    lanes = slice(t * LANES, (t + 1) * LANES)
                    rm_ref[pair, row : row + seqs, lanes] = (
                        right_ref[:, lanes] * plain + part_ref[:, lanes] * third
                    )
            return carry

        lax.fori_loop(first_pair(at_ref, labels_ref, 0), last_pair(at_ref, labels_ref, last) + 1, build, 0)

    def one_pair(pair, total):
        part = nn_dot(rm_ref[pair], back_ref[g])
        lab = lab_ref[:, lanes_of(g)]
        keep0, keep1 = lab == 2 * pair, lab == 2 * pair + 1
        return total + jnp.where(keep0, part[:seqs], 0.0) + jnp.where(keep1, part[seqs:], 0.0)

    total = lax.fori_loop(first_pair(at_ref, labels_ref, g), last_pair(at_ref, labels_ref, g) + 1, one_pair, jnp.zeros((seqs, WIDE), F32))
    left_out[:, lanes_of(g)] = total.astype(BF16)


def left_grad_call(at, labels, back, lab, right, tall):
    groups, span, _ = back.shape
    total = groups * WIDE
    seqs = right.shape[0]
    return pl.pallas_call(
        left_grad_body,
        grid_spec=pltpu.PrefetchScalarGridSpec(
            num_scalar_prefetch=2,
            grid=(total // WIDE,),
            in_specs=[
                VMEM,
                VMEM,
                VMEM,
                VMEM,
            ],
            out_specs=VMEM,
            scratch_shapes=[
                pltpu.VMEM((CHAINS // 2, 2 * seqs, span), BF16),
                pltpu.VMEM((seqs, span), BF16),
            ],
        ),
        out_shape=jax.ShapeDtypeStruct((seqs, total), BF16),
        compiler_params=KERNEL,
        cost_estimate=cost(10, span, total, seqs),
        name="left_grad",
    )(at, labels, back, lab, right, tall)


def outer_body(at_ref, labels_ref, left_ref, lab_ref, right_ref, wide_ref, grad_ref,
               outer_ref, weight_out, rm_ref, lb_ref, acc_ref, sum_ref, turn_ref, flip_ref, part_ref):
    g = pl.program_id(0)
    seqs = left_ref.shape[0]
    span = right_ref.shape[1]
    cols = span // PROJ
    rows_here, _, width = grad_ref.shape

    last = pl.num_programs(0) - 1

    @pl.when(g == 0)
    def _():
        for t in range(span // LANES):
            lanes = slice(t * LANES, (t + 1) * LANES)
            flipped = right_ref[:, lanes].astype(F32).T
            flip_ref[lanes] = flipped.astype(BF16)
            part_ref[lanes] = (flipped / 3).astype(BF16)

        def build(pair, carry):
            plain, third = wide_ref[pair, 0], wide_ref[pair, 1]
            for e in range(PROJ):
                rows = slice(e * cols, (e + 1) * cols)
                to = e % PER_TILE * (PROJ // PER_TILE) + e // PER_TILE
                into = slice(to * cols, (to + 1) * cols)
                for side in range(2):
                    lanes = slice(side * seqs, (side + 1) * seqs)
                    rm_ref[pair, into, lanes] = (
                        flip_ref[rows] * plain[:, lanes] + part_ref[rows] * third[:, lanes]
                    )
            return carry

        lax.fori_loop(first_pair(at_ref, labels_ref, 0), last_pair(at_ref, labels_ref, last) + 1, build, 0)
        sum_ref[...] = jnp.zeros_like(sum_ref)

    quarter = span // PER_TILE

    def product(pair, add):
        masked_left(left_ref, lab_ref, lb_ref, pair)
        for q in range(PER_TILE):
            rows = slice(q * quarter, (q + 1) * quarter)
            part = nn_dot(rm_ref[pair, rows], rolled(lb_ref[...], q))
            acc_ref[rows] = acc_ref[rows] + part if add else part

    product(first_pair(at_ref, labels_ref, g), False)

    def more(pair, carry):
        product(pair, True)
        return carry

    lax.fori_loop(
        first_pair(at_ref, labels_ref, g) + 1, last_pair(at_ref, labels_ref, g) + 1, more, 0
    )

    for half in range(WIDE // LANES):
        lanes = slice(half * LANES, (half + 1) * LANES)
        for t in range(PROJ // PER_TILE):
            parts = []
            for q in range(PER_TILE):
                e = q * (PROJ // PER_TILE) + t
                parts.append(acc_ref[e * cols : (e + 1) * cols, lanes].astype(BF16))
            turned = swap_blocks(parts)
            for p in range(PER_TILE):
                i = half * PER_TILE + p
                outer_ref[g, i * cols : (i + 1) * cols, t * LANES : (t + 1) * LANES] = turned[p]

    flat = grad_ref[...].reshape(rows_here * cols, width)
    sum_ref[...] += nn_dot(flat.T, outer_ref[g])

    @pl.when(g == last)
    def _():
        for t in range(PROJ * PROJ // LANES):
            part = slice(t * LANES, (t + 1) * LANES)
            turn_ref[part] = sum_ref[:, part].T
        for c in range(PROJ):
            weight_out[c * PROJ : (c + 1) * PROJ] = turn_ref[pl.ds(c, PROJ, stride=PROJ)]


def outer_call(at, labels, left, lab, right, wide, grad):
    rows, cols, width = grad.shape
    seqs, total = left.shape
    span = right.shape[1]
    step = WIDE // PROJ
    return pl.pallas_call(
        outer_body,
        grid_spec=pltpu.PrefetchScalarGridSpec(
            num_scalar_prefetch=2,
            grid=(total // WIDE,),
            in_specs=[
                VMEM,
                VMEM,
                VMEM,
                VMEM,
                pl.BlockSpec((step, cols, width), lambda g, *_: (g, 0, 0)),
            ],
            out_specs=[
                VMEM,
                VMEM,
            ],
            scratch_shapes=[
                pltpu.VMEM((CHAINS // 2, span, 2 * seqs), BF16),
                pltpu.VMEM((2 * seqs, WIDE), BF16),
                pltpu.VMEM((span, WIDE), F32),
                pltpu.VMEM((width, PROJ * PROJ), F32),
                pltpu.VMEM((PROJ * PROJ, width), F32),
                pltpu.VMEM((span, seqs), BF16),
                pltpu.VMEM((span, seqs), BF16),
            ],
        ),
        out_shape=[
            pltpu.VMEM((rows // step, step * cols, PROJ * PROJ), BF16),
            jax.ShapeDtypeStruct((PROJ * PROJ, width), F32),
        ],
        compiler_params=KERNEL,
        cost_estimate=cost(20, span, total, seqs),
        name="outer",
    )(at, labels, left, lab, right, wide, grad)


def pair_body(outer_ref, w_ref, offset_ref, pair_ref):
    pair = nn_dot(outer_ref[pl.program_id(0)], w_ref[...]) + offset_ref[...]
    pair_ref[...] = pair.astype(BF16)


def pair_call(outer, w, offset):
    groups, pairs, feats = outer.shape
    width = w.shape[1]
    return pl.pallas_call(
        pair_body,
        grid=(groups,),
        in_specs=[
            VMEM,
            VMEM,
            VMEM,
        ],
        out_specs=pl.BlockSpec((pairs, width), lambda g: (g, 0)),
        out_shape=jax.ShapeDtypeStruct((groups * pairs, width), BF16),
        compiler_params=KERNEL,
        cost_estimate=pl.CostEstimate(
            flops=2 * groups * pairs * feats * width,
            bytes_accessed=2 * groups * pairs * width,
            transcendentals=0,
        ),
        name="pair",
    )(outer, w, offset)


class Ring:
    def __init__(self, n_row, n_col):
        self.n_row, self.n_col = n_row, n_col
        self.per_row = n_col // n_row
        self.row = lax.axis_index("row").astype(jnp.uint32)
        self.col = lax.axis_index("col").astype(jnp.uint32)

    def col_shift(self, value, k):
        n = self.n_col
        return lax.ppermute(value, "col", [((t + k) % n, t) for t in range(n)])

    def row_shift(self, value, k):
        n = self.n_row
        return lax.ppermute(value, "row", [((t + k) % n, t) for t in range(n)])

    def right_along_row(self, right):
        others = [self.row_shift(right, k) for k in range(1, self.n_row)]
        return [right] + others

    def right_pieces(self, by_row):
        n, m = self.n_row, self.per_row
        here, lanes = by_row[0].shape
        lanes //= m
        by_row = jnp.stack(by_row)
        pieces = []
        for k in range(self.n_col):
            q = (self.col + (self.n_col - k)) % self.n_col
            at = ((q // m + (n - self.row)) % n, jnp.uint32(0), (q % m) * lanes)
            pieces.append(lax.dynamic_slice(by_row, at, (1, here, lanes))[0])
        return pieces

    def right_along_col(self, pieces):
        return jnp.concatenate([self.col_shift(p, k) if k else p for k, p in enumerate(pieces)])

    def right_grad_home(self, grad):
        n, m = self.n_col, self.per_row
        here, lanes = grad.shape[0] // n, grad.shape[1]
        total = jnp.zeros((m, here, lanes), F32)
        slot = lax.broadcasted_iota(jnp.uint32, (m, 1, 1), 0)
        for k in range(n):
            t = (self.row * m + self.col % m + k) % n
            block = lax.dynamic_slice_in_dim(grad, ((t + n - self.col) % n) * here, here, 0)
            pairs = []
            for r in range(self.n_row):
                for q in range(n):
                    pairs.append((r * n + q, (q // m) * n + (r * m + q % m + k) % n))
            got = lax.ppermute(block, ("row", "col"), pairs).astype(F32)[None]
            total += got if m == 1 else jnp.where(slot == (self.col + (n - k)) % n % m, got, 0)
        return total.swapaxes(0, 1).reshape(here, m * lanes).astype(BF16)

    def weight_over_row(self, weight):
        n = self.n_row
        size = weight.shape[0] // n
        sent = weight.astype(BF16).reshape(n, size, -1)
        total = lax.dynamic_index_in_dim(weight.reshape(n, size, -1), self.row, 0, keepdims=False)
        for k in range(1, n):
            piece = lax.dynamic_index_in_dim(sent, (self.row + k) % n, 0, keepdims=False)
            total += self.row_shift(piece, n - k).astype(F32)
        return total

    def weight_over_col(self, total):
        mine = total.astype(BF16)
        for k in range(1, self.n_col):
            total += self.col_shift(mine, k).astype(F32)
        return total.astype(BF16)

    def weight_to_all(self, mine):
        n = self.n_row
        which = (lax.broadcasted_iota(jnp.uint32, (n, 1, 1), 0) + (n - self.row)) % n
        shares = mine[None]
        for k in range(1, n):
            shares = jnp.where(which == k, self.row_shift(mine, k)[None], shares)
        return shares.reshape(n * mine.shape[0], mine.shape[1])


def after(value, *others):
    return lax.optimization_barrier((value,) + others)[0]


def shards(n_row, n_col, alignment_tensor, gain, shift, first_projector, second_projector,
           final_projector, final_offset, labels, counts, grad):
    ring = Ring(n_row, n_col)
    here, rows, _ = alignment_tensor.shape
    cols, width = grad.shape[1:]
    seqs = here * n_col
    left, right = project_call(
        alignment_tensor, gain[None, :], shift[None, :], first_projector.T, second_projector.T, cols
    )
    by_row = ring.right_along_row(right)
    left = jnp.concatenate([left] + [ring.col_shift(left, k) for k in range(1, n_col)])

    at = jnp.stack([ring.row * rows, ring.col * cols, ring.col * here]).astype(jnp.int32)
    lab, tall, wide, plain, w, wt = prep_call(
        at, labels, counts, after(final_projector, right), rows, cols, seqs
    )
    back = back_call(grad, wt)
    mine = ring.right_along_col(ring.right_pieces(by_row))
    back = in_vmem(back)
    right_grad = right_grad_call(at, labels, back, left, lab, plain)

    right = after(mine, right_grad)
    grad_right = ring.right_grad_home(right_grad)
    outer, weight = outer_call(
        at, labels, left, lab, right, wide, grad
    )
    share = ring.weight_over_row(weight)
    left_grad = left_grad_call(at, labels, back, after(lab, weight), right, tall)
    share = after(share, left_grad)

    total = left_grad[:here].astype(F32)
    for k in range(1, n_col):
        total += ring.col_shift(left_grad[k * here : (k + 1) * here], n_col - k).astype(F32)
    adjoint_first = total.astype(BF16)
    pair_update = pair_call(in_vmem(outer), after(w, left_grad, share), final_offset[None, :])
    pair_update = pair_update.reshape(rows, cols, width)
    mine = after(ring.weight_over_col(share), pair_update)
    grad_w_out = ring.weight_to_all(mine).astype(F32) / (n_row * rows)
    return pair_update, adjoint_first, grad_right, grad_w_out


def solution(mesh):
    in_specs = (
        P(("parts", "col"), "row", None),
        P(),
        P(),
        P(),
        P(),
        P(),
        P(),
        P("parts"),
        P("parts", None),
        P(("parts", "row"), "col", None),
    )
    out_specs = (
        P(("parts", "row"), "col", None),
        P(("parts", "col"), "row"),
        P(("parts", "col"), "row"),
        P("parts", None),
    )

    def body(*args):
        return shards(mesh.shape["row"], mesh.shape["col"], *args)

    return jax.shard_map(body, mesh=mesh, in_specs=in_specs, out_specs=out_specs, check_vma=False)
```

```python
import jax
import jax.numpy as jnp
from jax import lax
from jax.experimental import pallas as pl
from jax.experimental.pallas import tpu as pltpu
from jax.sharding import PartitionSpec as P


PROJ = 32
CHAINS = 8
LANES = 128
PER_TILE = LANES // PROJ
WIDE = 256
F32 = jnp.float32
BF16 = jnp.bfloat16
VMEM = pl.BlockSpec(memory_space=pltpu.VMEM)
KERNEL = pltpu.CompilerParams(vmem_limit_bytes=24 << 20)
HBM = pl.BlockSpec(memory_space=pltpu.HBM)
SMEM = pl.BlockSpec(memory_space=pltpu.SMEM)


def swap_blocks(parts):
    lane = lax.broadcasted_iota(jnp.int32, parts[0].shape, 1)
    outs = []
    for q in range(PER_TILE):
        out = parts[(PER_TILE - 1 - q) % PER_TILE]
        for block in range(PER_TILE - 2, -1, -1):
            out = jnp.where(lane < (block + 1) * PROJ, parts[(block - q) % PER_TILE], out)
        outs.append(pltpu.roll(out, LANES - q * PROJ, 1) if q else out)
    return outs


def rolled(value, p):
    if not p:
        return value
    return jnp.concatenate(
        [pltpu.roll(value[:, t : t + LANES], p * PROJ, 1) for t in range(0, value.shape[1], LANES)],
        axis=1,
    )


def nt_dot(a, b):
    return lax.dot_general(a, b, (((1,), (1,)), ((), ())), preferred_element_type=F32)


def nn_dot(a, b):
    return lax.dot_general(a, b, (((1,), (0,)), ((), ())), preferred_element_type=F32)


def in_vmem(value):
    return pltpu.with_memory_space_constraint(value, pltpu.VMEM)


def in_hbm(value):
    return pltpu.with_memory_space_constraint(value, pltpu.HBM)


def project_body(x_hbm, gain_hbm, shift_hbm, first_hbm, second_hbm, left_ref, right_ref,
                 x_ref, gain_ref, shift_ref, w_ref, proj_ref, turn_ref, out_ref, sems, *, cols):
    chunks, chunk, rows, feats = x_ref.shape
    small = [
        pltpu.make_async_copy(gain_hbm, gain_ref, sems.at[chunks]),
        pltpu.make_async_copy(shift_hbm, shift_ref, sems.at[chunks + 1]),
        pltpu.make_async_copy(first_hbm, w_ref.at[pl.ds(0, PROJ)], sems.at[chunks + 2]),
        pltpu.make_async_copy(second_hbm, w_ref.at[pl.ds(PROJ, PROJ)], sems.at[chunks + 3]),
    ]
    big = [
        pltpu.make_async_copy(x_hbm.at[pl.ds(g * chunk, chunk)], x_ref.at[g], sems.at[g])
        for g in range(chunks)
    ]
    for copy in big[:1] + small + big[1:]:
        copy.start()
    w_ref[2 * PROJ :] = jnp.zeros((LANES - 2 * PROJ, feats), BF16)
    for copy in small:
        copy.wait()
    for g in range(chunks):
        big[g].wait()
        x = x_ref[g].astype(F32).reshape(chunk * rows, feats)
        center = x - jnp.mean(x, axis=-1, keepdims=True)
        spread = jnp.mean(center * center, axis=-1, keepdims=True)
        normed = center * lax.rsqrt(spread + 1e-05) * gain_ref[...] + shift_ref[...]
        at = slice(g * chunk * rows, (g + 1) * chunk * rows)
        proj_ref[at] = nt_dot(normed.astype(BF16), w_ref[...])
    project_layout(proj_ref, turn_ref, out_ref, left_ref, right_ref, rows, cols)


def project_layout(proj_ref, turn_ref, out_ref, left_ref, right_ref, rows, cols):
    here = left_ref.shape[0]
    lane = lax.broadcasted_iota(jnp.int32, (here, LANES), 1)
    for t in range(rows // PER_TILE):
        tile = proj_ref[pl.ds(t * PER_TILE, here, stride=rows)]
        for p in range(1, PER_TILE):
            part = proj_ref[pl.ds(t * PER_TILE + p, here, stride=rows)]
            tile = jnp.where(lane < p * PROJ, tile, pltpu.roll(part, p * PROJ, 1))
        left_ref[:, t * LANES : (t + 1) * LANES] = tile.astype(BF16)

    tiles = here * rows // LANES
    for t in range(tiles):
        flipped = proj_ref[t * LANES : (t + 1) * LANES].T
        turn_ref[t * PROJ : (t + 1) * PROJ] = flipped[PROJ : 2 * PROJ]
    seqs = LANES // rows
    per = LANES // cols
    lane = lax.broadcasted_iota(jnp.int32, (tiles, LANES), 1)
    for block in range(rows // cols):
        for t in range(PROJ // per):
            at = (block * (PROJ // per) + t) * LANES
            parts = [turn_ref[pl.ds(t * per + p, tiles, stride=PROJ)] for p in range(per)]
            for u in range(seqs):
                start = u * rows + block * cols
                tile = None
                for p, part in enumerate(parts):
                    amount = (p * cols - start) % LANES
                    part = pltpu.roll(part, amount, 1) if amount else part
                    tile = part if tile is None else jnp.where(lane < p * cols, tile, part)
                out_ref[pl.ds(u, tiles, stride=seqs), :] = tile
            right_ref[:, at : at + LANES] = out_ref[...].astype(BF16)


def project_call(x, gain, shift, first, second, cols):
    here, rows, feats = x.shape
    chunk = min(here, max(1, 2 * WIDE // rows))
    return pl.pallas_call(
        lambda *refs: project_body(*refs, cols=cols),
        in_specs=[HBM] * 5,
        out_specs=[VMEM] * 2,
        out_shape=[jax.ShapeDtypeStruct((here, rows * PROJ), BF16)] * 2,
        scratch_shapes=[
            pltpu.VMEM((here // chunk, chunk, rows, feats), BF16),
            pltpu.VMEM(gain.shape, F32),
            pltpu.VMEM(shift.shape, F32),
            pltpu.VMEM((LANES, feats), BF16),
            pltpu.VMEM((here * rows, LANES), F32),
            pltpu.VMEM((here * rows // LANES * PROJ, LANES), F32),
            pltpu.VMEM((here, LANES), F32),
            pltpu.SemaphoreType.DMA((here // chunk + 4,)),
        ],
        compiler_params=KERNEL,
        name="project",
    )(*map(in_hbm, (x, gain, shift, first, second)))


def masks(at_ref, labels_ref, counts_ref, lab_ref, tall_ref, wide_ref, plain_ref, rows, cols, seqs):
    res = labels_ref.shape[1]
    labels = jnp.broadcast_to(labels_ref[...], (8, res))
    own = pltpu.roll(labels, (res - at_ref[0]) % res, 1)[:, :rows]
    spread = (
        lax.broadcasted_iota(jnp.int32, (rows, rows * PROJ), 1) // PROJ
        == lax.broadcasted_iota(jnp.int32, (rows, rows * PROJ), 0)
    )
    lab = nn_dot(own.astype(F32).astype(BF16), spread.astype(F32).astype(BF16))
    lab_ref[...] = lab[:1].astype(jnp.int32)

    there = pltpu.roll(labels, (res - at_ref[1]) % res, 1)[:, :LANES]
    there = jnp.where(lax.broadcasted_iota(jnp.int32, (8, LANES), 1) < cols, there, 0)
    reach = cols
    while reach < LANES:
        there = there + pltpu.roll(there, reach, 1)
        reach *= 2
    depth = jnp.zeros((CHAINS, LANES), jnp.int32)
    for b in range(CHAINS):
        depth += jnp.where(there == b, counts_ref[:, b : b + 1], 0)
    seq = (lax.broadcasted_iota(jnp.int32, (seqs, LANES), 0) + at_ref[2]) % seqs
    for a in range(CHAINS):
        deep = jnp.broadcast_to(depth[a : a + 1], (seqs, LANES))
        weight = jnp.where(seq < deep, 1.0 / deep.astype(F32), 0.0)
        three = deep % 3 == 0
        side = slice((a % 2) * seqs, (a % 2 + 1) * seqs)
        for x, part in enumerate((jnp.where(three, 0.0, weight), jnp.where(three, 3.0 * weight, 0.0))):
            tall_ref[a // 2, x, side] = part.astype(BF16)
            wide_ref[a // 2, x, :, side] = part.T[:cols].astype(BF16)
        plain_ref[a // 2, :, side] = weight.T[:cols]


def projector(w_ref, wide_w_ref, w_out, wt_ref):
    wide_w_ref[...] = w_ref[...].astype(F32)
    for t in range(PROJ // PER_TILE):
        for q in range(PER_TILE):
            e = t * PER_TILE + q
            w_out[e * PROJ : (e + 1) * PROJ] = wide_w_ref[pl.ds(e, PROJ, stride=PROJ)].astype(BF16)
        block = w_out[t * LANES : (t + 1) * LANES].astype(F32)
        for p in range(PER_TILE):
            wt_ref[p, :, t * LANES : (t + 1) * LANES] = rolled(block.T, p).astype(BF16)


def cost(passes, span, total, seqs):
    return pl.CostEstimate(
        flops=4 * passes * span * total * seqs, bytes_accessed=2 * span * total, transcendentals=0
    )


def back_body(at_ref, labels_hbm, counts_hbm, w_hbm, grad_hbm,
              lab_ref, tall_ref, wide_ref, plain_ref, w_out, back_ref, grad_ref,
              labels_ref, counts_ref, w_ref, wide_w_ref, wt_ref, sems, *, seqs):
    groups, step, cols, _ = grad_ref.shape
    copies = [
        pltpu.make_async_copy(w_hbm, w_ref, sems.at[groups]),
        pltpu.make_async_copy(labels_hbm, labels_ref, sems.at[groups + 1]),
        pltpu.make_async_copy(counts_hbm, counts_ref, sems.at[groups + 2]),
    ]
    for copy in copies:
        copy.start()

    def grad_of(g):
        return pltpu.make_async_copy(grad_hbm.at[pl.ds(g * step, step)], grad_ref.at[g], sems.at[g])

    for g in range(groups):
        grad_of(g).start()
    for copy in copies:
        copy.wait()
    projector(w_ref, wide_w_ref, w_out, wt_ref)
    masks(at_ref, labels_ref, counts_ref, lab_ref, tall_ref, wide_ref, plain_ref,
          groups * step, cols, seqs)
    halves = step // PER_TILE

    def group(g, carry):
        grad_of(g).wait()
        blocks = [
            jnp.concatenate([grad_ref[g, half * PER_TILE + p] for half in range(halves)], axis=0)
            for p in range(PER_TILE)
        ]
        for u in range(PROJ * PROJ // WIDE):
            prods = [
                nn_dot(block, wt_ref[p, :, u * WIDE : (u + 1) * WIDE]).astype(BF16)
                for p, block in enumerate(blocks)
            ]
            for half in range(halves):
                for t in range(WIDE // LANES):
                    parts = [
                        prod[half * cols : (half + 1) * cols, t * LANES : (t + 1) * LANES]
                        for prod in prods
                    ]
                    for q, part in enumerate(swap_blocks(parts)):
                        e = u * (WIDE // PROJ) + t * PER_TILE + q
                        at = (g, slice(e * cols, (e + 1) * cols))
                        back_ref[at + (slice(half * LANES, (half + 1) * LANES),)] = part
        return carry

    lax.fori_loop(0, groups, group, 0)


def back_call(at, labels, counts, w, grad, seqs):
    rows, cols, width = grad.shape
    step = WIDE // PROJ
    groups = rows // step
    pairs = CHAINS // 2
    labels = labels[None, :]
    return pl.pallas_call(
        lambda *refs: back_body(*refs, seqs=seqs),
        in_specs=[SMEM] + [HBM] * 4,
        out_specs=[VMEM] * 7,
        out_shape=[
            jax.ShapeDtypeStruct((1, rows * PROJ), jnp.int32),
            jax.ShapeDtypeStruct((pairs, 2, 2 * seqs, LANES), BF16),
            jax.ShapeDtypeStruct((pairs, 2, cols, 2 * seqs), BF16),
            jax.ShapeDtypeStruct((pairs, cols, 2 * seqs), F32),
            jax.ShapeDtypeStruct(w.shape, BF16),
            pltpu.VMEM((groups, PROJ * cols, WIDE), BF16),
            pltpu.VMEM((groups, step, cols, width), BF16),
        ],
        scratch_shapes=[
            pltpu.VMEM(labels.shape, jnp.int32),
            pltpu.VMEM(counts.shape, jnp.int32),
            pltpu.VMEM(w.shape, BF16),
            pltpu.VMEM(w.shape, F32),
            pltpu.VMEM((PER_TILE, width, PROJ * PROJ), BF16),
            pltpu.SemaphoreType.DMA((groups + 3,)),
        ],
        compiler_params=KERNEL,
        cost_estimate=cost(10, PROJ * cols, rows * PROJ, width),
        name="back",
    )(at, *map(in_hbm, (labels, counts, w, grad)))


def first_pair(at_ref, labels_ref, group):
    return labels_ref[at_ref[0] + group * (WIDE // PROJ)] // 2


def last_pair(at_ref, labels_ref, group):
    return labels_ref[at_ref[0] + (group + 1) * (WIDE // PROJ) - 1] // 2


def each(first, last, fn):
    def step(k, carry):
        fn(k)
        return carry

    lax.fori_loop(first, last + 1, step, 0)


def lanes_of(group):
    return pl.ds(pl.multiple_of(group * WIDE, WIDE), WIDE)


def masked_left(left_ref, lab_ref, lb_ref, pair, group):
    seqs = left_ref.shape[0]
    lanes = lanes_of(group)
    for side in range(2):
        keep = (lab_ref[:, lanes] == 2 * pair + side).astype(F32).astype(BF16)
        lb_ref[side * seqs : (side + 1) * seqs] = left_ref[:, lanes] * keep


def right_grad_body(at_ref, labels_ref, back_ref, left_ref, lab_ref, wide_ref,
                    right_out, q_ref, lb_ref, flip_ref, turn_ref):
    seqs = left_ref.shape[0]
    groups, span, _ = back_ref.shape
    cols = span // PROJ
    first = lambda g: first_pair(at_ref, labels_ref, g)
    last = lambda g: last_pair(at_ref, labels_ref, g)

    def clear(pair):
        q_ref[pair] = jnp.zeros(q_ref.shape[1:], F32)

    each(first(0), last(groups - 1), clear)

    def group(g):
        def one_pair(pair):
            masked_left(left_ref, lab_ref, lb_ref, pair, g)
            q_ref[pair] += nt_dot(back_ref[g], lb_ref[...])

        each(first(g), last(g), one_pair)

    each(0, groups - 1, group)

    def combine(pair, start):
        for e in range(PROJ):
            rows = slice(e * cols, (e + 1) * cols)
            both = q_ref[pair, rows] * wide_ref[pair]
            total = both[:, :seqs] + both[:, seqs:]
            flip_ref[rows] = total if start else flip_ref[rows] + total

    combine(first(0), True)
    each(first(0) + 1, last(groups - 1), lambda pair: combine(pair, False))
    for j in range(cols):
        turn_ref[j * PROJ : (j + 1) * PROJ] = flip_ref[pl.ds(j, PROJ, stride=cols)]
    for t in range(span // LANES):
        rows = slice(t * LANES, (t + 1) * LANES)
        right_out[:, rows] = turn_ref[rows].T.astype(BF16)


def right_grad_call(at, labels, back, left, lab, wide):
    groups, span, _ = back.shape
    total = groups * WIDE
    seqs = left.shape[0]
    return pl.pallas_call(
        right_grad_body,
        in_specs=[SMEM] * 2 + [VMEM] * 4,
        out_specs=VMEM,
        out_shape=jax.ShapeDtypeStruct((seqs, span), BF16),
        scratch_shapes=[
            pltpu.VMEM((CHAINS // 2, span, 2 * seqs), F32),
            pltpu.VMEM((2 * seqs, WIDE), BF16),
            pltpu.VMEM((span, seqs), F32),
            pltpu.VMEM((span, seqs), F32),
        ],
        compiler_params=KERNEL,
        cost_estimate=cost(10, span, total, seqs),
        name="right_grad",
    )(at, labels, back, left, lab, wide)


def left_grad_body(at_ref, labels_ref, back_ref, lab_ref, right_ref, tall_ref,
                   left_out, rm_ref, part_ref):
    seqs = right_ref.shape[0]
    groups, span, _ = back_ref.shape
    first = lambda g: first_pair(at_ref, labels_ref, g)
    last = lambda g: last_pair(at_ref, labels_ref, g)
    part_ref[...] = (right_ref[...].astype(F32) / 3).astype(BF16)

    def build(pair):
        for side in range(2):
            rows = slice(side * seqs, (side + 1) * seqs)
            plain, third = tall_ref[pair, 0, rows], tall_ref[pair, 1, rows]
            for t in range(span // LANES):
                lanes = slice(t * LANES, (t + 1) * LANES)
                rm_ref[pair, rows, lanes] = (
                    right_ref[:, lanes] * plain + part_ref[:, lanes] * third
                )

    each(first(0), last(groups - 1), build)

    def group(g):
        lab = lab_ref[:, lanes_of(g)]

        def one_pair(pair, total):
            part = nn_dot(rm_ref[pair], back_ref[g])
            keep0, keep1 = lab == 2 * pair, lab == 2 * pair + 1
            return total + jnp.where(keep0, part[:seqs], 0.0) + jnp.where(keep1, part[seqs:], 0.0)

        total = lax.fori_loop(first(g), last(g) + 1, one_pair, jnp.zeros((seqs, WIDE), F32))
        left_out[:, lanes_of(g)] = total.astype(BF16)

    each(0, groups - 1, group)


def left_grad_call(at, labels, back, lab, right, tall):
    groups, span, _ = back.shape
    total = groups * WIDE
    seqs = right.shape[0]
    return pl.pallas_call(
        left_grad_body,
        in_specs=[SMEM] * 2 + [VMEM] * 4,
        out_specs=VMEM,
        out_shape=jax.ShapeDtypeStruct((seqs, total), BF16),
        scratch_shapes=[
            pltpu.VMEM((CHAINS // 2, 2 * seqs, span), BF16),
            pltpu.VMEM((seqs, span), BF16),
        ],
        compiler_params=KERNEL,
        cost_estimate=cost(10, span, total, seqs),
        name="left_grad",
    )(at, labels, back, lab, right, tall)


def outer_body(at_ref, labels_ref, left_ref, lab_ref, right_ref, wide_ref, grad_ref,
               outer_ref, weight_out, rm_ref, lb_ref, acc_ref, sum_ref, turn_ref, flip_ref, part_ref):
    seqs = left_ref.shape[0]
    span = right_ref.shape[1]
    cols = span // PROJ
    groups, step, _, width = grad_ref.shape
    first = lambda g: first_pair(at_ref, labels_ref, g)
    last = lambda g: last_pair(at_ref, labels_ref, g)
    for t in range(span // LANES):
        lanes = slice(t * LANES, (t + 1) * LANES)
        flipped = right_ref[:, lanes].astype(F32).T
        flip_ref[lanes] = flipped.astype(BF16)
        part_ref[lanes] = (flipped / 3).astype(BF16)

    def build(pair):
        plain, third = wide_ref[pair, 0], wide_ref[pair, 1]
        for e in range(PROJ):
            rows = slice(e * cols, (e + 1) * cols)
            to = e % PER_TILE * (PROJ // PER_TILE) + e // PER_TILE
            into = slice(to * cols, (to + 1) * cols)
            for side in range(2):
                lanes = slice(side * seqs, (side + 1) * seqs)
                rm_ref[pair, into, lanes] = (
                    flip_ref[rows] * plain[:, lanes] + part_ref[rows] * third[:, lanes]
                )

    each(first(0), last(groups - 1), build)
    sum_ref[...] = jnp.zeros_like(sum_ref)
    quarter = span // PER_TILE

    def product(pair, g, add):
        masked_left(left_ref, lab_ref, lb_ref, pair, g)
        for q in range(PER_TILE):
            rows = slice(q * quarter, (q + 1) * quarter)
            part = nn_dot(rm_ref[pair, rows], rolled(lb_ref[...], q))
            acc_ref[rows] = acc_ref[rows] + part if add else part

    def group(g):
        product(first(g), g, False)
        each(first(g) + 1, last(g), lambda pair: product(pair, g, True))
        for half in range(WIDE // LANES):
            lanes = slice(half * LANES, (half + 1) * LANES)
            for t in range(PROJ // PER_TILE):
                parts = []
                for q in range(PER_TILE):
                    e = q * (PROJ // PER_TILE) + t
                    parts.append(acc_ref[e * cols : (e + 1) * cols, lanes].astype(BF16))
                turned = swap_blocks(parts)
                for p in range(PER_TILE):
                    i = half * PER_TILE + p
                    at = (g, slice(i * cols, (i + 1) * cols), slice(t * LANES, (t + 1) * LANES))
                    outer_ref[at] = turned[p]
        flat = grad_ref[g].reshape(step * cols, width)
        sum_ref[...] += nn_dot(flat.T, outer_ref[g])

    each(0, groups - 1, group)
    for t in range(PROJ * PROJ // LANES):
        part = slice(t * LANES, (t + 1) * LANES)
        turn_ref[part] = sum_ref[:, part].T
    for c in range(PROJ):
        weight_out[c * PROJ : (c + 1) * PROJ] = turn_ref[pl.ds(c, PROJ, stride=PROJ)]


def outer_call(at, labels, left, lab, right, wide, grad):
    groups, step, cols, width = grad.shape
    seqs, total = left.shape
    span = right.shape[1]
    return pl.pallas_call(
        outer_body,
        in_specs=[SMEM] * 2 + [VMEM] * 5,
        out_specs=[VMEM] * 2,
        out_shape=[
            pltpu.VMEM((groups, step * cols, PROJ * PROJ), BF16),
            jax.ShapeDtypeStruct((PROJ * PROJ, width), F32),
        ],
        scratch_shapes=[
            pltpu.VMEM((CHAINS // 2, span, 2 * seqs), BF16),
            pltpu.VMEM((2 * seqs, WIDE), BF16),
            pltpu.VMEM((span, WIDE), F32),
            pltpu.VMEM((width, PROJ * PROJ), F32),
            pltpu.VMEM((PROJ * PROJ, width), F32),
            pltpu.VMEM((span, seqs), BF16),
            pltpu.VMEM((span, seqs), BF16),
        ],
        compiler_params=KERNEL,
        cost_estimate=cost(20, span, total, seqs),
        name="outer",
    )(at, labels, left, lab, right, wide, grad)


def pair_body(outer_ref, w_ref, offset_ref, pair_ref):
    _, pairs, _ = outer_ref.shape
    here = pair_ref.shape[0] // pairs
    for g in range(here):
        pair = nn_dot(outer_ref[pl.program_id(0) * here + g], w_ref[...]) + offset_ref[...]
        pair_ref[g * pairs : (g + 1) * pairs] = pair.astype(BF16)


def pair_call(outer, w, offset):
    groups, pairs, feats = outer.shape
    width = w.shape[1]
    steps = 2
    return pl.pallas_call(
        pair_body,
        grid=(steps,),
        in_specs=[VMEM] * 3,
        out_specs=pl.BlockSpec((groups * pairs // steps, width), lambda g: (g, 0)),
        out_shape=jax.ShapeDtypeStruct((groups * pairs, width), BF16),
        compiler_params=KERNEL,
        cost_estimate=pl.CostEstimate(
            flops=2 * groups * pairs * feats * width,
            bytes_accessed=2 * groups * pairs * width,
            transcendentals=0,
        ),
        name="pair",
    )(outer, w, offset)


class Ring:
    def __init__(self, n_row, n_col):
        self.n_row, self.n_col = n_row, n_col
        self.per_row = n_col // n_row
        self.row = lax.axis_index("row").astype(jnp.uint32)
        self.col = lax.axis_index("col").astype(jnp.uint32)

    def col_shift(self, value, k):
        n = self.n_col
        return lax.ppermute(value, "col", [((t + k) % n, t) for t in range(n)])

    def row_shift(self, value, k):
        n = self.n_row
        return lax.ppermute(value, "row", [((t + k) % n, t) for t in range(n)])

    def right_along_row(self, right):
        others = [self.row_shift(right, k) for k in range(1, self.n_row)]
        return [right] + others

    def right_pieces(self, by_row):
        n, m = self.n_row, self.per_row
        here, lanes = by_row[0].shape
        lanes //= m
        by_row = jnp.stack(by_row)
        pieces = []
        for k in range(self.n_col):
            q = (self.col + (self.n_col - k)) % self.n_col
            at = ((q // m + (n - self.row)) % n, jnp.uint32(0), (q % m) * lanes)
            pieces.append(lax.dynamic_slice(by_row, at, (1, here, lanes))[0])
        return pieces

    def right_along_col(self, pieces):
        return jnp.concatenate([self.col_shift(p, k) if k else p for k, p in enumerate(pieces)])

    def right_grad_home(self, grad):
        n, m = self.n_col, self.per_row
        here, lanes = grad.shape[0] // n, grad.shape[1]
        total = jnp.zeros((m, here, lanes), F32)
        slot = lax.broadcasted_iota(jnp.uint32, (m, 1, 1), 0)
        for k in range(n):
            t = (self.row * m + self.col % m + k) % n
            block = lax.dynamic_slice_in_dim(grad, ((t + n - self.col) % n) * here, here, 0)
            pairs = []
            for r in range(self.n_row):
                for q in range(n):
                    pairs.append((r * n + q, (q // m) * n + (r * m + q % m + k) % n))
            got = lax.ppermute(block, ("row", "col"), pairs).astype(F32)[None]
            total += got if m == 1 else jnp.where(slot == (self.col + (n - k)) % n % m, got, 0)
        return total.swapaxes(0, 1).reshape(here, m * lanes).astype(BF16)

    def weight_over_row(self, weight):
        n = self.n_row
        size = weight.shape[0] // n
        sent = weight.astype(BF16).reshape(n, size, -1)
        total = lax.dynamic_index_in_dim(weight.reshape(n, size, -1), self.row, 0, keepdims=False)
        for k in range(1, n):
            piece = lax.dynamic_index_in_dim(sent, (self.row + k) % n, 0, keepdims=False)
            total += self.row_shift(piece, n - k).astype(F32)
        return total

    def weight_over_col(self, total):
        mine = total.astype(BF16)
        for k in range(1, self.n_col):
            total += self.col_shift(mine, k).astype(F32)
        return total.astype(BF16)

    def weight_to_all(self, mine):
        n = self.n_row
        which = (lax.broadcasted_iota(jnp.uint32, (n, 1, 1), 0) + (n - self.row)) % n
        shares = mine[None]
        for k in range(1, n):
            shares = jnp.where(which == k, self.row_shift(mine, k)[None], shares)
        return shares.reshape(n * mine.shape[0], mine.shape[1])


def after(value, *others):
    return lax.optimization_barrier((value,) + others)[0]


def shards(n_row, n_col, alignment_tensor, gain, shift, first_projector, second_projector,
           final_projector, final_offset, labels, counts, grad):
    ring = Ring(n_row, n_col)
    here, rows, _ = alignment_tensor.shape
    cols, width = grad.shape[1:]
    seqs = here * n_col
    left, right = project_call(
        alignment_tensor, gain[None, :], shift[None, :], first_projector.T, second_projector.T, cols
    )
    by_row = ring.right_along_row(right)
    left = jnp.concatenate([left] + [ring.col_shift(left, k) for k in range(1, n_col)])

    at = jnp.stack([ring.row * rows, ring.col * cols, ring.col * here]).astype(jnp.int32)
    lab, tall, wide, plain, w, back, grad = back_call(
        at, labels, counts, after(final_projector, right), grad, seqs
    )
    mine = ring.right_along_col(ring.right_pieces(by_row))
    back, grad = in_vmem(back), in_vmem(grad)
    right_grad = right_grad_call(at, labels, back, left, lab, plain)

    right = after(mine, right_grad)
    grad_right = ring.right_grad_home(right_grad)
    outer, weight = outer_call(
        at, labels, left, lab, right, wide, grad
    )
    share = ring.weight_over_row(weight)
    left_grad = left_grad_call(at, labels, back, after(lab, weight), right, tall)
    share = after(share, left_grad)

    total = left_grad[:here].astype(F32)
    for k in range(1, n_col):
        total += ring.col_shift(left_grad[k * here : (k + 1) * here], n_col - k).astype(F32)
    adjoint_first = total.astype(BF16)
    pair_update = pair_call(in_vmem(outer), after(w, left_grad, share), final_offset[None, :])
    pair_update = pair_update.reshape(rows, cols, width)
    mine = after(ring.weight_over_col(share), pair_update)
    grad_w_out = ring.weight_to_all(mine).astype(F32) / (n_row * rows)
    return pair_update, adjoint_first, grad_right, grad_w_out


def solution(mesh):
    in_specs = (
        P(("parts", "col"), "row", None),
        P(),
        P(),
        P(),
        P(),
        P(),
        P(),
        P("parts"),
        P("parts", None),
        P(("parts", "row"), "col", None),
    )
    out_specs = (
        P(("parts", "row"), "col", None),
        P(("parts", "col"), "row"),
        P(("parts", "col"), "row"),
        P("parts", None),
    )

    def body(*args):
        return shards(mesh.shape["row"], mesh.shape["col"], *args)

    return jax.shard_map(body, mesh=mesh, in_specs=in_specs, out_specs=out_specs, check_vma=False)
```

```python
import jax
import jax.numpy as jnp
from jax import lax
from jax.experimental import pallas as pl
from jax.experimental.pallas import tpu as pltpu
from jax.sharding import PartitionSpec as P


PROJ = 32
CHAINS = 8
LANES = 128
PER_TILE = LANES // PROJ
WIDE = 256
F32 = jnp.float32
BF16 = jnp.bfloat16
VMEM = pl.BlockSpec(memory_space=pltpu.VMEM)
KERNEL = pltpu.CompilerParams(vmem_limit_bytes=24 << 20)
HBM = pl.BlockSpec(memory_space=pltpu.HBM)
SMEM = pl.BlockSpec(memory_space=pltpu.SMEM)


def swap_blocks(parts):
    lane = lax.broadcasted_iota(jnp.int32, parts[0].shape, 1)
    outs = []
    for q in range(PER_TILE):
        out = parts[(PER_TILE - 1 - q) % PER_TILE]
        for block in range(PER_TILE - 2, -1, -1):
            out = jnp.where(lane < (block + 1) * PROJ, parts[(block - q) % PER_TILE], out)
        outs.append(pltpu.roll(out, LANES - q * PROJ, 1) if q else out)
    return outs


def rolled(value, p):
    if not p:
        return value
    return jnp.concatenate(
        [pltpu.roll(value[:, t : t + LANES], p * PROJ, 1) for t in range(0, value.shape[1], LANES)],
        axis=1,
    )


def nt_dot(a, b):
    return lax.dot_general(a, b, (((1,), (1,)), ((), ())), preferred_element_type=F32)


def nn_dot(a, b):
    return lax.dot_general(a, b, (((1,), (0,)), ((), ())), preferred_element_type=F32)


def in_vmem(value):
    return pltpu.with_memory_space_constraint(value, pltpu.VMEM)


def in_hbm(value):
    return pltpu.with_memory_space_constraint(value, pltpu.HBM)


def project_body(x_hbm, gain_hbm, shift_hbm, first_hbm, second_hbm, left_ref, right_ref,
                 x_ref, gain_ref, shift_ref, w_ref, proj_ref, turn_ref, out_ref, sems, *, cols):
    chunks, chunk, rows, feats = x_ref.shape
    small = [
        pltpu.make_async_copy(gain_hbm, gain_ref, sems.at[chunks]),
        pltpu.make_async_copy(shift_hbm, shift_ref, sems.at[chunks + 1]),
        pltpu.make_async_copy(first_hbm, w_ref.at[pl.ds(0, PROJ)], sems.at[chunks + 2]),
        pltpu.make_async_copy(second_hbm, w_ref.at[pl.ds(PROJ, PROJ)], sems.at[chunks + 3]),
    ]
    big = [
        pltpu.make_async_copy(x_hbm.at[pl.ds(g * chunk, chunk)], x_ref.at[g], sems.at[g])
        for g in range(chunks)
    ]
    for copy in big[:1] + small + big[1:]:
        copy.start()
    w_ref[2 * PROJ :] = jnp.zeros((LANES - 2 * PROJ, feats), BF16)
    for copy in small:
        copy.wait()
    for g in range(chunks):
        big[g].wait()
        x = x_ref[g].astype(F32).reshape(chunk * rows, feats)
        center = x - jnp.mean(x, axis=-1, keepdims=True)
        spread = jnp.mean(center * center, axis=-1, keepdims=True)
        normed = center * lax.rsqrt(spread + 1e-05) * gain_ref[...] + shift_ref[...]
        at = slice(g * chunk * rows, (g + 1) * chunk * rows)
        proj_ref[at] = nt_dot(normed.astype(BF16), w_ref[...])
    project_layout(proj_ref, turn_ref, out_ref, left_ref, right_ref, rows, cols)


def project_layout(proj_ref, turn_ref, out_ref, left_ref, right_ref, rows, cols):
    here = left_ref.shape[0]
    lane = lax.broadcasted_iota(jnp.int32, (here, LANES), 1)
    for t in range(rows // PER_TILE):
        tile = proj_ref[pl.ds(t * PER_TILE, here, stride=rows)]
        for p in range(1, PER_TILE):
            part = proj_ref[pl.ds(t * PER_TILE + p, here, stride=rows)]
            tile = jnp.where(lane < p * PROJ, tile, pltpu.roll(part, p * PROJ, 1))
        left_ref[:, t * LANES : (t + 1) * LANES] = tile.astype(BF16)

    tiles = here * rows // LANES
    for t in range(tiles):
        flipped = proj_ref[t * LANES : (t + 1) * LANES].T
        turn_ref[t * PROJ : (t + 1) * PROJ] = flipped[PROJ : 2 * PROJ]
    seqs = LANES // rows
    per = LANES // cols
    lane = lax.broadcasted_iota(jnp.int32, (tiles, LANES), 1)
    for block in range(rows // cols):
        for t in range(PROJ // per):
            at = (block * (PROJ // per) + t) * LANES
            parts = [turn_ref[pl.ds(t * per + p, tiles, stride=PROJ)] for p in range(per)]
            for u in range(seqs):
                start = u * rows + block * cols
                tile = None
                for p, part in enumerate(parts):
                    amount = (p * cols - start) % LANES
                    part = pltpu.roll(part, amount, 1) if amount else part
                    tile = part if tile is None else jnp.where(lane < p * cols, tile, part)
                out_ref[pl.ds(u, tiles, stride=seqs), :] = tile
            right_ref[:, at : at + LANES] = out_ref[...].astype(BF16)


def project_call(x, gain, shift, first, second, cols):
    here, rows, feats = x.shape
    chunk = min(here, max(1, 2 * WIDE // rows))
    return pl.pallas_call(
        lambda *refs: project_body(*refs, cols=cols),
        in_specs=[HBM] * 5,
        out_specs=[VMEM] * 2,
        out_shape=[jax.ShapeDtypeStruct((here, rows * PROJ), BF16)] * 2,
        scratch_shapes=[
            pltpu.VMEM((here // chunk, chunk, rows, feats), BF16),
            pltpu.VMEM(gain.shape, F32),
            pltpu.VMEM(shift.shape, F32),
            pltpu.VMEM((LANES, feats), BF16),
            pltpu.VMEM((here * rows, LANES), F32),
            pltpu.VMEM((here * rows // LANES * PROJ, LANES), F32),
            pltpu.VMEM((here, LANES), F32),
            pltpu.SemaphoreType.DMA((here // chunk + 4,)),
        ],
        compiler_params=KERNEL,
        name="project",
    )(*map(in_hbm, (x, gain, shift, first, second)))


def masks(at_ref, labels_ref, counts_ref, lab_ref, tall_ref, wide_ref, plain_ref, rows, cols, seqs):
    res = labels_ref.shape[1]
    labels = jnp.broadcast_to(labels_ref[...], (8, res))
    own = pltpu.roll(labels, (res - at_ref[0]) % res, 1)[:, :rows]
    spread = (
        lax.broadcasted_iota(jnp.int32, (rows, rows * PROJ), 1) // PROJ
        == lax.broadcasted_iota(jnp.int32, (rows, rows * PROJ), 0)
    )
    lab = nn_dot(own.astype(F32).astype(BF16), spread.astype(F32).astype(BF16))
    lab_ref[...] = lab[:1].astype(jnp.int32)

    there = pltpu.roll(labels, (res - at_ref[1]) % res, 1)[:, :LANES]
    there = jnp.where(lax.broadcasted_iota(jnp.int32, (8, LANES), 1) < cols, there, 0)
    reach = cols
    while reach < LANES:
        there = there + pltpu.roll(there, reach, 1)
        reach *= 2
    depth = jnp.zeros((CHAINS, LANES), jnp.int32)
    for b in range(CHAINS):
        depth += jnp.where(there == b, counts_ref[:, b : b + 1], 0)
    seq = (lax.broadcasted_iota(jnp.int32, (seqs, LANES), 0) + at_ref[2]) % seqs
    for a in range(CHAINS):
        deep = jnp.broadcast_to(depth[a : a + 1], (seqs, LANES))
        weight = jnp.where(seq < deep, 1.0 / deep.astype(F32), 0.0)
        three = deep % 3 == 0
        for x, part in enumerate((jnp.where(three, 0.0, weight), jnp.where(three, 3.0 * weight, 0.0))):
            tall_ref[a, x] = part.astype(BF16)
            wide_ref[a, x] = part.T[:cols].astype(BF16)
        plain_ref[a] = weight.T[:cols]


def projector(w_ref, wide_w_ref, w_out, wt_ref):
    wide_w_ref[...] = w_ref[...].astype(F32)
    for t in range(PROJ // PER_TILE):
        for q in range(PER_TILE):
            e = t * PER_TILE + q
            w_out[e * PROJ : (e + 1) * PROJ] = wide_w_ref[pl.ds(e, PROJ, stride=PROJ)].astype(BF16)
        block = w_out[t * LANES : (t + 1) * LANES].astype(F32)
        for p in range(PER_TILE):
            wt_ref[p, :, t * LANES : (t + 1) * LANES] = rolled(block.T, p).astype(BF16)


def cost(passes, span, total, seqs):
    return pl.CostEstimate(
        flops=4 * passes * span * total * seqs, bytes_accessed=2 * span * total, transcendentals=0
    )


def back_body(at_ref, labels_hbm, counts_hbm, w_hbm, grad_hbm,
              lab_ref, tall_ref, wide_ref, plain_ref, w_out, back_ref, grad_ref,
              labels_ref, counts_ref, w_ref, wide_w_ref, wt_ref, sems, *, seqs):
    groups, step, cols, _ = grad_ref.shape
    copies = [
        pltpu.make_async_copy(w_hbm, w_ref, sems.at[groups]),
        pltpu.make_async_copy(labels_hbm, labels_ref, sems.at[groups + 1]),
        pltpu.make_async_copy(counts_hbm, counts_ref, sems.at[groups + 2]),
    ]
    for copy in copies:
        copy.start()

    def grad_of(g):
        return pltpu.make_async_copy(grad_hbm.at[pl.ds(g * step, step)], grad_ref.at[g], sems.at[g])

    for g in range(groups):
        grad_of(g).start()
    for copy in copies:
        copy.wait()
    projector(w_ref, wide_w_ref, w_out, wt_ref)
    masks(at_ref, labels_ref, counts_ref, lab_ref, tall_ref, wide_ref, plain_ref,
          groups * step, cols, seqs)
    halves = step // PER_TILE

    def group(g, carry):
        grad_of(g).wait()
        blocks = [
            jnp.concatenate([grad_ref[g, half * PER_TILE + p] for half in range(halves)], axis=0)
            for p in range(PER_TILE)
        ]
        for u in range(PROJ * PROJ // WIDE):
            prods = [
                nn_dot(block, wt_ref[p, :, u * WIDE : (u + 1) * WIDE]).astype(BF16)
                for p, block in enumerate(blocks)
            ]
            for half in range(halves):
                for t in range(WIDE // LANES):
                    parts = [
                        prod[half * cols : (half + 1) * cols, t * LANES : (t + 1) * LANES]
                        for prod in prods
                    ]
                    for q, part in enumerate(swap_blocks(parts)):
                        e = u * (WIDE // PROJ) + t * PER_TILE + q
                        at = (g, slice(e * cols, (e + 1) * cols))
                        back_ref[at + (slice(half * LANES, (half + 1) * LANES),)] = part
        return carry

    lax.fori_loop(0, groups, group, 0)


def back_call(at, labels, counts, w, grad, seqs):
    rows, cols, width = grad.shape
    step = WIDE // PROJ
    groups = rows // step
    labels = labels[None, :]
    return pl.pallas_call(
        lambda *refs: back_body(*refs, seqs=seqs),
        in_specs=[SMEM] + [HBM] * 4,
        out_specs=[VMEM] * 7,
        out_shape=[
            jax.ShapeDtypeStruct((1, rows * PROJ), jnp.int32),
            jax.ShapeDtypeStruct((CHAINS, 2, seqs, LANES), BF16),
            jax.ShapeDtypeStruct((CHAINS, 2, cols, seqs), BF16),
            jax.ShapeDtypeStruct((CHAINS, cols, seqs), F32),
            jax.ShapeDtypeStruct(w.shape, BF16),
            pltpu.VMEM((groups, PROJ * cols, WIDE), BF16),
            pltpu.VMEM((groups, step, cols, width), BF16),
        ],
        scratch_shapes=[
            pltpu.VMEM(labels.shape, jnp.int32),
            pltpu.VMEM(counts.shape, jnp.int32),
            pltpu.VMEM(w.shape, BF16),
            pltpu.VMEM(w.shape, F32),
            pltpu.VMEM((PER_TILE, width, PROJ * PROJ), BF16),
            pltpu.SemaphoreType.DMA((groups + 3,)),
        ],
        compiler_params=KERNEL,
        cost_estimate=cost(10, PROJ * cols, rows * PROJ, width),
        name="back",
    )(at, *map(in_hbm, (labels, counts, w, grad)))


def first_chain(at_ref, labels_ref, group):
    return labels_ref[at_ref[0] + group * (WIDE // PROJ)]


def last_chain(at_ref, labels_ref, group):
    return labels_ref[at_ref[0] + (group + 1) * (WIDE // PROJ) - 1]


def slots(chain, count, seqs):
    return pl.ds(pl.multiple_of(chain * seqs, seqs), count * seqs)


def each(first, last, fn):
    def step(k, carry):
        fn(k)
        return carry

    lax.fori_loop(first, last + 1, step, 0)


def lanes_of(group):
    return pl.ds(pl.multiple_of(group * WIDE, WIDE), WIDE)


def masked_left(left_ref, lab_ref, lb_ref, chain, group):
    seqs = left_ref.shape[0]
    lanes = lanes_of(group)
    for side in range(2):
        keep = (lab_ref[:, lanes] == chain + side).astype(F32).astype(BF16)
        lb_ref[side * seqs : (side + 1) * seqs] = left_ref[:, lanes] * keep


def right_grad_body(at_ref, labels_ref, back_ref, left_ref, lab_ref, wide_ref,
                    right_out, q_ref, lb_ref, flip_ref, turn_ref):
    seqs = left_ref.shape[0]
    groups, span, _ = back_ref.shape
    cols = span // PROJ
    first = lambda g: first_chain(at_ref, labels_ref, g)
    last = lambda g: last_chain(at_ref, labels_ref, g)

    def clear(chain):
        q_ref[:, slots(chain, 1, seqs)] = jnp.zeros((span, seqs), F32)

    each(first(0), last(groups - 1) + 1, clear)

    def group(g):
        def two_chains(k):
            chain = first(g) + 2 * k
            masked_left(left_ref, lab_ref, lb_ref, chain, g)
            q_ref[:, slots(chain, 2, seqs)] += nt_dot(back_ref[g], lb_ref[...])

        each(0, (last(g) - first(g)) // 2, two_chains)

    each(0, groups - 1, group)

    def combine(chain, start):
        for e in range(PROJ):
            rows = slice(e * cols, (e + 1) * cols)
            part = q_ref[rows, slots(chain, 1, seqs)] * wide_ref[chain]
            flip_ref[rows] = part if start else flip_ref[rows] + part

    combine(first(0), True)
    each(first(0) + 1, last(groups - 1), lambda chain: combine(chain, False))
    for j in range(cols):
        turn_ref[j * PROJ : (j + 1) * PROJ] = flip_ref[pl.ds(j, PROJ, stride=cols)]
    for t in range(span // LANES):
        rows = slice(t * LANES, (t + 1) * LANES)
        right_out[:, rows] = turn_ref[rows].T.astype(BF16)


def right_grad_call(at, labels, back, left, lab, wide):
    groups, span, _ = back.shape
    total = groups * WIDE
    seqs = left.shape[0]
    return pl.pallas_call(
        right_grad_body,
        in_specs=[SMEM] * 2 + [VMEM] * 4,
        out_specs=VMEM,
        out_shape=jax.ShapeDtypeStruct((seqs, span), BF16),
        scratch_shapes=[
            pltpu.VMEM((span, (CHAINS + 1) * seqs), F32),
            pltpu.VMEM((2 * seqs, WIDE), BF16),
            pltpu.VMEM((span, seqs), F32),
            pltpu.VMEM((span, seqs), F32),
        ],
        compiler_params=KERNEL,
        cost_estimate=cost(10, span, total, seqs),
        name="right_grad",
    )(at, labels, back, left, lab, wide)


def left_grad_body(at_ref, labels_ref, back_ref, lab_ref, right_ref, tall_ref,
                   left_out, rm_ref, part_ref):
    seqs = right_ref.shape[0]
    groups, span, _ = back_ref.shape
    first = lambda g: first_chain(at_ref, labels_ref, g)
    last = lambda g: last_chain(at_ref, labels_ref, g)
    part_ref[...] = (right_ref[...].astype(F32) / 3).astype(BF16)

    def build(chain):
        plain, third = tall_ref[chain, 0], tall_ref[chain, 1]
        for t in range(span // LANES):
            lanes = slice(t * LANES, (t + 1) * LANES)
            rm_ref[slots(chain, 1, seqs), lanes] = (
                right_ref[:, lanes] * plain + part_ref[:, lanes] * third
            )

    each(first(0), last(groups - 1), build)
    rm_ref[slots(last(groups - 1) + 1, 1, seqs)] = jnp.zeros((seqs, span), BF16)

    def group(g):
        lab = lab_ref[:, lanes_of(g)]

        def two_chains(k, total):
            chain = first(g) + 2 * k
            part = nn_dot(rm_ref[slots(chain, 2, seqs)], back_ref[g])
            keep0, keep1 = lab == chain, lab == chain + 1
            return total + jnp.where(keep0, part[:seqs], 0.0) + jnp.where(keep1, part[seqs:], 0.0)

        passes = (last(g) - first(g)) // 2 + 1
        total = lax.fori_loop(0, passes, two_chains, jnp.zeros((seqs, WIDE), F32))
        left_out[:, lanes_of(g)] = total.astype(BF16)

    each(0, groups - 1, group)


def left_grad_call(at, labels, back, lab, right, tall):
    groups, span, _ = back.shape
    total = groups * WIDE
    seqs = right.shape[0]
    return pl.pallas_call(
        left_grad_body,
        in_specs=[SMEM] * 2 + [VMEM] * 4,
        out_specs=VMEM,
        out_shape=jax.ShapeDtypeStruct((seqs, total), BF16),
        scratch_shapes=[
            pltpu.VMEM(((CHAINS + 1) * seqs, span), BF16),
            pltpu.VMEM((seqs, span), BF16),
        ],
        compiler_params=KERNEL,
        cost_estimate=cost(10, span, total, seqs),
        name="left_grad",
    )(at, labels, back, lab, right, tall)


def outer_body(at_ref, labels_ref, left_ref, lab_ref, right_ref, wide_ref, grad_ref,
               outer_ref, weight_out, rm_ref, lb_ref, acc_ref, sum_ref, turn_ref, flip_ref, part_ref):
    seqs = left_ref.shape[0]
    span = right_ref.shape[1]
    cols = span // PROJ
    groups, step, _, width = grad_ref.shape
    first = lambda g: first_chain(at_ref, labels_ref, g)
    last = lambda g: last_chain(at_ref, labels_ref, g)
    for t in range(span // LANES):
        lanes = slice(t * LANES, (t + 1) * LANES)
        flipped = right_ref[:, lanes].astype(F32).T
        flip_ref[lanes] = flipped.astype(BF16)
        part_ref[lanes] = (flipped / 3).astype(BF16)

    def build(chain):
        plain, third = wide_ref[chain, 0], wide_ref[chain, 1]
        for e in range(PROJ):
            rows = slice(e * cols, (e + 1) * cols)
            to = e % PER_TILE * (PROJ // PER_TILE) + e // PER_TILE
            rm_ref[to * cols : (to + 1) * cols, slots(chain, 1, seqs)] = (
                flip_ref[rows] * plain + part_ref[rows] * third
            )

    each(first(0), last(groups - 1), build)
    rm_ref[:, slots(last(groups - 1) + 1, 1, seqs)] = jnp.zeros((span, seqs), BF16)
    sum_ref[...] = jnp.zeros_like(sum_ref)
    quarter = span // PER_TILE

    def product(chain, g, add):
        masked_left(left_ref, lab_ref, lb_ref, chain, g)
        for q in range(PER_TILE):
            rows = slice(q * quarter, (q + 1) * quarter)
            part = nn_dot(rm_ref[rows, slots(chain, 2, seqs)], rolled(lb_ref[...], q))
            acc_ref[rows] = acc_ref[rows] + part if add else part

    def group(g):
        product(first(g), g, False)
        each(1, (last(g) - first(g)) // 2, lambda k: product(first(g) + 2 * k, g, True))
        for half in range(WIDE // LANES):
            lanes = slice(half * LANES, (half + 1) * LANES)
            for t in range(PROJ // PER_TILE):
                parts = []
                for q in range(PER_TILE):
                    e = q * (PROJ // PER_TILE) + t
                    parts.append(acc_ref[e * cols : (e + 1) * cols, lanes].astype(BF16))
                turned = swap_blocks(parts)
                for p in range(PER_TILE):
                    i = half * PER_TILE + p
                    at = (g, slice(i * cols, (i + 1) * cols), slice(t * LANES, (t + 1) * LANES))
                    outer_ref[at] = turned[p]
        flat = grad_ref[g].reshape(step * cols, width)
        sum_ref[...] += nn_dot(flat.T, outer_ref[g])

    each(0, groups - 1, group)
    for t in range(PROJ * PROJ // LANES):
        part = slice(t * LANES, (t + 1) * LANES)
        turn_ref[part] = sum_ref[:, part].T
    for c in range(PROJ):
        weight_out[c * PROJ : (c + 1) * PROJ] = turn_ref[pl.ds(c, PROJ, stride=PROJ)]


def outer_call(at, labels, left, lab, right, wide, grad):
    groups, step, cols, width = grad.shape
    seqs, total = left.shape
    span = right.shape[1]
    return pl.pallas_call(
        outer_body,
        in_specs=[SMEM] * 2 + [VMEM] * 5,
        out_specs=[VMEM] * 2,
        out_shape=[
            pltpu.VMEM((groups, step * cols, PROJ * PROJ), BF16),
            jax.ShapeDtypeStruct((PROJ * PROJ, width), F32),
        ],
        scratch_shapes=[
            pltpu.VMEM((span, (CHAINS + 1) * seqs), BF16),
            pltpu.VMEM((2 * seqs, WIDE), BF16),
            pltpu.VMEM((span, WIDE), F32),
            pltpu.VMEM((width, PROJ * PROJ), F32),
            pltpu.VMEM((PROJ * PROJ, width), F32),
            pltpu.VMEM((span, seqs), BF16),
            pltpu.VMEM((span, seqs), BF16),
        ],
        compiler_params=KERNEL,
        cost_estimate=cost(20, span, total, seqs),
        name="outer",
    )(at, labels, left, lab, right, wide, grad)


def pair_body(outer_ref, w_ref, offset_ref, pair_ref):
    _, pairs, _ = outer_ref.shape
    here = pair_ref.shape[0] // pairs
    for g in range(here):
        pair = nn_dot(outer_ref[pl.program_id(0) * here + g], w_ref[...]) + offset_ref[...]
        pair_ref[g * pairs : (g + 1) * pairs] = pair.astype(BF16)


def pair_call(outer, w, offset):
    groups, pairs, feats = outer.shape
    width = w.shape[1]
    steps = 2
    return pl.pallas_call(
        pair_body,
        grid=(steps,),
        in_specs=[VMEM] * 3,
        out_specs=pl.BlockSpec((groups * pairs // steps, width), lambda g: (g, 0)),
        out_shape=jax.ShapeDtypeStruct((groups * pairs, width), BF16),
        compiler_params=KERNEL,
        cost_estimate=pl.CostEstimate(
            flops=2 * groups * pairs * feats * width,
            bytes_accessed=2 * groups * pairs * width,
            transcendentals=0,
        ),
        name="pair",
    )(outer, w, offset)


class Ring:
    def __init__(self, n_row, n_col):
        self.n_row, self.n_col = n_row, n_col
        self.per_row = n_col // n_row
        self.row = lax.axis_index("row").astype(jnp.uint32)
        self.col = lax.axis_index("col").astype(jnp.uint32)

    def col_shift(self, value, k):
        n = self.n_col
        return lax.ppermute(value, "col", [((t + k) % n, t) for t in range(n)])

    def row_shift(self, value, k):
        n = self.n_row
        return lax.ppermute(value, "row", [((t + k) % n, t) for t in range(n)])

    def right_along_row(self, right):
        others = [self.row_shift(right, k) for k in range(1, self.n_row)]
        return [right] + others

    def right_pieces(self, by_row):
        n, m = self.n_row, self.per_row
        here, lanes = by_row[0].shape
        lanes //= m
        by_row = jnp.stack(by_row)
        pieces = []
        for k in range(self.n_col):
            q = (self.col + (self.n_col - k)) % self.n_col
            at = ((q // m + (n - self.row)) % n, jnp.uint32(0), (q % m) * lanes)
            pieces.append(lax.dynamic_slice(by_row, at, (1, here, lanes))[0])
        return pieces

    def right_along_col(self, pieces):
        return jnp.concatenate([self.col_shift(p, k) if k else p for k, p in enumerate(pieces)])

    def right_grad_home(self, grad):
        n, m = self.n_col, self.per_row
        here, lanes = grad.shape[0] // n, grad.shape[1]
        total = jnp.zeros((m, here, lanes), F32)
        slot = lax.broadcasted_iota(jnp.uint32, (m, 1, 1), 0)
        for k in range(n):
            t = (self.row * m + self.col % m + k) % n
            block = lax.dynamic_slice_in_dim(grad, ((t + n - self.col) % n) * here, here, 0)
            pairs = []
            for r in range(self.n_row):
                for q in range(n):
                    pairs.append((r * n + q, (q // m) * n + (r * m + q % m + k) % n))
            got = lax.ppermute(block, ("row", "col"), pairs).astype(F32)[None]
            total += got if m == 1 else jnp.where(slot == (self.col + (n - k)) % n % m, got, 0)
        return total.swapaxes(0, 1).reshape(here, m * lanes).astype(BF16)

    def weight_over_row(self, weight):
        n = self.n_row
        size = weight.shape[0] // n
        sent = weight.astype(BF16).reshape(n, size, -1)
        total = lax.dynamic_index_in_dim(weight.reshape(n, size, -1), self.row, 0, keepdims=False)
        for k in range(1, n):
            piece = lax.dynamic_index_in_dim(sent, (self.row + k) % n, 0, keepdims=False)
            total += self.row_shift(piece, n - k).astype(F32)
        return total

    def weight_over_col(self, total):
        mine = total.astype(BF16)
        for k in range(1, self.n_col):
            total += self.col_shift(mine, k).astype(F32)
        return total.astype(BF16)

    def weight_to_all(self, mine):
        n = self.n_row
        which = (lax.broadcasted_iota(jnp.uint32, (n, 1, 1), 0) + (n - self.row)) % n
        shares = mine[None]
        for k in range(1, n):
            shares = jnp.where(which == k, self.row_shift(mine, k)[None], shares)
        return shares.reshape(n * mine.shape[0], mine.shape[1])


def after(value, *others):
    return lax.optimization_barrier((value,) + others)[0]


def shards(n_row, n_col, alignment_tensor, gain, shift, first_projector, second_projector,
           final_projector, final_offset, labels, counts, grad):
    ring = Ring(n_row, n_col)
    here, rows, _ = alignment_tensor.shape
    cols, width = grad.shape[1:]
    seqs = here * n_col
    left, right = project_call(
        alignment_tensor, gain[None, :], shift[None, :], first_projector.T, second_projector.T, cols
    )
    by_row = ring.right_along_row(right)
    left = jnp.concatenate([left] + [ring.col_shift(left, k) for k in range(1, n_col)])

    at = jnp.stack([ring.row * rows, ring.col * cols, ring.col * here]).astype(jnp.int32)
    lab, tall, wide, plain, w, back, grad = back_call(
        at, labels, counts, after(final_projector, right), grad, seqs
    )
    mine = ring.right_along_col(ring.right_pieces(by_row))
    back, grad = in_vmem(back), in_vmem(grad)
    right_grad = right_grad_call(at, labels, back, left, lab, plain)

    right = after(mine, right_grad)
    grad_right = ring.right_grad_home(right_grad)
    outer, weight = outer_call(
        at, labels, left, lab, right, wide, grad
    )
    share = ring.weight_over_row(weight)
    left_grad = left_grad_call(at, labels, back, after(lab, weight), right, tall)
    share = after(share, left_grad)

    total = left_grad[:here].astype(F32)
    for k in range(1, n_col):
        total += ring.col_shift(left_grad[k * here : (k + 1) * here], n_col - k).astype(F32)
    adjoint_first = total.astype(BF16)
    pair_update = pair_call(in_vmem(outer), after(w, left_grad, share), final_offset[None, :])
    pair_update = pair_update.reshape(rows, cols, width)
    mine = after(ring.weight_over_col(share), pair_update)
    grad_w_out = ring.weight_to_all(mine).astype(F32) / (n_row * rows)
    return pair_update, adjoint_first, grad_right, grad_w_out


def solution(mesh):
    in_specs = (
        P(("parts", "col"), "row", None),
        P(),
        P(),
        P(),
        P(),
        P(),
        P(),
        P("parts"),
        P("parts", None),
        P(("parts", "row"), "col", None),
    )
    out_specs = (
        P(("parts", "row"), "col", None),
        P(("parts", "col"), "row"),
        P(("parts", "col"), "row"),
        P("parts", None),
    )

    def body(*args):
        return shards(mesh.shape["row"], mesh.shape["col"], *args)

    return jax.shard_map(body, mesh=mesh, in_specs=in_specs, out_specs=out_specs, check_vma=False)
```

```python
import jax
import jax.numpy as jnp
from jax import lax
from jax.experimental import pallas as pl
from jax.experimental.pallas import tpu as pltpu
from jax.sharding import PartitionSpec as P


PROJ = 32
CHAINS = 8
LANES = 128
PER_TILE = LANES // PROJ
WIDE = 256
F32 = jnp.float32
BF16 = jnp.bfloat16
VMEM = pl.BlockSpec(memory_space=pltpu.VMEM)
KERNEL = pltpu.CompilerParams(vmem_limit_bytes=24 << 20)
HBM = pl.BlockSpec(memory_space=pltpu.HBM)
SMEM = pl.BlockSpec(memory_space=pltpu.SMEM)


def swap_blocks(parts):
    lane = lax.broadcasted_iota(jnp.int32, parts[0].shape, 1)
    outs = []
    for q in range(PER_TILE):
        out = parts[(PER_TILE - 1 - q) % PER_TILE]
        for block in range(PER_TILE - 2, -1, -1):
            out = jnp.where(lane < (block + 1) * PROJ, parts[(block - q) % PER_TILE], out)
        outs.append(pltpu.roll(out, LANES - q * PROJ, 1) if q else out)
    return outs


def rolled(value, p):
    if not p:
        return value
    return jnp.concatenate(
        [pltpu.roll(value[:, t : t + LANES], p * PROJ, 1) for t in range(0, value.shape[1], LANES)],
        axis=1,
    )


def nt_dot(a, b):
    return lax.dot_general(a, b, (((1,), (1,)), ((), ())), preferred_element_type=F32)


def nn_dot(a, b):
    return lax.dot_general(a, b, (((1,), (0,)), ((), ())), preferred_element_type=F32)


def in_vmem(value):
    return pltpu.with_memory_space_constraint(value, pltpu.VMEM)


def in_hbm(value):
    return pltpu.with_memory_space_constraint(value, pltpu.HBM)


def project_body(x_hbm, gain_hbm, shift_hbm, first_hbm, second_hbm, left_ref, right_ref,
                 x_ref, gain_ref, shift_ref, w_ref, proj_ref, turn_ref, out_ref, sems, *, cols):
    chunks, chunk, rows, feats = x_ref.shape
    small = [
        pltpu.make_async_copy(gain_hbm, gain_ref, sems.at[chunks]),
        pltpu.make_async_copy(shift_hbm, shift_ref, sems.at[chunks + 1]),
        pltpu.make_async_copy(first_hbm, w_ref.at[pl.ds(0, PROJ)], sems.at[chunks + 2]),
        pltpu.make_async_copy(second_hbm, w_ref.at[pl.ds(PROJ, PROJ)], sems.at[chunks + 3]),
    ]
    big = [
        pltpu.make_async_copy(x_hbm.at[pl.ds(g * chunk, chunk)], x_ref.at[g], sems.at[g])
        for g in range(chunks)
    ]
    for copy in big[:1] + small + big[1:]:
        copy.start()
    w_ref[2 * PROJ :] = jnp.zeros((LANES - 2 * PROJ, feats), BF16)
    for copy in small:
        copy.wait()
    for g in range(chunks):
        big[g].wait()
        x = x_ref[g].astype(F32).reshape(chunk * rows, feats)
        center = x - jnp.mean(x, axis=-1, keepdims=True)
        spread = jnp.mean(center * center, axis=-1, keepdims=True)
        normed = center * lax.rsqrt(spread + 1e-05) * gain_ref[...] + shift_ref[...]
        at = slice(g * chunk * rows, (g + 1) * chunk * rows)
        proj_ref[at] = nt_dot(normed.astype(BF16), w_ref[...])
    project_layout(proj_ref, turn_ref, out_ref, left_ref, right_ref, rows, cols)


def project_layout(proj_ref, turn_ref, out_ref, left_ref, right_ref, rows, cols):
    here = left_ref.shape[0]
    lane = lax.broadcasted_iota(jnp.int32, (here, LANES), 1)
    for t in range(rows // PER_TILE):
        tile = proj_ref[pl.ds(t * PER_TILE, here, stride=rows)]
        for p in range(1, PER_TILE):
            part = proj_ref[pl.ds(t * PER_TILE + p, here, stride=rows)]
            tile = jnp.where(lane < p * PROJ, tile, pltpu.roll(part, p * PROJ, 1))
        left_ref[:, t * LANES : (t + 1) * LANES] = tile.astype(BF16)

    tiles = here * rows // LANES
    for t in range(tiles):
        flipped = proj_ref[t * LANES : (t + 1) * LANES].T
        turn_ref[t * PROJ : (t + 1) * PROJ] = flipped[PROJ : 2 * PROJ]
    seqs = LANES // rows
    per = LANES // cols
    lane = lax.broadcasted_iota(jnp.int32, (tiles, LANES), 1)
    for block in range(rows // cols):
        for t in range(PROJ // per):
            at = (block * (PROJ // per) + t) * LANES
            parts = [turn_ref[pl.ds(t * per + p, tiles, stride=PROJ)] for p in range(per)]
            for u in range(seqs):
                start = u * rows + block * cols
                tile = None
                for p, part in enumerate(parts):
                    amount = (p * cols - start) % LANES
                    part = pltpu.roll(part, amount, 1) if amount else part
                    tile = part if tile is None else jnp.where(lane < p * cols, tile, part)
                out_ref[pl.ds(u, tiles, stride=seqs), :] = tile
            right_ref[:, at : at + LANES] = out_ref[...].astype(BF16)


def project_call(x, gain, shift, first, second, cols):
    here, rows, feats = x.shape
    chunk = min(here, max(1, 2 * WIDE // rows))
    return pl.pallas_call(
        lambda *refs: project_body(*refs, cols=cols),
        in_specs=[HBM] * 5,
        out_specs=[VMEM] * 2,
        out_shape=[jax.ShapeDtypeStruct((here, rows * PROJ), BF16)] * 2,
        scratch_shapes=[
            pltpu.VMEM((here // chunk, chunk, rows, feats), BF16),
            pltpu.VMEM(gain.shape, F32),
            pltpu.VMEM(shift.shape, F32),
            pltpu.VMEM((LANES, feats), BF16),
            pltpu.VMEM((here * rows, LANES), F32),
            pltpu.VMEM((here * rows // LANES * PROJ, LANES), F32),
            pltpu.VMEM((here, LANES), F32),
            pltpu.SemaphoreType.DMA((here // chunk + 4,)),
        ],
        compiler_params=KERNEL,
        name="project",
    )(*map(in_hbm, (x, gain, shift, first, second)))


def masks(at_ref, labels_ref, counts_ref, lab_ref, tall_ref, wide_ref, plain_ref, rows, cols, seqs,
          n_row, n_col):
    res = labels_ref.shape[1]
    labels = jnp.broadcast_to(labels_ref[...], (8, res))
    own = pltpu.roll(labels, (res - at_ref[0]) % res, 1)[:, :rows]
    spread = (
        lax.broadcasted_iota(jnp.int32, (rows, rows * PROJ), 1) // PROJ
        == lax.broadcasted_iota(jnp.int32, (rows, rows * PROJ), 0)
    )
    lab = nn_dot(own.astype(F32).astype(BF16), spread.astype(F32).astype(BF16))
    lab_ref[...] = lab[:1].astype(jnp.int32)

    there = pltpu.roll(labels, (res - at_ref[1]) % res, 1)[:, :LANES]
    there = jnp.where(lax.broadcasted_iota(jnp.int32, (8, LANES), 1) < cols, there, 0)
    reach = cols
    while reach < LANES:
        there = there + pltpu.roll(there, reach, 1)
        reach *= 2
    depth = jnp.zeros((CHAINS, LANES), jnp.int32)
    for b in range(CHAINS):
        depth += jnp.where(there == b, counts_ref[:, b : b + 1], 0)
    here, m = seqs // n_col, n_col // n_row
    within = lax.broadcasted_iota(jnp.int32, (here, LANES), 0)
    blocks = []
    for k in range(n_row):
        for u in range(m):
            t = (at_ref[2] ^ k) * m + (lax.rem(at_ref[3] + (m - u), m) if m > 1 else 0)
            blocks.append(within + t * here)
    seq = jnp.concatenate(blocks, axis=0)
    for a in range(CHAINS):
        deep = jnp.broadcast_to(depth[a : a + 1], (seqs, LANES))
        weight = jnp.where(seq < deep, 1.0 / deep.astype(F32), 0.0)
        three = deep % 3 == 0
        for x, part in enumerate((jnp.where(three, 0.0, weight), jnp.where(three, 3.0 * weight, 0.0))):
            tall_ref[a, x] = part.astype(BF16)
            wide_ref[a, x] = part.T[:cols].astype(BF16)
        plain_ref[a] = weight.T[:cols]


def projector(w_ref, wide_w_ref, w_out, wt_ref):
    wide_w_ref[...] = w_ref[...].astype(F32)
    for t in range(PROJ // PER_TILE):
        for q in range(PER_TILE):
            e = t * PER_TILE + q
            w_out[e * PROJ : (e + 1) * PROJ] = wide_w_ref[pl.ds(e, PROJ, stride=PROJ)].astype(BF16)
        block = w_out[t * LANES : (t + 1) * LANES].astype(F32)
        for p in range(PER_TILE):
            wt_ref[p, :, t * LANES : (t + 1) * LANES] = rolled(block.T, p).astype(BF16)


def cost(passes, span, total, seqs):
    return pl.CostEstimate(
        flops=4 * passes * span * total * seqs, bytes_accessed=2 * span * total, transcendentals=0
    )


def back_body(at_ref, labels_hbm, counts_hbm, w_hbm, grad_hbm,
              lab_ref, tall_ref, wide_ref, plain_ref, w_out, back_ref, grad_ref,
              labels_ref, counts_ref, w_ref, wide_w_ref, wt_ref, sems, *, seqs, n_row, n_col):
    groups, step, cols, _ = grad_ref.shape
    copies = [
        pltpu.make_async_copy(w_hbm, w_ref, sems.at[groups]),
        pltpu.make_async_copy(labels_hbm, labels_ref, sems.at[groups + 1]),
        pltpu.make_async_copy(counts_hbm, counts_ref, sems.at[groups + 2]),
    ]
    for copy in copies:
        copy.start()

    def grad_of(g):
        return pltpu.make_async_copy(grad_hbm.at[pl.ds(g * step, step)], grad_ref.at[g], sems.at[g])

    for g in range(groups):
        grad_of(g).start()
    for copy in copies:
        copy.wait()
    projector(w_ref, wide_w_ref, w_out, wt_ref)
    masks(at_ref, labels_ref, counts_ref, lab_ref, tall_ref, wide_ref, plain_ref,
          groups * step, cols, seqs, n_row, n_col)
    halves = step // PER_TILE

    def group(g, carry):
        grad_of(g).wait()
        blocks = [
            jnp.concatenate([grad_ref[g, half * PER_TILE + p] for half in range(halves)], axis=0)
            for p in range(PER_TILE)
        ]
        for u in range(PROJ * PROJ // WIDE):
            prods = [
                nn_dot(block, wt_ref[p, :, u * WIDE : (u + 1) * WIDE]).astype(BF16)
                for p, block in enumerate(blocks)
            ]
            for half in range(halves):
                for t in range(WIDE // LANES):
                    parts = [
                        prod[half * cols : (half + 1) * cols, t * LANES : (t + 1) * LANES]
                        for prod in prods
                    ]
                    for q, part in enumerate(swap_blocks(parts)):
                        e = u * (WIDE // PROJ) + t * PER_TILE + q
                        at = (g, slice(e * cols, (e + 1) * cols))
                        back_ref[at + (slice(half * LANES, (half + 1) * LANES),)] = part
        return carry

    lax.fori_loop(0, groups, group, 0)


def back_call(at, labels, counts, w, grad, seqs, n_row, n_col):
    rows, cols, width = grad.shape
    step = WIDE // PROJ
    groups = rows // step
    labels = labels[None, :]
    return pl.pallas_call(
        lambda *refs: back_body(*refs, seqs=seqs, n_row=n_row, n_col=n_col),
        in_specs=[SMEM] + [HBM] * 4,
        out_specs=[VMEM] * 7,
        out_shape=[
            jax.ShapeDtypeStruct((1, rows * PROJ), jnp.int32),
            jax.ShapeDtypeStruct((CHAINS, 2, seqs, LANES), BF16),
            jax.ShapeDtypeStruct((CHAINS, 2, cols, seqs), BF16),
            jax.ShapeDtypeStruct((CHAINS, cols, seqs), F32),
            jax.ShapeDtypeStruct(w.shape, BF16),
            pltpu.VMEM((groups, PROJ * cols, WIDE), BF16),
            pltpu.VMEM((groups, step, cols, width), BF16),
        ],
        scratch_shapes=[
            pltpu.VMEM(labels.shape, jnp.int32),
            pltpu.VMEM(counts.shape, jnp.int32),
            pltpu.VMEM(w.shape, BF16),
            pltpu.VMEM(w.shape, F32),
            pltpu.VMEM((PER_TILE, width, PROJ * PROJ), BF16),
            pltpu.SemaphoreType.DMA((groups + 3,)),
        ],
        compiler_params=KERNEL,
        cost_estimate=cost(10, PROJ * cols, rows * PROJ, width),
        name="back",
    )(at, *map(in_hbm, (labels, counts, w, grad)))


def first_chain(at_ref, labels_ref, group):
    return labels_ref[at_ref[0] + group * (WIDE // PROJ)]


def last_chain(at_ref, labels_ref, group):
    return labels_ref[at_ref[0] + (group + 1) * (WIDE // PROJ) - 1]


def slots(chain, count, seqs):
    return pl.ds(pl.multiple_of(chain * seqs, seqs), count * seqs)


def each(first, last, fn):
    def step(k, carry):
        fn(k)
        return carry

    lax.fori_loop(first, last + 1, step, 0)


def lanes_of(group):
    return pl.ds(pl.multiple_of(group * WIDE, WIDE), WIDE)


def masked_left(left_ref, lab_ref, lb_ref, chain, group):
    seqs = left_ref.shape[0]
    lanes = lanes_of(group)
    for side in range(2):
        keep = (lab_ref[:, lanes] == chain + side).astype(F32).astype(BF16)
        lb_ref[side * seqs : (side + 1) * seqs] = left_ref[:, lanes] * keep


def right_grad_body(at_ref, labels_ref, back_ref, left_ref, lab_ref, wide_ref,
                    right_out, q_ref, lb_ref, flip_ref, turn_ref):
    seqs = left_ref.shape[0]
    groups, span, _ = back_ref.shape
    cols = span // PROJ
    first = lambda g: first_chain(at_ref, labels_ref, g)
    last = lambda g: last_chain(at_ref, labels_ref, g)

    def clear(chain):
        q_ref[:, slots(chain, 1, seqs)] = jnp.zeros((span, seqs), F32)

    each(first(0), last(groups - 1) + 1, clear)

    def group(g):
        def two_chains(k):
            chain = first(g) + 2 * k
            masked_left(left_ref, lab_ref, lb_ref, chain, g)
            q_ref[:, slots(chain, 2, seqs)] += nt_dot(back_ref[g], lb_ref[...])

        each(0, (last(g) - first(g)) // 2, two_chains)

    each(0, groups - 1, group)

    def combine(chain, start):
        for e in range(PROJ):
            rows = slice(e * cols, (e + 1) * cols)
            part = q_ref[rows, slots(chain, 1, seqs)] * wide_ref[chain]
            flip_ref[rows] = part if start else flip_ref[rows] + part

    combine(first(0), True)
    each(first(0) + 1, last(groups - 1), lambda chain: combine(chain, False))
    for j in range(cols):
        turn_ref[j * PROJ : (j + 1) * PROJ] = flip_ref[pl.ds(j, PROJ, stride=cols)]
    for t in range(span // LANES):
        rows = slice(t * LANES, (t + 1) * LANES)
        right_out[:, rows] = turn_ref[rows].T.astype(BF16)


def right_grad_call(at, labels, back, left, lab, wide):
    groups, span, _ = back.shape
    total = groups * WIDE
    seqs = left.shape[0]
    return pl.pallas_call(
        right_grad_body,
        in_specs=[SMEM] * 2 + [VMEM] * 4,
        out_specs=VMEM,
        out_shape=jax.ShapeDtypeStruct((seqs, span), BF16),
        scratch_shapes=[
            pltpu.VMEM((span, (CHAINS + 1) * seqs), F32),
            pltpu.VMEM((2 * seqs, WIDE), BF16),
            pltpu.VMEM((span, seqs), F32),
            pltpu.VMEM((span, seqs), F32),
        ],
        compiler_params=KERNEL,
        cost_estimate=cost(10, span, total, seqs),
        name="right_grad",
    )(at, labels, back, left, lab, wide)


def left_grad_body(at_ref, labels_ref, back_ref, lab_ref, right_ref, tall_ref,
                   left_out, rm_ref, part_ref):
    seqs = right_ref.shape[0]
    groups, span, _ = back_ref.shape
    first = lambda g: first_chain(at_ref, labels_ref, g)
    last = lambda g: last_chain(at_ref, labels_ref, g)
    part_ref[...] = (right_ref[...].astype(F32) / 3).astype(BF16)

    def build(chain):
        plain, third = tall_ref[chain, 0], tall_ref[chain, 1]
        for t in range(span // LANES):
            lanes = slice(t * LANES, (t + 1) * LANES)
            rm_ref[slots(chain, 1, seqs), lanes] = (
                right_ref[:, lanes] * plain + part_ref[:, lanes] * third
            )

    each(first(0), last(groups - 1), build)
    rm_ref[slots(last(groups - 1) + 1, 1, seqs)] = jnp.zeros((seqs, span), BF16)

    def group(g):
        lab = lab_ref[:, lanes_of(g)]

        def two_chains(k, total):
            chain = first(g) + 2 * k
            part = nn_dot(rm_ref[slots(chain, 2, seqs)], back_ref[g])
            keep0, keep1 = lab == chain, lab == chain + 1
            return total + jnp.where(keep0, part[:seqs], 0.0) + jnp.where(keep1, part[seqs:], 0.0)

        passes = (last(g) - first(g)) // 2 + 1
        total = lax.fori_loop(0, passes, two_chains, jnp.zeros((seqs, WIDE), F32))
        left_out[:, lanes_of(g)] = total.astype(BF16)

    each(0, groups - 1, group)


def left_grad_call(at, labels, back, lab, right, tall):
    groups, span, _ = back.shape
    total = groups * WIDE
    seqs = right.shape[0]
    return pl.pallas_call(
        left_grad_body,
        in_specs=[SMEM] * 2 + [VMEM] * 4,
        out_specs=VMEM,
        out_shape=jax.ShapeDtypeStruct((seqs, total), BF16),
        scratch_shapes=[
            pltpu.VMEM(((CHAINS + 1) * seqs, span), BF16),
            pltpu.VMEM((seqs, span), BF16),
        ],
        compiler_params=KERNEL,
        cost_estimate=cost(10, span, total, seqs),
        name="left_grad",
    )(at, labels, back, lab, right, tall)


def outer_body(at_ref, labels_ref, left_ref, lab_ref, right_ref, wide_ref, grad_ref,
               outer_ref, weight_out, rm_ref, lb_ref, acc_ref, sum_ref, turn_ref, flip_ref, part_ref):
    seqs = left_ref.shape[0]
    span = right_ref.shape[1]
    cols = span // PROJ
    groups, step, _, width = grad_ref.shape
    first = lambda g: first_chain(at_ref, labels_ref, g)
    last = lambda g: last_chain(at_ref, labels_ref, g)
    for t in range(span // LANES):
        lanes = slice(t * LANES, (t + 1) * LANES)
        flipped = right_ref[:, lanes].astype(F32).T
        flip_ref[lanes] = flipped.astype(BF16)
        part_ref[lanes] = (flipped / 3).astype(BF16)

    def build(chain):
        plain, third = wide_ref[chain, 0], wide_ref[chain, 1]
        for e in range(PROJ):
            rows = slice(e * cols, (e + 1) * cols)
            to = e % PER_TILE * (PROJ // PER_TILE) + e // PER_TILE
            rm_ref[to * cols : (to + 1) * cols, slots(chain, 1, seqs)] = (
                flip_ref[rows] * plain + part_ref[rows] * third
            )

    each(first(0), last(groups - 1), build)
    rm_ref[:, slots(last(groups - 1) + 1, 1, seqs)] = jnp.zeros((span, seqs), BF16)
    sum_ref[...] = jnp.zeros_like(sum_ref)
    quarter = span // PER_TILE

    def product(chain, g, add):
        masked_left(left_ref, lab_ref, lb_ref, chain, g)
        for q in range(PER_TILE):
            rows = slice(q * quarter, (q + 1) * quarter)
            part = nn_dot(rm_ref[rows, slots(chain, 2, seqs)], rolled(lb_ref[...], q))
            acc_ref[rows] = acc_ref[rows] + part if add else part

    def group(g):
        product(first(g), g, False)
        each(1, (last(g) - first(g)) // 2, lambda k: product(first(g) + 2 * k, g, True))
        for half in range(WIDE // LANES):
            lanes = slice(half * LANES, (half + 1) * LANES)
            for t in range(PROJ // PER_TILE):
                parts = []
                for q in range(PER_TILE):
                    e = q * (PROJ // PER_TILE) + t
                    parts.append(acc_ref[e * cols : (e + 1) * cols, lanes].astype(BF16))
                turned = swap_blocks(parts)
                for p in range(PER_TILE):
                    i = half * PER_TILE + p
                    at = (g, slice(i * cols, (i + 1) * cols), slice(t * LANES, (t + 1) * LANES))
                    outer_ref[at] = turned[p]
        flat = grad_ref[g].reshape(step * cols, width)
        sum_ref[...] += nn_dot(flat.T, outer_ref[g])

    each(0, groups - 1, group)
    for t in range(PROJ * PROJ // LANES):
        part = slice(t * LANES, (t + 1) * LANES)
        turn_ref[part] = sum_ref[:, part].T
    for c in range(PROJ):
        weight_out[c * PROJ : (c + 1) * PROJ] = turn_ref[pl.ds(c, PROJ, stride=PROJ)]


def outer_call(at, labels, left, lab, right, wide, grad):
    groups, step, cols, width = grad.shape
    seqs, total = left.shape
    span = right.shape[1]
    return pl.pallas_call(
        outer_body,
        in_specs=[SMEM] * 2 + [VMEM] * 5,
        out_specs=[VMEM] * 2,
        out_shape=[
            pltpu.VMEM((groups, step * cols, PROJ * PROJ), BF16),
            jax.ShapeDtypeStruct((PROJ * PROJ, width), F32),
        ],
        scratch_shapes=[
            pltpu.VMEM((span, (CHAINS + 1) * seqs), BF16),
            pltpu.VMEM((2 * seqs, WIDE), BF16),
            pltpu.VMEM((span, WIDE), F32),
            pltpu.VMEM((width, PROJ * PROJ), F32),
            pltpu.VMEM((PROJ * PROJ, width), F32),
            pltpu.VMEM((span, seqs), BF16),
            pltpu.VMEM((span, seqs), BF16),
        ],
        compiler_params=KERNEL,
        cost_estimate=cost(20, span, total, seqs),
        name="outer",
    )(at, labels, left, lab, right, wide, grad)


def pair_body(outer_ref, w_ref, offset_ref, pair_ref):
    _, pairs, _ = outer_ref.shape
    here = pair_ref.shape[0] // pairs
    for g in range(here):
        pair = nn_dot(outer_ref[pl.program_id(0) * here + g], w_ref[...]) + offset_ref[...]
        pair_ref[g * pairs : (g + 1) * pairs] = pair.astype(BF16)


def pair_call(outer, w, offset):
    groups, pairs, feats = outer.shape
    width = w.shape[1]
    steps = 2
    return pl.pallas_call(
        pair_body,
        grid=(steps,),
        in_specs=[VMEM] * 3,
        out_specs=pl.BlockSpec((groups * pairs // steps, width), lambda g: (g, 0)),
        out_shape=jax.ShapeDtypeStruct((groups * pairs, width), BF16),
        compiler_params=KERNEL,
        cost_estimate=pl.CostEstimate(
            flops=2 * groups * pairs * feats * width,
            bytes_accessed=2 * groups * pairs * width,
            transcendentals=0,
        ),
        name="pair",
    )(outer, w, offset)


class Pairs:
    def __init__(self, n_row, n_col):
        self.n_row, self.n_col = n_row, n_col
        self.per_row = n_col // n_row
        self.row = lax.axis_index("row").astype(jnp.uint32)
        self.col = lax.axis_index("col").astype(jnp.uint32)

    def col_swap(self, value, k):
        return lax.ppermute(value, "col", [(t ^ k, t) for t in range(self.n_col)])

    def row_swap(self, value, k):
        return lax.ppermute(value, "row", [(t ^ k, t) for t in range(self.n_row)])

    def place_of(self, t):
        m = self.per_row
        return ((t // m) ^ self.row) * m + (self.col + (m - t % m)) % m

    def home_pairs(self, u):
        n, m = self.n_col, self.per_row
        return [
            (a * n + t, (t // m) * n + a * m + (t + u) % m) for a in range(self.n_row) for t in range(n)
        ]

    def right_to_col(self, right):
        m = self.per_row
        lanes = right.shape[1] // m
        pieces = []
        for u in range(m):
            at = (self.col + u) % m * lanes
            block = lax.dynamic_slice_in_dim(right, at, lanes, 1) if m > 1 else right
            pieces.append(lax.ppermute(block, ("row", "col"), self.home_pairs(u)))
        return jnp.concatenate(pieces)

    def right_along_row(self, mine):
        swaps = [self.row_swap(mine, k) for k in range(1, self.n_row)]
        return jnp.concatenate([mine] + swaps)

    def right_grad_along_row(self, grad):
        size = grad.shape[0] // self.n_row
        total = grad[:size].astype(F32)
        for k in range(1, self.n_row):
            total += self.row_swap(grad[k * size : (k + 1) * size], k).astype(F32)
        return total.astype(BF16)

    def right_grad_home(self, mine):
        m = self.per_row
        here, lanes = mine.shape[0] // m, mine.shape[1]
        slot = lax.broadcasted_iota(jnp.uint32, (m, 1, 1), 0)
        home = jnp.zeros((m, here, lanes), BF16)
        for u in range(m):
            pairs = [(there, origin) for origin, there in self.home_pairs(u)]
            got = lax.ppermute(mine[u * here : (u + 1) * here], ("row", "col"), pairs)[None]
            home = got if m == 1 else jnp.where(slot == (self.col + u) % m, got, home)
        return home.swapaxes(0, 1).reshape(here, m * lanes)

    def left_along_col(self, left):
        here = left.shape[0]
        out = jnp.zeros((self.n_col * here, left.shape[1]), left.dtype)
        for k in range(self.n_col):
            block = self.col_swap(left, k) if k else left
            out = lax.dynamic_update_slice_in_dim(out, block, self.place_of(self.col ^ k) * here, 0)
        return out

    def left_grad_along_col(self, grad):
        here = grad.shape[0] // self.n_col
        blocks = [
            lax.dynamic_slice_in_dim(grad, self.place_of(self.col ^ k) * here, here, 0)
            for k in range(self.n_col)
        ]
        total = blocks[0].astype(F32)
        for k in range(1, self.n_col):
            total += self.col_swap(blocks[k], k).astype(F32)
        return total.astype(BF16)

    def weight_over_row(self, weight):
        n = self.n_row
        size = weight.shape[0] // n
        sent = weight.astype(BF16).reshape(n, size, -1)
        total = lax.dynamic_index_in_dim(weight.reshape(n, size, -1), self.row, 0, keepdims=False)
        for k in range(1, n):
            piece = lax.dynamic_index_in_dim(sent, self.row ^ k, 0, keepdims=False)
            total += self.row_swap(piece, k).astype(F32)
        return total

    def weight_over_col(self, total):
        mine = total.astype(BF16)
        for k in range(1, self.n_col):
            total += self.col_swap(mine, k).astype(F32)
        return total.astype(BF16)

    def weight_to_all(self, mine):
        n = self.n_row
        which = lax.broadcasted_iota(jnp.uint32, (n, 1, 1), 0) ^ self.row
        shares = mine[None]
        for k in range(1, n):
            shares = jnp.where(which == k, self.row_swap(mine, k)[None], shares)
        return shares.reshape(n * mine.shape[0], mine.shape[1])


def after(value, *others):
    return lax.optimization_barrier((value,) + others)[0]


def shards(n_row, n_col, alignment_tensor, gain, shift, first_projector, second_projector,
           final_projector, final_offset, labels, counts, grad):
    ring = Pairs(n_row, n_col)
    here, rows, _ = alignment_tensor.shape
    cols, width = grad.shape[1:]
    seqs = here * n_col
    left, right = project_call(
        alignment_tensor, gain[None, :], shift[None, :], first_projector.T, second_projector.T, cols
    )
    mine = ring.right_to_col(right)
    left = ring.left_along_col(left)

    at = jnp.stack([ring.row * rows, ring.col * cols, ring.row, ring.col]).astype(jnp.int32)
    lab, tall, wide, plain, w, back, grad = back_call(
        at, labels, counts, after(final_projector, right), grad, seqs, n_row, n_col
    )
    right = ring.right_along_row(mine)
    back, grad = in_vmem(back), in_vmem(grad)
    right_grad = right_grad_call(at, labels, back, left, lab, plain)

    right = after(right, right_grad)
    mine = ring.right_grad_along_row(right_grad)
    outer, weight = outer_call(
        at, labels, left, lab, right, wide, grad
    )
    share = ring.weight_over_row(weight)
    left_grad = left_grad_call(at, labels, back, after(lab, weight), right, tall)
    share = after(share, left_grad)

    grad_right = ring.right_grad_home(after(mine, weight))
    adjoint_first = ring.left_grad_along_col(left_grad)
    pair_update = pair_call(in_vmem(outer), after(w, left_grad, share), final_offset[None, :])
    pair_update = pair_update.reshape(rows, cols, width)
    mine = after(ring.weight_over_col(share), pair_update)
    grad_w_out = ring.weight_to_all(mine).astype(F32) / (n_row * rows)
    return pair_update, adjoint_first, grad_right, grad_w_out


def solution(mesh):
    in_specs = (
        P(("parts", "col"), "row", None),
        P(),
        P(),
        P(),
        P(),
        P(),
        P(),
        P("parts"),
        P("parts", None),
        P(("parts", "row"), "col", None),
    )
    out_specs = (
        P(("parts", "row"), "col", None),
        P(("parts", "col"), "row"),
        P(("parts", "col"), "row"),
        P("parts", None),
    )

    def body(*args):
        return shards(mesh.shape["row"], mesh.shape["col"], *args)

    return jax.shard_map(body, mesh=mesh, in_specs=in_specs, out_specs=out_specs, check_vma=False)
```

```python
import jax
import jax.numpy as jnp
from jax import lax
from jax.experimental import pallas as pl
from jax.experimental.pallas import tpu as pltpu
from jax.sharding import PartitionSpec as P


PROJ = 32
CHAINS = 8
LANES = 128
PER_TILE = LANES // PROJ
WIDE = 256
F32 = jnp.float32
BF16 = jnp.bfloat16
VMEM = pl.BlockSpec(memory_space=pltpu.VMEM)
KERNEL = pltpu.CompilerParams(vmem_limit_bytes=24 << 20)
HBM = pl.BlockSpec(memory_space=pltpu.HBM)
SMEM = pl.BlockSpec(memory_space=pltpu.SMEM)


def swap_blocks(parts):
    lane = lax.broadcasted_iota(jnp.int32, parts[0].shape, 1)
    outs = []
    for q in range(PER_TILE):
        out = parts[(PER_TILE - 1 - q) % PER_TILE]
        for block in range(PER_TILE - 2, -1, -1):
            out = jnp.where(lane < (block + 1) * PROJ, parts[(block - q) % PER_TILE], out)
        outs.append(pltpu.roll(out, LANES - q * PROJ, 1) if q else out)
    return outs


def rolled(value, p):
    if not p:
        return value
    return jnp.concatenate(
        [pltpu.roll(value[:, t : t + LANES], p * PROJ, 1) for t in range(0, value.shape[1], LANES)],
        axis=1,
    )


def nt_dot(a, b):
    return lax.dot_general(a, b, (((1,), (1,)), ((), ())), preferred_element_type=F32)


def nn_dot(a, b):
    return lax.dot_general(a, b, (((1,), (0,)), ((), ())), preferred_element_type=F32)


def in_vmem(value):
    return pltpu.with_memory_space_constraint(value, pltpu.VMEM)


def in_hbm(value):
    return pltpu.with_memory_space_constraint(value, pltpu.HBM)


def project_body(x_hbm, gain_hbm, shift_hbm, first_hbm, second_hbm, left_ref, right_ref,
                 x_ref, gain_ref, shift_ref, w_ref, proj_ref, turn_ref, out_ref, sems, *, cols):
    chunks, chunk, rows, feats = x_ref.shape
    small = [
        pltpu.make_async_copy(gain_hbm, gain_ref, sems.at[chunks]),
        pltpu.make_async_copy(shift_hbm, shift_ref, sems.at[chunks + 1]),
        pltpu.make_async_copy(first_hbm, w_ref.at[pl.ds(0, PROJ)], sems.at[chunks + 2]),
        pltpu.make_async_copy(second_hbm, w_ref.at[pl.ds(PROJ, PROJ)], sems.at[chunks + 3]),
    ]
    big = [
        pltpu.make_async_copy(x_hbm.at[pl.ds(g * chunk, chunk)], x_ref.at[g], sems.at[g])
        for g in range(chunks)
    ]
    for copy in big[:1] + small + big[1:]:
        copy.start()
    w_ref[2 * PROJ :] = jnp.zeros((LANES - 2 * PROJ, feats), BF16)
    for copy in small:
        copy.wait()
    for g in range(chunks):
        big[g].wait()
        x = x_ref[g].astype(F32).reshape(chunk * rows, feats)
        center = x - jnp.mean(x, axis=-1, keepdims=True)
        spread = jnp.mean(center * center, axis=-1, keepdims=True)
        normed = center * lax.rsqrt(spread + 1e-05) * gain_ref[...] + shift_ref[...]
        at = slice(g * chunk * rows, (g + 1) * chunk * rows)
        proj_ref[at] = nt_dot(normed.astype(BF16), w_ref[...])
    project_layout(proj_ref, turn_ref, out_ref, left_ref, right_ref, rows, cols)


def project_layout(proj_ref, turn_ref, out_ref, left_ref, right_ref, rows, cols):
    here = left_ref.shape[0]
    lane = lax.broadcasted_iota(jnp.int32, (here, LANES), 1)
    for t in range(rows // PER_TILE):
        tile = proj_ref[pl.ds(t * PER_TILE, here, stride=rows)]
        for p in range(1, PER_TILE):
            part = proj_ref[pl.ds(t * PER_TILE + p, here, stride=rows)]
            tile = jnp.where(lane < p * PROJ, tile, pltpu.roll(part, p * PROJ, 1))
        left_ref[:, t * LANES : (t + 1) * LANES] = tile.astype(BF16)

    tiles = here * rows // LANES
    for t in range(tiles):
        flipped = proj_ref[t * LANES : (t + 1) * LANES].T
        turn_ref[t * PROJ : (t + 1) * PROJ] = flipped[PROJ : 2 * PROJ]
    seqs = LANES // rows
    per = LANES // cols
    lane = lax.broadcasted_iota(jnp.int32, (tiles, LANES), 1)
    for block in range(rows // cols):
        for t in range(PROJ // per):
            at = (block * (PROJ // per) + t) * LANES
            parts = [turn_ref[pl.ds(t * per + p, tiles, stride=PROJ)] for p in range(per)]
            for u in range(seqs):
                start = u * rows + block * cols
                tile = None
                for p, part in enumerate(parts):
                    amount = (p * cols - start) % LANES
                    part = pltpu.roll(part, amount, 1) if amount else part
                    tile = part if tile is None else jnp.where(lane < p * cols, tile, part)
                out_ref[pl.ds(u, tiles, stride=seqs), :] = tile
            right_ref[:, at : at + LANES] = out_ref[...].astype(BF16)


def project_call(x, gain, shift, first, second, cols):
    here, rows, feats = x.shape
    chunk = min(here, max(1, 2 * WIDE // rows))
    return pl.pallas_call(
        lambda *refs: project_body(*refs, cols=cols),
        in_specs=[HBM] * 5,
        out_specs=[VMEM] * 2,
        out_shape=[jax.ShapeDtypeStruct((here, rows * PROJ), BF16)] * 2,
        scratch_shapes=[
            pltpu.VMEM((here // chunk, chunk, rows, feats), BF16),
            pltpu.VMEM(gain.shape, F32),
            pltpu.VMEM(shift.shape, F32),
            pltpu.VMEM((LANES, feats), BF16),
            pltpu.VMEM((here * rows, LANES), F32),
            pltpu.VMEM((here * rows // LANES * PROJ, LANES), F32),
            pltpu.VMEM((here, LANES), F32),
            pltpu.SemaphoreType.DMA((here // chunk + 4,)),
        ],
        compiler_params=KERNEL,
        name="project",
    )(*map(in_hbm, (x, gain, shift, first, second)))


def masks(at_ref, labels_ref, counts_ref, lab_ref, tall_ref, wide_ref, plain_ref, rows, cols, seqs,
          n_row, n_col):
    res = labels_ref.shape[1]
    labels = jnp.broadcast_to(labels_ref[...], (8, res))
    own = pltpu.roll(labels, (res - at_ref[0]) % res, 1)[:, :rows]
    spread = (
        lax.broadcasted_iota(jnp.int32, (rows, rows * PROJ), 1) // PROJ
        == lax.broadcasted_iota(jnp.int32, (rows, rows * PROJ), 0)
    )
    lab = nn_dot(own.astype(F32).astype(BF16), spread.astype(F32).astype(BF16))
    lab_ref[...] = lab[:1].astype(jnp.int32)

    there = pltpu.roll(labels, (res - at_ref[1]) % res, 1)[:, :LANES]
    there = jnp.where(lax.broadcasted_iota(jnp.int32, (8, LANES), 1) < cols, there, 0)
    reach = cols
    while reach < LANES:
        there = there + pltpu.roll(there, reach, 1)
        reach *= 2
    depth = jnp.zeros((CHAINS, LANES), jnp.int32)
    for b in range(CHAINS):
        depth += jnp.where(there == b, counts_ref[:, b : b + 1], 0)
    here, m = seqs // n_col, n_col // n_row
    within = lax.broadcasted_iota(jnp.int32, (here, LANES), 0)
    blocks = []
    for k in range(n_row):
        for u in range(m):
            t = (at_ref[2] ^ k) * m + (lax.rem(at_ref[3] + (m - u), m) if m > 1 else 0)
            blocks.append(within + t * here)
    seq = jnp.concatenate(blocks, axis=0)
    for a in range(CHAINS):
        deep = jnp.broadcast_to(depth[a : a + 1], (seqs, LANES))
        weight = jnp.where(seq < deep, 1.0 / deep.astype(F32), 0.0)
        three = deep % 3 == 0
        for x, part in enumerate((jnp.where(three, 0.0, weight), jnp.where(three, 3.0 * weight, 0.0))):
            tall_ref[a, x] = part.astype(BF16)
            wide_ref[a, x] = part.T[:cols].astype(BF16)
        plain_ref[a] = weight.T[:cols]


def projector(w_ref, wide_w_ref, w_out, wt_ref):
    wide_w_ref[...] = w_ref[...].astype(F32)
    for t in range(PROJ // PER_TILE):
        for q in range(PER_TILE):
            e = t * PER_TILE + q
            w_out[e * PROJ : (e + 1) * PROJ] = wide_w_ref[pl.ds(e, PROJ, stride=PROJ)].astype(BF16)
        block = w_out[t * LANES : (t + 1) * LANES].astype(F32)
        for p in range(PER_TILE):
            wt_ref[p, :, t * LANES : (t + 1) * LANES] = rolled(block.T, p).astype(BF16)


def cost(passes, span, total, seqs):
    return pl.CostEstimate(
        flops=4 * passes * span * total * seqs, bytes_accessed=2 * span * total, transcendentals=0
    )


def back_body(at_ref, labels_hbm, counts_hbm, w_hbm, grad_hbm,
              lab_ref, tall_ref, wide_ref, plain_ref, w_out, back_ref, grad_ref,
              labels_ref, counts_ref, w_ref, wide_w_ref, wt_ref, sems, *, seqs, n_row, n_col):
    groups, step, cols, _ = grad_ref.shape
    copies = [
        pltpu.make_async_copy(w_hbm, w_ref, sems.at[groups]),
        pltpu.make_async_copy(labels_hbm, labels_ref, sems.at[groups + 1]),
        pltpu.make_async_copy(counts_hbm, counts_ref, sems.at[groups + 2]),
    ]
    for copy in copies:
        copy.start()

    def grad_of(g):
        return pltpu.make_async_copy(grad_hbm.at[pl.ds(g * step, step)], grad_ref.at[g], sems.at[g])

    for g in range(groups):
        grad_of(g).start()
    for copy in copies:
        copy.wait()
    projector(w_ref, wide_w_ref, w_out, wt_ref)
    masks(at_ref, labels_ref, counts_ref, lab_ref, tall_ref, wide_ref, plain_ref,
          groups * step, cols, seqs, n_row, n_col)
    halves = step // PER_TILE

    def group(g, carry):
        grad_of(g).wait()
        blocks = [
            jnp.concatenate([grad_ref[g, half * PER_TILE + p] for half in range(halves)], axis=0)
            for p in range(PER_TILE)
        ]
        for u in range(PROJ * PROJ // WIDE):
            prods = [
                nn_dot(block, wt_ref[p, :, u * WIDE : (u + 1) * WIDE]).astype(BF16)
                for p, block in enumerate(blocks)
            ]
            for half in range(halves):
                for t in range(WIDE // LANES):
                    parts = [
                        prod[half * cols : (half + 1) * cols, t * LANES : (t + 1) * LANES]
                        for prod in prods
                    ]
                    for q, part in enumerate(swap_blocks(parts)):
                        e = u * (WIDE // PROJ) + t * PER_TILE + q
                        at = (g, slice(e * cols, (e + 1) * cols))
                        back_ref[at + (slice(half * LANES, (half + 1) * LANES),)] = part
        return carry

    lax.fori_loop(0, groups, group, 0)


def back_call(at, labels, counts, w, grad, seqs, n_row, n_col):
    rows, cols, width = grad.shape
    step = WIDE // PROJ
    groups = rows // step
    labels = labels[None, :]
    return pl.pallas_call(
        lambda *refs: back_body(*refs, seqs=seqs, n_row=n_row, n_col=n_col),
        in_specs=[SMEM] + [HBM] * 4,
        out_specs=[VMEM] * 7,
        out_shape=[
            jax.ShapeDtypeStruct((1, rows * PROJ), jnp.int32),
            jax.ShapeDtypeStruct((CHAINS, 2, seqs, LANES), BF16),
            jax.ShapeDtypeStruct((CHAINS, 2, cols, seqs), BF16),
            jax.ShapeDtypeStruct((CHAINS, cols, seqs), F32),
            jax.ShapeDtypeStruct(w.shape, BF16),
            pltpu.VMEM((groups, PROJ * cols, WIDE), BF16),
            pltpu.VMEM((groups, step, cols, width), BF16),
        ],
        scratch_shapes=[
            pltpu.VMEM(labels.shape, jnp.int32),
            pltpu.VMEM(counts.shape, jnp.int32),
            pltpu.VMEM(w.shape, BF16),
            pltpu.VMEM(w.shape, F32),
            pltpu.VMEM((PER_TILE, width, PROJ * PROJ), BF16),
            pltpu.SemaphoreType.DMA((groups + 3,)),
        ],
        compiler_params=KERNEL,
        cost_estimate=cost(10, PROJ * cols, rows * PROJ, width),
        name="back",
    )(at, *map(in_hbm, (labels, counts, w, grad)))


def first_chain(at_ref, labels_ref, group):
    return labels_ref[at_ref[0] + group * (WIDE // PROJ)]


def last_chain(at_ref, labels_ref, group):
    return labels_ref[at_ref[0] + (group + 1) * (WIDE // PROJ) - 1]


def slots(chain, count, seqs):
    return pl.ds(pl.multiple_of(chain * seqs, seqs), count * seqs)


def each(first, last, fn):
    def step(k, carry):
        fn(k)
        return carry

    lax.fori_loop(first, last + 1, step, 0)


def lanes_of(group):
    return pl.ds(pl.multiple_of(group * WIDE, WIDE), WIDE)


def masked_left(left_ref, lab_ref, lb_ref, chain, group):
    seqs = left_ref.shape[0]
    lanes = lanes_of(group)
    for side in range(2):
        keep = (lab_ref[:, lanes] == chain + side).astype(F32).astype(BF16)
        lb_ref[side * seqs : (side + 1) * seqs] = left_ref[:, lanes] * keep


def right_grad_body(at_ref, labels_ref, back_ref, left_ref, lab_ref, wide_ref,
                    right_out, q_ref, lb_ref, flip_ref, turn_ref):
    seqs = left_ref.shape[0]
    groups, span, _ = back_ref.shape
    cols = span // PROJ
    first = lambda g: first_chain(at_ref, labels_ref, g)
    last = lambda g: last_chain(at_ref, labels_ref, g)

    def clear(chain):
        q_ref[:, slots(chain, 1, seqs)] = jnp.zeros((span, seqs), F32)

    each(first(0), last(groups - 1) + 1, clear)

    def group(g):
        def two_chains(k):
            chain = first(g) + 2 * k
            masked_left(left_ref, lab_ref, lb_ref, chain, g)
            q_ref[:, slots(chain, 2, seqs)] += nt_dot(back_ref[g], lb_ref[...])

        each(0, (last(g) - first(g)) // 2, two_chains)

    each(0, groups - 1, group)

    def combine(chain, start):
        for e in range(PROJ):
            rows = slice(e * cols, (e + 1) * cols)
            part = q_ref[rows, slots(chain, 1, seqs)] * wide_ref[chain]
            flip_ref[rows] = part if start else flip_ref[rows] + part

    combine(first(0), True)
    each(first(0) + 1, last(groups - 1), lambda chain: combine(chain, False))
    for j in range(cols):
        turn_ref[j * PROJ : (j + 1) * PROJ] = flip_ref[pl.ds(j, PROJ, stride=cols)]
    for t in range(span // LANES):
        rows = slice(t * LANES, (t + 1) * LANES)
        right_out[:, rows] = turn_ref[rows].T.astype(BF16)


def right_grad_call(at, labels, back, left, lab, wide):
    groups, span, _ = back.shape
    total = groups * WIDE
    seqs = left.shape[0]
    return pl.pallas_call(
        right_grad_body,
        in_specs=[SMEM] * 2 + [VMEM] * 4,
        out_specs=VMEM,
        out_shape=jax.ShapeDtypeStruct((seqs, span), BF16),
        scratch_shapes=[
            pltpu.VMEM((span, (CHAINS + 1) * seqs), F32),
            pltpu.VMEM((2 * seqs, WIDE), BF16),
            pltpu.VMEM((span, seqs), F32),
            pltpu.VMEM((span, seqs), F32),
        ],
        compiler_params=KERNEL,
        cost_estimate=cost(10, span, total, seqs),
        name="right_grad",
    )(at, labels, back, left, lab, wide)


def left_grad_body(at_ref, labels_ref, back_ref, lab_ref, right_ref, tall_ref,
                   left_out, rm_ref, part_ref):
    seqs = right_ref.shape[0]
    groups, span, _ = back_ref.shape
    first = lambda g: first_chain(at_ref, labels_ref, g)
    last = lambda g: last_chain(at_ref, labels_ref, g)
    part_ref[...] = (right_ref[...].astype(F32) / 3).astype(BF16)

    def build(chain):
        plain, third = tall_ref[chain, 0], tall_ref[chain, 1]
        for t in range(span // LANES):
            lanes = slice(t * LANES, (t + 1) * LANES)
            rm_ref[slots(chain, 1, seqs), lanes] = (
                right_ref[:, lanes] * plain + part_ref[:, lanes] * third
            )

    each(first(0), last(groups - 1), build)
    rm_ref[slots(last(groups - 1) + 1, 1, seqs)] = jnp.zeros((seqs, span), BF16)

    def group(g):
        lab = lab_ref[:, lanes_of(g)]

        def two_chains(k, total):
            chain = first(g) + 2 * k
            part = nn_dot(rm_ref[slots(chain, 2, seqs)], back_ref[g])
            keep0, keep1 = lab == chain, lab == chain + 1
            return total + jnp.where(keep0, part[:seqs], 0.0) + jnp.where(keep1, part[seqs:], 0.0)

        passes = (last(g) - first(g)) // 2 + 1
        total = lax.fori_loop(0, passes, two_chains, jnp.zeros((seqs, WIDE), F32))
        left_out[:, lanes_of(g)] = total.astype(BF16)

    each(0, groups - 1, group)


def left_grad_call(at, labels, back, lab, right, tall):
    groups, span, _ = back.shape
    total = groups * WIDE
    seqs = right.shape[0]
    return pl.pallas_call(
        left_grad_body,
        in_specs=[SMEM] * 2 + [VMEM] * 4,
        out_specs=VMEM,
        out_shape=jax.ShapeDtypeStruct((seqs, total), BF16),
        scratch_shapes=[
            pltpu.VMEM(((CHAINS + 1) * seqs, span), BF16),
            pltpu.VMEM((seqs, span), BF16),
        ],
        compiler_params=KERNEL,
        cost_estimate=cost(10, span, total, seqs),
        name="left_grad",
    )(at, labels, back, lab, right, tall)


def outer_body(at_ref, labels_ref, left_ref, lab_ref, right_ref, wide_ref, grad_ref,
               outer_ref, weight_out, rm_ref, lb_ref, acc_ref, sum_ref, turn_ref, flip_ref, part_ref):
    seqs = left_ref.shape[0]
    span = right_ref.shape[1]
    cols = span // PROJ
    groups, step, _, width = grad_ref.shape
    first = lambda g: first_chain(at_ref, labels_ref, g)
    last = lambda g: last_chain(at_ref, labels_ref, g)
    for t in range(span // LANES):
        lanes = slice(t * LANES, (t + 1) * LANES)
        flipped = right_ref[:, lanes].astype(F32).T
        flip_ref[lanes] = flipped.astype(BF16)
        part_ref[lanes] = (flipped / 3).astype(BF16)

    def build(chain):
        plain, third = wide_ref[chain, 0], wide_ref[chain, 1]
        for e in range(PROJ):
            rows = slice(e * cols, (e + 1) * cols)
            to = e % PER_TILE * (PROJ // PER_TILE) + e // PER_TILE
            rm_ref[to * cols : (to + 1) * cols, slots(chain, 1, seqs)] = (
                flip_ref[rows] * plain + part_ref[rows] * third
            )

    each(first(0), last(groups - 1), build)
    rm_ref[:, slots(last(groups - 1) + 1, 1, seqs)] = jnp.zeros((span, seqs), BF16)
    sum_ref[...] = jnp.zeros_like(sum_ref)
    quarter = span // PER_TILE

    def product(chain, g, add):
        masked_left(left_ref, lab_ref, lb_ref, chain, g)
        for q in range(PER_TILE):
            rows = slice(q * quarter, (q + 1) * quarter)
            part = nn_dot(rm_ref[rows, slots(chain, 2, seqs)], rolled(lb_ref[...], q))
            acc_ref[rows] = acc_ref[rows] + part if add else part

    def group(g):
        product(first(g), g, False)
        each(1, (last(g) - first(g)) // 2, lambda k: product(first(g) + 2 * k, g, True))
        for half in range(WIDE // LANES):
            lanes = slice(half * LANES, (half + 1) * LANES)
            for t in range(PROJ // PER_TILE):
                parts = []
                for q in range(PER_TILE):
                    e = q * (PROJ // PER_TILE) + t
                    parts.append(acc_ref[e * cols : (e + 1) * cols, lanes].astype(BF16))
                turned = swap_blocks(parts)
                for p in range(PER_TILE):
                    i = half * PER_TILE + p
                    at = (g, slice(i * cols, (i + 1) * cols), slice(t * LANES, (t + 1) * LANES))
                    outer_ref[at] = turned[p]
        flat = grad_ref[g].reshape(step * cols, width)
        sum_ref[...] += nn_dot(flat.T, outer_ref[g])

    each(0, groups - 1, group)
    for t in range(PROJ * PROJ // LANES):
        part = slice(t * LANES, (t + 1) * LANES)
        turn_ref[part] = sum_ref[:, part].T
    for c in range(PROJ):
        weight_out[c * PROJ : (c + 1) * PROJ] = turn_ref[pl.ds(c, PROJ, stride=PROJ)]


def outer_call(at, labels, left, lab, right, wide, grad):
    groups, step, cols, width = grad.shape
    seqs, total = left.shape
    span = right.shape[1]
    return pl.pallas_call(
        outer_body,
        in_specs=[SMEM] * 2 + [VMEM] * 5,
        out_specs=[VMEM] * 2,
        out_shape=[
            pltpu.VMEM((groups, step * cols, PROJ * PROJ), BF16),
            jax.ShapeDtypeStruct((PROJ * PROJ, width), F32),
        ],
        scratch_shapes=[
            pltpu.VMEM((span, (CHAINS + 1) * seqs), BF16),
            pltpu.VMEM((2 * seqs, WIDE), BF16),
            pltpu.VMEM((span, WIDE), F32),
            pltpu.VMEM((width, PROJ * PROJ), F32),
            pltpu.VMEM((PROJ * PROJ, width), F32),
            pltpu.VMEM((span, seqs), BF16),
            pltpu.VMEM((span, seqs), BF16),
        ],
        compiler_params=KERNEL,
        cost_estimate=cost(20, span, total, seqs),
        name="outer",
    )(at, labels, left, lab, right, wide, grad)


def pair_body(outer_ref, w_ref, offset_ref, pair_ref):
    _, pairs, _ = outer_ref.shape
    here = pair_ref.shape[0] // pairs
    for g in range(here):
        pair = nn_dot(outer_ref[pl.program_id(0) * here + g], w_ref[...]) + offset_ref[...]
        pair_ref[g * pairs : (g + 1) * pairs] = pair.astype(BF16)


def pair_call(outer, w, offset):
    groups, pairs, feats = outer.shape
    width = w.shape[1]
    steps = 2
    return pl.pallas_call(
        pair_body,
        grid=(steps,),
        in_specs=[VMEM] * 3,
        out_specs=pl.BlockSpec((groups * pairs // steps, width), lambda g: (g, 0)),
        out_shape=jax.ShapeDtypeStruct((groups * pairs, width), BF16),
        compiler_params=KERNEL,
        cost_estimate=pl.CostEstimate(
            flops=2 * groups * pairs * feats * width,
            bytes_accessed=2 * groups * pairs * width,
            transcendentals=0,
        ),
        name="pair",
    )(outer, w, offset)


class Pairs:
    def __init__(self, n_row, n_col):
        self.n_row, self.n_col = n_row, n_col
        self.per_row = n_col // n_row
        self.row = lax.axis_index("row").astype(jnp.uint32)
        self.col = lax.axis_index("col").astype(jnp.uint32)

    def col_swap(self, value, k):
        return lax.ppermute(value, "col", [(t ^ k, t) for t in range(self.n_col)])

    def row_swap(self, value, k):
        return lax.ppermute(value, "row", [(t ^ k, t) for t in range(self.n_row)])

    def place_of(self, t):
        m = self.per_row
        return ((t // m) ^ self.row) * m + (self.col + (m - t % m)) % m

    def home_pairs(self, u):
        n, m = self.n_col, self.per_row
        return [
            (a * n + t, (t // m) * n + a * m + (t + u) % m) for a in range(self.n_row) for t in range(n)
        ]

    def right_to_col(self, right):
        m = self.per_row
        lanes = right.shape[1] // m
        pieces = []
        for u in range(m):
            at = (self.col + u) % m * lanes
            block = lax.dynamic_slice_in_dim(right, at, lanes, 1) if m > 1 else right
            pieces.append(lax.ppermute(block, ("row", "col"), self.home_pairs(u)))
        return jnp.concatenate(pieces)

    def right_along_row(self, mine):
        swaps = [self.row_swap(mine, k) for k in range(1, self.n_row)]
        return jnp.concatenate([mine] + swaps)

    def right_grad_along_row(self, grad):
        size = grad.shape[0] // self.n_row
        swaps = [self.row_swap(grad[k * size : (k + 1) * size], k) for k in range(1, self.n_row)]
        return [grad[:size]] + swaps

    def right_grad_home(self, mine):
        m = self.per_row
        here, lanes = mine.shape[0] // m, mine.shape[1]
        slot = lax.broadcasted_iota(jnp.uint32, (m, 1, 1), 0)
        home = jnp.zeros((m, here, lanes), BF16)
        for u in range(m):
            pairs = [(there, origin) for origin, there in self.home_pairs(u)]
            got = lax.ppermute(mine[u * here : (u + 1) * here], ("row", "col"), pairs)[None]
            home = got if m == 1 else jnp.where(slot == (self.col + u) % m, got, home)
        return home.swapaxes(0, 1).reshape(here, m * lanes)

    def left_along_col(self, left):
        here = left.shape[0]
        out = jnp.zeros((self.n_col * here, left.shape[1]), left.dtype)
        for k in range(self.n_col):
            block = self.col_swap(left, k) if k else left
            out = lax.dynamic_update_slice_in_dim(out, block, self.place_of(self.col ^ k) * here, 0)
        return out

    def left_grad_along_col(self, grad):
        here = grad.shape[0] // self.n_col
        blocks = [
            lax.dynamic_slice_in_dim(grad, self.place_of(self.col ^ k) * here, here, 0)
            for k in range(self.n_col)
        ]
        total = blocks[0].astype(F32)
        for k in range(1, self.n_col):
            total += self.col_swap(blocks[k], k).astype(F32)
        return total.astype(BF16)

    def weight_over_row(self, weight):
        n = self.n_row
        size = weight.shape[0] // n
        sent = weight.astype(BF16).reshape(n, size, -1)
        total = lax.dynamic_index_in_dim(weight.reshape(n, size, -1), self.row, 0, keepdims=False)
        for k in range(1, n):
            piece = lax.dynamic_index_in_dim(sent, self.row ^ k, 0, keepdims=False)
            total += self.row_swap(piece, k).astype(F32)
        return total

    def weight_over_col(self, total):
        mine = total.astype(BF16)
        for k in range(1, self.n_col):
            total += self.col_swap(mine, k).astype(F32)
        return total.astype(BF16)

    def weight_to_all(self, mine):
        n = self.n_row
        which = lax.broadcasted_iota(jnp.uint32, (n, 1, 1), 0) ^ self.row
        shares = mine[None]
        for k in range(1, n):
            shares = jnp.where(which == k, self.row_swap(mine, k)[None], shares)
        return shares.reshape(n * mine.shape[0], mine.shape[1])


def after(value, *others):
    return lax.optimization_barrier((value,) + others)[0]


def shards(n_row, n_col, alignment_tensor, gain, shift, first_projector, second_projector,
           final_projector, final_offset, labels, counts, grad):
    ring = Pairs(n_row, n_col)
    here, rows, _ = alignment_tensor.shape
    cols, width = grad.shape[1:]
    seqs = here * n_col
    left, right = project_call(
        alignment_tensor, gain[None, :], shift[None, :], first_projector.T, second_projector.T, cols
    )
    mine = ring.right_to_col(right)
    left = ring.left_along_col(left)

    at = jnp.stack([ring.row * rows, ring.col * cols, ring.row, ring.col]).astype(jnp.int32)
    lab, tall, wide, plain, w, back, grad = back_call(
        at, labels, counts, after(final_projector, right), grad, seqs, n_row, n_col
    )
    right = ring.right_along_row(mine)
    back, grad = in_vmem(back), in_vmem(grad)
    right_grad = right_grad_call(at, labels, back, left, lab, plain)

    right = after(right, right_grad)
    parts = ring.right_grad_along_row(right_grad)
    outer, weight = outer_call(
        at, labels, left, lab, right, wide, grad
    )
    share = ring.weight_over_row(weight)
    left_grad = left_grad_call(at, labels, back, after(lab, weight), right, tall)
    share = after(share, left_grad)

    parts = lax.optimization_barrier((*parts, share))[:-1]
    mine = sum(part.astype(F32) for part in parts).astype(BF16)
    grad_right = ring.right_grad_home(mine)
    adjoint_first = ring.left_grad_along_col(left_grad)
    pair_update = pair_call(in_vmem(outer), after(w, left_grad, share), final_offset[None, :])
    pair_update = pair_update.reshape(rows, cols, width)
    mine = after(ring.weight_over_col(share), pair_update)
    grad_w_out = ring.weight_to_all(mine).astype(F32) / (n_row * rows)
    return pair_update, adjoint_first, grad_right, grad_w_out


def solution(mesh):
    in_specs = (
        P(("parts", "col"), "row", None),
        P(),
        P(),
        P(),
        P(),
        P(),
        P(),
        P("parts"),
        P("parts", None),
        P(("parts", "row"), "col", None),
    )
    out_specs = (
        P(("parts", "row"), "col", None),
        P(("parts", "col"), "row"),
        P(("parts", "col"), "row"),
        P("parts", None),
    )

    def body(*args):
        return shards(mesh.shape["row"], mesh.shape["col"], *args)

    return jax.shard_map(body, mesh=mesh, in_specs=in_specs, out_specs=out_specs, check_vma=False)
```

```python
import jax
import jax.numpy as jnp
from jax import lax
from jax.experimental import pallas as pl
from jax.experimental.pallas import tpu as pltpu
from jax.sharding import PartitionSpec as P


PROJ = 32
CHAINS = 8
LANES = 128
PER_TILE = LANES // PROJ
WIDE = 256
F32 = jnp.float32
BF16 = jnp.bfloat16
VMEM = pl.BlockSpec(memory_space=pltpu.VMEM)
KERNEL = pltpu.CompilerParams(vmem_limit_bytes=24 << 20)
HBM = pl.BlockSpec(memory_space=pltpu.HBM)
SMEM = pl.BlockSpec(memory_space=pltpu.SMEM)


def swap_blocks(parts):
    lane = lax.broadcasted_iota(jnp.int32, parts[0].shape, 1)
    outs = []
    for q in range(PER_TILE):
        out = parts[(PER_TILE - 1 - q) % PER_TILE]
        for block in range(PER_TILE - 2, -1, -1):
            out = jnp.where(lane < (block + 1) * PROJ, parts[(block - q) % PER_TILE], out)
        outs.append(pltpu.roll(out, LANES - q * PROJ, 1) if q else out)
    return outs


def rolled(value, p):
    if not p:
        return value
    return jnp.concatenate(
        [pltpu.roll(value[:, t : t + LANES], p * PROJ, 1) for t in range(0, value.shape[1], LANES)],
        axis=1,
    )


def nt_dot(a, b):
    return lax.dot_general(a, b, (((1,), (1,)), ((), ())), preferred_element_type=F32)


def nn_dot(a, b):
    return lax.dot_general(a, b, (((1,), (0,)), ((), ())), preferred_element_type=F32)


def in_vmem(value):
    return pltpu.with_memory_space_constraint(value, pltpu.VMEM)


def in_hbm(value):
    return pltpu.with_memory_space_constraint(value, pltpu.HBM)


def project_body(x_hbm, gain_hbm, shift_hbm, first_hbm, second_hbm, left_ref, right_ref,
                 x_ref, gain_ref, shift_ref, w_ref, proj_ref, turn_ref, out_ref, sems, *, cols):
    chunks, chunk, rows, feats = x_ref.shape
    small = [
        pltpu.make_async_copy(gain_hbm, gain_ref, sems.at[chunks]),
        pltpu.make_async_copy(shift_hbm, shift_ref, sems.at[chunks + 1]),
        pltpu.make_async_copy(first_hbm, w_ref.at[pl.ds(0, PROJ)], sems.at[chunks + 2]),
        pltpu.make_async_copy(second_hbm, w_ref.at[pl.ds(PROJ, PROJ)], sems.at[chunks + 3]),
    ]
    big = [
        pltpu.make_async_copy(x_hbm.at[pl.ds(g * chunk, chunk)], x_ref.at[g], sems.at[g])
        for g in range(chunks)
    ]
    for copy in big[:1] + small + big[1:]:
        copy.start()
    w_ref[2 * PROJ :] = jnp.zeros((LANES - 2 * PROJ, feats), BF16)
    for copy in small:
        copy.wait()
    for g in range(chunks):
        big[g].wait()
        x = x_ref[g].astype(F32).reshape(chunk * rows, feats)
        center = x - jnp.mean(x, axis=-1, keepdims=True)
        spread = jnp.mean(center * center, axis=-1, keepdims=True)
        normed = center * lax.rsqrt(spread + 1e-05) * gain_ref[...] + shift_ref[...]
        at = slice(g * chunk * rows, (g + 1) * chunk * rows)
        proj_ref[at] = nt_dot(normed.astype(BF16), w_ref[...])
    project_layout(proj_ref, turn_ref, out_ref, left_ref, right_ref, rows, cols)


def project_layout(proj_ref, turn_ref, out_ref, left_ref, right_ref, rows, cols):
    here = left_ref.shape[0]
    lane = lax.broadcasted_iota(jnp.int32, (here, LANES), 1)
    for t in range(rows // PER_TILE):
        tile = proj_ref[pl.ds(t * PER_TILE, here, stride=rows)]
        for p in range(1, PER_TILE):
            part = proj_ref[pl.ds(t * PER_TILE + p, here, stride=rows)]
            tile = jnp.where(lane < p * PROJ, tile, pltpu.roll(part, p * PROJ, 1))
        left_ref[:, t * LANES : (t + 1) * LANES] = tile.astype(BF16)

    tiles = here * rows // LANES
    for t in range(tiles):
        flipped = proj_ref[t * LANES : (t + 1) * LANES].T
        turn_ref[t * PROJ : (t + 1) * PROJ] = flipped[PROJ : 2 * PROJ]
    seqs = LANES // rows
    per = LANES // cols
    lane = lax.broadcasted_iota(jnp.int32, (tiles, LANES), 1)
    for block in range(rows // cols):
        for t in range(PROJ // per):
            at = (block * (PROJ // per) + t) * LANES
            parts = [turn_ref[pl.ds(t * per + p, tiles, stride=PROJ)] for p in range(per)]
            for u in range(seqs):
                start = u * rows + block * cols
                tile = None
                for p, part in enumerate(parts):
                    amount = (p * cols - start) % LANES
                    part = pltpu.roll(part, amount, 1) if amount else part
                    tile = part if tile is None else jnp.where(lane < p * cols, tile, part)
                out_ref[pl.ds(u, tiles, stride=seqs), :] = tile
            right_ref[:, at : at + LANES] = out_ref[...].astype(BF16)


def project_call(x, gain, shift, first, second, cols):
    here, rows, feats = x.shape
    chunk = min(here, max(1, 2 * WIDE // rows))
    return pl.pallas_call(
        lambda *refs: project_body(*refs, cols=cols),
        in_specs=[HBM] * 5,
        out_specs=[VMEM] * 2,
        out_shape=[jax.ShapeDtypeStruct((here, rows * PROJ), BF16)] * 2,
        scratch_shapes=[
            pltpu.VMEM((here // chunk, chunk, rows, feats), BF16),
            pltpu.VMEM(gain.shape, F32),
            pltpu.VMEM(shift.shape, F32),
            pltpu.VMEM((LANES, feats), BF16),
            pltpu.VMEM((here * rows, LANES), F32),
            pltpu.VMEM((here * rows // LANES * PROJ, LANES), F32),
            pltpu.VMEM((here, LANES), F32),
            pltpu.SemaphoreType.DMA((here // chunk + 4,)),
        ],
        compiler_params=KERNEL,
        name="project",
    )(*map(in_hbm, (x, gain, shift, first, second)))


def masks(at_ref, labels_ref, counts_ref, lab_ref, tall_ref, wide_ref, plain_ref, rows, cols, seqs, n_col):
    res = labels_ref.shape[1]
    labels = jnp.broadcast_to(labels_ref[...], (8, res))
    own = pltpu.roll(labels, (res - at_ref[0]) % res, 1)[:, :rows]
    spread = (
        lax.broadcasted_iota(jnp.int32, (rows, rows * PROJ), 1) // PROJ
        == lax.broadcasted_iota(jnp.int32, (rows, rows * PROJ), 0)
    )
    lab = nn_dot(own.astype(F32).astype(BF16), spread.astype(F32).astype(BF16))
    lab_ref[...] = lab[:1].astype(jnp.int32)

    there = pltpu.roll(labels, (res - at_ref[1]) % res, 1)[:, :LANES]
    there = jnp.where(lax.broadcasted_iota(jnp.int32, (8, LANES), 1) < cols, there, 0)
    reach = cols
    while reach < LANES:
        there = there + pltpu.roll(there, reach, 1)
        reach *= 2
    depth = jnp.zeros((CHAINS, LANES), jnp.int32)
    for b in range(CHAINS):
        depth += jnp.where(there == b, counts_ref[:, b : b + 1], 0)
    here = lax.broadcasted_iota(jnp.int32, (seqs // n_col, LANES), 0)
    seq = jnp.concatenate([here + (at_ref[2] ^ k) * (seqs // n_col) for k in range(n_col)], axis=0)
    for a in range(CHAINS):
        deep = jnp.broadcast_to(depth[a : a + 1], (seqs, LANES))
        weight = jnp.where(seq < deep, 1.0 / deep.astype(F32), 0.0)
        three = deep % 3 == 0
        for x, part in enumerate((jnp.where(three, 0.0, weight), jnp.where(three, 3.0 * weight, 0.0))):
            tall_ref[a, x] = part.astype(BF16)
            wide_ref[a, x] = part.T[:cols].astype(BF16)
        plain_ref[a] = weight.T[:cols]


def projector(w_ref, wide_w_ref, w_out, wt_ref):
    wide_w_ref[...] = w_ref[...].astype(F32)
    for t in range(PROJ // PER_TILE):
        for q in range(PER_TILE):
            e = t * PER_TILE + q
            w_out[e * PROJ : (e + 1) * PROJ] = wide_w_ref[pl.ds(e, PROJ, stride=PROJ)].astype(BF16)
        block = w_out[t * LANES : (t + 1) * LANES].astype(F32)
        for p in range(PER_TILE):
            wt_ref[p, :, t * LANES : (t + 1) * LANES] = rolled(block.T, p).astype(BF16)


def cost(passes, span, total, seqs):
    return pl.CostEstimate(
        flops=4 * passes * span * total * seqs, bytes_accessed=2 * span * total, transcendentals=0
    )


def back_body(at_ref, labels_hbm, counts_hbm, w_hbm, grad_hbm,
              lab_ref, tall_ref, wide_ref, plain_ref, w_out, back_ref, grad_ref,
              labels_ref, counts_ref, w_ref, wide_w_ref, wt_ref, sems, *, seqs, n_col):
    groups, step, cols, _ = grad_ref.shape
    copies = [
        pltpu.make_async_copy(w_hbm, w_ref, sems.at[groups]),
        pltpu.make_async_copy(labels_hbm, labels_ref, sems.at[groups + 1]),
        pltpu.make_async_copy(counts_hbm, counts_ref, sems.at[groups + 2]),
    ]
    for copy in copies:
        copy.start()

    def grad_of(g):
        return pltpu.make_async_copy(grad_hbm.at[pl.ds(g * step, step)], grad_ref.at[g], sems.at[g])

    for g in range(groups):
        grad_of(g).start()
    for copy in copies:
        copy.wait()
    projector(w_ref, wide_w_ref, w_out, wt_ref)
    masks(at_ref, labels_ref, counts_ref, lab_ref, tall_ref, wide_ref, plain_ref,
          groups * step, cols, seqs, n_col)
    halves = step // PER_TILE

    def group(g, carry):
        grad_of(g).wait()
        blocks = [
            jnp.concatenate([grad_ref[g, half * PER_TILE + p] for half in range(halves)], axis=0)
            for p in range(PER_TILE)
        ]
        for u in range(PROJ * PROJ // WIDE):
            prods = [
                nn_dot(block, wt_ref[p, :, u * WIDE : (u + 1) * WIDE]).astype(BF16)
                for p, block in enumerate(blocks)
            ]
            for half in range(halves):
                for t in range(WIDE // LANES):
                    parts = [
                        prod[half * cols : (half + 1) * cols, t * LANES : (t + 1) * LANES]
                        for prod in prods
                    ]
                    for q, part in enumerate(swap_blocks(parts)):
                        e = u * (WIDE // PROJ) + t * PER_TILE + q
                        at = (g, slice(e * cols, (e + 1) * cols))
                        back_ref[at + (slice(half * LANES, (half + 1) * LANES),)] = part
        return carry

    lax.fori_loop(0, groups, group, 0)


def back_call(at, labels, counts, w, grad, seqs, n_col):
    rows, cols, width = grad.shape
    step = WIDE // PROJ
    groups = rows // step
    labels = labels[None, :]
    return pl.pallas_call(
        lambda *refs: back_body(*refs, seqs=seqs, n_col=n_col),
        in_specs=[SMEM] + [HBM] * 4,
        out_specs=[VMEM] * 7,
        out_shape=[
            jax.ShapeDtypeStruct((1, rows * PROJ), jnp.int32),
            jax.ShapeDtypeStruct((CHAINS, 2, seqs, LANES), BF16),
            jax.ShapeDtypeStruct((CHAINS, 2, cols, seqs), BF16),
            jax.ShapeDtypeStruct((CHAINS, cols, seqs), F32),
            jax.ShapeDtypeStruct(w.shape, BF16),
            pltpu.VMEM((groups, PROJ * cols, WIDE), BF16),
            pltpu.VMEM((groups, step, cols, width), BF16),
        ],
        scratch_shapes=[
            pltpu.VMEM(labels.shape, jnp.int32),
            pltpu.VMEM(counts.shape, jnp.int32),
            pltpu.VMEM(w.shape, BF16),
            pltpu.VMEM(w.shape, F32),
            pltpu.VMEM((PER_TILE, width, PROJ * PROJ), BF16),
            pltpu.SemaphoreType.DMA((groups + 3,)),
        ],
        compiler_params=KERNEL,
        cost_estimate=cost(10, PROJ * cols, rows * PROJ, width),
        name="back",
    )(at, *map(in_hbm, (labels, counts, w, grad)))


def first_chain(at_ref, labels_ref, group):
    return labels_ref[at_ref[0] + group * (WIDE // PROJ)]


def last_chain(at_ref, labels_ref, group):
    return labels_ref[at_ref[0] + (group + 1) * (WIDE // PROJ) - 1]


def slots(chain, count, seqs):
    return pl.ds(pl.multiple_of(chain * seqs, seqs), count * seqs)


def each(first, last, fn):
    def step(k, carry):
        fn(k)
        return carry

    lax.fori_loop(first, last + 1, step, 0)


def lanes_of(group):
    return pl.ds(pl.multiple_of(group * WIDE, WIDE), WIDE)


def masked_left(left_ref, lab_ref, lb_ref, chain, group):
    seqs = left_ref.shape[0]
    lanes = lanes_of(group)
    for side in range(2):
        keep = (lab_ref[:, lanes] == chain + side).astype(F32).astype(BF16)
        lb_ref[side * seqs : (side + 1) * seqs] = left_ref[:, lanes] * keep


def right_grad_body(at_ref, labels_ref, back_ref, left_ref, lab_ref, wide_ref,
                    right_out, q_ref, lb_ref, flip_ref, turn_ref):
    seqs = left_ref.shape[0]
    groups, span, _ = back_ref.shape
    cols = span // PROJ
    first = lambda g: first_chain(at_ref, labels_ref, g)
    last = lambda g: last_chain(at_ref, labels_ref, g)

    def clear(chain):
        q_ref[:, slots(chain, 1, seqs)] = jnp.zeros((span, seqs), F32)

    each(first(0), last(groups - 1) + 1, clear)

    def group(g):
        def two_chains(k):
            chain = first(g) + 2 * k
            masked_left(left_ref, lab_ref, lb_ref, chain, g)
            q_ref[:, slots(chain, 2, seqs)] += nt_dot(back_ref[g], lb_ref[...])

        each(0, (last(g) - first(g)) // 2, two_chains)

    each(0, groups - 1, group)

    def combine(chain, start):
        for e in range(PROJ):
            rows = slice(e * cols, (e + 1) * cols)
            part = q_ref[rows, slots(chain, 1, seqs)] * wide_ref[chain]
            flip_ref[rows] = part if start else flip_ref[rows] + part

    combine(first(0), True)
    each(first(0) + 1, last(groups - 1), lambda chain: combine(chain, False))
    for j in range(cols):
        turn_ref[j * PROJ : (j + 1) * PROJ] = flip_ref[pl.ds(j, PROJ, stride=cols)]
    for t in range(span // LANES):
        rows = slice(t * LANES, (t + 1) * LANES)
        right_out[:, rows] = turn_ref[rows].T.astype(BF16)


def right_grad_call(at, labels, back, left, lab, wide):
    groups, span, _ = back.shape
    total = groups * WIDE
    seqs = left.shape[0]
    return pl.pallas_call(
        right_grad_body,
        in_specs=[SMEM] * 2 + [VMEM] * 4,
        out_specs=VMEM,
        out_shape=jax.ShapeDtypeStruct((seqs, span), BF16),
        scratch_shapes=[
            pltpu.VMEM((span, (CHAINS + 1) * seqs), F32),
            pltpu.VMEM((2 * seqs, WIDE), BF16),
            pltpu.VMEM((span, seqs), F32),
            pltpu.VMEM((span, seqs), F32),
        ],
        compiler_params=KERNEL,
        cost_estimate=cost(10, span, total, seqs),
        name="right_grad",
    )(at, labels, back, left, lab, wide)


def left_grad_body(at_ref, labels_ref, back_ref, lab_ref, right_ref, tall_ref,
                   left_out, rm_ref, part_ref):
    seqs = right_ref.shape[0]
    groups, span, _ = back_ref.shape
    first = lambda g: first_chain(at_ref, labels_ref, g)
    last = lambda g: last_chain(at_ref, labels_ref, g)
    part_ref[...] = (right_ref[...].astype(F32) / 3).astype(BF16)

    def build(chain):
        plain, third = tall_ref[chain, 0], tall_ref[chain, 1]
        for t in range(span // LANES):
            lanes = slice(t * LANES, (t + 1) * LANES)
            rm_ref[slots(chain, 1, seqs), lanes] = (
                right_ref[:, lanes] * plain + part_ref[:, lanes] * third
            )

    each(first(0), last(groups - 1), build)
    rm_ref[slots(last(groups - 1) + 1, 1, seqs)] = jnp.zeros((seqs, span), BF16)

    def group(g):
        lab = lab_ref[:, lanes_of(g)]

        def two_chains(k, total):
            chain = first(g) + 2 * k
            part = nn_dot(rm_ref[slots(chain, 2, seqs)], back_ref[g])
            keep0, keep1 = lab == chain, lab == chain + 1
            return total + jnp.where(keep0, part[:seqs], 0.0) + jnp.where(keep1, part[seqs:], 0.0)

        passes = (last(g) - first(g)) // 2 + 1
        total = lax.fori_loop(0, passes, two_chains, jnp.zeros((seqs, WIDE), F32))
        left_out[:, lanes_of(g)] = total.astype(BF16)

    each(0, groups - 1, group)


def left_grad_call(at, labels, back, lab, right, tall):
    groups, span, _ = back.shape
    total = groups * WIDE
    seqs = right.shape[0]
    return pl.pallas_call(
        left_grad_body,
        in_specs=[SMEM] * 2 + [VMEM] * 4,
        out_specs=VMEM,
        out_shape=jax.ShapeDtypeStruct((seqs, total), BF16),
        scratch_shapes=[
            pltpu.VMEM(((CHAINS + 1) * seqs, span), BF16),
            pltpu.VMEM((seqs, span), BF16),
        ],
        compiler_params=KERNEL,
        cost_estimate=cost(10, span, total, seqs),
        name="left_grad",
    )(at, labels, back, lab, right, tall)


def outer_body(at_ref, labels_ref, left_ref, lab_ref, right_ref, wide_ref, grad_ref,
               outer_ref, weight_out, rm_ref, lb_ref, acc_ref, sum_ref, turn_ref, flip_ref, part_ref):
    seqs = left_ref.shape[0]
    span = right_ref.shape[1]
    cols = span // PROJ
    groups, step, _, width = grad_ref.shape
    first = lambda g: first_chain(at_ref, labels_ref, g)
    last = lambda g: last_chain(at_ref, labels_ref, g)
    for t in range(span // LANES):
        lanes = slice(t * LANES, (t + 1) * LANES)
        flipped = right_ref[:, lanes].astype(F32).T
        flip_ref[lanes] = flipped.astype(BF16)
        part_ref[lanes] = (flipped / 3).astype(BF16)

    def build(chain):
        plain, third = wide_ref[chain, 0], wide_ref[chain, 1]
        for e in range(PROJ):
            rows = slice(e * cols, (e + 1) * cols)
            to = e % PER_TILE * (PROJ // PER_TILE) + e // PER_TILE
            rm_ref[to * cols : (to + 1) * cols, slots(chain, 1, seqs)] = (
                flip_ref[rows] * plain + part_ref[rows] * third
            )

    each(first(0), last(groups - 1), build)
    rm_ref[:, slots(last(groups - 1) + 1, 1, seqs)] = jnp.zeros((span, seqs), BF16)
    sum_ref[...] = jnp.zeros_like(sum_ref)
    quarter = span // PER_TILE

    def product(chain, g, add):
        masked_left(left_ref, lab_ref, lb_ref, chain, g)
        for q in range(PER_TILE):
            rows = slice(q * quarter, (q + 1) * quarter)
            part = nn_dot(rm_ref[rows, slots(chain, 2, seqs)], rolled(lb_ref[...], q))
            acc_ref[rows] = acc_ref[rows] + part if add else part

    def group(g):
        product(first(g), g, False)
        each(1, (last(g) - first(g)) // 2, lambda k: product(first(g) + 2 * k, g, True))
        for half in range(WIDE // LANES):
            lanes = slice(half * LANES, (half + 1) * LANES)
            for t in range(PROJ // PER_TILE):
                parts = []
                for q in range(PER_TILE):
                    e = q * (PROJ // PER_TILE) + t
                    parts.append(acc_ref[e * cols : (e + 1) * cols, lanes].astype(BF16))
                turned = swap_blocks(parts)
                for p in range(PER_TILE):
                    i = half * PER_TILE + p
                    at = (g, slice(i * cols, (i + 1) * cols), slice(t * LANES, (t + 1) * LANES))
                    outer_ref[at] = turned[p]
        flat = grad_ref[g].reshape(step * cols, width)
        sum_ref[...] += nn_dot(flat.T, outer_ref[g])

    each(0, groups - 1, group)
    for t in range(PROJ * PROJ // LANES):
        part = slice(t * LANES, (t + 1) * LANES)
        turn_ref[part] = sum_ref[:, part].T
    for c in range(PROJ):
        weight_out[c * PROJ : (c + 1) * PROJ] = turn_ref[pl.ds(c, PROJ, stride=PROJ)]


def outer_call(at, labels, left, lab, right, wide, grad):
    groups, step, cols, width = grad.shape
    seqs, total = left.shape
    span = right.shape[1]
    return pl.pallas_call(
        outer_body,
        in_specs=[SMEM] * 2 + [VMEM] * 5,
        out_specs=[VMEM] * 2,
        out_shape=[
            pltpu.VMEM((groups, step * cols, PROJ * PROJ), BF16),
            jax.ShapeDtypeStruct((PROJ * PROJ, width), F32),
        ],
        scratch_shapes=[
            pltpu.VMEM((span, (CHAINS + 1) * seqs), BF16),
            pltpu.VMEM((2 * seqs, WIDE), BF16),
            pltpu.VMEM((span, WIDE), F32),
            pltpu.VMEM((width, PROJ * PROJ), F32),
            pltpu.VMEM((PROJ * PROJ, width), F32),
            pltpu.VMEM((span, seqs), BF16),
            pltpu.VMEM((span, seqs), BF16),
        ],
        compiler_params=KERNEL,
        cost_estimate=cost(20, span, total, seqs),
        name="outer",
    )(at, labels, left, lab, right, wide, grad)


def pair_body(outer_ref, w_ref, offset_ref, pair_ref):
    _, pairs, _ = outer_ref.shape
    here = pair_ref.shape[0] // pairs
    for g in range(here):
        pair = nn_dot(outer_ref[pl.program_id(0) * here + g], w_ref[...]) + offset_ref[...]
        pair_ref[g * pairs : (g + 1) * pairs] = pair.astype(BF16)


def pair_call(outer, w, offset):
    groups, pairs, feats = outer.shape
    width = w.shape[1]
    steps = 2
    return pl.pallas_call(
        pair_body,
        grid=(steps,),
        in_specs=[VMEM] * 3,
        out_specs=pl.BlockSpec((groups * pairs // steps, width), lambda g: (g, 0)),
        out_shape=jax.ShapeDtypeStruct((groups * pairs, width), BF16),
        compiler_params=KERNEL,
        cost_estimate=pl.CostEstimate(
            flops=2 * groups * pairs * feats * width,
            bytes_accessed=2 * groups * pairs * width,
            transcendentals=0,
        ),
        name="pair",
    )(outer, w, offset)


class Pairs:
    def __init__(self, n_row, n_col):
        self.n_row, self.n_col = n_row, n_col
        self.per_row = n_col // n_row
        self.row = lax.axis_index("row").astype(jnp.uint32)
        self.col = lax.axis_index("col").astype(jnp.uint32)

    def col_swap(self, value, k):
        return lax.ppermute(value, "col", [(t ^ k, t) for t in range(self.n_col)])

    def row_swap(self, value, k):
        return lax.ppermute(value, "row", [(t ^ k, t) for t in range(self.n_row)])

    def right_along_row(self, right):
        others = [self.row_swap(right, k) for k in range(1, self.n_row)]
        return [right] + others

    def right_pieces(self, by_row):
        m = self.per_row
        here, lanes = by_row[0].shape
        lanes //= m
        by_row = jnp.stack(by_row)
        pieces = []
        for k in range(self.n_col):
            q = self.col ^ k
            at = ((q // m) ^ self.row, jnp.uint32(0), (q % m) * lanes)
            pieces.append(lax.dynamic_slice(by_row, at, (1, here, lanes))[0])
        return pieces

    def right_along_col(self, pieces):
        return jnp.concatenate([self.col_swap(p, k) if k else p for k, p in enumerate(pieces)])

    def right_grad_home(self, grad):
        n, m = self.n_col, self.per_row
        here, lanes = grad.shape[0] // n, grad.shape[1]
        total = jnp.zeros((m, here, lanes), F32)
        slot = lax.broadcasted_iota(jnp.uint32, (m, 1, 1), 0)
        for k in range(n):
            t = (self.row * m + self.col % m) ^ k
            block = lax.dynamic_slice_in_dim(grad, (t ^ self.col) * here, here, 0)
            pairs = []
            for r in range(self.n_row):
                for q in range(n):
                    pairs.append((r * n + q, (q // m) * n + ((r * m + q % m) ^ k)))
            got = lax.ppermute(block, ("row", "col"), pairs).astype(F32)[None]
            total += got if m == 1 else jnp.where(slot == (self.col ^ k) % m, got, 0)
        return total.swapaxes(0, 1).reshape(here, m * lanes).astype(BF16)

    def weight_over_row(self, weight):
        n = self.n_row
        size = weight.shape[0] // n
        sent = weight.astype(BF16).reshape(n, size, -1)
        total = lax.dynamic_index_in_dim(weight.reshape(n, size, -1), self.row, 0, keepdims=False)
        for k in range(1, n):
            piece = lax.dynamic_index_in_dim(sent, self.row ^ k, 0, keepdims=False)
            total += self.row_swap(piece, k).astype(F32)
        return total

    def weight_over_col(self, total):
        mine = total.astype(BF16)
        for k in range(1, self.n_col):
            total += self.col_swap(mine, k).astype(F32)
        return total.astype(BF16)

    def weight_to_all(self, mine):
        n = self.n_row
        which = lax.broadcasted_iota(jnp.uint32, (n, 1, 1), 0) ^ self.row
        shares = mine[None]
        for k in range(1, n):
            shares = jnp.where(which == k, self.row_swap(mine, k)[None], shares)
        return shares.reshape(n * mine.shape[0], mine.shape[1])


def after(value, *others):
    return lax.optimization_barrier((value,) + others)[0]


def shards(n_row, n_col, alignment_tensor, gain, shift, first_projector, second_projector,
           final_projector, final_offset, labels, counts, grad):
    ring = Pairs(n_row, n_col)
    here, rows, _ = alignment_tensor.shape
    cols, width = grad.shape[1:]
    seqs = here * n_col
    left, right = project_call(
        alignment_tensor, gain[None, :], shift[None, :], first_projector.T, second_projector.T, cols
    )
    by_row = ring.right_along_row(right)
    left = jnp.concatenate([left] + [ring.col_swap(left, k) for k in range(1, n_col)])

    at = jnp.stack([ring.row * rows, ring.col * cols, ring.col]).astype(jnp.int32)
    lab, tall, wide, plain, w, back, grad = back_call(
        at, labels, counts, after(final_projector, right), grad, seqs, n_col
    )
    mine = ring.right_along_col(ring.right_pieces(by_row))
    back, grad = in_vmem(back), in_vmem(grad)
    right_grad = right_grad_call(at, labels, back, left, lab, plain)

    right = after(mine, right_grad)
    grad_right = ring.right_grad_home(right_grad)
    outer, weight = outer_call(
        at, labels, left, lab, right, wide, grad
    )
    share = ring.weight_over_row(weight)
    left_grad = left_grad_call(at, labels, back, after(lab, weight), right, tall)
    share = after(share, left_grad)

    total = left_grad[:here].astype(F32)
    for k in range(1, n_col):
        total += ring.col_swap(left_grad[k * here : (k + 1) * here], k).astype(F32)
    adjoint_first = total.astype(BF16)
    pair_update = pair_call(in_vmem(outer), after(w, left_grad, share), final_offset[None, :])
    pair_update = pair_update.reshape(rows, cols, width)
    mine = after(ring.weight_over_col(share), pair_update)
    grad_w_out = ring.weight_to_all(mine).astype(F32) / (n_row * rows)
    return pair_update, adjoint_first, grad_right, grad_w_out


def solution(mesh):
    in_specs = (
        P(("parts", "col"), "row", None),
        P(),
        P(),
        P(),
        P(),
        P(),
        P(),
        P("parts"),
        P("parts", None),
        P(("parts", "row"), "col", None),
    )
    out_specs = (
        P(("parts", "row"), "col", None),
        P(("parts", "col"), "row"),
        P(("parts", "col"), "row"),
        P("parts", None),
    )

    def body(*args):
        return shards(mesh.shape["row"], mesh.shape["col"], *args)

    return jax.shard_map(body, mesh=mesh, in_specs=in_specs, out_specs=out_specs, check_vma=False)
```

```python
import jax
import jax.numpy as jnp
from jax import lax
from jax.experimental import pallas as pl
from jax.experimental.pallas import tpu as pltpu
from jax.sharding import PartitionSpec as P


PROJ = 32
CHAINS = 8
LANES = 128
PER_TILE = LANES // PROJ
WIDE = 256
F32 = jnp.float32
BF16 = jnp.bfloat16
VMEM = pl.BlockSpec(memory_space=pltpu.VMEM)
KERNEL = pltpu.CompilerParams(vmem_limit_bytes=24 << 20)
HBM = pl.BlockSpec(memory_space=pltpu.HBM)
SMEM = pl.BlockSpec(memory_space=pltpu.SMEM)


def swap_blocks(parts):
    lane = lax.broadcasted_iota(jnp.int32, parts[0].shape, 1)
    outs = []
    for q in range(PER_TILE):
        out = parts[(PER_TILE - 1 - q) % PER_TILE]
        for block in range(PER_TILE - 2, -1, -1):
            out = jnp.where(lane < (block + 1) * PROJ, parts[(block - q) % PER_TILE], out)
        outs.append(pltpu.roll(out, LANES - q * PROJ, 1) if q else out)
    return outs


def rolled(value, p):
    if not p:
        return value
    return jnp.concatenate(
        [pltpu.roll(value[:, t : t + LANES], p * PROJ, 1) for t in range(0, value.shape[1], LANES)],
        axis=1,
    )


def nt_dot(a, b):
    return lax.dot_general(a, b, (((1,), (1,)), ((), ())), preferred_element_type=F32)


def nn_dot(a, b):
    return lax.dot_general(a, b, (((1,), (0,)), ((), ())), preferred_element_type=F32)


def in_vmem(value):
    return pltpu.with_memory_space_constraint(value, pltpu.VMEM)


def in_hbm(value):
    return pltpu.with_memory_space_constraint(value, pltpu.HBM)


def project_body(x_hbm, gain_hbm, shift_hbm, first_hbm, second_hbm, left_ref, right_ref,
                 x_ref, gain_ref, shift_ref, w_ref, proj_ref, turn_ref, out_ref, sems, *, cols):
    chunks, chunk, rows, feats = x_ref.shape
    small = [
        pltpu.make_async_copy(gain_hbm, gain_ref, sems.at[chunks]),
        pltpu.make_async_copy(shift_hbm, shift_ref, sems.at[chunks + 1]),
        pltpu.make_async_copy(first_hbm, w_ref.at[pl.ds(0, PROJ)], sems.at[chunks + 2]),
        pltpu.make_async_copy(second_hbm, w_ref.at[pl.ds(PROJ, PROJ)], sems.at[chunks + 3]),
    ]
    big = [
        pltpu.make_async_copy(x_hbm.at[pl.ds(g * chunk, chunk)], x_ref.at[g], sems.at[g])
        for g in range(chunks)
    ]
    for copy in big[:1] + small + big[1:]:
        copy.start()
    w_ref[2 * PROJ :] = jnp.zeros((LANES - 2 * PROJ, feats), BF16)
    for copy in small:
        copy.wait()
    for g in range(chunks):
        big[g].wait()
        x = x_ref[g].astype(F32).reshape(chunk * rows, feats)
        center = x - jnp.mean(x, axis=-1, keepdims=True)
        spread = jnp.mean(center * center, axis=-1, keepdims=True)
        normed = center * lax.rsqrt(spread + 1e-05) * gain_ref[...] + shift_ref[...]
        at = slice(g * chunk * rows, (g + 1) * chunk * rows)
        proj_ref[at] = nt_dot(normed.astype(BF16), w_ref[...])
    project_layout(proj_ref, turn_ref, out_ref, left_ref, right_ref, rows, cols)


def project_layout(proj_ref, turn_ref, out_ref, left_ref, right_ref, rows, cols):
    here = left_ref.shape[0]
    lane = lax.broadcasted_iota(jnp.int32, (here, LANES), 1)
    for t in range(rows // PER_TILE):
        tile = proj_ref[pl.ds(t * PER_TILE, here, stride=rows)]
        for p in range(1, PER_TILE):
            part = proj_ref[pl.ds(t * PER_TILE + p, here, stride=rows)]
            tile = jnp.where(lane < p * PROJ, tile, pltpu.roll(part, p * PROJ, 1))
        left_ref[:, t * LANES : (t + 1) * LANES] = tile.astype(BF16)

    tiles = here * rows // LANES
    for t in range(tiles):
        flipped = proj_ref[t * LANES : (t + 1) * LANES].T
        turn_ref[t * PROJ : (t + 1) * PROJ] = flipped[PROJ : 2 * PROJ]
    seqs = LANES // rows
    per = LANES // cols
    lane = lax.broadcasted_iota(jnp.int32, (tiles, LANES), 1)
    for block in range(rows // cols):
        for t in range(PROJ // per):
            at = (block * (PROJ // per) + t) * LANES
            parts = [turn_ref[pl.ds(t * per + p, tiles, stride=PROJ)] for p in range(per)]
            for u in range(seqs):
                start = u * rows + block * cols
                tile = None
                for p, part in enumerate(parts):
                    amount = (p * cols - start) % LANES
                    part = pltpu.roll(part, amount, 1) if amount else part
                    tile = part if tile is None else jnp.where(lane < p * cols, tile, part)
                out_ref[pl.ds(u, tiles, stride=seqs), :] = tile
            right_ref[:, at : at + LANES] = out_ref[...].astype(BF16)


def project_call(x, gain, shift, first, second, cols):
    here, rows, feats = x.shape
    chunk = min(here, max(1, 2 * WIDE // rows))
    return pl.pallas_call(
        lambda *refs: project_body(*refs, cols=cols),
        in_specs=[HBM] * 5,
        out_specs=[VMEM] * 2,
        out_shape=[jax.ShapeDtypeStruct((here, rows * PROJ), BF16)] * 2,
        scratch_shapes=[
            pltpu.VMEM((here // chunk, chunk, rows, feats), BF16),
            pltpu.VMEM(gain.shape, F32),
            pltpu.VMEM(shift.shape, F32),
            pltpu.VMEM((LANES, feats), BF16),
            pltpu.VMEM((here * rows, LANES), F32),
            pltpu.VMEM((here * rows // LANES * PROJ, LANES), F32),
            pltpu.VMEM((here, LANES), F32),
            pltpu.SemaphoreType.DMA((here // chunk + 4,)),
        ],
        compiler_params=KERNEL,
        name="project",
    )(*map(in_hbm, (x, gain, shift, first, second)))


def masks(at_ref, labels_ref, counts_ref, lab_ref, tall_ref, wide_ref, plain_ref, rows, cols, seqs, n_col):
    res = labels_ref.shape[1]
    labels = jnp.broadcast_to(labels_ref[...], (8, res))
    own = pltpu.roll(labels, (res - at_ref[0]) % res, 1)[:, :rows]
    spread = (
        lax.broadcasted_iota(jnp.int32, (rows, rows * PROJ), 1) // PROJ
        == lax.broadcasted_iota(jnp.int32, (rows, rows * PROJ), 0)
    )
    lab = nn_dot(own.astype(F32).astype(BF16), spread.astype(F32).astype(BF16))
    lab_ref[...] = lab[:1].astype(jnp.int32)

    there = pltpu.roll(labels, (res - at_ref[1]) % res, 1)[:, :LANES]
    there = jnp.where(lax.broadcasted_iota(jnp.int32, (8, LANES), 1) < cols, there, 0)
    reach = cols
    while reach < LANES:
        there = there + pltpu.roll(there, reach, 1)
        reach *= 2
    depth = jnp.zeros((CHAINS, LANES), jnp.int32)
    for b in range(CHAINS):
        depth += jnp.where(there == b, counts_ref[:, b : b + 1], 0)
    here = lax.broadcasted_iota(jnp.int32, (seqs // n_col, LANES), 0)
    seq = jnp.concatenate([here + (at_ref[2] ^ k) * (seqs // n_col) for k in range(n_col)], axis=0)
    for a in range(CHAINS):
        deep = jnp.broadcast_to(depth[a : a + 1], (seqs, LANES))
        weight = jnp.where(seq < deep, 1.0 / deep.astype(F32), 0.0)
        three = deep % 3 == 0
        for x, part in enumerate((jnp.where(three, 0.0, weight), jnp.where(three, 3.0 * weight, 0.0))):
            tall_ref[a, x] = part.astype(BF16)
            wide_ref[a, x] = part.T[:cols].astype(BF16)
        plain_ref[a] = weight.T[:cols]


def projector(w_ref, wide_w_ref, w_out, wt_ref):
    wide_w_ref[...] = w_ref[...].astype(F32)
    for t in range(PROJ // PER_TILE):
        for q in range(PER_TILE):
            e = t * PER_TILE + q
            w_out[e * PROJ : (e + 1) * PROJ] = wide_w_ref[pl.ds(e, PROJ, stride=PROJ)].astype(BF16)
        block = w_out[t * LANES : (t + 1) * LANES].astype(F32)
        for p in range(PER_TILE):
            wt_ref[p, :, t * LANES : (t + 1) * LANES] = rolled(block.T, p).astype(BF16)


def cost(passes, span, total, seqs):
    return pl.CostEstimate(
        flops=4 * passes * span * total * seqs, bytes_accessed=2 * span * total, transcendentals=0
    )


def back_body(at_ref, labels_hbm, counts_hbm, w_hbm, grad_hbm,
              lab_ref, tall_ref, wide_ref, plain_ref, w_out, back_ref, grad_ref,
              labels_ref, counts_ref, w_ref, wide_w_ref, wt_ref, sems, *, seqs, n_col):
    groups, step, cols, _ = grad_ref.shape
    copies = [
        pltpu.make_async_copy(w_hbm, w_ref, sems.at[groups]),
        pltpu.make_async_copy(labels_hbm, labels_ref, sems.at[groups + 1]),
        pltpu.make_async_copy(counts_hbm, counts_ref, sems.at[groups + 2]),
    ]
    for copy in copies:
        copy.start()

    def grad_of(g):
        return pltpu.make_async_copy(grad_hbm.at[pl.ds(g * step, step)], grad_ref.at[g], sems.at[g])

    for g in range(groups):
        grad_of(g).start()
    for copy in copies:
        copy.wait()
    projector(w_ref, wide_w_ref, w_out, wt_ref)
    masks(at_ref, labels_ref, counts_ref, lab_ref, tall_ref, wide_ref, plain_ref,
          groups * step, cols, seqs, n_col)
    halves = step // PER_TILE

    def group(g, carry):
        grad_of(g).wait()
        blocks = [
            jnp.concatenate([grad_ref[g, half * PER_TILE + p] for half in range(halves)], axis=0)
            for p in range(PER_TILE)
        ]
        for u in range(PROJ * PROJ // WIDE):
            prods = [
                nn_dot(block, wt_ref[p, :, u * WIDE : (u + 1) * WIDE]).astype(BF16)
                for p, block in enumerate(blocks)
            ]
            for half in range(halves):
                for t in range(WIDE // LANES):
                    parts = [
                        prod[half * cols : (half + 1) * cols, t * LANES : (t + 1) * LANES]
                        for prod in prods
                    ]
                    for q, part in enumerate(swap_blocks(parts)):
                        e = u * (WIDE // PROJ) + t * PER_TILE + q
                        at = (g, slice(e * cols, (e + 1) * cols))
                        back_ref[at + (slice(half * LANES, (half + 1) * LANES),)] = part
        return carry

    lax.fori_loop(0, groups, group, 0)


def back_call(at, labels, counts, w, grad, seqs, n_col):
    rows, cols, width = grad.shape
    step = WIDE // PROJ
    groups = rows // step
    labels = labels[None, :]
    return pl.pallas_call(
        lambda *refs: back_body(*refs, seqs=seqs, n_col=n_col),
        in_specs=[SMEM] + [HBM] * 4,
        out_specs=[VMEM] * 7,
        out_shape=[
            jax.ShapeDtypeStruct((1, rows * PROJ), jnp.int32),
            jax.ShapeDtypeStruct((CHAINS, 2, seqs, LANES), BF16),
            jax.ShapeDtypeStruct((CHAINS, 2, cols, seqs), BF16),
            jax.ShapeDtypeStruct((CHAINS, cols, seqs), F32),
            jax.ShapeDtypeStruct(w.shape, BF16),
            pltpu.VMEM((groups, PROJ * cols, WIDE), BF16),
            pltpu.VMEM((groups, step, cols, width), BF16),
        ],
        scratch_shapes=[
            pltpu.VMEM(labels.shape, jnp.int32),
            pltpu.VMEM(counts.shape, jnp.int32),
            pltpu.VMEM(w.shape, BF16),
            pltpu.VMEM(w.shape, F32),
            pltpu.VMEM((PER_TILE, width, PROJ * PROJ), BF16),
            pltpu.SemaphoreType.DMA((groups + 3,)),
        ],
        compiler_params=KERNEL,
        cost_estimate=cost(10, PROJ * cols, rows * PROJ, width),
        name="back",
    )(at, *map(in_hbm, (labels, counts, w, grad)))


def first_chain(at_ref, labels_ref, group):
    return labels_ref[at_ref[0] + group * (WIDE // PROJ)]


def last_chain(at_ref, labels_ref, group):
    return labels_ref[at_ref[0] + (group + 1) * (WIDE // PROJ) - 1]


def slots(chain, count, seqs):
    return pl.ds(pl.multiple_of(chain * seqs, seqs), count * seqs)


def each(first, last, fn):
    def step(k, carry):
        fn(k)
        return carry

    lax.fori_loop(first, last + 1, step, 0)


def lanes_of(group):
    return pl.ds(pl.multiple_of(group * WIDE, WIDE), WIDE)


def masked_left(left_ref, lab_ref, lb_ref, chain, group):
    seqs = left_ref.shape[0]
    lanes = lanes_of(group)
    for side in range(2):
        keep = (lab_ref[:, lanes] == chain + side).astype(F32).astype(BF16)
        lb_ref[side * seqs : (side + 1) * seqs] = left_ref[:, lanes] * keep


def right_grad_body(at_ref, labels_ref, back_ref, left_ref, lab_ref, wide_ref,
                    right_out, q_ref, lb_ref, flip_ref, turn_ref):
    seqs = left_ref.shape[0]
    groups, span, _ = back_ref.shape
    cols = span // PROJ
    first = lambda g: first_chain(at_ref, labels_ref, g)
    last = lambda g: last_chain(at_ref, labels_ref, g)

    def clear(chain):
        q_ref[:, slots(chain, 1, seqs)] = jnp.zeros((span, seqs), F32)

    each(first(0), last(groups - 1) + 1, clear)

    def group(g):
        def two_chains(k):
            chain = first(g) + 2 * k
            masked_left(left_ref, lab_ref, lb_ref, chain, g)
            q_ref[:, slots(chain, 2, seqs)] += nt_dot(back_ref[g], lb_ref[...])

        each(0, (last(g) - first(g)) // 2, two_chains)

    each(0, groups - 1, group)

    def combine(chain, start):
        for e in range(PROJ):
            rows = slice(e * cols, (e + 1) * cols)
            part = q_ref[rows, slots(chain, 1, seqs)] * wide_ref[chain]
            flip_ref[rows] = part if start else flip_ref[rows] + part

    combine(first(0), True)
    each(first(0) + 1, last(groups - 1), lambda chain: combine(chain, False))
    for j in range(cols):
        turn_ref[j * PROJ : (j + 1) * PROJ] = flip_ref[pl.ds(j, PROJ, stride=cols)]
    for t in range(span // LANES):
        rows = slice(t * LANES, (t + 1) * LANES)
        right_out[:, rows] = turn_ref[rows].T.astype(BF16)


def right_grad_call(at, labels, back, left, lab, wide):
    groups, span, _ = back.shape
    total = groups * WIDE
    seqs = left.shape[0]
    return pl.pallas_call(
        right_grad_body,
        in_specs=[SMEM] * 2 + [VMEM] * 4,
        out_specs=VMEM,
        out_shape=jax.ShapeDtypeStruct((seqs, span), BF16),
        scratch_shapes=[
            pltpu.VMEM((span, (CHAINS + 1) * seqs), F32),
            pltpu.VMEM((2 * seqs, WIDE), BF16),
            pltpu.VMEM((span, seqs), F32),
            pltpu.VMEM((span, seqs), F32),
        ],
        compiler_params=KERNEL,
        cost_estimate=cost(10, span, total, seqs),
        name="right_grad",
    )(at, labels, back, left, lab, wide)


def left_grad_body(at_ref, labels_ref, back_ref, lab_ref, right_ref, tall_ref,
                   left_out, rm_ref, part_ref):
    seqs = right_ref.shape[0]
    groups, span, _ = back_ref.shape
    first = lambda g: first_chain(at_ref, labels_ref, g)
    last = lambda g: last_chain(at_ref, labels_ref, g)
    part_ref[...] = (right_ref[...].astype(F32) / 3).astype(BF16)

    def build(chain):
        plain, third = tall_ref[chain, 0], tall_ref[chain, 1]
        for t in range(span // LANES):
            lanes = slice(t * LANES, (t + 1) * LANES)
            rm_ref[slots(chain, 1, seqs), lanes] = (
                right_ref[:, lanes] * plain + part_ref[:, lanes] * third
            )

    each(first(0), last(groups - 1), build)
    rm_ref[slots(last(groups - 1) + 1, 1, seqs)] = jnp.zeros((seqs, span), BF16)

    def group(g):
        lab = lab_ref[:, lanes_of(g)]

        def two_chains(k, total):
            chain = first(g) + 2 * k
            part = nn_dot(rm_ref[slots(chain, 2, seqs)], back_ref[g])
            keep0, keep1 = lab == chain, lab == chain + 1
            return total + jnp.where(keep0, part[:seqs], 0.0) + jnp.where(keep1, part[seqs:], 0.0)

        passes = (last(g) - first(g)) // 2 + 1
        total = lax.fori_loop(0, passes, two_chains, jnp.zeros((seqs, WIDE), F32))
        left_out[:, lanes_of(g)] = total.astype(BF16)

    each(0, groups - 1, group)


def left_grad_call(at, labels, back, lab, right, tall):
    groups, span, _ = back.shape
    total = groups * WIDE
    seqs = right.shape[0]
    return pl.pallas_call(
        left_grad_body,
        in_specs=[SMEM] * 2 + [VMEM] * 4,
        out_specs=VMEM,
        out_shape=jax.ShapeDtypeStruct((seqs, total), BF16),
        scratch_shapes=[
            pltpu.VMEM(((CHAINS + 1) * seqs, span), BF16),
            pltpu.VMEM((seqs, span), BF16),
        ],
        compiler_params=KERNEL,
        cost_estimate=cost(10, span, total, seqs),
        name="left_grad",
    )(at, labels, back, lab, right, tall)


def outer_body(at_ref, labels_ref, left_ref, lab_ref, right_ref, wide_ref, grad_ref,
               outer_ref, weight_out, rm_ref, lb_ref, even_ref, odd_ref, sum_ref, turn_ref, flip_ref, part_ref):
    seqs = left_ref.shape[0]
    span = right_ref.shape[1]
    cols = span // PROJ
    groups, step, _, width = grad_ref.shape
    first = lambda g: first_chain(at_ref, labels_ref, g)
    last = lambda g: last_chain(at_ref, labels_ref, g)
    for t in range(span // LANES):
        lanes = slice(t * LANES, (t + 1) * LANES)
        flipped = right_ref[:, lanes].astype(F32).T
        flip_ref[lanes] = flipped.astype(BF16)
        part_ref[lanes] = (flipped / 3).astype(BF16)

    def build(chain):
        plain, third = wide_ref[chain, 0], wide_ref[chain, 1]
        for e in range(PROJ):
            rows = slice(e * cols, (e + 1) * cols)
            to = e % PER_TILE * (PROJ // PER_TILE) + e // PER_TILE
            rm_ref[to * cols : (to + 1) * cols, slots(chain, 1, seqs)] = (
                flip_ref[rows] * plain + part_ref[rows] * third
            )

    each(first(0), last(groups - 1), build)
    rm_ref[:, slots(last(groups - 1) + 1, 1, seqs)] = jnp.zeros((span, seqs), BF16)
    sum_ref[...] = jnp.zeros_like(sum_ref)
    quarter = span // PER_TILE

    def product(chain, g, acc_ref, add):
        masked_left(left_ref, lab_ref, lb_ref, chain, g)
        for q in range(PER_TILE):
            rows = slice(q * quarter, (q + 1) * quarter)
            part = nn_dot(rm_ref[rows, slots(chain, 2, seqs)], rolled(lb_ref[...], q))
            acc_ref[rows] = acc_ref[rows] + part if add else part

    def rest(g, acc_ref):
        each(1, (last(g) - first(g)) // 2, lambda k: product(first(g) + 2 * k, g, acc_ref, True))

    def finish(g, acc_ref):
        for half in range(WIDE // LANES):
            lanes = slice(half * LANES, (half + 1) * LANES)
            for t in range(PROJ // PER_TILE):
                parts = []
                for q in range(PER_TILE):
                    e = q * (PROJ // PER_TILE) + t
                    parts.append(acc_ref[e * cols : (e + 1) * cols, lanes].astype(BF16))
                turned = swap_blocks(parts)
                for p in range(PER_TILE):
                    i = half * PER_TILE + p
                    at = (g, slice(i * cols, (i + 1) * cols), slice(t * LANES, (t + 1) * LANES))
                    outer_ref[at] = turned[p]
        flat = grad_ref[g].reshape(step * cols, width)
        sum_ref[...] += nn_dot(flat.T, outer_ref[g])

    def turn(g, acc_ref, next_ref):
        product(first(g + 1), g + 1, next_ref, False)
        finish(g, acc_ref)
        rest(g + 1, next_ref)

    def two_groups(i):
        turn(2 * i, even_ref, odd_ref)
        turn(2 * i + 1, odd_ref, even_ref)

    product(first(0), 0, even_ref, False)
    rest(0, even_ref)
    each(0, groups // 2 - 2, two_groups)
    turn(groups - 2, even_ref, odd_ref)
    finish(groups - 1, odd_ref)
    for t in range(PROJ * PROJ // LANES):
        part = slice(t * LANES, (t + 1) * LANES)
        turn_ref[part] = sum_ref[:, part].T
    for c in range(PROJ):
        weight_out[c * PROJ : (c + 1) * PROJ] = turn_ref[pl.ds(c, PROJ, stride=PROJ)]


def outer_call(at, labels, left, lab, right, wide, grad):
    groups, step, cols, width = grad.shape
    seqs, total = left.shape
    span = right.shape[1]
    return pl.pallas_call(
        outer_body,
        in_specs=[SMEM] * 2 + [VMEM] * 5,
        out_specs=[VMEM] * 2,
        out_shape=[
            pltpu.VMEM((groups, step * cols, PROJ * PROJ), BF16),
            jax.ShapeDtypeStruct((PROJ * PROJ, width), F32),
        ],
        scratch_shapes=[
            pltpu.VMEM((span, (CHAINS + 1) * seqs), BF16),
            pltpu.VMEM((2 * seqs, WIDE), BF16),
            pltpu.VMEM((span, WIDE), F32),
            pltpu.VMEM((span, WIDE), F32),
            pltpu.VMEM((width, PROJ * PROJ), F32),
            pltpu.VMEM((PROJ * PROJ, width), F32),
            pltpu.VMEM((span, seqs), BF16),
            pltpu.VMEM((span, seqs), BF16),
        ],
        compiler_params=KERNEL,
        cost_estimate=cost(20, span, total, seqs),
        name="outer",
    )(at, labels, left, lab, right, wide, grad)


def pair_body(outer_ref, w_ref, offset_ref, pair_ref):
    _, pairs, _ = outer_ref.shape
    here = pair_ref.shape[0] // pairs
    for g in range(here):
        pair = nn_dot(outer_ref[pl.program_id(0) * here + g], w_ref[...]) + offset_ref[...]
        pair_ref[g * pairs : (g + 1) * pairs] = pair.astype(BF16)


def pair_call(outer, w, offset):
    groups, pairs, feats = outer.shape
    width = w.shape[1]
    steps = 2
    return pl.pallas_call(
        pair_body,
        grid=(steps,),
        in_specs=[VMEM] * 3,
        out_specs=pl.BlockSpec((groups * pairs // steps, width), lambda g: (g, 0)),
        out_shape=jax.ShapeDtypeStruct((groups * pairs, width), BF16),
        compiler_params=KERNEL,
        cost_estimate=pl.CostEstimate(
            flops=2 * groups * pairs * feats * width,
            bytes_accessed=2 * groups * pairs * width,
            transcendentals=0,
        ),
        name="pair",
    )(outer, w, offset)


class Pairs:
    def __init__(self, n_row, n_col):
        self.n_row, self.n_col = n_row, n_col
        self.per_row = n_col // n_row
        self.row = lax.axis_index("row").astype(jnp.uint32)
        self.col = lax.axis_index("col").astype(jnp.uint32)

    def col_swap(self, value, k):
        return lax.ppermute(value, "col", [(t ^ k, t) for t in range(self.n_col)])

    def row_swap(self, value, k):
        return lax.ppermute(value, "row", [(t ^ k, t) for t in range(self.n_row)])

    def right_along_row(self, right):
        others = [self.row_swap(right, k) for k in range(1, self.n_row)]
        return [right] + others

    def right_pieces(self, by_row):
        m = self.per_row
        here, lanes = by_row[0].shape
        lanes //= m
        by_row = jnp.stack(by_row)
        pieces = []
        for k in range(self.n_col):
            q = self.col ^ k
            at = ((q // m) ^ self.row, jnp.uint32(0), (q % m) * lanes)
            pieces.append(lax.dynamic_slice(by_row, at, (1, here, lanes))[0])
        return pieces

    def right_along_col(self, pieces):
        return jnp.concatenate([self.col_swap(p, k) if k else p for k, p in enumerate(pieces)])

    def right_grad_home(self, grad):
        n, m = self.n_col, self.per_row
        here, lanes = grad.shape[0] // n, grad.shape[1]
        total = jnp.zeros((m, here, lanes), F32)
        slot = lax.broadcasted_iota(jnp.uint32, (m, 1, 1), 0)
        for k in range(n):
            t = (self.row * m + self.col % m) ^ k
            block = lax.dynamic_slice_in_dim(grad, (t ^ self.col) * here, here, 0)
            pairs = []
            for r in range(self.n_row):
                for q in range(n):
                    pairs.append((r * n + q, (q // m) * n + ((r * m + q % m) ^ k)))
            got = lax.ppermute(block, ("row", "col"), pairs).astype(F32)[None]
            total += got if m == 1 else jnp.where(slot == (self.col ^ k) % m, got, 0)
        return total.swapaxes(0, 1).reshape(here, m * lanes).astype(BF16)

    def weight_over_row(self, weight):
        n = self.n_row
        size = weight.shape[0] // n
        sent = weight.astype(BF16).reshape(n, size, -1)
        total = lax.dynamic_index_in_dim(weight.reshape(n, size, -1), self.row, 0, keepdims=False)
        for k in range(1, n):
            piece = lax.dynamic_index_in_dim(sent, self.row ^ k, 0, keepdims=False)
            total += self.row_swap(piece, k).astype(F32)
        return total

    def weight_over_col(self, total):
        mine = total.astype(BF16)
        for k in range(1, self.n_col):
            total += self.col_swap(mine, k).astype(F32)
        return total.astype(BF16)

    def weight_to_all(self, mine):
        n = self.n_row
        which = lax.broadcasted_iota(jnp.uint32, (n, 1, 1), 0) ^ self.row
        shares = mine[None]
        for k in range(1, n):
            shares = jnp.where(which == k, self.row_swap(mine, k)[None], shares)
        return shares.reshape(n * mine.shape[0], mine.shape[1])


def after(value, *others):
    return lax.optimization_barrier((value,) + others)[0]


def shards(n_row, n_col, alignment_tensor, gain, shift, first_projector, second_projector,
           final_projector, final_offset, labels, counts, grad):
    ring = Pairs(n_row, n_col)
    here, rows, _ = alignment_tensor.shape
    cols, width = grad.shape[1:]
    seqs = here * n_col
    left, right = project_call(
        alignment_tensor, gain[None, :], shift[None, :], first_projector.T, second_projector.T, cols
    )
    by_row = ring.right_along_row(right)
    left = jnp.concatenate([left] + [ring.col_swap(left, k) for k in range(1, n_col)])

    at = jnp.stack([ring.row * rows, ring.col * cols, ring.col]).astype(jnp.int32)
    lab, tall, wide, plain, w, back, grad = back_call(
        at, labels, counts, after(final_projector, right), grad, seqs, n_col
    )
    mine = ring.right_along_col(ring.right_pieces(by_row))
    back, grad = in_vmem(back), in_vmem(grad)
    right_grad = right_grad_call(at, labels, back, left, lab, plain)

    right = after(mine, right_grad)
    grad_right = ring.right_grad_home(right_grad)
    outer, weight = outer_call(
        at, labels, left, lab, right, wide, grad
    )
    share = ring.weight_over_row(weight)
    left_grad = left_grad_call(at, labels, back, after(lab, weight), right, tall)
    share = after(share, left_grad)

    total = left_grad[:here].astype(F32)
    for k in range(1, n_col):
        total += ring.col_swap(left_grad[k * here : (k + 1) * here], k).astype(F32)
    adjoint_first = total.astype(BF16)
    pair_update = pair_call(in_vmem(outer), after(w, left_grad, share), final_offset[None, :])
    pair_update = pair_update.reshape(rows, cols, width)
    mine = after(ring.weight_over_col(share), pair_update)
    grad_w_out = ring.weight_to_all(mine).astype(F32) / (n_row * rows)
    return pair_update, adjoint_first, grad_right, grad_w_out


def solution(mesh):
    in_specs = (
        P(("parts", "col"), "row", None),
        P(),
        P(),
        P(),
        P(),
        P(),
        P(),
        P("parts"),
        P("parts", None),
        P(("parts", "row"), "col", None),
    )
    out_specs = (
        P(("parts", "row"), "col", None),
        P(("parts", "col"), "row"),
        P(("parts", "col"), "row"),
        P("parts", None),
    )

    def body(*args):
        return shards(mesh.shape["row"], mesh.shape["col"], *args)

    return jax.shard_map(body, mesh=mesh, in_specs=in_specs, out_specs=out_specs, check_vma=False)
```

```python
import functools

import jax
import jax.numpy as jnp
from jax import lax
from jax.experimental import pallas as pl
from jax.experimental.pallas import tpu as pltpu
from jax.sharding import PartitionSpec as P


PROJ = 32
CHAINS = 8
LANES = 128
PER_TILE = LANES // PROJ
WIDE = 256
F32 = jnp.float32
BF16 = jnp.bfloat16
VMEM = pl.BlockSpec(memory_space=pltpu.VMEM)
KERNEL = pltpu.CompilerParams(vmem_limit_bytes=24 << 20)
HBM = pl.BlockSpec(memory_space=pltpu.HBM)
SMEM = pl.BlockSpec(memory_space=pltpu.SMEM)


def swap_blocks(parts):
    lane = lax.broadcasted_iota(jnp.int32, parts[0].shape, 1)
    outs = []
    for q in range(PER_TILE):
        out = parts[(PER_TILE - 1 - q) % PER_TILE]
        for block in range(PER_TILE - 2, -1, -1):
            out = jnp.where(lane < (block + 1) * PROJ, parts[(block - q) % PER_TILE], out)
        outs.append(pltpu.roll(out, LANES - q * PROJ, 1) if q else out)
    return outs


def rolled(value, p):
    if not p:
        return value
    return jnp.concatenate(
        [pltpu.roll(value[:, t : t + LANES], p * PROJ, 1) for t in range(0, value.shape[1], LANES)],
        axis=1,
    )


def nt_dot(a, b):
    return lax.dot_general(a, b, (((1,), (1,)), ((), ())), preferred_element_type=F32)


def nn_dot(a, b):
    return lax.dot_general(a, b, (((1,), (0,)), ((), ())), preferred_element_type=F32)


def in_vmem(value):
    return pltpu.with_memory_space_constraint(value, pltpu.VMEM)


def in_hbm(value):
    return pltpu.with_memory_space_constraint(value, pltpu.HBM)


def project_body(x_hbm, gain_hbm, shift_hbm, first_hbm, second_hbm, left_ref, right_ref,
                 x_ref, gain_ref, shift_ref, w_ref, proj_ref, turn_ref, out_ref, sems, *, cols):
    chunks, chunk, rows, feats = x_ref.shape
    small = [
        pltpu.make_async_copy(gain_hbm, gain_ref, sems.at[chunks]),
        pltpu.make_async_copy(shift_hbm, shift_ref, sems.at[chunks + 1]),
        pltpu.make_async_copy(first_hbm, w_ref.at[pl.ds(0, PROJ)], sems.at[chunks + 2]),
        pltpu.make_async_copy(second_hbm, w_ref.at[pl.ds(PROJ, PROJ)], sems.at[chunks + 3]),
    ]
    big = [
        pltpu.make_async_copy(x_hbm.at[pl.ds(g * chunk, chunk)], x_ref.at[g], sems.at[g])
        for g in range(chunks)
    ]
    for copy in big[:1] + small + big[1:]:
        copy.start()
    w_ref[2 * PROJ :] = jnp.zeros((LANES - 2 * PROJ, feats), BF16)
    for copy in small:
        copy.wait()
    for g in range(chunks):
        big[g].wait()
        x = x_ref[g].astype(F32).reshape(chunk * rows, feats)
        center = x - jnp.mean(x, axis=-1, keepdims=True)
        spread = jnp.mean(center * center, axis=-1, keepdims=True)
        normed = center * lax.rsqrt(spread + 1e-05) * gain_ref[...] + shift_ref[...]
        at = slice(g * chunk * rows, (g + 1) * chunk * rows)
        proj_ref[at] = nt_dot(normed.astype(BF16), w_ref[...])
    project_layout(proj_ref, turn_ref, out_ref, left_ref, right_ref, rows, cols)


def project_layout(proj_ref, turn_ref, out_ref, left_ref, right_ref, rows, cols):
    here = left_ref.shape[0]
    lane = lax.broadcasted_iota(jnp.int32, (here, LANES), 1)
    for t in range(rows // PER_TILE):
        tile = proj_ref[pl.ds(t * PER_TILE, here, stride=rows)]
        for p in range(1, PER_TILE):
            part = proj_ref[pl.ds(t * PER_TILE + p, here, stride=rows)]
            tile = jnp.where(lane < p * PROJ, tile, pltpu.roll(part, p * PROJ, 1))
        left_ref[:, t * LANES : (t + 1) * LANES] = tile.astype(BF16)

    tiles = here * rows // LANES
    for t in range(tiles):
        flipped = proj_ref[t * LANES : (t + 1) * LANES].T
        turn_ref[t * PROJ : (t + 1) * PROJ] = flipped[PROJ : 2 * PROJ]
    seqs = LANES // rows
    per = LANES // cols
    lane = lax.broadcasted_iota(jnp.int32, (tiles, LANES), 1)
    for block in range(rows // cols):
        for t in range(PROJ // per):
            at = (block * (PROJ // per) + t) * LANES
            parts = [turn_ref[pl.ds(t * per + p, tiles, stride=PROJ)] for p in range(per)]
            for u in range(seqs):
                start = u * rows + block * cols
                tile = None
                for p, part in enumerate(parts):
                    amount = (p * cols - start) % LANES
                    part = pltpu.roll(part, amount, 1) if amount else part
                    tile = part if tile is None else jnp.where(lane < p * cols, tile, part)
                out_ref[pl.ds(u, tiles, stride=seqs), :] = tile
            right_ref[:, at : at + LANES] = out_ref[...].astype(BF16)


def project_call(x, gain, shift, first, second, cols):
    here, rows, feats = x.shape
    chunk = min(here, max(1, 2 * WIDE // rows))
    return pl.pallas_call(
        lambda *refs: project_body(*refs, cols=cols),
        in_specs=[HBM] * 5,
        out_specs=[VMEM] * 2,
        out_shape=[jax.ShapeDtypeStruct((here, rows * PROJ), BF16)] * 2,
        scratch_shapes=[
            pltpu.VMEM((here // chunk, chunk, rows, feats), BF16),
            pltpu.VMEM(gain.shape, F32),
            pltpu.VMEM(shift.shape, F32),
            pltpu.VMEM((LANES, feats), BF16),
            pltpu.VMEM((here * rows, LANES), F32),
            pltpu.VMEM((here * rows // LANES * PROJ, LANES), F32),
            pltpu.VMEM((here, LANES), F32),
            pltpu.SemaphoreType.DMA((here // chunk + 4,)),
        ],
        compiler_params=KERNEL,
        name="project",
    )(*map(in_hbm, (x, gain, shift, first, second)))


def masks(at_ref, labels_ref, counts_ref, lab_ref, tall_ref, wide_ref, plain_ref, rows, cols, seqs, n_col):
    res = labels_ref.shape[1]
    labels = jnp.broadcast_to(labels_ref[...], (8, res))
    own = pltpu.roll(labels, (res - at_ref[0]) % res, 1)[:, :rows]
    spread = (
        lax.broadcasted_iota(jnp.int32, (rows, rows * PROJ), 1) // PROJ
        == lax.broadcasted_iota(jnp.int32, (rows, rows * PROJ), 0)
    )
    lab = nn_dot(own.astype(F32).astype(BF16), spread.astype(F32).astype(BF16))
    lab_ref[...] = lab[:1].astype(jnp.int32)

    there = pltpu.roll(labels, (res - at_ref[1]) % res, 1)[:, :LANES]
    there = jnp.where(lax.broadcasted_iota(jnp.int32, (8, LANES), 1) < cols, there, 0)
    reach = cols
    while reach < LANES:
        there = there + pltpu.roll(there, reach, 1)
        reach *= 2
    depth = jnp.zeros((CHAINS, LANES), jnp.int32)
    for b in range(CHAINS):
        depth += jnp.where(there == b, counts_ref[:, b : b + 1], 0)
    here = lax.broadcasted_iota(jnp.int32, (seqs // n_col, LANES), 0)
    seq = jnp.concatenate([here + (at_ref[2] ^ k) * (seqs // n_col) for k in range(n_col)], axis=0)
    for a in range(CHAINS):
        deep = jnp.broadcast_to(depth[a : a + 1], (seqs, LANES))
        weight = jnp.where(seq < deep, 1.0 / deep.astype(F32), 0.0)
        three = deep % 3 == 0
        for x, part in enumerate((jnp.where(three, 0.0, weight), jnp.where(three, 3.0 * weight, 0.0))):
            tall_ref[a, x] = part.astype(BF16)
            wide_ref[a, x] = part.T[:cols].astype(BF16)
        plain_ref[a] = weight.T[:cols]


def projector(w_ref, wide_w_ref, w_out, wt_ref):
    wide_w_ref[...] = w_ref[...].astype(F32)
    for t in range(PROJ // PER_TILE):
        for q in range(PER_TILE):
            e = t * PER_TILE + q
            w_out[e * PROJ : (e + 1) * PROJ] = wide_w_ref[pl.ds(e, PROJ, stride=PROJ)].astype(BF16)
        block = w_out[t * LANES : (t + 1) * LANES].astype(F32)
        for p in range(PER_TILE):
            wt_ref[p, :, t * LANES : (t + 1) * LANES] = rolled(block.T, p).astype(BF16)


def cost(passes, span, total, seqs):
    return pl.CostEstimate(
        flops=4 * passes * span * total * seqs, bytes_accessed=2 * span * total, transcendentals=0
    )


def back_body(at_ref, labels_hbm, counts_hbm, w_hbm, grad_hbm,
              lab_ref, tall_ref, wide_ref, plain_ref, w_out, back_ref, grad_ref,
              labels_ref, counts_ref, w_ref, wide_w_ref, wt_ref, sems, *, seqs, n_col):
    groups, step, cols, _ = grad_ref.shape
    copies = [
        pltpu.make_async_copy(w_hbm, w_ref, sems.at[groups]),
        pltpu.make_async_copy(labels_hbm, labels_ref, sems.at[groups + 1]),
        pltpu.make_async_copy(counts_hbm, counts_ref, sems.at[groups + 2]),
    ]
    for copy in copies:
        copy.start()

    def grad_of(g):
        return pltpu.make_async_copy(grad_hbm.at[pl.ds(g * step, step)], grad_ref.at[g], sems.at[g])

    for g in range(groups):
        grad_of(g).start()
    for copy in copies:
        copy.wait()
    projector(w_ref, wide_w_ref, w_out, wt_ref)
    masks(at_ref, labels_ref, counts_ref, lab_ref, tall_ref, wide_ref, plain_ref,
          groups * step, cols, seqs, n_col)
    halves = step // PER_TILE

    def group(g):
        blocks = [
            jnp.concatenate([grad_ref[g, half * PER_TILE + p] for half in range(halves)], axis=0)
            for p in range(PER_TILE)
        ]
        for u in range(PROJ * PROJ // WIDE):
            prods = [
                nn_dot(block, wt_ref[p, :, u * WIDE : (u + 1) * WIDE]).astype(BF16)
                for p, block in enumerate(blocks)
            ]
            for half in range(halves):
                for t in range(WIDE // LANES):
                    parts = [
                        prod[half * cols : (half + 1) * cols, t * LANES : (t + 1) * LANES]
                        for prod in prods
                    ]
                    for q, part in enumerate(swap_blocks(parts)):
                        e = u * (WIDE // PROJ) + t * PER_TILE + q
                        at = (g, slice(e * cols, (e + 1) * cols))
                        back_ref[at + (slice(half * LANES, (half + 1) * LANES),)] = part

    def two_groups(i):
        grad_of(2 * i).wait()
        grad_of(2 * i + 1).wait()
        group(2 * i)
        group(2 * i + 1)

    each(0, groups // 2 - 1, two_groups)


def back_call(at, labels, counts, w, grad, seqs, n_col):
    rows, cols, width = grad.shape
    step = WIDE // PROJ
    groups = rows // step
    labels = labels[None, :]
    return pl.pallas_call(
        lambda *refs: back_body(*refs, seqs=seqs, n_col=n_col),
        in_specs=[SMEM] + [HBM] * 4,
        out_specs=[VMEM] * 7,
        out_shape=[
            jax.ShapeDtypeStruct((1, rows * PROJ), jnp.int32),
            jax.ShapeDtypeStruct((CHAINS, 2, seqs, LANES), BF16),
            jax.ShapeDtypeStruct((CHAINS, 2, cols, seqs), BF16),
            jax.ShapeDtypeStruct((CHAINS, cols, seqs), F32),
            jax.ShapeDtypeStruct(w.shape, BF16),
            pltpu.VMEM((groups, PROJ * cols, WIDE), BF16),
            pltpu.VMEM((groups, step, cols, width), BF16),
        ],
        scratch_shapes=[
            pltpu.VMEM(labels.shape, jnp.int32),
            pltpu.VMEM(counts.shape, jnp.int32),
            pltpu.VMEM(w.shape, BF16),
            pltpu.VMEM(w.shape, F32),
            pltpu.VMEM((PER_TILE, width, PROJ * PROJ), BF16),
            pltpu.SemaphoreType.DMA((groups + 3,)),
        ],
        compiler_params=KERNEL,
        cost_estimate=cost(10, PROJ * cols, rows * PROJ, width),
        name="back",
    )(at, *map(in_hbm, (labels, counts, w, grad)))


def first_chain(at_ref, labels_ref, group):
    return labels_ref[at_ref[0] + group * (WIDE // PROJ)]


def last_chain(at_ref, labels_ref, group):
    return labels_ref[at_ref[0] + (group + 1) * (WIDE // PROJ) - 1]


def slots(chain, count, seqs):
    return pl.ds(pl.multiple_of(chain * seqs, seqs), count * seqs)


def each(first, last, fn):
    def step(k, carry):
        fn(k)
        return carry

    lax.fori_loop(first, last + 1, step, 0)


def lanes_of(group):
    return pl.ds(pl.multiple_of(group * WIDE, WIDE), WIDE)


def masked_left(left_ref, lab_ref, lb_ref, chain, group):
    seqs = left_ref.shape[0]
    lanes = lanes_of(group)
    for side in range(2):
        keep = (lab_ref[:, lanes] == chain + side).astype(F32).astype(BF16)
        lb_ref[side * seqs : (side + 1) * seqs] = left_ref[:, lanes] * keep


def right_grad_body(at_ref, labels_ref, back_ref, left_ref, lab_ref, wide_ref,
                    right_out, q_ref, lb_ref, flip_ref, turn_ref):
    seqs = left_ref.shape[0]
    groups, span, _ = back_ref.shape
    cols = span // PROJ
    first = lambda g: first_chain(at_ref, labels_ref, g)
    last = lambda g: last_chain(at_ref, labels_ref, g)

    def clear(chain):
        q_ref[:, slots(chain, 1, seqs)] = jnp.zeros((span, seqs), F32)

    each(first(0), last(groups - 1) + 1, clear)

    def group(g):
        def two_chains(k):
            chain = first(g) + 2 * k
            masked_left(left_ref, lab_ref, lb_ref, chain, g)
            q_ref[:, slots(chain, 2, seqs)] += nt_dot(back_ref[g], lb_ref[...])

        each(0, (last(g) - first(g)) // 2, two_chains)

    each(0, groups - 1, group)

    def combine(chain, start):
        for e in range(PROJ):
            rows = slice(e * cols, (e + 1) * cols)
            part = q_ref[rows, slots(chain, 1, seqs)] * wide_ref[chain]
            flip_ref[rows] = part if start else flip_ref[rows] + part

    combine(first(0), True)
    each(first(0) + 1, last(groups - 1), lambda chain: combine(chain, False))
    for j in range(cols):
        turn_ref[j * PROJ : (j + 1) * PROJ] = flip_ref[pl.ds(j, PROJ, stride=cols)]
    for t in range(span // LANES):
        rows = slice(t * LANES, (t + 1) * LANES)
        right_out[:, rows] = turn_ref[rows].T.astype(BF16)


def right_grad_call(at, labels, back, left, lab, wide):
    groups, span, _ = back.shape
    total = groups * WIDE
    seqs = left.shape[0]
    return pl.pallas_call(
        right_grad_body,
        in_specs=[SMEM] * 2 + [VMEM] * 4,
        out_specs=VMEM,
        out_shape=jax.ShapeDtypeStruct((seqs, span), BF16),
        scratch_shapes=[
            pltpu.VMEM((span, (CHAINS + 1) * seqs), F32),
            pltpu.VMEM((2 * seqs, WIDE), BF16),
            pltpu.VMEM((span, seqs), F32),
            pltpu.VMEM((span, seqs), F32),
        ],
        compiler_params=KERNEL,
        cost_estimate=cost(10, span, total, seqs),
        name="right_grad",
    )(at, labels, back, left, lab, wide)


def left_grad_body(at_ref, labels_ref, back_ref, lab_ref, right_ref, tall_ref,
                   left_out, rm_ref, part_ref):
    seqs = right_ref.shape[0]
    groups, span, _ = back_ref.shape
    first = lambda g: first_chain(at_ref, labels_ref, g)
    last = lambda g: last_chain(at_ref, labels_ref, g)
    part_ref[...] = (right_ref[...].astype(F32) / 3).astype(BF16)

    def build(chain):
        plain, third = tall_ref[chain, 0], tall_ref[chain, 1]
        for t in range(span // LANES):
            lanes = slice(t * LANES, (t + 1) * LANES)
            rm_ref[slots(chain, 1, seqs), lanes] = (
                right_ref[:, lanes] * plain + part_ref[:, lanes] * third
            )

    each(first(0), last(groups - 1), build)
    rm_ref[slots(last(groups - 1) + 1, 1, seqs)] = jnp.zeros((seqs, span), BF16)

    def two_chains(g, k, total):
        lab = lab_ref[:, lanes_of(g)]
        chain = first(g) + 2 * k
        part = nn_dot(rm_ref[slots(chain, 2, seqs)], back_ref[g])
        keep0, keep1 = lab == chain, lab == chain + 1
        part = jnp.where(keep0, part[:seqs], 0.0) + jnp.where(keep1, part[seqs:], 0.0)
        return part if total is None else total + part

    def two_groups(i):
        totals = [two_chains(g, 0, None) for g in (2 * i, 2 * i + 1)]
        for g, total in zip((2 * i, 2 * i + 1), totals):
            more = functools.partial(two_chains, g)
            total = lax.fori_loop(1, (last(g) - first(g)) // 2 + 1, more, total)
            left_out[:, lanes_of(g)] = total.astype(BF16)

    each(0, groups // 2 - 1, two_groups)


def left_grad_call(at, labels, back, lab, right, tall):
    groups, span, _ = back.shape
    total = groups * WIDE
    seqs = right.shape[0]
    return pl.pallas_call(
        left_grad_body,
        in_specs=[SMEM] * 2 + [VMEM] * 4,
        out_specs=VMEM,
        out_shape=jax.ShapeDtypeStruct((seqs, total), BF16),
        scratch_shapes=[
            pltpu.VMEM(((CHAINS + 1) * seqs, span), BF16),
            pltpu.VMEM((seqs, span), BF16),
        ],
        compiler_params=KERNEL,
        cost_estimate=cost(10, span, total, seqs),
        name="left_grad",
    )(at, labels, back, lab, right, tall)


def outer_body(at_ref, labels_ref, left_ref, lab_ref, right_ref, wide_ref, grad_ref,
               outer_ref, weight_out, rm_ref, lb_ref, even_ref, odd_ref, sum_ref, turn_ref, flip_ref, part_ref):
    seqs = left_ref.shape[0]
    span = right_ref.shape[1]
    cols = span // PROJ
    groups, step, _, width = grad_ref.shape
    first = lambda g: first_chain(at_ref, labels_ref, g)
    last = lambda g: last_chain(at_ref, labels_ref, g)
    for t in range(span // LANES):
        lanes = slice(t * LANES, (t + 1) * LANES)
        flipped = right_ref[:, lanes].astype(F32).T
        flip_ref[lanes] = flipped.astype(BF16)
        part_ref[lanes] = (flipped / 3).astype(BF16)

    def build(chain):
        plain, third = wide_ref[chain, 0], wide_ref[chain, 1]
        for e in range(PROJ):
            rows = slice(e * cols, (e + 1) * cols)
            to = e % PER_TILE * (PROJ // PER_TILE) + e // PER_TILE
            rm_ref[to * cols : (to + 1) * cols, slots(chain, 1, seqs)] = (
                flip_ref[rows] * plain + part_ref[rows] * third
            )

    each(first(0), last(groups - 1), build)
    rm_ref[:, slots(last(groups - 1) + 1, 1, seqs)] = jnp.zeros((span, seqs), BF16)
    sum_ref[...] = jnp.zeros_like(sum_ref)
    quarter = span // PER_TILE

    def product(chain, g, acc_ref, add):
        masked_left(left_ref, lab_ref, lb_ref, chain, g)
        for q in range(PER_TILE):
            rows = slice(q * quarter, (q + 1) * quarter)
            part = nn_dot(rm_ref[rows, slots(chain, 2, seqs)], rolled(lb_ref[...], q))
            acc_ref[rows] = acc_ref[rows] + part if add else part

    def rest(g, acc_ref):
        each(1, (last(g) - first(g)) // 2, lambda k: product(first(g) + 2 * k, g, acc_ref, True))

    def finish(g, acc_ref):
        for half in range(WIDE // LANES):
            lanes = slice(half * LANES, (half + 1) * LANES)
            for t in range(PROJ // PER_TILE):
                parts = []
                for q in range(PER_TILE):
                    e = q * (PROJ // PER_TILE) + t
                    parts.append(acc_ref[e * cols : (e + 1) * cols, lanes].astype(BF16))
                turned = swap_blocks(parts)
                for p in range(PER_TILE):
                    i = half * PER_TILE + p
                    at = (g, slice(i * cols, (i + 1) * cols), slice(t * LANES, (t + 1) * LANES))
                    outer_ref[at] = turned[p]
        flat = grad_ref[g].reshape(step * cols, width)
        sum_ref[...] += nn_dot(flat.T, outer_ref[g])

    def turn(g, acc_ref, next_ref):
        product(first(g + 1), g + 1, next_ref, False)
        finish(g, acc_ref)
        rest(g + 1, next_ref)

    def two_groups(i):
        turn(2 * i, even_ref, odd_ref)
        turn(2 * i + 1, odd_ref, even_ref)

    product(first(0), 0, even_ref, False)
    rest(0, even_ref)
    each(0, groups // 2 - 2, two_groups)
    turn(groups - 2, even_ref, odd_ref)
    finish(groups - 1, odd_ref)
    for t in range(PROJ * PROJ // LANES):
        part = slice(t * LANES, (t + 1) * LANES)
        turn_ref[part] = sum_ref[:, part].T
    for c in range(PROJ):
        weight_out[c * PROJ : (c + 1) * PROJ] = turn_ref[pl.ds(c, PROJ, stride=PROJ)]


def outer_call(at, labels, left, lab, right, wide, grad):
    groups, step, cols, width = grad.shape
    seqs, total = left.shape
    span = right.shape[1]
    return pl.pallas_call(
        outer_body,
        in_specs=[SMEM] * 2 + [VMEM] * 5,
        out_specs=[VMEM] * 2,
        out_shape=[
            pltpu.VMEM((groups, step * cols, PROJ * PROJ), BF16),
            jax.ShapeDtypeStruct((PROJ * PROJ, width), F32),
        ],
        scratch_shapes=[
            pltpu.VMEM((span, (CHAINS + 1) * seqs), BF16),
            pltpu.VMEM((2 * seqs, WIDE), BF16),
            pltpu.VMEM((span, WIDE), F32),
            pltpu.VMEM((span, WIDE), F32),
            pltpu.VMEM((width, PROJ * PROJ), F32),
            pltpu.VMEM((PROJ * PROJ, width), F32),
            pltpu.VMEM((span, seqs), BF16),
            pltpu.VMEM((span, seqs), BF16),
        ],
        compiler_params=KERNEL,
        cost_estimate=cost(20, span, total, seqs),
        name="outer",
    )(at, labels, left, lab, right, wide, grad)


def pair_body(outer_ref, w_ref, offset_ref, pair_ref):
    _, pairs, _ = outer_ref.shape
    here = pair_ref.shape[0] // pairs
    for g in range(here):
        pair = nn_dot(outer_ref[pl.program_id(0) * here + g], w_ref[...]) + offset_ref[...]
        pair_ref[g * pairs : (g + 1) * pairs] = pair.astype(BF16)


def pair_call(outer, w, offset):
    groups, pairs, feats = outer.shape
    width = w.shape[1]
    steps = 2
    return pl.pallas_call(
        pair_body,
        grid=(steps,),
        in_specs=[VMEM] * 3,
        out_specs=pl.BlockSpec((groups * pairs // steps, width), lambda g: (g, 0)),
        out_shape=jax.ShapeDtypeStruct((groups * pairs, width), BF16),
        compiler_params=KERNEL,
        cost_estimate=pl.CostEstimate(
            flops=2 * groups * pairs * feats * width,
            bytes_accessed=2 * groups * pairs * width,
            transcendentals=0,
        ),
        name="pair",
    )(outer, w, offset)


class Pairs:
    def __init__(self, n_row, n_col):
        self.n_row, self.n_col = n_row, n_col
        self.per_row = n_col // n_row
        self.row = lax.axis_index("row").astype(jnp.uint32)
        self.col = lax.axis_index("col").astype(jnp.uint32)

    def col_swap(self, value, k):
        return lax.ppermute(value, "col", [(t ^ k, t) for t in range(self.n_col)])

    def row_swap(self, value, k):
        return lax.ppermute(value, "row", [(t ^ k, t) for t in range(self.n_row)])

    def right_along_row(self, right):
        others = [self.row_swap(right, k) for k in range(1, self.n_row)]
        return [right] + others

    def right_pieces(self, by_row):
        m = self.per_row
        here, lanes = by_row[0].shape
        lanes //= m
        by_row = jnp.stack(by_row)
        pieces = []
        for k in range(self.n_col):
            q = self.col ^ k
            at = ((q // m) ^ self.row, jnp.uint32(0), (q % m) * lanes)
            pieces.append(lax.dynamic_slice(by_row, at, (1, here, lanes))[0])
        return pieces

    def right_along_col(self, pieces):
        return jnp.concatenate([self.col_swap(p, k) if k else p for k, p in enumerate(pieces)])

    def right_grad_home(self, grad):
        n, m = self.n_col, self.per_row
        here, lanes = grad.shape[0] // n, grad.shape[1]
        total = jnp.zeros((m, here, lanes), F32)
        slot = lax.broadcasted_iota(jnp.uint32, (m, 1, 1), 0)
        for k in range(n):
            t = (self.row * m + self.col % m) ^ k
            block = lax.dynamic_slice_in_dim(grad, (t ^ self.col) * here, here, 0)
            pairs = []
            for r in range(self.n_row):
                for q in range(n):
                    pairs.append((r * n + q, (q // m) * n + ((r * m + q % m) ^ k)))
            got = lax.ppermute(block, ("row", "col"), pairs).astype(F32)[None]
            total += got if m == 1 else jnp.where(slot == (self.col ^ k) % m, got, 0)
        return total.swapaxes(0, 1).reshape(here, m * lanes).astype(BF16)

    def weight_over_row(self, weight):
        n = self.n_row
        size = weight.shape[0] // n
        sent = weight.astype(BF16).reshape(n, size, -1)
        total = lax.dynamic_index_in_dim(weight.reshape(n, size, -1), self.row, 0, keepdims=False)
        for k in range(1, n):
            piece = lax.dynamic_index_in_dim(sent, self.row ^ k, 0, keepdims=False)
            total += self.row_swap(piece, k).astype(F32)
        return total

    def weight_over_col(self, total):
        mine = total.astype(BF16)
        for k in range(1, self.n_col):
            total += self.col_swap(mine, k).astype(F32)
        return total.astype(BF16)

    def weight_to_all(self, mine):
        n = self.n_row
        which = lax.broadcasted_iota(jnp.uint32, (n, 1, 1), 0) ^ self.row
        shares = mine[None]
        for k in range(1, n):
            shares = jnp.where(which == k, self.row_swap(mine, k)[None], shares)
        return shares.reshape(n * mine.shape[0], mine.shape[1])


def after(value, *others):
    return lax.optimization_barrier((value,) + others)[0]


def shards(n_row, n_col, alignment_tensor, gain, shift, first_projector, second_projector,
           final_projector, final_offset, labels, counts, grad):
    ring = Pairs(n_row, n_col)
    here, rows, _ = alignment_tensor.shape
    cols, width = grad.shape[1:]
    seqs = here * n_col
    left, right = project_call(
        alignment_tensor, gain[None, :], shift[None, :], first_projector.T, second_projector.T, cols
    )
    by_row = ring.right_along_row(right)
    left = jnp.concatenate([left] + [ring.col_swap(left, k) for k in range(1, n_col)])

    at = jnp.stack([ring.row * rows, ring.col * cols, ring.col]).astype(jnp.int32)
    lab, tall, wide, plain, w, back, grad = back_call(
        at, labels, counts, after(final_projector, right), grad, seqs, n_col
    )
    mine = ring.right_along_col(ring.right_pieces(by_row))
    back, grad = in_vmem(back), in_vmem(grad)
    right_grad = right_grad_call(at, labels, back, left, lab, plain)

    right = after(mine, right_grad)
    grad_right = ring.right_grad_home(right_grad)
    outer, weight = outer_call(
        at, labels, left, lab, right, wide, grad
    )
    share = ring.weight_over_row(weight)
    left_grad = left_grad_call(at, labels, back, after(lab, weight), right, tall)
    share = after(share, left_grad)

    total = left_grad[:here].astype(F32)
    for k in range(1, n_col):
        total += ring.col_swap(left_grad[k * here : (k + 1) * here], k).astype(F32)
    adjoint_first = total.astype(BF16)
    pair_update = pair_call(in_vmem(outer), after(w, left_grad, share), final_offset[None, :])
    pair_update = pair_update.reshape(rows, cols, width)
    mine = after(ring.weight_over_col(share), pair_update)
    grad_w_out = ring.weight_to_all(mine).astype(F32) / (n_row * rows)
    return pair_update, adjoint_first, grad_right, grad_w_out


def solution(mesh):
    in_specs = (
        P(("parts", "col"), "row", None),
        P(),
        P(),
        P(),
        P(),
        P(),
        P(),
        P("parts"),
        P("parts", None),
        P(("parts", "row"), "col", None),
    )
    out_specs = (
        P(("parts", "row"), "col", None),
        P(("parts", "col"), "row"),
        P(("parts", "col"), "row"),
        P("parts", None),
    )

    def body(*args):
        return shards(mesh.shape["row"], mesh.shape["col"], *args)

    return jax.shard_map(body, mesh=mesh, in_specs=in_specs, out_specs=out_specs, check_vma=False)
```

```python
import functools

import jax
import jax.numpy as jnp
from jax import lax
from jax.experimental import pallas as pl
from jax.experimental.pallas import tpu as pltpu
from jax.sharding import PartitionSpec as P


PROJ = 32
CHAINS = 8
LANES = 128
PER_TILE = LANES // PROJ
WIDE = 256
F32 = jnp.float32
BF16 = jnp.bfloat16
VMEM = pl.BlockSpec(memory_space=pltpu.VMEM)
KERNEL = pltpu.CompilerParams(vmem_limit_bytes=24 << 20)
HBM = pl.BlockSpec(memory_space=pltpu.HBM)
SMEM = pl.BlockSpec(memory_space=pltpu.SMEM)


def swap_blocks(parts):
    lane = lax.broadcasted_iota(jnp.int32, parts[0].shape, 1)
    outs = []
    for q in range(PER_TILE):
        out = parts[(PER_TILE - 1 - q) % PER_TILE]
        for block in range(PER_TILE - 2, -1, -1):
            out = jnp.where(lane < (block + 1) * PROJ, parts[(block - q) % PER_TILE], out)
        outs.append(pltpu.roll(out, LANES - q * PROJ, 1) if q else out)
    return outs


def rolled(value, p):
    if not p:
        return value
    return jnp.concatenate(
        [pltpu.roll(value[:, t : t + LANES], p * PROJ, 1) for t in range(0, value.shape[1], LANES)],
        axis=1,
    )


def nt_dot(a, b):
    return lax.dot_general(a, b, (((1,), (1,)), ((), ())), preferred_element_type=F32)


def nn_dot(a, b):
    return lax.dot_general(a, b, (((1,), (0,)), ((), ())), preferred_element_type=F32)


def in_vmem(value):
    return pltpu.with_memory_space_constraint(value, pltpu.VMEM)


def in_hbm(value):
    return pltpu.with_memory_space_constraint(value, pltpu.HBM)


def project_body(x_hbm, gain_hbm, shift_hbm, first_hbm, second_hbm, left_ref, right_ref,
                 x_ref, gain_ref, shift_ref, w_ref, proj_ref, turn_ref, out_ref, sems, *, cols):
    chunks, chunk, rows, feats = x_ref.shape
    small = [
        pltpu.make_async_copy(gain_hbm, gain_ref, sems.at[chunks]),
        pltpu.make_async_copy(shift_hbm, shift_ref, sems.at[chunks + 1]),
        pltpu.make_async_copy(first_hbm, w_ref.at[pl.ds(0, PROJ)], sems.at[chunks + 2]),
        pltpu.make_async_copy(second_hbm, w_ref.at[pl.ds(PROJ, PROJ)], sems.at[chunks + 3]),
    ]
    big = [
        pltpu.make_async_copy(x_hbm.at[pl.ds(g * chunk, chunk)], x_ref.at[g], sems.at[g])
        for g in range(chunks)
    ]
    for copy in big[:1] + small + big[1:]:
        copy.start()
    w_ref[2 * PROJ :] = jnp.zeros((LANES - 2 * PROJ, feats), BF16)
    for copy in small:
        copy.wait()
    for g in range(chunks):
        big[g].wait()
        x = x_ref[g].astype(F32).reshape(chunk * rows, feats)
        center = x - jnp.mean(x, axis=-1, keepdims=True)
        spread = jnp.mean(center * center, axis=-1, keepdims=True)
        normed = center * lax.rsqrt(spread + 1e-05) * gain_ref[...] + shift_ref[...]
        at = slice(g * chunk * rows, (g + 1) * chunk * rows)
        proj_ref[at] = nt_dot(normed.astype(BF16), w_ref[...])
    project_layout(proj_ref, turn_ref, out_ref, left_ref, right_ref, rows, cols)


def project_layout(proj_ref, turn_ref, out_ref, left_ref, right_ref, rows, cols):
    here = left_ref.shape[0]
    lane = lax.broadcasted_iota(jnp.int32, (here, LANES), 1)
    for t in range(rows // PER_TILE):
        tile = proj_ref[pl.ds(t * PER_TILE, here, stride=rows)]
        for p in range(1, PER_TILE):
            part = proj_ref[pl.ds(t * PER_TILE + p, here, stride=rows)]
            tile = jnp.where(lane < p * PROJ, tile, pltpu.roll(part, p * PROJ, 1))
        left_ref[:, t * LANES : (t + 1) * LANES] = tile.astype(BF16)

    tiles = here * rows // LANES
    for t in range(tiles):
        flipped = proj_ref[t * LANES : (t + 1) * LANES].T
        turn_ref[t * PROJ : (t + 1) * PROJ] = flipped[PROJ : 2 * PROJ]
    seqs = LANES // rows
    per = LANES // cols
    lane = lax.broadcasted_iota(jnp.int32, (tiles, LANES), 1)
    for block in range(rows // cols):
        for t in range(PROJ // per):
            at = (block * (PROJ // per) + t) * LANES
            parts = [turn_ref[pl.ds(t * per + p, tiles, stride=PROJ)] for p in range(per)]
            for u in range(seqs):
                start = u * rows + block * cols
                tile = None
                for p, part in enumerate(parts):
                    amount = (p * cols - start) % LANES
                    part = pltpu.roll(part, amount, 1) if amount else part
                    tile = part if tile is None else jnp.where(lane < p * cols, tile, part)
                out_ref[pl.ds(u, tiles, stride=seqs), :] = tile
            right_ref[:, at : at + LANES] = out_ref[...].astype(BF16)


def project_call(x, gain, shift, first, second, cols):
    here, rows, feats = x.shape
    chunk = min(here, max(1, 2 * WIDE // rows))
    return pl.pallas_call(
        lambda *refs: project_body(*refs, cols=cols),
        in_specs=[HBM] * 5,
        out_specs=[VMEM] * 2,
        out_shape=[jax.ShapeDtypeStruct((here, rows * PROJ), BF16)] * 2,
        scratch_shapes=[
            pltpu.VMEM((here // chunk, chunk, rows, feats), BF16),
            pltpu.VMEM(gain.shape, F32),
            pltpu.VMEM(shift.shape, F32),
            pltpu.VMEM((LANES, feats), BF16),
            pltpu.VMEM((here * rows, LANES), F32),
            pltpu.VMEM((here * rows // LANES * PROJ, LANES), F32),
            pltpu.VMEM((here, LANES), F32),
            pltpu.SemaphoreType.DMA((here // chunk + 4,)),
        ],
        compiler_params=KERNEL,
        name="project",
    )(*map(in_hbm, (x, gain, shift, first, second)))


def masks(at_ref, labels_ref, counts_ref, lab_ref, tall_ref, wide_ref, plain_ref, rows, cols, seqs, n_col):
    res = labels_ref.shape[1]
    labels = jnp.broadcast_to(labels_ref[...], (8, res))
    own = pltpu.roll(labels, (res - at_ref[0]) % res, 1)[:, :rows]
    spread = (
        lax.broadcasted_iota(jnp.int32, (rows, rows * PROJ), 1) // PROJ
        == lax.broadcasted_iota(jnp.int32, (rows, rows * PROJ), 0)
    )
    lab = nn_dot(own.astype(F32).astype(BF16), spread.astype(F32).astype(BF16))
    lab_ref[...] = lab[:1].astype(jnp.int32)

    there = pltpu.roll(labels, (res - at_ref[1]) % res, 1)[:, :LANES]
    there = jnp.where(lax.broadcasted_iota(jnp.int32, (8, LANES), 1) < cols, there, 0)
    reach = cols
    while reach < LANES:
        there = there + pltpu.roll(there, reach, 1)
        reach *= 2
    depth = jnp.zeros((CHAINS, LANES), jnp.int32)
    for b in range(CHAINS):
        depth += jnp.where(there == b, counts_ref[:, b : b + 1], 0)
    here = lax.broadcasted_iota(jnp.int32, (seqs // n_col, LANES), 0)
    seq = jnp.concatenate([here + (at_ref[2] ^ k) * (seqs // n_col) for k in range(n_col)], axis=0)
    for a in range(CHAINS):
        deep = jnp.broadcast_to(depth[a : a + 1], (seqs, LANES))
        weight = jnp.where(seq < deep, 1.0 / deep.astype(F32), 0.0)
        three = deep % 3 == 0
        for x, part in enumerate((jnp.where(three, 0.0, weight), jnp.where(three, 3.0 * weight, 0.0))):
            tall_ref[a, x] = part.astype(BF16)
            wide_ref[a, x] = part.T[:cols].astype(BF16)
        plain_ref[a] = weight.T[:cols]


def projector(w_ref, wide_w_ref, w_out, wt_ref):
    wide_w_ref[...] = w_ref[...].astype(F32)
    for t in range(PROJ // PER_TILE):
        for q in range(PER_TILE):
            e = t * PER_TILE + q
            w_out[e * PROJ : (e + 1) * PROJ] = wide_w_ref[pl.ds(e, PROJ, stride=PROJ)].astype(BF16)
        block = w_out[t * LANES : (t + 1) * LANES].astype(F32)
        for p in range(PER_TILE):
            wt_ref[p, :, t * LANES : (t + 1) * LANES] = rolled(block.T, p).astype(BF16)


def cost(passes, span, total, seqs):
    return pl.CostEstimate(
        flops=4 * passes * span * total * seqs, bytes_accessed=2 * span * total, transcendentals=0
    )


def back_body(at_ref, labels_hbm, counts_hbm, w_hbm, grad_hbm,
              lab_ref, tall_ref, wide_ref, plain_ref, w_out, back_ref, grad_ref,
              labels_ref, counts_ref, w_ref, wide_w_ref, wt_ref, sems, *, seqs, n_col):
    groups, step, cols, _ = grad_ref.shape
    copies = [
        pltpu.make_async_copy(w_hbm, w_ref, sems.at[groups]),
        pltpu.make_async_copy(labels_hbm, labels_ref, sems.at[groups + 1]),
        pltpu.make_async_copy(counts_hbm, counts_ref, sems.at[groups + 2]),
    ]
    for copy in copies:
        copy.start()

    def grad_of(g):
        return pltpu.make_async_copy(grad_hbm.at[pl.ds(g * step, step)], grad_ref.at[g], sems.at[g])

    for g in range(groups):
        grad_of(g).start()
    for copy in copies:
        copy.wait()
    projector(w_ref, wide_w_ref, w_out, wt_ref)
    masks(at_ref, labels_ref, counts_ref, lab_ref, tall_ref, wide_ref, plain_ref,
          groups * step, cols, seqs, n_col)
    halves = step // PER_TILE

    def group(g):
        blocks = [
            jnp.concatenate([grad_ref[g, half * PER_TILE + p] for half in range(halves)], axis=0)
            for p in range(PER_TILE)
        ]
        for u in range(PROJ * PROJ // WIDE):
            prods = [
                nn_dot(block, wt_ref[p, :, u * WIDE : (u + 1) * WIDE]).astype(BF16)
                for p, block in enumerate(blocks)
            ]
            for half in range(halves):
                for t in range(WIDE // LANES):
                    parts = [
                        prod[half * cols : (half + 1) * cols, t * LANES : (t + 1) * LANES]
                        for prod in prods
                    ]
                    for q, part in enumerate(swap_blocks(parts)):
                        e = u * (WIDE // PROJ) + t * PER_TILE + q
                        at = (g, slice(e * cols, (e + 1) * cols))
                        back_ref[at + (slice(half * LANES, (half + 1) * LANES),)] = part

    def two_groups(i):
        grad_of(2 * i).wait()
        grad_of(2 * i + 1).wait()
        group(2 * i)
        group(2 * i + 1)

    each(0, groups // 2 - 1, two_groups)


def back_call(at, labels, counts, w, grad, seqs, n_col):
    rows, cols, width = grad.shape
    step = WIDE // PROJ
    groups = rows // step
    labels = labels[None, :]
    return pl.pallas_call(
        lambda *refs: back_body(*refs, seqs=seqs, n_col=n_col),
        in_specs=[SMEM] + [HBM] * 4,
        out_specs=[VMEM] * 7,
        out_shape=[
            jax.ShapeDtypeStruct((1, rows * PROJ), jnp.int32),
            jax.ShapeDtypeStruct((CHAINS, 2, seqs, LANES), BF16),
            jax.ShapeDtypeStruct((CHAINS, 2, cols, seqs), BF16),
            jax.ShapeDtypeStruct((CHAINS, cols, seqs), F32),
            jax.ShapeDtypeStruct(w.shape, BF16),
            pltpu.VMEM((groups, PROJ * cols, WIDE), BF16),
            pltpu.VMEM((groups, step, cols, width), BF16),
        ],
        scratch_shapes=[
            pltpu.VMEM(labels.shape, jnp.int32),
            pltpu.VMEM(counts.shape, jnp.int32),
            pltpu.VMEM(w.shape, BF16),
            pltpu.VMEM(w.shape, F32),
            pltpu.VMEM((PER_TILE, width, PROJ * PROJ), BF16),
            pltpu.SemaphoreType.DMA((groups + 3,)),
        ],
        compiler_params=KERNEL,
        cost_estimate=cost(10, PROJ * cols, rows * PROJ, width),
        name="back",
    )(at, *map(in_hbm, (labels, counts, w, grad)))


def first_chain(at_ref, labels_ref, group):
    return labels_ref[at_ref[0] + group * (WIDE // PROJ)]


def last_chain(at_ref, labels_ref, group):
    return labels_ref[at_ref[0] + (group + 1) * (WIDE // PROJ) - 1]


def slots(chain, count, seqs):
    return pl.ds(pl.multiple_of(chain * seqs, seqs), count * seqs)


def each(first, last, fn):
    def step(k, carry):
        fn(k)
        return carry

    lax.fori_loop(first, last + 1, step, 0)


def lanes_of(group):
    return pl.ds(pl.multiple_of(group * WIDE, WIDE), WIDE)


def masked_left(left_ref, lab_ref, lb_ref, chain, group):
    seqs = left_ref.shape[0]
    lanes = lanes_of(group)
    for side in range(2):
        keep = (lab_ref[:, lanes] == chain + side).astype(F32).astype(BF16)
        lb_ref[side * seqs : (side + 1) * seqs] = left_ref[:, lanes] * keep


def right_grad_body(at_ref, labels_ref, back_ref, left_ref, lab_ref, wide_ref,
                    right_out, q_ref, lb_ref, next_ref, flip_ref, turn_ref):
    seqs = left_ref.shape[0]
    groups, span, _ = back_ref.shape
    cols = span // PROJ
    first = lambda g: first_chain(at_ref, labels_ref, g)
    last = lambda g: last_chain(at_ref, labels_ref, g)

    def clear(chain):
        q_ref[:, slots(chain, 1, seqs)] = jnp.zeros((span, seqs), F32)

    each(first(0), last(groups - 1) + 1, clear)

    def two_chains(g, k):
        chain = first(g) + 2 * k
        masked_left(left_ref, lab_ref, lb_ref, chain, g)
        q_ref[:, slots(chain, 2, seqs)] += nt_dot(back_ref[g], lb_ref[...])

    def two_groups(i):
        g = 2 * i
        chain = first(g)
        same = first(g + 1) == chain

        @pl.when(same)
        def _():
            masked_left(left_ref, lab_ref, lb_ref, chain, g)
            masked_left(left_ref, lab_ref, next_ref, chain, g + 1)
            q_ref[:, slots(chain, 2, seqs)] += nt_dot(back_ref[g], lb_ref[...]) + nt_dot(
                back_ref[g + 1], next_ref[...]
            )

        @pl.when(jnp.logical_not(same))
        def _():
            two_chains(g, 0)
            two_chains(g + 1, 0)

        each(1, (last(g) - first(g)) // 2, lambda k: two_chains(g, k))
        each(1, (last(g + 1) - first(g + 1)) // 2, lambda k: two_chains(g + 1, k))

    each(0, groups // 2 - 1, two_groups)

    def combine(chain, start):
        for e in range(PROJ):
            rows = slice(e * cols, (e + 1) * cols)
            part = q_ref[rows, slots(chain, 1, seqs)] * wide_ref[chain]
            flip_ref[rows] = part if start else flip_ref[rows] + part

    combine(first(0), True)
    each(first(0) + 1, last(groups - 1), lambda chain: combine(chain, False))
    for j in range(cols):
        turn_ref[j * PROJ : (j + 1) * PROJ] = flip_ref[pl.ds(j, PROJ, stride=cols)]
    for t in range(span // LANES):
        rows = slice(t * LANES, (t + 1) * LANES)
        right_out[:, rows] = turn_ref[rows].T.astype(BF16)


def right_grad_call(at, labels, back, left, lab, wide):
    groups, span, _ = back.shape
    total = groups * WIDE
    seqs = left.shape[0]
    return pl.pallas_call(
        right_grad_body,
        in_specs=[SMEM] * 2 + [VMEM] * 4,
        out_specs=VMEM,
        out_shape=jax.ShapeDtypeStruct((seqs, span), BF16),
        scratch_shapes=[
            pltpu.VMEM((span, (CHAINS + 1) * seqs), F32),
            pltpu.VMEM((2 * seqs, WIDE), BF16),
            pltpu.VMEM((2 * seqs, WIDE), BF16),
            pltpu.VMEM((span, seqs), F32),
            pltpu.VMEM((span, seqs), F32),
        ],
        compiler_params=KERNEL,
        cost_estimate=cost(10, span, total, seqs),
        name="right_grad",
    )(at, labels, back, left, lab, wide)


def left_grad_body(at_ref, labels_ref, back_ref, lab_ref, right_ref, tall_ref,
                   left_out, rm_ref, part_ref):
    seqs = right_ref.shape[0]
    groups, span, _ = back_ref.shape
    first = lambda g: first_chain(at_ref, labels_ref, g)
    last = lambda g: last_chain(at_ref, labels_ref, g)
    part_ref[...] = (right_ref[...].astype(F32) / 3).astype(BF16)

    def build(chain):
        plain, third = tall_ref[chain, 0], tall_ref[chain, 1]
        for t in range(span // LANES):
            lanes = slice(t * LANES, (t + 1) * LANES)
            rm_ref[slots(chain, 1, seqs), lanes] = (
                right_ref[:, lanes] * plain + part_ref[:, lanes] * third
            )

    each(first(0), last(groups - 1), build)
    rm_ref[slots(last(groups - 1) + 1, 1, seqs)] = jnp.zeros((seqs, span), BF16)

    def two_chains(g, k, total):
        lab = lab_ref[:, lanes_of(g)]
        chain = first(g) + 2 * k
        part = nn_dot(rm_ref[slots(chain, 2, seqs)], back_ref[g])
        keep0, keep1 = lab == chain, lab == chain + 1
        part = jnp.where(keep0, part[:seqs], 0.0) + jnp.where(keep1, part[seqs:], 0.0)
        return part if total is None else total + part

    def two_groups(i):
        totals = [two_chains(g, 0, None) for g in (2 * i, 2 * i + 1)]
        for g, total in zip((2 * i, 2 * i + 1), totals):
            more = functools.partial(two_chains, g)
            total = lax.fori_loop(1, (last(g) - first(g)) // 2 + 1, more, total)
            left_out[:, lanes_of(g)] = total.astype(BF16)

    each(0, groups // 2 - 1, two_groups)


def left_grad_call(at, labels, back, lab, right, tall):
    groups, span, _ = back.shape
    total = groups * WIDE
    seqs = right.shape[0]
    return pl.pallas_call(
        left_grad_body,
        in_specs=[SMEM] * 2 + [VMEM] * 4,
        out_specs=VMEM,
        out_shape=jax.ShapeDtypeStruct((seqs, total), BF16),
        scratch_shapes=[
            pltpu.VMEM(((CHAINS + 1) * seqs, span), BF16),
            pltpu.VMEM((seqs, span), BF16),
        ],
        compiler_params=KERNEL,
        cost_estimate=cost(10, span, total, seqs),
        name="left_grad",
    )(at, labels, back, lab, right, tall)


def outer_body(at_ref, labels_ref, left_ref, lab_ref, right_ref, wide_ref, grad_ref,
               outer_ref, weight_out, rm_ref, lb_ref, even_ref, odd_ref, sum_ref, turn_ref, flip_ref, part_ref):
    seqs = left_ref.shape[0]
    span = right_ref.shape[1]
    cols = span // PROJ
    groups, step, _, width = grad_ref.shape
    first = lambda g: first_chain(at_ref, labels_ref, g)
    last = lambda g: last_chain(at_ref, labels_ref, g)
    for t in range(span // LANES):
        lanes = slice(t * LANES, (t + 1) * LANES)
        flipped = right_ref[:, lanes].astype(F32).T
        flip_ref[lanes] = flipped.astype(BF16)
        part_ref[lanes] = (flipped / 3).astype(BF16)

    def build(chain):
        plain, third = wide_ref[chain, 0], wide_ref[chain, 1]
        for e in range(PROJ):
            rows = slice(e * cols, (e + 1) * cols)
            to = e % PER_TILE * (PROJ // PER_TILE) + e // PER_TILE
            rm_ref[to * cols : (to + 1) * cols, slots(chain, 1, seqs)] = (
                flip_ref[rows] * plain + part_ref[rows] * third
            )

    each(first(0), last(groups - 1), build)
    rm_ref[:, slots(last(groups - 1) + 1, 1, seqs)] = jnp.zeros((span, seqs), BF16)
    sum_ref[...] = jnp.zeros_like(sum_ref)
    quarter = span // PER_TILE

    def product(chain, g, acc_ref, add):
        masked_left(left_ref, lab_ref, lb_ref, chain, g)
        for q in range(PER_TILE):
            rows = slice(q * quarter, (q + 1) * quarter)
            part = nn_dot(rm_ref[rows, slots(chain, 2, seqs)], rolled(lb_ref[...], q))
            acc_ref[rows] = acc_ref[rows] + part if add else part

    def rest(g, acc_ref):
        each(1, (last(g) - first(g)) // 2, lambda k: product(first(g) + 2 * k, g, acc_ref, True))

    def finish(g, acc_ref):
        for half in range(WIDE // LANES):
            lanes = slice(half * LANES, (half + 1) * LANES)
            for t in range(PROJ // PER_TILE):
                parts = []
                for q in range(PER_TILE):
                    e = q * (PROJ // PER_TILE) + t
                    parts.append(acc_ref[e * cols : (e + 1) * cols, lanes].astype(BF16))
                turned = swap_blocks(parts)
                for p in range(PER_TILE):
                    i = half * PER_TILE + p
                    at = (g, slice(i * cols, (i + 1) * cols), slice(t * LANES, (t + 1) * LANES))
                    outer_ref[at] = turned[p]
        flat = grad_ref[g].reshape(step * cols, width)
        sum_ref[...] += nn_dot(flat.T, outer_ref[g])

    def turn(g, acc_ref, next_ref):
        product(first(g + 1), g + 1, next_ref, False)
        finish(g, acc_ref)
        rest(g + 1, next_ref)

    def two_groups(i):
        turn(2 * i, even_ref, odd_ref)
        turn(2 * i + 1, odd_ref, even_ref)

    product(first(0), 0, even_ref, False)
    rest(0, even_ref)
    each(0, groups // 2 - 2, two_groups)
    turn(groups - 2, even_ref, odd_ref)
    finish(groups - 1, odd_ref)
    for t in range(PROJ * PROJ // LANES):
        part = slice(t * LANES, (t + 1) * LANES)
        turn_ref[part] = sum_ref[:, part].T
    for c in range(PROJ):
        weight_out[c * PROJ : (c + 1) * PROJ] = turn_ref[pl.ds(c, PROJ, stride=PROJ)]


def outer_call(at, labels, left, lab, right, wide, grad):
    groups, step, cols, width = grad.shape
    seqs, total = left.shape
    span = right.shape[1]
    return pl.pallas_call(
        outer_body,
        in_specs=[SMEM] * 2 + [VMEM] * 5,
        out_specs=[VMEM] * 2,
        out_shape=[
            pltpu.VMEM((groups, step * cols, PROJ * PROJ), BF16),
            jax.ShapeDtypeStruct((PROJ * PROJ, width), F32),
        ],
        scratch_shapes=[
            pltpu.VMEM((span, (CHAINS + 1) * seqs), BF16),
            pltpu.VMEM((2 * seqs, WIDE), BF16),
            pltpu.VMEM((span, WIDE), F32),
            pltpu.VMEM((span, WIDE), F32),
            pltpu.VMEM((width, PROJ * PROJ), F32),
            pltpu.VMEM((PROJ * PROJ, width), F32),
            pltpu.VMEM((span, seqs), BF16),
            pltpu.VMEM((span, seqs), BF16),
        ],
        compiler_params=KERNEL,
        cost_estimate=cost(20, span, total, seqs),
        name="outer",
    )(at, labels, left, lab, right, wide, grad)


def pair_body(outer_ref, w_ref, offset_ref, pair_ref):
    _, pairs, _ = outer_ref.shape
    here = pair_ref.shape[0] // pairs
    for g in range(here):
        pair = nn_dot(outer_ref[pl.program_id(0) * here + g], w_ref[...]) + offset_ref[...]
        pair_ref[g * pairs : (g + 1) * pairs] = pair.astype(BF16)


def pair_call(outer, w, offset):
    groups, pairs, feats = outer.shape
    width = w.shape[1]
    steps = 2
    return pl.pallas_call(
        pair_body,
        grid=(steps,),
        in_specs=[VMEM] * 3,
        out_specs=pl.BlockSpec((groups * pairs // steps, width), lambda g: (g, 0)),
        out_shape=jax.ShapeDtypeStruct((groups * pairs, width), BF16),
        compiler_params=KERNEL,
        cost_estimate=pl.CostEstimate(
            flops=2 * groups * pairs * feats * width,
            bytes_accessed=2 * groups * pairs * width,
            transcendentals=0,
        ),
        name="pair",
    )(outer, w, offset)


class Pairs:
    def __init__(self, n_row, n_col):
        self.n_row, self.n_col = n_row, n_col
        self.per_row = n_col // n_row
        self.row = lax.axis_index("row").astype(jnp.uint32)
        self.col = lax.axis_index("col").astype(jnp.uint32)

    def col_swap(self, value, k):
        return lax.ppermute(value, "col", [(t ^ k, t) for t in range(self.n_col)])

    def row_swap(self, value, k):
        return lax.ppermute(value, "row", [(t ^ k, t) for t in range(self.n_row)])

    def right_along_row(self, right):
        others = [self.row_swap(right, k) for k in range(1, self.n_row)]
        return [right] + others

    def right_pieces(self, by_row):
        m = self.per_row
        here, lanes = by_row[0].shape
        lanes //= m
        by_row = jnp.stack(by_row)
        pieces = []
        for k in range(self.n_col):
            q = self.col ^ k
            at = ((q // m) ^ self.row, jnp.uint32(0), (q % m) * lanes)
            pieces.append(lax.dynamic_slice(by_row, at, (1, here, lanes))[0])
        return pieces

    def right_along_col(self, pieces):
        return jnp.concatenate([self.col_swap(p, k) if k else p for k, p in enumerate(pieces)])

    def right_grad_home(self, grad):
        n, m = self.n_col, self.per_row
        here, lanes = grad.shape[0] // n, grad.shape[1]
        total = jnp.zeros((m, here, lanes), F32)
        slot = lax.broadcasted_iota(jnp.uint32, (m, 1, 1), 0)
        for k in range(n):
            t = (self.row * m + self.col % m) ^ k
            block = lax.dynamic_slice_in_dim(grad, (t ^ self.col) * here, here, 0)
            pairs = []
            for r in range(self.n_row):
                for q in range(n):
                    pairs.append((r * n + q, (q // m) * n + ((r * m + q % m) ^ k)))
            got = lax.ppermute(block, ("row", "col"), pairs).astype(F32)[None]
            total += got if m == 1 else jnp.where(slot == (self.col ^ k) % m, got, 0)
        return total.swapaxes(0, 1).reshape(here, m * lanes).astype(BF16)

    def weight_over_row(self, weight):
        n = self.n_row
        size = weight.shape[0] // n
        sent = weight.astype(BF16).reshape(n, size, -1)
        total = lax.dynamic_index_in_dim(weight.reshape(n, size, -1), self.row, 0, keepdims=False)
        for k in range(1, n):
            piece = lax.dynamic_index_in_dim(sent, self.row ^ k, 0, keepdims=False)
            total += self.row_swap(piece, k).astype(F32)
        return total

    def weight_over_col(self, total):
        mine = total.astype(BF16)
        for k in range(1, self.n_col):
            total += self.col_swap(mine, k).astype(F32)
        return total.astype(BF16)

    def weight_to_all(self, mine):
        n = self.n_row
        which = lax.broadcasted_iota(jnp.uint32, (n, 1, 1), 0) ^ self.row
        shares = mine[None]
        for k in range(1, n):
            shares = jnp.where(which == k, self.row_swap(mine, k)[None], shares)
        return shares.reshape(n * mine.shape[0], mine.shape[1])


def after(value, *others):
    return lax.optimization_barrier((value,) + others)[0]


def shards(n_row, n_col, alignment_tensor, gain, shift, first_projector, second_projector,
           final_projector, final_offset, labels, counts, grad):
    ring = Pairs(n_row, n_col)
    here, rows, _ = alignment_tensor.shape
    cols, width = grad.shape[1:]
    seqs = here * n_col
    left, right = project_call(
        alignment_tensor, gain[None, :], shift[None, :], first_projector.T, second_projector.T, cols
    )
    by_row = ring.right_along_row(right)
    left = jnp.concatenate([left] + [ring.col_swap(left, k) for k in range(1, n_col)])

    at = jnp.stack([ring.row * rows, ring.col * cols, ring.col]).astype(jnp.int32)
    lab, tall, wide, plain, w, back, grad = back_call(
        at, labels, counts, after(final_projector, right), grad, seqs, n_col
    )
    mine = ring.right_along_col(ring.right_pieces(by_row))
    back, grad = in_vmem(back), in_vmem(grad)
    right_grad = right_grad_call(at, labels, back, left, lab, plain)

    right = after(mine, right_grad)
    grad_right = ring.right_grad_home(right_grad)
    outer, weight = outer_call(
        at, labels, left, lab, right, wide, grad
    )
    share = ring.weight_over_row(weight)
    left_grad = left_grad_call(at, labels, back, after(lab, weight), right, tall)
    share = after(share, left_grad)

    total = left_grad[:here].astype(F32)
    for k in range(1, n_col):
        total += ring.col_swap(left_grad[k * here : (k + 1) * here], k).astype(F32)
    adjoint_first = total.astype(BF16)
    pair_update = pair_call(in_vmem(outer), after(w, left_grad, share), final_offset[None, :])
    pair_update = pair_update.reshape(rows, cols, width)
    mine = after(ring.weight_over_col(share), pair_update)
    grad_w_out = ring.weight_to_all(mine).astype(F32) / (n_row * rows)
    return pair_update, adjoint_first, grad_right, grad_w_out


def solution(mesh):
    in_specs = (
        P(("parts", "col"), "row", None),
        P(),
        P(),
        P(),
        P(),
        P(),
        P(),
        P("parts"),
        P("parts", None),
        P(("parts", "row"), "col", None),
    )
    out_specs = (
        P(("parts", "row"), "col", None),
        P(("parts", "col"), "row"),
        P(("parts", "col"), "row"),
        P("parts", None),
    )

    def body(*args):
        return shards(mesh.shape["row"], mesh.shape["col"], *args)

    return jax.shard_map(body, mesh=mesh, in_specs=in_specs, out_specs=out_specs, check_vma=False)
```

```python
import functools

import jax
import jax.numpy as jnp
from jax import lax
from jax.experimental import pallas as pl
from jax.experimental.pallas import tpu as pltpu
from jax.sharding import PartitionSpec as P


PROJ = 32
CHAINS = 8
LANES = 128
PER_TILE = LANES // PROJ
WIDE = 256
F32 = jnp.float32
BF16 = jnp.bfloat16
VMEM = pl.BlockSpec(memory_space=pltpu.VMEM)
KERNEL = pltpu.CompilerParams(vmem_limit_bytes=24 << 20)
HBM = pl.BlockSpec(memory_space=pltpu.HBM)
SMEM = pl.BlockSpec(memory_space=pltpu.SMEM)


def swap_blocks(parts):
    lane = lax.broadcasted_iota(jnp.int32, parts[0].shape, 1)
    outs = []
    for q in range(PER_TILE):
        out = parts[(PER_TILE - 1 - q) % PER_TILE]
        for block in range(PER_TILE - 2, -1, -1):
            out = jnp.where(lane < (block + 1) * PROJ, parts[(block - q) % PER_TILE], out)
        outs.append(pltpu.roll(out, LANES - q * PROJ, 1) if q else out)
    return outs


def rolled(value, p):
    if not p:
        return value
    return jnp.concatenate(
        [pltpu.roll(value[:, t : t + LANES], p * PROJ, 1) for t in range(0, value.shape[1], LANES)],
        axis=1,
    )


def nt_dot(a, b):
    return lax.dot_general(a, b, (((1,), (1,)), ((), ())), preferred_element_type=F32)


def nn_dot(a, b):
    return lax.dot_general(a, b, (((1,), (0,)), ((), ())), preferred_element_type=F32)


def in_vmem(value):
    return pltpu.with_memory_space_constraint(value, pltpu.VMEM)


def in_hbm(value):
    return pltpu.with_memory_space_constraint(value, pltpu.HBM)


def project_body(x_hbm, gain_hbm, shift_hbm, first_hbm, second_hbm, left_ref, right_ref,
                 x_ref, gain_ref, shift_ref, w_ref, proj_ref, turn_ref, out_ref, sems, *, cols):
    chunks, chunk, rows, feats = x_ref.shape
    small = [
        pltpu.make_async_copy(gain_hbm, gain_ref, sems.at[chunks]),
        pltpu.make_async_copy(shift_hbm, shift_ref, sems.at[chunks + 1]),
        pltpu.make_async_copy(first_hbm, w_ref.at[pl.ds(0, PROJ)], sems.at[chunks + 2]),
        pltpu.make_async_copy(second_hbm, w_ref.at[pl.ds(PROJ, PROJ)], sems.at[chunks + 3]),
    ]
    big = [
        pltpu.make_async_copy(x_hbm.at[pl.ds(g * chunk, chunk)], x_ref.at[g], sems.at[g])
        for g in range(chunks)
    ]
    for copy in big[:1] + small + big[1:]:
        copy.start()
    w_ref[2 * PROJ :] = jnp.zeros((LANES - 2 * PROJ, feats), BF16)
    for copy in small:
        copy.wait()
    for g in range(chunks):
        big[g].wait()
        x = x_ref[g].astype(F32).reshape(chunk * rows, feats)
        center = x - jnp.mean(x, axis=-1, keepdims=True)
        spread = jnp.mean(center * center, axis=-1, keepdims=True)
        normed = center * lax.rsqrt(spread + 1e-05) * gain_ref[...] + shift_ref[...]
        at = slice(g * chunk * rows, (g + 1) * chunk * rows)
        proj_ref[at] = nt_dot(normed.astype(BF16), w_ref[...])
    project_layout(proj_ref, turn_ref, out_ref, left_ref, right_ref, rows, cols)


def project_layout(proj_ref, turn_ref, out_ref, left_ref, right_ref, rows, cols):
    here = left_ref.shape[0]
    lane = lax.broadcasted_iota(jnp.int32, (here, LANES), 1)
    for t in range(rows // PER_TILE):
        tile = proj_ref[pl.ds(t * PER_TILE, here, stride=rows)]
        for p in range(1, PER_TILE):
            part = proj_ref[pl.ds(t * PER_TILE + p, here, stride=rows)]
            tile = jnp.where(lane < p * PROJ, tile, pltpu.roll(part, p * PROJ, 1))
        left_ref[:, t * LANES : (t + 1) * LANES] = tile.astype(BF16)

    tiles = here * rows // LANES
    for t in range(tiles):
        flipped = proj_ref[t * LANES : (t + 1) * LANES].T
        turn_ref[t * PROJ : (t + 1) * PROJ] = flipped[PROJ : 2 * PROJ]
    seqs = LANES // rows
    per = LANES // cols
    lane = lax.broadcasted_iota(jnp.int32, (tiles, LANES), 1)
    for block in range(rows // cols):
        for t in range(PROJ // per):
            at = (block * (PROJ // per) + t) * LANES
            parts = [turn_ref[pl.ds(t * per + p, tiles, stride=PROJ)] for p in range(per)]
            for u in range(seqs):
                start = u * rows + block * cols
                tile = None
                for p, part in enumerate(parts):
                    amount = (p * cols - start) % LANES
                    part = pltpu.roll(part, amount, 1) if amount else part
                    tile = part if tile is None else jnp.where(lane < p * cols, tile, part)
                out_ref[pl.ds(u, tiles, stride=seqs), :] = tile
            right_ref[:, at : at + LANES] = out_ref[...].astype(BF16)


def project_call(x, gain, shift, first, second, cols):
    here, rows, feats = x.shape
    chunk = min(here, max(1, 2 * WIDE // rows))
    return pl.pallas_call(
        lambda *refs: project_body(*refs, cols=cols),
        in_specs=[HBM] * 5,
        out_specs=[VMEM] * 2,
        out_shape=[jax.ShapeDtypeStruct((here, rows * PROJ), BF16)] * 2,
        scratch_shapes=[
            pltpu.VMEM((here // chunk, chunk, rows, feats), BF16),
            pltpu.VMEM(gain.shape, F32),
            pltpu.VMEM(shift.shape, F32),
            pltpu.VMEM((LANES, feats), BF16),
            pltpu.VMEM((here * rows, LANES), F32),
            pltpu.VMEM((here * rows // LANES * PROJ, LANES), F32),
            pltpu.VMEM((here, LANES), F32),
            pltpu.SemaphoreType.DMA((here // chunk + 4,)),
        ],
        compiler_params=KERNEL,
        name="project",
    )(*map(in_hbm, (x, gain, shift, first, second)))


def masks(at_ref, labels_ref, counts_ref, lab_ref, tall_ref, wide_ref, plain_ref, rows, cols, seqs, n_col):
    res = labels_ref.shape[1]
    labels = jnp.broadcast_to(labels_ref[...], (8, res))
    own = pltpu.roll(labels, (res - at_ref[0]) % res, 1)[:, :rows]
    spread = (
        lax.broadcasted_iota(jnp.int32, (rows, rows * PROJ), 1) // PROJ
        == lax.broadcasted_iota(jnp.int32, (rows, rows * PROJ), 0)
    )
    lab = nn_dot(own.astype(F32).astype(BF16), spread.astype(F32).astype(BF16))
    lab_ref[...] = lab[:1].astype(jnp.int32)

    there = pltpu.roll(labels, (res - at_ref[1]) % res, 1)[:, :LANES]
    there = jnp.where(lax.broadcasted_iota(jnp.int32, (8, LANES), 1) < cols, there, 0)
    reach = cols
    while reach < LANES:
        there = there + pltpu.roll(there, reach, 1)
        reach *= 2
    depth = jnp.zeros((CHAINS, LANES), jnp.int32)
    for b in range(CHAINS):
        depth += jnp.where(there == b, counts_ref[:, b : b + 1], 0)
    here = lax.broadcasted_iota(jnp.int32, (seqs // n_col, LANES), 0)
    seq = jnp.concatenate([here + (at_ref[2] ^ k) * (seqs // n_col) for k in range(n_col)], axis=0)
    for a in range(CHAINS):
        deep = jnp.broadcast_to(depth[a : a + 1], (seqs, LANES))
        weight = jnp.where(seq < deep, 1.0 / deep.astype(F32), 0.0)
        three = deep % 3 == 0
        for x, part in enumerate((jnp.where(three, 0.0, weight), jnp.where(three, 3.0 * weight, 0.0))):
            tall_ref[a, x] = part.astype(BF16)
            wide_ref[a, x] = part.T[:cols].astype(BF16)
        plain_ref[a] = weight.T[:cols]


def projector(w_ref, wide_w_ref, w_out, wt_ref):
    wide_w_ref[...] = w_ref[...].astype(F32)
    for t in range(PROJ // PER_TILE):
        for q in range(PER_TILE):
            e = t * PER_TILE + q
            w_out[e * PROJ : (e + 1) * PROJ] = wide_w_ref[pl.ds(e, PROJ, stride=PROJ)].astype(BF16)
        block = w_out[t * LANES : (t + 1) * LANES].astype(F32)
        for p in range(PER_TILE):
            wt_ref[p, :, t * LANES : (t + 1) * LANES] = rolled(block.T, p).astype(BF16)


def cost(passes, span, total, seqs):
    return pl.CostEstimate(
        flops=4 * passes * span * total * seqs, bytes_accessed=2 * span * total, transcendentals=0
    )


def back_body(at_ref, labels_hbm, counts_hbm, w_hbm, grad_hbm,
              lab_ref, tall_ref, wide_ref, plain_ref, w_out, back_ref, grad_ref,
              labels_ref, counts_ref, w_ref, wide_w_ref, wt_ref, sems, *, seqs, n_col):
    groups, step, cols, _ = grad_ref.shape
    copies = [
        pltpu.make_async_copy(w_hbm, w_ref, sems.at[groups]),
        pltpu.make_async_copy(labels_hbm, labels_ref, sems.at[groups + 1]),
        pltpu.make_async_copy(counts_hbm, counts_ref, sems.at[groups + 2]),
    ]
    for copy in copies:
        copy.start()

    def grad_of(g):
        return pltpu.make_async_copy(grad_hbm.at[pl.ds(g * step, step)], grad_ref.at[g], sems.at[g])

    for g in range(groups):
        grad_of(g).start()
    for copy in copies:
        copy.wait()
    projector(w_ref, wide_w_ref, w_out, wt_ref)
    masks(at_ref, labels_ref, counts_ref, lab_ref, tall_ref, wide_ref, plain_ref,
          groups * step, cols, seqs, n_col)
    halves = step // PER_TILE

    def group(g):
        blocks = [
            jnp.concatenate([grad_ref[g, half * PER_TILE + p] for half in range(halves)], axis=0)
            for p in range(PER_TILE)
        ]
        for u in range(PROJ * PROJ // WIDE):
            prods = [
                nn_dot(block, wt_ref[p, :, u * WIDE : (u + 1) * WIDE]).astype(BF16)
                for p, block in enumerate(blocks)
            ]
            for half in range(halves):
                for t in range(WIDE // LANES):
                    parts = [
                        prod[half * cols : (half + 1) * cols, t * LANES : (t + 1) * LANES]
                        for prod in prods
                    ]
                    for q, part in enumerate(swap_blocks(parts)):
                        e = u * (WIDE // PROJ) + t * PER_TILE + q
                        at = (g, slice(e * cols, (e + 1) * cols))
                        back_ref[at + (slice(half * LANES, (half + 1) * LANES),)] = part

    def four_groups(i):
        for g in range(4):
            grad_of(4 * i + g).wait()
        for g in range(4):
            group(4 * i + g)

    each(0, groups // 4 - 1, four_groups)


def back_call(at, labels, counts, w, grad, seqs, n_col):
    rows, cols, width = grad.shape
    step = WIDE // PROJ
    groups = rows // step
    labels = labels[None, :]
    return pl.pallas_call(
        lambda *refs: back_body(*refs, seqs=seqs, n_col=n_col),
        in_specs=[SMEM] + [HBM] * 4,
        out_specs=[VMEM] * 7,
        out_shape=[
            jax.ShapeDtypeStruct((1, rows * PROJ), jnp.int32),
            jax.ShapeDtypeStruct((CHAINS, 2, seqs, LANES), BF16),
            jax.ShapeDtypeStruct((CHAINS, 2, cols, seqs), BF16),
            jax.ShapeDtypeStruct((CHAINS, cols, seqs), F32),
            jax.ShapeDtypeStruct(w.shape, BF16),
            pltpu.VMEM((groups, PROJ * cols, WIDE), BF16),
            pltpu.VMEM((groups, step, cols, width), BF16),
        ],
        scratch_shapes=[
            pltpu.VMEM(labels.shape, jnp.int32),
            pltpu.VMEM(counts.shape, jnp.int32),
            pltpu.VMEM(w.shape, BF16),
            pltpu.VMEM(w.shape, F32),
            pltpu.VMEM((PER_TILE, width, PROJ * PROJ), BF16),
            pltpu.SemaphoreType.DMA((groups + 3,)),
        ],
        compiler_params=KERNEL,
        cost_estimate=cost(10, PROJ * cols, rows * PROJ, width),
        name="back",
    )(at, *map(in_hbm, (labels, counts, w, grad)))


def first_chain(at_ref, labels_ref, group):
    return labels_ref[at_ref[0] + group * (WIDE // PROJ)]


def last_chain(at_ref, labels_ref, group):
    return labels_ref[at_ref[0] + (group + 1) * (WIDE // PROJ) - 1]


def slots(chain, count, seqs):
    return pl.ds(pl.multiple_of(chain * seqs, seqs), count * seqs)


def each(first, last, fn):
    def step(k, carry):
        fn(k)
        return carry

    lax.fori_loop(first, last + 1, step, 0)


def lanes_of(group):
    return pl.ds(pl.multiple_of(group * WIDE, WIDE), WIDE)


def masked_left(left_ref, lab_ref, lb_ref, chain, group):
    seqs = left_ref.shape[0]
    lanes = lanes_of(group)
    for side in range(2):
        keep = (lab_ref[:, lanes] == chain + side).astype(F32).astype(BF16)
        lb_ref[side * seqs : (side + 1) * seqs] = left_ref[:, lanes] * keep


def right_grad_body(at_ref, labels_ref, back_ref, left_ref, lab_ref, wide_ref,
                    right_out, q_ref, lb_ref, flip_ref, turn_ref):
    seqs = left_ref.shape[0]
    groups, span, _ = back_ref.shape
    cols = span // PROJ
    first = lambda g: first_chain(at_ref, labels_ref, g)
    last = lambda g: last_chain(at_ref, labels_ref, g)

    def clear(chain):
        q_ref[:, slots(chain, 1, seqs)] = jnp.zeros((span, seqs), F32)

    each(first(0), last(groups - 1) + 1, clear)

    def group(g):
        def two_chains(k):
            chain = first(g) + 2 * k
            masked_left(left_ref, lab_ref, lb_ref, chain, g)
            q_ref[:, slots(chain, 2, seqs)] += nt_dot(back_ref[g], lb_ref[...])

        each(0, (last(g) - first(g)) // 2, two_chains)

    each(0, groups - 1, group)

    def combine(chain, start):
        for e in range(PROJ):
            rows = slice(e * cols, (e + 1) * cols)
            part = q_ref[rows, slots(chain, 1, seqs)] * wide_ref[chain]
            flip_ref[rows] = part if start else flip_ref[rows] + part

    combine(first(0), True)
    each(first(0) + 1, last(groups - 1), lambda chain: combine(chain, False))
    for j in range(cols):
        turn_ref[j * PROJ : (j + 1) * PROJ] = flip_ref[pl.ds(j, PROJ, stride=cols)]
    for t in range(span // LANES):
        rows = slice(t * LANES, (t + 1) * LANES)
        right_out[:, rows] = turn_ref[rows].T.astype(BF16)


def right_grad_call(at, labels, back, left, lab, wide):
    groups, span, _ = back.shape
    total = groups * WIDE
    seqs = left.shape[0]
    return pl.pallas_call(
        right_grad_body,
        in_specs=[SMEM] * 2 + [VMEM] * 4,
        out_specs=VMEM,
        out_shape=jax.ShapeDtypeStruct((seqs, span), BF16),
        scratch_shapes=[
            pltpu.VMEM((span, (CHAINS + 1) * seqs), F32),
            pltpu.VMEM((2 * seqs, WIDE), BF16),
            pltpu.VMEM((span, seqs), F32),
            pltpu.VMEM((span, seqs), F32),
        ],
        compiler_params=KERNEL,
        cost_estimate=cost(10, span, total, seqs),
        name="right_grad",
    )(at, labels, back, left, lab, wide)


def left_grad_body(at_ref, labels_ref, back_ref, lab_ref, right_ref, tall_ref,
                   left_out, rm_ref, part_ref):
    seqs = right_ref.shape[0]
    groups, span, _ = back_ref.shape
    first = lambda g: first_chain(at_ref, labels_ref, g)
    last = lambda g: last_chain(at_ref, labels_ref, g)
    part_ref[...] = (right_ref[...].astype(F32) / 3).astype(BF16)

    def build(chain):
        plain, third = tall_ref[chain, 0], tall_ref[chain, 1]
        for t in range(span // LANES):
            lanes = slice(t * LANES, (t + 1) * LANES)
            rm_ref[slots(chain, 1, seqs), lanes] = (
                right_ref[:, lanes] * plain + part_ref[:, lanes] * third
            )

    each(first(0), last(groups - 1), build)
    rm_ref[slots(last(groups - 1) + 1, 1, seqs)] = jnp.zeros((seqs, span), BF16)

    def two_chains(g, k, total):
        lab = lab_ref[:, lanes_of(g)]
        chain = first(g) + 2 * k
        part = nn_dot(rm_ref[slots(chain, 2, seqs)], back_ref[g])
        keep0, keep1 = lab == chain, lab == chain + 1
        part = jnp.where(keep0, part[:seqs], 0.0) + jnp.where(keep1, part[seqs:], 0.0)
        return part if total is None else total + part

    def four_groups(i):
        some = [4 * i + g for g in range(4)]
        totals = [two_chains(g, 0, None) for g in some]
        for g, total in zip(some, totals):
            more = functools.partial(two_chains, g)
            total = lax.fori_loop(1, (last(g) - first(g)) // 2 + 1, more, total)
            left_out[:, lanes_of(g)] = total.astype(BF16)

    each(0, groups // 4 - 1, four_groups)


def left_grad_call(at, labels, back, lab, right, tall):
    groups, span, _ = back.shape
    total = groups * WIDE
    seqs = right.shape[0]
    return pl.pallas_call(
        left_grad_body,
        in_specs=[SMEM] * 2 + [VMEM] * 4,
        out_specs=VMEM,
        out_shape=jax.ShapeDtypeStruct((seqs, total), BF16),
        scratch_shapes=[
            pltpu.VMEM(((CHAINS + 1) * seqs, span), BF16),
            pltpu.VMEM((seqs, span), BF16),
        ],
        compiler_params=KERNEL,
        cost_estimate=cost(10, span, total, seqs),
        name="left_grad",
    )(at, labels, back, lab, right, tall)


def outer_body(at_ref, labels_ref, left_ref, lab_ref, right_ref, wide_ref, grad_ref,
               outer_ref, weight_out, rm_ref, lb_ref, even_ref, odd_ref, sum_ref, turn_ref, flip_ref, part_ref):
    seqs = left_ref.shape[0]
    span = right_ref.shape[1]
    cols = span // PROJ
    groups, step, _, width = grad_ref.shape
    first = lambda g: first_chain(at_ref, labels_ref, g)
    last = lambda g: last_chain(at_ref, labels_ref, g)
    for t in range(span // LANES):
        lanes = slice(t * LANES, (t + 1) * LANES)
        flipped = right_ref[:, lanes].astype(F32).T
        flip_ref[lanes] = flipped.astype(BF16)
        part_ref[lanes] = (flipped / 3).astype(BF16)

    def build(chain):
        plain, third = wide_ref[chain, 0], wide_ref[chain, 1]
        for e in range(PROJ):
            rows = slice(e * cols, (e + 1) * cols)
            to = e % PER_TILE * (PROJ // PER_TILE) + e // PER_TILE
            rm_ref[to * cols : (to + 1) * cols, slots(chain, 1, seqs)] = (
                flip_ref[rows] * plain + part_ref[rows] * third
            )

    each(first(0), last(groups - 1), build)
    rm_ref[:, slots(last(groups - 1) + 1, 1, seqs)] = jnp.zeros((span, seqs), BF16)
    sum_ref[...] = jnp.zeros_like(sum_ref)
    quarter = span // PER_TILE

    def product(chain, g, acc_ref, add):
        masked_left(left_ref, lab_ref, lb_ref, chain, g)
        for q in range(PER_TILE):
            rows = slice(q * quarter, (q + 1) * quarter)
            part = nn_dot(rm_ref[rows, slots(chain, 2, seqs)], rolled(lb_ref[...], q))
            acc_ref[rows] = acc_ref[rows] + part if add else part

    def rest(g, acc_ref):
        each(1, (last(g) - first(g)) // 2, lambda k: product(first(g) + 2 * k, g, acc_ref, True))

    def finish(g, acc_ref):
        for half in range(WIDE // LANES):
            lanes = slice(half * LANES, (half + 1) * LANES)
            for t in range(PROJ // PER_TILE):
                parts = []
                for q in range(PER_TILE):
                    e = q * (PROJ // PER_TILE) + t
                    parts.append(acc_ref[e * cols : (e + 1) * cols, lanes].astype(BF16))
                turned = swap_blocks(parts)
                for p in range(PER_TILE):
                    i = half * PER_TILE + p
                    at = (g, slice(i * cols, (i + 1) * cols), slice(t * LANES, (t + 1) * LANES))
                    outer_ref[at] = turned[p]
        flat = grad_ref[g].reshape(step * cols, width)
        sum_ref[...] += nn_dot(flat.T, outer_ref[g])

    def turn(g, acc_ref, next_ref):
        product(first(g + 1), g + 1, next_ref, False)
        finish(g, acc_ref)
        rest(g + 1, next_ref)

    def two_groups(i):
        turn(2 * i, even_ref, odd_ref)
        turn(2 * i + 1, odd_ref, even_ref)

    product(first(0), 0, even_ref, False)
    rest(0, even_ref)
    each(0, groups // 2 - 2, two_groups)
    turn(groups - 2, even_ref, odd_ref)
    finish(groups - 1, odd_ref)
    for t in range(PROJ * PROJ // LANES):
        part = slice(t * LANES, (t + 1) * LANES)
        turn_ref[part] = sum_ref[:, part].T
    for c in range(PROJ):
        weight_out[c * PROJ : (c + 1) * PROJ] = turn_ref[pl.ds(c, PROJ, stride=PROJ)]


def outer_call(at, labels, left, lab, right, wide, grad):
    groups, step, cols, width = grad.shape
    seqs, total = left.shape
    span = right.shape[1]
    return pl.pallas_call(
        outer_body,
        in_specs=[SMEM] * 2 + [VMEM] * 5,
        out_specs=[VMEM] * 2,
        out_shape=[
            pltpu.VMEM((groups, step * cols, PROJ * PROJ), BF16),
            jax.ShapeDtypeStruct((PROJ * PROJ, width), F32),
        ],
        scratch_shapes=[
            pltpu.VMEM((span, (CHAINS + 1) * seqs), BF16),
            pltpu.VMEM((2 * seqs, WIDE), BF16),
            pltpu.VMEM((span, WIDE), F32),
            pltpu.VMEM((span, WIDE), F32),
            pltpu.VMEM((width, PROJ * PROJ), F32),
            pltpu.VMEM((PROJ * PROJ, width), F32),
            pltpu.VMEM((span, seqs), BF16),
            pltpu.VMEM((span, seqs), BF16),
        ],
        compiler_params=KERNEL,
        cost_estimate=cost(20, span, total, seqs),
        name="outer",
    )(at, labels, left, lab, right, wide, grad)


def pair_body(outer_ref, w_ref, offset_ref, pair_ref):
    _, pairs, _ = outer_ref.shape
    here = pair_ref.shape[0] // pairs
    for g in range(here):
        pair = nn_dot(outer_ref[pl.program_id(0) * here + g], w_ref[...]) + offset_ref[...]
        pair_ref[g * pairs : (g + 1) * pairs] = pair.astype(BF16)


def pair_call(outer, w, offset):
    groups, pairs, feats = outer.shape
    width = w.shape[1]
    steps = 2
    return pl.pallas_call(
        pair_body,
        grid=(steps,),
        in_specs=[VMEM] * 3,
        out_specs=pl.BlockSpec((groups * pairs // steps, width), lambda g: (g, 0)),
        out_shape=jax.ShapeDtypeStruct((groups * pairs, width), BF16),
        compiler_params=KERNEL,
        cost_estimate=pl.CostEstimate(
            flops=2 * groups * pairs * feats * width,
            bytes_accessed=2 * groups * pairs * width,
            transcendentals=0,
        ),
        name="pair",
    )(outer, w, offset)


class Pairs:
    def __init__(self, n_row, n_col):
        self.n_row, self.n_col = n_row, n_col
        self.per_row = n_col // n_row
        self.row = lax.axis_index("row").astype(jnp.uint32)
        self.col = lax.axis_index("col").astype(jnp.uint32)

    def col_swap(self, value, k):
        return lax.ppermute(value, "col", [(t ^ k, t) for t in range(self.n_col)])

    def row_swap(self, value, k):
        return lax.ppermute(value, "row", [(t ^ k, t) for t in range(self.n_row)])

    def right_along_row(self, right):
        others = [self.row_swap(right, k) for k in range(1, self.n_row)]
        return [right] + others

    def right_pieces(self, by_row):
        m = self.per_row
        here, lanes = by_row[0].shape
        lanes //= m
        by_row = jnp.stack(by_row)
        pieces = []
        for k in range(self.n_col):
            q = self.col ^ k
            at = ((q // m) ^ self.row, jnp.uint32(0), (q % m) * lanes)
            pieces.append(lax.dynamic_slice(by_row, at, (1, here, lanes))[0])
        return pieces

    def right_along_col(self, pieces):
        return jnp.concatenate([self.col_swap(p, k) if k else p for k, p in enumerate(pieces)])

    def right_grad_home(self, grad):
        n, m = self.n_col, self.per_row
        here, lanes = grad.shape[0] // n, grad.shape[1]
        total = jnp.zeros((m, here, lanes), F32)
        slot = lax.broadcasted_iota(jnp.uint32, (m, 1, 1), 0)
        for k in range(n):
            t = (self.row * m + self.col % m) ^ k
            block = lax.dynamic_slice_in_dim(grad, (t ^ self.col) * here, here, 0)
            pairs = []
            for r in range(self.n_row):
                for q in range(n):
                    pairs.append((r * n + q, (q // m) * n + ((r * m + q % m) ^ k)))
            got = lax.ppermute(block, ("row", "col"), pairs).astype(F32)[None]
            total += got if m == 1 else jnp.where(slot == (self.col ^ k) % m, got, 0)
        return total.swapaxes(0, 1).reshape(here, m * lanes).astype(BF16)

    def weight_over_row(self, weight):
        n = self.n_row
        size = weight.shape[0] // n
        sent = weight.astype(BF16).reshape(n, size, -1)
        total = lax.dynamic_index_in_dim(weight.reshape(n, size, -1), self.row, 0, keepdims=False)
        for k in range(1, n):
            piece = lax.dynamic_index_in_dim(sent, self.row ^ k, 0, keepdims=False)
            total += self.row_swap(piece, k).astype(F32)
        return total

    def weight_over_col(self, total):
        mine = total.astype(BF16)
        for k in range(1, self.n_col):
            total += self.col_swap(mine, k).astype(F32)
        return total.astype(BF16)

    def weight_to_all(self, mine):
        n = self.n_row
        which = lax.broadcasted_iota(jnp.uint32, (n, 1, 1), 0) ^ self.row
        shares = mine[None]
        for k in range(1, n):
            shares = jnp.where(which == k, self.row_swap(mine, k)[None], shares)
        return shares.reshape(n * mine.shape[0], mine.shape[1])


def after(value, *others):
    return lax.optimization_barrier((value,) + others)[0]


def shards(n_row, n_col, alignment_tensor, gain, shift, first_projector, second_projector,
           final_projector, final_offset, labels, counts, grad):
    ring = Pairs(n_row, n_col)
    here, rows, _ = alignment_tensor.shape
    cols, width = grad.shape[1:]
    seqs = here * n_col
    left, right = project_call(
        alignment_tensor, gain[None, :], shift[None, :], first_projector.T, second_projector.T, cols
    )
    by_row = ring.right_along_row(right)
    left = jnp.concatenate([left] + [ring.col_swap(left, k) for k in range(1, n_col)])

    at = jnp.stack([ring.row * rows, ring.col * cols, ring.col]).astype(jnp.int32)
    lab, tall, wide, plain, w, back, grad = back_call(
        at, labels, counts, after(final_projector, right), grad, seqs, n_col
    )
    mine = ring.right_along_col(ring.right_pieces(by_row))
    back, grad = in_vmem(back), in_vmem(grad)
    right_grad = right_grad_call(at, labels, back, left, lab, plain)

    right = after(mine, right_grad)
    grad_right = ring.right_grad_home(right_grad)
    outer, weight = outer_call(
        at, labels, left, lab, right, wide, grad
    )
    share = ring.weight_over_row(weight)
    left_grad = left_grad_call(at, labels, back, after(lab, weight), right, tall)
    share = after(share, left_grad)

    total = left_grad[:here].astype(F32)
    for k in range(1, n_col):
        total += ring.col_swap(left_grad[k * here : (k + 1) * here], k).astype(F32)
    adjoint_first = total.astype(BF16)
    pair_update = pair_call(in_vmem(outer), after(w, left_grad, share), final_offset[None, :])
    pair_update = pair_update.reshape(rows, cols, width)
    mine = after(ring.weight_over_col(share), pair_update)
    grad_w_out = ring.weight_to_all(mine).astype(F32) / (n_row * rows)
    return pair_update, adjoint_first, grad_right, grad_w_out


def solution(mesh):
    in_specs = (
        P(("parts", "col"), "row", None),
        P(),
        P(),
        P(),
        P(),
        P(),
        P(),
        P("parts"),
        P("parts", None),
        P(("parts", "row"), "col", None),
    )
    out_specs = (
        P(("parts", "row"), "col", None),
        P(("parts", "col"), "row"),
        P(("parts", "col"), "row"),
        P("parts", None),
    )

    def body(*args):
        return shards(mesh.shape["row"], mesh.shape["col"], *args)

    return jax.shard_map(body, mesh=mesh, in_specs=in_specs, out_specs=out_specs, check_vma=False)
```
